32 devices in a mesh: dp: 2 (over core), ctx: 4 (over y, x), tp: 4 (over z).
Axes of the slice: x: 2, y: 2, z: 4, core: 2. Of those that a mesh axis runs over, the one named last changes fastest.
Arguments:
- layer_in: bfloat16 [4096, 2304], P(('dp', 'ctx', 'tp')), may hold values from -6 to 6
- cotangent: bfloat16 [4096, 2304], P(('dp', 'ctx', 'tp')), may hold values from -6 to 6
- norm_gains: float32 [4, 2304], replicated, may hold values from 0.25 to 1.75
- w_query: bfloat16 [2304, 2048], P('dp', 'tp'), may hold values from -1.25 to 1.25
- w_key: bfloat16 [2304, 1024], P('dp', 'tp'), may hold values from -0.125 to 0.125
- w_value: bfloat16 [2304, 1024], P('dp', 'tp'), may hold values from -0.125 to 0.125
- w_out: bfloat16 [2048, 2304], P('tp', 'dp'), may hold values from -0.125 to 0.125
- w_gate: bfloat16 [2304, 9216], P('dp', 'tp'), may hold values from -0.125 to 0.125
- w_up: bfloat16 [2304, 9216], P('dp', 'tp'), may hold values from -0.125 to 0.125
- w_down: bfloat16 [9216, 2304], P('tp', 'dp'), may hold values from -0.0625 to 0.0625
Outputs:
- layer_out: bfloat16 [4096, 2304], P(('dp', 'ctx', 'tp'))
- input_grad: float32 [4096, 2304], P(('dp', 'ctx', 'tp'))
- gain_grads: float32 [4, 2304], P(None, ('dp', 'ctx', 'tp'))
- grad_query: float32 [2304, 2048], P(('dp', 'ctx'), 'tp')
- grad_key: float32 [2304, 1024], P(('dp', 'ctx'), 'tp')
- grad_value: float32 [2304, 1024], P(('dp', 'ctx'), 'tp')
- grad_out: float32 [2048, 2304], P('tp', ('dp', 'ctx'))
- grad_gate: float32 [2304, 9216], P(('dp', 'ctx'), 'tp')
- grad_up: float32 [2304, 9216], P(('dp', 'ctx'), 'tp')
- grad_down: float32 [9216, 2304], P('tp', ('dp', 'ctx'))
The draws below stay inside these ranges and needn't reach their ends.
All inputs are finite; a program needn't handle non-finite values.
Results may differ from the reference program's by a relative error of at most 0.028.
The reference program's roundings to bfloat16 on the way (of `normed_one`, `weights`, `head_rows`, `normed_two`, `hidden`, `branch_half`, `attention_half` and `heads_delta`) count: a program that leaves them out, or rounds other values in their place, can miss the bound.
Values may be sent and summed in bfloat16 or wider, within the bound.
A program may use at most 256 MiB of HBM per device.

```python
import math
import jax
import jax.numpy as jnp
from jax import lax

D = 2304
FF = 9216
QH = 8
KVH = 4
HEAD = 256
SEQ_LEN = 2048
TOKENS = 4096


def draw_w_query(key, part):
    own_key = jax.random.fold_in(key, 11)
    base_key, order_key = jax.random.split(own_key)
    base = jnp.clip(jax.random.normal(base_key, (D, QH * HEAD), jnp.float32), -6.0, 6.0)
    levels = 10.0 ** (jnp.arange(QH, dtype=jnp.float32) / (QH - 1))
    order = jax.random.permutation(order_key, QH)
    head_factor = levels[order]
    column_factor = jnp.repeat(head_factor, HEAD)
    scaled = base * (1.0 / math.sqrt(D)) * column_factor[None, :]
    return scaled.astype(jnp.bfloat16)


def raised(entries, rng, source, target, blocks, factor):
    def block_of(axis_at):
        return (jnp.arange(entries.shape[axis_at]) // (entries.shape[axis_at] // blocks)).reshape((-1,) + (1,) * (entries.ndim - 1 - axis_at))

    near = jax.random.permutation(rng, blocks)[block_of(target)]
    far = (block_of(target) + blocks // 2) % blocks
    return jnp.where((block_of(source) == near) | (block_of(source) == far), factor * entries, entries)


def block_scale(key, shape, cuts, smallest, high):
    factor_of = 1.0
    for position, shards_of in cuts:
        steps = jax.random.uniform(jax.random.fold_in(jax.random.fold_in(key, 6), position), (shards_of,), jnp.float32, smallest / len(cuts), high / len(cuts))
        factor_of = factor_of * jnp.repeat(jnp.exp(steps), shape[position] // shards_of).reshape((-1,) + (1,) * (len(shape) - 1 - position))
    return factor_of


def bell_draw(rng, shape, deviation, bound, cuts=(), kind=jnp.bfloat16):
    factor_of = block_scale(rng, shape, cuts, -0.22, 0.18) if cuts else 1.0
    entries = jax.random.normal(rng, shape, jnp.float32) * deviation * factor_of
    return jnp.minimum(jnp.maximum(entries, -bound), bound).astype(kind)


def bell_draw_with(key, shape, scale, most, cuts, heavy, held_as=jnp.bfloat16):
    result = scale * jax.random.normal(key, shape, jnp.float32)
    if cuts:
        result = result * block_scale(key, shape, cuts, -0.22, 0.18)
    return jnp.clip(raised(result, jax.random.fold_in(key, 3), *heavy), -most, most).astype(held_as)


def setup_inputs(seed: int = 0) -> dict:
    seeds = jax.random.split(jax.random.key(seed), 11)
    layer_in = bell_draw(seeds[0], (TOKENS, D), 1.0, 6.0, ((0, 32),))
    cotangent = bell_draw_with(seeds[1], (TOKENS, D), 1.0, 6.0, ((0, 32),), (0, 1, 32, 2.75))
    norm_gains = jnp.clip(1.0 + 0.15 * jax.random.normal(seeds[2], (4, D), jnp.float32), 0.25, 1.75)
    w_query = draw_w_query(jax.random.fold_in(seeds[10], 71), 0)
    w_key = bell_draw(seeds[4], (D, KVH * HEAD), D ** -0.5, 0.125, ((0, 2), (1, 4)))
    w_value = bell_draw(seeds[5], (D, KVH * HEAD), D ** -0.5, 0.125, ((0, 2), (1, 4)))
    w_out = bell_draw(seeds[6], (QH * HEAD, D), (QH * HEAD) ** -0.5, 0.125, ((0, 4), (1, 2)))
    w_gate = bell_draw(seeds[7], (D, FF), D ** -0.5, 0.125, ((0, 2), (1, 4)))
    w_up = bell_draw(seeds[8], (D, FF), D ** -0.5, 0.125, ((0, 2), (1, 4)))
    w_down = bell_draw(seeds[9], (FF, D), FF ** -0.5, 0.0625, ((0, 4), (1, 2)))
    return dict(layer_in=layer_in, cotangent=cotangent, norm_gains=norm_gains, w_query=w_query, w_key=w_key, w_value=w_value, w_out=w_out, w_gate=w_gate, w_up=w_up, w_down=w_down)


EPS = 1e-06
CAP = 50.0
THETA = 10000.0

def rms_scale(values, gain_row):
    return values * lax.rsqrt(lax.optimization_barrier(jnp.mean(values * values, axis=-1, keepdims=True)) + EPS) * gain_row

def glu_product(gate_proj, up_proj):
    return jax.nn.gelu(gate_proj, approximate=True) * up_proj

def rope_tables(positions, head_width):
    half_width = head_width // 2
    frequency = THETA ** (-(jnp.arange(half_width, dtype=jnp.float32) * 2.0) / head_width)
    angles = positions.astype(jnp.float32)[:, None] * frequency[None, :]
    cosine = jnp.concatenate([jnp.cos(angles), jnp.cos(angles)], axis=1)
    sine_table = jnp.concatenate([jnp.sin(angles), jnp.sin(angles)], axis=1)
    return (cosine, sine_table)

def rotate(values, cosine, sine_table, sine_sign):
    half_width = values.shape[-1] // 2
    turned = jnp.concatenate([-values[..., half_width:], values[..., :half_width]], axis=-1)
    return values * cosine[:, None, :] + turned * (sine_sign * sine_table)[:, None, :]

def inner_rows(former, latter):
    return lax.dot_general(former, latter, (((0,), (0,)), ((), ())), preferred_element_type=jnp.float32)

def times_transposed(former, latter):
    return lax.dot_general(former, latter, (((1,), (1,)), ((), ())), preferred_element_type=jnp.float32)

def block_scores(query, key_float, block_index, query_block):
    row_start = block_index * query_block
    query_part = lax.dynamic_slice_in_dim(query, row_start, query_block, 0).astype(jnp.float32)
    raw_scores = jnp.einsum('bkgh,lkh->kgbl', query_part, key_float) * HEAD ** (-0.5)
    capped = CAP * jnp.tanh(raw_scores / CAP)
    query_pos = row_start + jnp.arange(query_block, dtype=jnp.int32)
    key_pos = jnp.arange(SEQ_LEN, dtype=jnp.int32)
    allowed = key_pos[None, :] <= query_pos[:, None]
    return (query_part, capped, allowed)

def attend_forward(query, key_rows, value_rows):
    query_block = math.gcd(SEQ_LEN, 512)
    key_float = key_rows.astype(jnp.float32)
    value_float = value_rows.astype(jnp.float32)

    def one_block(block_index):
        query_part, capped, allowed = block_scores(query, key_float, block_index, query_block)
        exp_scores = jnp.where(allowed, jnp.exp(capped), 0.0)
        totals = lax.optimization_barrier(jnp.sum(exp_scores, axis=-1))
        weights = lax.optimization_barrier(exp_scores.astype(jnp.bfloat16)).astype(jnp.float32)
        summed = jnp.einsum('kgbl,lkh->bkgh', weights, value_float)
        head_rows = (summed / jnp.transpose(totals, (2, 0, 1))[..., None]).astype(jnp.bfloat16)
        return (head_rows, jnp.log(totals))
    head_rows, log_totals = lax.map(one_block, jnp.arange(SEQ_LEN // query_block, dtype=jnp.int32))
    return (head_rows.reshape(query.shape), log_totals)

def attend_backward(query, key_rows, value_rows, head_rows, heads_delta, log_totals):
    query_block = math.gcd(SEQ_LEN, 512)
    key_float = key_rows.astype(jnp.float32)
    value_float = value_rows.astype(jnp.float32)
    score_scale = HEAD ** (-0.5)

    def one_block(state_in, block_index):
        key_acc, value_acc = state_in
        query_part, capped, allowed = block_scores(query, key_float, block_index, query_block)
        row_start = block_index * query_block
        block_logs = log_totals[block_index]
        prob_rows = jnp.where(allowed, jnp.exp(capped - block_logs[..., None]), 0.0)
        prob_half = lax.optimization_barrier(prob_rows.astype(jnp.bfloat16)).astype(jnp.float32)
        delta_part = lax.dynamic_slice_in_dim(heads_delta, row_start, query_block, 0).astype(jnp.float32)
        heads_part = lax.dynamic_slice_in_dim(head_rows, row_start, query_block, 0).astype(jnp.float32)
        value_acc = value_acc + jnp.einsum('kgbl,bkgh->lkh', prob_half, delta_part)
        prob_delta = jnp.einsum('bkgh,lkh->kgbl', delta_part, value_float)
        row_delta = jnp.transpose(lax.optimization_barrier(jnp.sum(delta_part * heads_part, axis=-1)), (1, 2, 0))
        score_grad = prob_rows * (prob_delta - row_delta[..., None]) * (1.0 - (capped / CAP) ** 2)
        score_half = lax.optimization_barrier(score_grad.astype(jnp.bfloat16)).astype(jnp.float32)
        query_grad = jnp.einsum('kgbl,lkh->bkgh', score_half, key_float) * score_scale
        key_acc = key_acc + jnp.einsum('kgbl,bkgh->lkh', score_half, query_part) * score_scale
        return ((key_acc, value_acc), query_grad)
    zero_rows = jnp.zeros((SEQ_LEN, KVH, HEAD), jnp.float32)
    (key_grad, value_grad), query_grad = lax.scan(one_block, (zero_rows, zero_rows), jnp.arange(SEQ_LEN // query_block, dtype=jnp.int32))
    return (query_grad.reshape(query.shape), key_grad, value_grad)

def reference(layer_in, cotangent, norm_gains, w_query, w_key, w_value, w_out, w_gate, w_up, w_down):
    group_size = QH // KVH
    seq_count = TOKENS // SEQ_LEN
    input_float = layer_in.astype(jnp.float32)
    normed_one = rms_scale(input_float, norm_gains[0]).astype(jnp.bfloat16)
    positions = jnp.arange(TOKENS, dtype=jnp.int32) % SEQ_LEN
    cosine, sine_table = rope_tables(positions, HEAD)
    query_proj = jnp.dot(normed_one, w_query, preferred_element_type=jnp.float32).reshape(TOKENS, QH, HEAD)
    query_rot = rotate(query_proj, cosine, sine_table, 1.0).astype(jnp.bfloat16)
    key_proj = jnp.dot(normed_one, w_key, preferred_element_type=jnp.float32).reshape(TOKENS, KVH, HEAD)
    key_rot = rotate(key_proj, cosine, sine_table, 1.0).astype(jnp.bfloat16)
    value_rows = jnp.dot(normed_one, w_value, preferred_element_type=jnp.float32).astype(jnp.bfloat16).reshape(TOKENS, KVH, HEAD)
    query_seq = query_rot.reshape(seq_count, SEQ_LEN, KVH, group_size, HEAD)
    key_seq = key_rot.reshape(seq_count, SEQ_LEN, KVH, HEAD)
    value_seq = value_rows.reshape(seq_count, SEQ_LEN, KVH, HEAD)
    heads_seq, logs_seq = lax.map(lambda seq_items: attend_forward(seq_items[0], seq_items[1], seq_items[2]), (query_seq, key_seq, value_seq))
    head_flat = heads_seq.reshape(TOKENS, QH * HEAD)
    attention = jnp.dot(head_flat, w_out, preferred_element_type=jnp.float32)
    middle = input_float + rms_scale(attention, norm_gains[1])
    row_block = math.gcd(TOKENS, 4096)

    def ffn_block(state_in, block_index):
        grad_gate, grad_up, grad_down, gain_two, gain_three = state_in
        row_start = block_index * row_block
        middle_part = lax.dynamic_slice_in_dim(middle, row_start, row_block, 0)
        seed_part = lax.dynamic_slice_in_dim(cotangent, row_start, row_block, 0).astype(jnp.float32)
        normed_two = rms_scale(middle_part, norm_gains[2]).astype(jnp.bfloat16)
        gate_proj = jnp.dot(normed_two, w_gate, preferred_element_type=jnp.float32)
        up_proj = jnp.dot(normed_two, w_up, preferred_element_type=jnp.float32)
        hidden = glu_product(gate_proj, up_proj).astype(jnp.bfloat16)
        branch_two = jnp.dot(hidden, w_down, preferred_element_type=jnp.float32)
        out_part = (middle_part + rms_scale(branch_two, norm_gains[3])).astype(jnp.bfloat16)
        unused_three, back_three = jax.vjp(rms_scale, branch_two, norm_gains[3])
        branch_delta, gain_delta_three = back_three(seed_part)
        branch_half = branch_delta.astype(jnp.bfloat16)
        grad_down = grad_down + inner_rows(hidden, branch_half)
        hidden_delta = times_transposed(branch_half, w_down)
        unused_glu, back_glu = jax.vjp(glu_product, gate_proj, up_proj)
        gate_delta, up_delta = back_glu(hidden_delta)
        gate_half = gate_delta.astype(jnp.bfloat16)
        up_half = up_delta.astype(jnp.bfloat16)
        grad_gate = grad_gate + inner_rows(normed_two, gate_half)
        grad_up = grad_up + inner_rows(normed_two, up_half)
        normed_delta_two = times_transposed(gate_half, w_gate) + times_transposed(up_half, w_up)
        unused_two, back_two = jax.vjp(rms_scale, middle_part, norm_gains[2])
        middle_part_delta, gain_delta_two = back_two(normed_delta_two)
        state_out = (grad_gate, grad_up, grad_down, gain_two + gain_delta_two, gain_three + gain_delta_three)
        return (state_out, (out_part, seed_part + middle_part_delta))
    start_state = (jnp.zeros((D, FF), jnp.float32), jnp.zeros((D, FF), jnp.float32), jnp.zeros((FF, D), jnp.float32), jnp.zeros((D,), jnp.float32), jnp.zeros((D,), jnp.float32))
    final_state, stacked = lax.scan(ffn_block, start_state, jnp.arange(TOKENS // row_block, dtype=jnp.int32))
    grad_gate, grad_up, grad_down, gain_two, gain_three = final_state
    layer_out = stacked[0].reshape(TOKENS, D)
    middle_delta = stacked[1].reshape(TOKENS, D)
    unused_one, back_one = jax.vjp(rms_scale, attention, norm_gains[1])
    attention_delta, gain_one = back_one(middle_delta)
    attention_half = attention_delta.astype(jnp.bfloat16)
    grad_out = inner_rows(head_flat, attention_half)
    heads_delta = times_transposed(attention_half, w_out).astype(jnp.bfloat16).reshape(seq_count, SEQ_LEN, KVH, group_size, HEAD)
    query_grad, key_grad, value_grad = lax.map(lambda seq_items: attend_backward(seq_items[0], seq_items[1], seq_items[2], seq_items[3], seq_items[4], seq_items[5]), (query_seq, key_seq, value_seq, heads_seq, heads_delta, logs_seq))
    query_delta = rotate(query_grad.reshape(TOKENS, QH, HEAD), cosine, sine_table, -1.0).astype(jnp.bfloat16).reshape(TOKENS, QH * HEAD)
    key_delta = rotate(key_grad.reshape(TOKENS, KVH, HEAD), cosine, sine_table, -1.0).astype(jnp.bfloat16).reshape(TOKENS, KVH * HEAD)
    value_delta = value_grad.astype(jnp.bfloat16).reshape(TOKENS, KVH * HEAD)
    grad_query = inner_rows(normed_one, query_delta)
    grad_key = inner_rows(normed_one, key_delta)
    grad_value = inner_rows(normed_one, value_delta)
    normed_delta_one = times_transposed(query_delta, w_query) + times_transposed(key_delta, w_key) + times_transposed(value_delta, w_value)
    unused_zero, back_zero = jax.vjp(rms_scale, input_float, norm_gains[0])
    input_delta, gain_zero = back_zero(normed_delta_one)
    input_grad = middle_delta + input_delta
    gain_grads = jnp.stack([gain_zero, gain_one, gain_two, gain_three])
    return (layer_out, input_grad, gain_grads, grad_query, grad_key, grad_value, grad_out, grad_gate, grad_up, grad_down)
```

```python
import functools

import jax
import jax.numpy as jnp
from jax import lax
from jax.experimental import pallas as pl
from jax.experimental.pallas import tpu as pltpu
from jax.sharding import PartitionSpec as P

HEAD = 256
EPS = 1e-06
CAP = 50.0
THETA = 10000.0
MESH = pl.DeviceIdType.MESH
BF = jnp.bfloat16
F32 = jnp.float32


def tile_of(width):
    for tile in (768, 512, 256, 128):
        if width % tile == 0:
            return tile
    return width


def inverse_rms(values):
    return lax.rsqrt(jnp.mean(values * values, axis=-1, keepdims=True) + EPS)


def rms_back(values, scale, gain, delta):
    weighted = delta * gain
    inner = jnp.mean(weighted * values, axis=-1, keepdims=True)
    grad = scale * weighted - values * (scale * scale * scale * inner)
    return grad, jnp.sum(delta * values * scale, axis=0, keepdims=True)


def dot_nt(former, latter):
    return lax.dot_general(former, latter, (((1,), (1,)), ((), ())), preferred_element_type=F32)


def dot_nn(former, latter):
    return jnp.dot(former, latter, preferred_element_type=F32)


def barrier(count_of, peers):
    sem = pltpu.get_barrier_semaphore()
    for present, device_id in peers:

        @pl.when(present)
        def _():
            pl.semaphore_signal(sem, inc=1, device_id=device_id, device_id_type=MESH)

    pl.semaphore_wait(sem, count_of)


def core_kernel(
    T, C, NDP,
    x_ref, ct_ref, gain_ref, heads_ref, wo_ref, wg_ref, wu_ref, wd_ref,
    out_ref, mdelta_ref, gsum_ref, hdelta_ref,
    rows_pair, hid_pair, branch_pair, gate_pair, up_pair, attn_pair, head_pair,
    wo_v, wg_v, wu_v, wd_v, X, Pb, Rb, hid, Ab, Bb, att, mid, acc,
    w_sem, rs_send, rs_recv, ag_send, ag_recv, pair_sem,
):
    t = lax.axis_index("tp")
    dp = lax.axis_index("dp")
    D = x_ref.shape[1]
    rc = x_ref.shape[0] // C
    Dh = D // NDP
    F = wg_v.shape[1]
    M = T * rc
    has_left, has_right = t > 0, t < T - 1
    left, right = {"tp": jnp.maximum(t - 1, 0)}, {"tp": jnp.minimum(t + 1, T - 1)}
    partners = [{"dp": lax.rem(dp + o, NDP)} for o in range(1, NDP)]

    barrier(
        has_left.astype(jnp.int32) + has_right.astype(jnp.int32) + (NDP - 1),
        [(has_left, left), (has_right, right)] + [(t >= 0, p) for p in partners],
    )

    rows_at = pl.ds(pl.multiple_of(dp * Dh, 128), Dh)
    weights = [
        (wo_ref, lambda: wo_v.at[:, rows_at]),
        (wg_ref, lambda: wg_v.at[rows_at]),
        (wu_ref, lambda: wu_v.at[rows_at]),
        (wd_ref, lambda: wd_v.at[:, rows_at]),
    ]

    def weight_copies(i):
        src, dst = weights[i]
        copies = [pltpu.make_async_copy(src, dst(), w_sem.at[0, i])]
        for o, partner in enumerate(partners):
            copies.append(
                pltpu.make_async_remote_copy(
                    src, dst(), w_sem.at[1 + 2 * o, i], w_sem.at[2 + 2 * o, i],
                    device_id=partner, device_id_type=MESH,
                )
            )
        return copies

    for i in range(4):
        for copy in weight_copies(i):
            copy.start()

    def weight_wait(i):
        src, dst = weights[i]
        for o, copy in enumerate(weight_copies(i)):
            if o == 0:
                copy.wait()
            else:
                copy.wait_recv()

    def pair_copies(kind, s, src, half, dst):
        def cut(owner):
            if half:
                return src.at[..., pl.ds(pl.multiple_of(owner * Dh, 128), Dh)]
            return src

        copies = [pltpu.make_async_copy(cut(dp), dst.at[dp, s], pair_sem.at[0, kind, s])]
        for o, partner in enumerate(partners):
            copies.append(
                pltpu.make_async_remote_copy(
                    cut(partner["dp"]), dst.at[dp, s],
                    pair_sem.at[1 + 2 * o, kind, s], pair_sem.at[2 + 2 * o, kind, s],
                    device_id=partner, device_id_type=MESH,
                )
            )
        return copies

    def pair_of(kind, s):
        return pair_copies(
            kind, s,
            *[
                (X.at[s], True, rows_pair),
                (hid.at[s], False, hid_pair),
                (X.at[s], True, branch_pair),
                (Ab.at[s], False, gate_pair),
                (Bb.at[s], False, up_pair),
                (X.at[s], True, attn_pair),
                (heads_ref.at[:, s], False, head_pair),
            ][kind],
        )

    def pair_start(kind, s):
        for copy in pair_of(kind, s):
            copy.start()

    def pair_sent(kind, s):
        for o, copy in enumerate(pair_of(kind, s)):
            if o == 0:
                copy.wait()
            else:
                copy.wait_send()

    def pair_received(kind, s):
        for copy in pair_of(kind, s)[1:]:
            copy.wait_recv()

    def rs_copy(s, side, k, j):
        if side == 0:
            slot, peer = j, right
        else:
            slot, peer = jnp.where(j == t - 1, T, j), left
        return pltpu.make_async_remote_copy(
            Pb.at[s, j], Rb.at[s, slot], rs_send.at[s, side, k], rs_recv.at[s, side, k],
            device_id=peer, device_id_type=MESH,
        )

    def rs_block(side, k):
        return (T - 1 - k + t) if side == 0 else (k - (T - 1 - t))

    def rs_sends(side, k):
        return (t <= k) if side == 0 else (T - 1 - t <= k)

    def ag_copy(s, side, k, j):
        return pltpu.make_async_remote_copy(
            X.at[s, j], X.at[s, j], ag_send.at[s, side, k], ag_recv.at[s, side, k],
            device_id=right if side == 0 else left, device_id_type=MESH,
        )

    def ag_block(side, k):
        return (t - k) if side == 0 else (t + k)

    def ag_sends(side, k):
        return (t >= k) & has_right if side == 0 else (t + k <= T - 1) & has_left

    def rs_start(s):
        for side in (0, 1):

            @pl.when(rs_sends(side, 0))
            def _():
                rs_copy(s, side, 0, rs_block(side, 0)).start()

    def rs_step(s, k):
        for side in (0, 1):
            j = rs_block(side, k)
            came = has_left if side == 0 else has_right

            @pl.when(rs_sends(side, k))
            def _():
                @pl.when(came)
                def _():
                    rs_copy(s, side, k - 1, j).wait_recv()
                    Pb[s, j] = (Pb[s, j].astype(F32) + Rb[s, j].astype(F32)).astype(BF)

                rs_copy(s, side, k, j).start()

    def rs_sent(s):
        for side in (0, 1):
            for k in range(T - 1):

                @pl.when(rs_sends(side, k))
                def _():
                    rs_copy(s, side, k, rs_block(side, k)).wait_send()

    def rs_finish(s):
        acc[...] = Pb[s, t].astype(F32)

        @pl.when(has_left)
        def _():
            rs_copy(s, 0, T - 2, t).wait_recv()
            acc[...] += Rb[s, t].astype(F32)

        @pl.when(has_right)
        def _():
            rs_copy(s, 1, T - 2, t).wait_recv()
            acc[...] += Rb[s, T].astype(F32)

    def ag_start(s):
        for side in (0, 1):

            @pl.when(ag_sends(side, 0))
            def _():
                ag_copy(s, side, 0, t).start()

    def ag_step(s, k):
        for side in (0, 1):
            j = ag_block(side, k)
            there = (j >= 0) if side == 0 else (j <= T - 1)

            @pl.when(there)
            def _():
                ag_copy(s, side, k - 1, j).wait_recv()
                if k <= T - 2:

                    @pl.when(has_right if side == 0 else has_left)
                    def _():
                        ag_copy(s, side, k, j).start()

    def ag_sent(s):
        for side in (0, 1):
            for k in range(T - 1):

                @pl.when(ag_sends(side, k))
                def _():
                    ag_copy(s, side, k, ag_block(side, k)).wait_send()

    def local_rows(n, s):
        own = pl.ds(pl.multiple_of(s * rc, rc), rc)
        total = acc[...]

        @pl.when(n == 0)
        def _():
            att[s] = total
            middle = x_ref[own].astype(F32) + total * inverse_rms(total) * gain_ref[1:2]
            mid[s] = middle
            X[s, t] = (middle * inverse_rms(middle) * gain_ref[2:3]).astype(BF)

        @pl.when(n == 1)
        def _():
            scale = inverse_rms(total)
            out_ref[own] = (mid[s] + total * scale * gain_ref[3:4]).astype(BF)
            grad, terms = rms_back(total, scale, gain_ref[3:4], ct_ref[own].astype(F32))
            gsum_ref[2:3] += terms
            X[s, t] = grad.astype(BF)

        @pl.when(n == 2)
        def _():
            middle, attention = mid[s], att[s]
            grad, terms = rms_back(middle, inverse_rms(middle), gain_ref[2:3], total)
            gsum_ref[1:2] += terms
            middle_delta = ct_ref[own].astype(F32) + grad
            mdelta_ref[own] = middle_delta
            grad, terms = rms_back(attention, inverse_rms(attention), gain_ref[1:2], middle_delta)
            gsum_ref[0:1] += terms
            X[s, t] = grad.astype(BF)

    def comm(tau, w, a):
        back = tau - a

        @pl.when((back >= 0) & (back < 3 * C))
        def _():
            n, s = back // C, lax.rem(back, C)
            if w <= T - 2:
                rs_step(s, w)
            elif w == T - 1:
                rs_finish(s)
                local_rows(n, s)
                ag_start(s)
            else:
                ag_step(s, w - (T - 1))

    def tiles(width, body):
        tile = tile_of(width)

        def step(i, carry):
            body(pl.ds(pl.multiple_of(i * tile, tile), tile), tile)
            return carry

        lax.fori_loop(0, width // tile, step, 0)

    def rows_of(s):
        return X[s].reshape(M, D)

    def store_part(s, at, tile, value):
        Pb[s, :, :, at] = value.astype(BF).reshape(T, rc, tile)

    def tick(tau, carry):
        n, s = tau // C, lax.rem(tau, C)

        @pl.when((n >= 1) & (n <= 2))
        def _():
            rs_sent(s)

        @pl.when(n == 1)
        def _():
            @pl.when(s == 0)
            def _():
                weight_wait(1)
                weight_wait(2)

            pair_start(0, s)

            def gate_up(at, tile):
                gate = dot_nn(rows_of(s), wg_v[:, at])
                up = dot_nn(rows_of(s), wu_v[:, at])
                inner = jnp.tanh(0.7978845608028654 * (gate + 0.044715 * gate * gate * gate))
                half = 0.5 * (1.0 + inner)
                gelu = gate * half
                slope = half + 0.5 * gate * (1.0 - inner * inner) * (
                    0.7978845608028654 * (1.0 + 0.134145 * gate * gate)
                )
                hid[s, :, at] = (gelu * up).astype(BF)
                Ab[s, :, at] = (up * slope).astype(BF)
                Bb[s, :, at] = gelu.astype(BF)

            tiles(F, gate_up)
            pair_start(1, s)

        @pl.when(n == 2)
        def _():
            pair_start(2, s)

            def gate_up_delta(at, tile):
                delta = dot_nt(rows_of(s), wd_v[at, :])
                Ab[s, :, at] = (delta * Ab[s, :, at].astype(F32)).astype(BF)
                Bb[s, :, at] = (delta * Bb[s, :, at].astype(F32)).astype(BF)

            tiles(F, gate_up_delta)
            pair_start(3, s)
            pair_start(4, s)

        for a in range(1, T):
            comm(tau, 2 * a - 1, a)

        @pl.when(n == 0)
        def _():
            pair_start(6, s)
            heads = heads_ref[:, s].reshape(M, heads_ref.shape[3])
            tiles(D, lambda at, tile: store_part(s, at, tile, dot_nn(heads, wo_v[:, at])))

        @pl.when(n == 1)
        def _():
            @pl.when(s == 0)
            def _():
                weight_wait(3)

            tiles(D, lambda at, tile: store_part(s, at, tile, dot_nn(hid[s], wd_v[:, at])))
            pair_sent(0, s)
            ag_sent(s)

        @pl.when(n == 2)
        def _():
            tiles(
                D,
                lambda at, tile: store_part(
                    s, at, tile, dot_nt(Ab[s], wg_v[at, :]) + dot_nt(Bb[s], wu_v[at, :])
                ),
            )
            pair_sent(2, s)
            ag_sent(s)

        @pl.when(n <= 2)
        def _():
            rs_start(s)

        @pl.when(n == 3)
        def _():
            pair_start(5, s)
            hdelta_ref[:, s] = (
                dot_nt(rows_of(s), wo_v[...]).astype(BF).reshape(T, rc, heads_ref.shape[3])
            )

        for a in range(1, T):
            comm(tau, 2 * a, a)
        return carry

    gsum_ref[...] = jnp.zeros_like(gsum_ref)
    weight_wait(0)
    lax.fori_loop(0, 4 * C, tick, 0)

    for i in range(4):
        for copy in weight_copies(i)[1:]:
            copy.wait_send()

    def close(s, carry):
        for kind in (1, 3, 4, 5, 6):
            pair_sent(kind, s)
        for kind in range(7):
            pair_received(kind, s)
        rs_sent(s)
        ag_sent(s)
        return carry

    lax.fori_loop(0, C, close, 0)


def core_call(layer_in, cotangent, norm_gains, head_flat, w_out, w_gate, w_up, w_down):
    T, NDP = lax.axis_size("tp"), lax.axis_size("dp")
    C = T
    Lr, D = layer_in.shape
    rc = Lr // C
    Hq = w_out.shape[0]
    Dh = D // NDP
    F = w_gate.shape[1]
    M = T * rc
    any_spec = pl.BlockSpec(memory_space=pl.ANY)
    vm = pl.BlockSpec(memory_space=pltpu.VMEM)
    sds = jax.ShapeDtypeStruct
    outs = pl.pallas_call(
        functools.partial(core_kernel, T, C, NDP),
        out_shape=(
            sds((Lr, D), BF), sds((Lr, D), F32), sds((3, D), F32), sds((T, C, rc, Hq), BF),
            sds((NDP, C, T, rc, Dh), BF), sds((NDP, C, M, F), BF), sds((NDP, C, T, rc, Dh), BF),
            sds((NDP, C, M, F), BF), sds((NDP, C, M, F), BF), sds((NDP, C, T, rc, Dh), BF),
            sds((NDP, C, T, rc, Hq), BF),
        ),
        in_specs=[vm, vm, vm, vm] + [any_spec] * 4,
        out_specs=[vm, vm, vm, vm] + [any_spec] * 7,
        scratch_shapes=[
            pltpu.VMEM((Hq, D), BF), pltpu.VMEM((D, F), BF), pltpu.VMEM((D, F), BF), pltpu.VMEM((F, D), BF),
            pltpu.VMEM((C, T, rc, D), BF), pltpu.VMEM((C, T, rc, D), BF), pltpu.VMEM((C, T + 1, rc, D), BF),
            pltpu.VMEM((C, M, F), BF), pltpu.VMEM((C, M, F), BF), pltpu.VMEM((C, M, F), BF),
            pltpu.VMEM((C, rc, D), F32), pltpu.VMEM((C, rc, D), F32), pltpu.VMEM((rc, D), F32),
            pltpu.SemaphoreType.DMA((2 * NDP - 1, 4)),
            pltpu.SemaphoreType.DMA((C, 2, T - 1)), pltpu.SemaphoreType.DMA((C, 2, T - 1)),
            pltpu.SemaphoreType.DMA((C, 2, T - 1)), pltpu.SemaphoreType.DMA((C, 2, T - 1)),
            pltpu.SemaphoreType.DMA((2 * NDP - 1, 7, C)),
        ],
        compiler_params=pltpu.CompilerParams(
            collective_id=0, has_side_effects=True, vmem_limit_bytes=66_000_000
        ),
        name="core",
    )(layer_in, cotangent, norm_gains, head_flat.reshape(T, C, rc, Hq), w_out, w_gate, w_up, w_down)
    out, mdelta, gsum, hdelta, rows, hidden, branch, gate, up, attn, heads = outs
    flat = lambda a: a.reshape(NDP * T * Lr, a.shape[-1])
    return (
        out, mdelta, gsum, hdelta.reshape(T * Lr, Hq),
        flat(rows), flat(hidden), flat(branch), flat(gate), flat(up), flat(attn), flat(heads),
    )


def rms_scale(values, gain_row):
    return values * lax.rsqrt(jnp.mean(values * values, axis=-1, keepdims=True) + EPS) * gain_row


def rope_tables(positions, head_width):
    half_width = head_width // 2
    frequency = THETA ** (-(jnp.arange(half_width, dtype=jnp.float32) * 2.0) / head_width)
    angles = positions.astype(jnp.float32)[:, None] * frequency[None, :]
    cosine = jnp.concatenate([jnp.cos(angles), jnp.cos(angles)], axis=1)
    sine_table = jnp.concatenate([jnp.sin(angles), jnp.sin(angles)], axis=1)
    return (cosine, sine_table)


def rotate(values, cosine, sine_table, sine_sign):
    half_width = values.shape[-1] // 2
    turned = jnp.concatenate([-values[..., half_width:], values[..., :half_width]], axis=-1)
    return values * cosine[:, None, :] + turned * (sine_sign * sine_table)[:, None, :]


def inner_rows(former, latter):
    return lax.dot_general(
        former, latter, (((0,), (0,)), ((), ())), preferred_element_type=jnp.float32
    )


def times_transposed(former, latter):
    return lax.dot_general(
        former, latter, (((1,), (1,)), ((), ())), preferred_element_type=jnp.float32
    )


def fetch_weights(query_part, key_part, value_part):
    return (
        lax.all_gather(query_part, "dp", axis=0, tiled=True),
        lax.all_gather(key_part, "dp", axis=0, tiled=True),
        lax.all_gather(value_part, "dp", axis=0, tiled=True),
    )


def spread_rows(rows_part):
    return lax.all_gather(rows_part, "tp", axis=0, tiled=True)


def collect_rows(term_fn, row_total):
    return lax.psum_scatter(
        term_fn(jnp.int32(0), row_total * lax.axis_size("tp")).astype(jnp.bfloat16),
        "tp",
        scatter_dimension=0,
        tiled=True,
    ).astype(jnp.float32)


def over_ctx(terms, dim):
    return lax.psum_scatter(terms.astype(BF), "ctx", scatter_dimension=dim, tiled=True).astype(F32)


def shards(layer_in, cotangent, norm_gains, w_query, w_key, w_value, w_out, w_gate, w_up, w_down):
    tp_count = lax.axis_size("tp")
    ctx_count = lax.axis_size("ctx")
    local_rows = layer_in.shape[0]
    block_rows = local_rows * tp_count
    seq_rows = block_rows * ctx_count
    positions = lax.axis_index("ctx") * block_rows + jnp.arange(block_rows, dtype=jnp.int32)
    last_pos = positions[block_rows - 1]
    cosine, sine_table = rope_tables(positions, HEAD)
    score_scale = HEAD ** (-0.5)
    query_full, key_full, value_full = fetch_weights(w_query, w_key, w_value)
    query_heads = query_full.shape[1] // HEAD
    key_heads = key_full.shape[1] // HEAD
    group_size = query_heads // key_heads
    input_float = layer_in.astype(jnp.float32)
    normed_one = rms_scale(input_float, norm_gains[0]).astype(jnp.bfloat16)
    rows_one = spread_rows(normed_one)
    query_proj = jnp.dot(rows_one, query_full, preferred_element_type=jnp.float32).reshape(
        block_rows, query_heads, HEAD
    )
    query_rot = (
        rotate(query_proj, cosine, sine_table, 1.0)
        .astype(jnp.bfloat16)
        .reshape(block_rows, key_heads, group_size, HEAD)
    )
    key_proj = jnp.dot(rows_one, key_full, preferred_element_type=jnp.float32).reshape(
        block_rows, key_heads, HEAD
    )
    key_rot = rotate(key_proj, cosine, sine_table, 1.0).astype(jnp.bfloat16)
    value_rows = (
        jnp.dot(rows_one, value_full, preferred_element_type=jnp.float32)
        .astype(jnp.bfloat16)
        .reshape(block_rows, key_heads, HEAD)
    )

    def scores_for(key_block):
        piece_len = key_block.shape[0]
        raw_scores = (
            jnp.einsum("bkgh,lkh->kgbl", query_rot, key_block, preferred_element_type=jnp.float32)
            * score_scale
        )
        capped = CAP * jnp.tanh(raw_scores / CAP)
        key_pos = jnp.arange(piece_len, dtype=jnp.int32)
        allowed = key_pos[None, :] <= positions[:, None]
        return (capped, allowed)

    accum_zero = jnp.zeros((block_rows, key_heads, group_size, HEAD), jnp.float32)
    totals_zero = jnp.zeros((key_heads, group_size, block_rows), jnp.float32)
    accumulated = accum_zero
    totals = totals_zero
    key_block = lax.all_gather(key_rot, "ctx", axis=0, tiled=True)
    value_block = lax.all_gather(value_rows, "ctx", axis=0, tiled=True)

    def attend_compute_piece():
        capped, allowed = scores_for(key_block)
        exp_scores = jnp.where(allowed, jnp.exp(capped), 0.0)
        weights = exp_scores.astype(jnp.bfloat16)
        summed = jnp.einsum(
            "kgbl,lkh->bkgh", weights, value_block, preferred_element_type=jnp.float32
        )
        return (summed, jnp.sum(exp_scores, axis=-1))

    def attend_keep_piece():
        return (accumulated, totals)

    accumulated, totals = lax.cond(
        jnp.int32(0) <= last_pos, attend_compute_piece, attend_keep_piece
    )
    head_rows = (accumulated / jnp.transpose(totals, (2, 0, 1))[..., None]).astype(jnp.bfloat16)
    log_totals = jnp.log(totals)
    head_flat = head_rows.reshape(block_rows, query_heads * HEAD)

    core = core_call(layer_in, cotangent, norm_gains, head_flat, w_out, w_gate, w_up, w_down)
    layer_out, middle_delta, gain_sums, heads_delta, *pairs = core
    rows_pair, hid_pair, branch_pair, gate_pair, up_pair, attn_pair, head_pair = pairs
    heads_delta = heads_delta.reshape(block_rows, key_heads, group_size, HEAD)
    row_delta = jnp.einsum(
        "bkgh,bkgh->kgb", heads_delta, head_rows, preferred_element_type=jnp.float32
    )
    buffer_zero = jnp.zeros((seq_rows, key_heads, HEAD), jnp.float32)
    key_buffer = buffer_zero
    value_buffer = buffer_zero
    back_key_block = lax.all_gather(key_rot, "ctx", axis=0, tiled=True)
    back_value_block = lax.all_gather(value_rows, "ctx", axis=0, tiled=True)

    def back_compute_piece():
        capped, allowed = scores_for(back_key_block)
        prob_rows = jnp.where(allowed, jnp.exp(capped - log_totals[..., None]), 0.0)
        value_part = jnp.einsum(
            "kgbl,bkgh->lkh",
            prob_rows.astype(jnp.bfloat16),
            heads_delta,
            preferred_element_type=jnp.float32,
        )
        prob_delta = jnp.einsum(
            "bkgh,lkh->kgbl", heads_delta, back_value_block, preferred_element_type=jnp.float32
        )
        score_grad = prob_rows * (prob_delta - row_delta[..., None]) * (1.0 - (capped / CAP) ** 2)
        score_half = score_grad.astype(jnp.bfloat16)
        query_part = (
            jnp.einsum(
                "kgbl,lkh->bkgh", score_half, back_key_block, preferred_element_type=jnp.float32
            )
            * score_scale
        )
        key_part = (
            jnp.einsum("kgbl,bkgh->lkh", score_half, query_rot, preferred_element_type=jnp.float32)
            * score_scale
        )
        return (query_part, key_part, value_part)

    def back_keep_piece():
        return (accum_zero, key_buffer, value_buffer)

    query_grad, key_buffer, value_buffer = lax.cond(
        jnp.int32(0) <= last_pos, back_compute_piece, back_keep_piece
    )
    key_grad, value_grad = (
        lax.psum_scatter(
            key_buffer.astype(jnp.bfloat16), "ctx", scatter_dimension=0, tiled=True
        ).astype(jnp.float32),
        lax.psum_scatter(
            value_buffer.astype(jnp.bfloat16), "ctx", scatter_dimension=0, tiled=True
        ).astype(jnp.float32),
    )
    query_delta = (
        rotate(query_grad.reshape(block_rows, query_heads, HEAD), cosine, sine_table, -1.0)
        .astype(jnp.bfloat16)
        .reshape(block_rows, query_heads * HEAD)
    )
    key_delta = (
        rotate(key_grad, cosine, sine_table, -1.0)
        .astype(jnp.bfloat16)
        .reshape(block_rows, key_heads * HEAD)
    )
    value_delta = value_grad.astype(jnp.bfloat16).reshape(block_rows, key_heads * HEAD)
    grad_query = inner_rows(rows_one, query_delta)
    grad_key = inner_rows(rows_one, key_delta)
    grad_value = inner_rows(rows_one, value_delta)

    def normed_one_term(row_start, row_count):
        first_term = times_transposed(query_delta, query_full)
        second_term = times_transposed(key_delta, key_full)
        return first_term + second_term + times_transposed(value_delta, value_full)

    normed_delta_one = collect_rows(normed_one_term, local_rows)
    unused_zero, back_zero = jax.vjp(rms_scale, input_float, norm_gains[0])
    input_delta, gain_zero = back_zero(normed_delta_one)
    input_grad = middle_delta + input_delta
    gain_terms = jnp.concatenate([gain_zero[None], gain_sums])
    gain_grads = lax.psum_scatter(gain_terms, ("dp", "ctx", "tp"), scatter_dimension=1, tiled=True)
    summed = (
        lax.psum_scatter(
            grad_query.astype(jnp.bfloat16), ("dp", "ctx"), scatter_dimension=0, tiled=True
        ).astype(jnp.float32),
        lax.psum_scatter(
            grad_key.astype(jnp.bfloat16), ("dp", "ctx"), scatter_dimension=0, tiled=True
        ).astype(jnp.float32),
        lax.psum_scatter(
            grad_value.astype(jnp.bfloat16), ("dp", "ctx"), scatter_dimension=0, tiled=True
        ).astype(jnp.float32),
        over_ctx(inner_rows(head_pair, attn_pair), 1),
        over_ctx(inner_rows(rows_pair, gate_pair), 0),
        over_ctx(inner_rows(rows_pair, up_pair), 0),
        over_ctx(inner_rows(hid_pair, branch_pair), 1),
    )
    grad_query, grad_key, grad_value, grad_out, grad_gate, grad_up, grad_down = summed
    return (
        layer_out,
        input_grad,
        gain_grads,
        grad_query,
        grad_key,
        grad_value,
        grad_out,
        grad_gate,
        grad_up,
        grad_down,
    )


def solution(mesh):
    return jax.shard_map(
        shards,
        mesh=mesh,
        in_specs=(
            P(("dp", "ctx", "tp"), None),
            P(("dp", "ctx", "tp"), None),
            P(),
            P("dp", "tp"),
            P("dp", "tp"),
            P("dp", "tp"),
            P("tp", "dp"),
            P("dp", "tp"),
            P("dp", "tp"),
            P("tp", "dp"),
        ),
        out_specs=(
            P(("dp", "ctx", "tp"), None),
            P(("dp", "ctx", "tp"), None),
            P(None, ("dp", "ctx", "tp")),
            P(("dp", "ctx"), "tp"),
            P(("dp", "ctx"), "tp"),
            P(("dp", "ctx"), "tp"),
            P("tp", ("dp", "ctx")),
            P(("dp", "ctx"), "tp"),
            P(("dp", "ctx"), "tp"),
            P("tp", ("dp", "ctx")),
        ),
        check_vma=False,
    )
```

```python
import functools

import jax
import jax.numpy as jnp
from jax import lax
from jax.experimental import pallas as pl
from jax.experimental.pallas import tpu as pltpu
from jax.sharding import PartitionSpec as P

HEAD = 256
EPS = 1e-06
CAP = 50.0
THETA = 10000.0
MESH = pl.DeviceIdType.MESH
BF = jnp.bfloat16
F32 = jnp.float32


def tile_of(width):
    for tile in (768, 512, 256, 128):
        if width % tile == 0:
            return tile
    return width


def inverse_rms(values):
    return lax.rsqrt(jnp.mean(values * values, axis=-1, keepdims=True) + EPS)


def rms_back(values, scale, gain, delta):
    weighted = delta * gain
    inner = jnp.mean(weighted * values, axis=-1, keepdims=True)
    grad = scale * weighted - values * (scale * scale * scale * inner)
    return grad, jnp.sum(delta * values * scale, axis=0, keepdims=True)


def dot_nt(former, latter):
    return lax.dot_general(former, latter, (((1,), (1,)), ((), ())), preferred_element_type=F32)


def dot_nn(former, latter):
    return jnp.dot(former, latter, preferred_element_type=F32)


def barrier(count_of, peers):
    sem = pltpu.get_barrier_semaphore()
    for present, device_id in peers:

        @pl.when(present)
        def _():
            pl.semaphore_signal(sem, inc=1, device_id=device_id, device_id_type=MESH)

    pl.semaphore_wait(sem, count_of)


def core_kernel(
    T, C, NDP,
    x_ref, ct_ref, gain_ref, heads_ref, wo_ref, wg_ref, wu_ref, wd_ref,
    out_ref, mdelta_ref, gsum_ref, hdelta_ref,
    rows_pair, hid_pair, branch_pair, gate_pair, up_pair, attn_pair, head_pair,
    wo_v, wg_v, wu_v, wd_v, X, Pb, Rb, hid, Ab, Bb, att, mid, acc,
    w_sem, rs_send, rs_recv, ag_send, ag_recv, pair_sem,
):
    t = lax.axis_index("tp")
    dp = lax.axis_index("dp")
    D = x_ref.shape[1]
    rc = x_ref.shape[0] // C
    Dh = D // NDP
    F = wg_v.shape[1]
    M = T * rc
    has_left, has_right = t > 0, t < T - 1
    left, right = {"tp": jnp.maximum(t - 1, 0)}, {"tp": jnp.minimum(t + 1, T - 1)}
    partners = [{"dp": lax.rem(dp + o, NDP)} for o in range(1, NDP)]

    barrier(
        has_left.astype(jnp.int32) + has_right.astype(jnp.int32) + (NDP - 1),
        [(has_left, left), (has_right, right)] + [(t >= 0, p) for p in partners],
    )

    rows_at = pl.ds(pl.multiple_of(dp * Dh, 128), Dh)
    weights = [
        (wo_ref, lambda: wo_v.at[:, rows_at]),
        (wg_ref, lambda: wg_v.at[rows_at]),
        (wu_ref, lambda: wu_v.at[rows_at]),
        (wd_ref, lambda: wd_v.at[:, rows_at]),
    ]

    def weight_copies(i):
        src, dst = weights[i]
        copies = [pltpu.make_async_copy(src, dst(), w_sem.at[0, i])]
        for o, partner in enumerate(partners):
            copies.append(
                pltpu.make_async_remote_copy(
                    src, dst(), w_sem.at[1 + 2 * o, i], w_sem.at[2 + 2 * o, i],
                    device_id=partner, device_id_type=MESH,
                )
            )
        return copies

    for i in range(4):
        for copy in weight_copies(i):
            copy.start()

    def weight_wait(i):
        src, dst = weights[i]
        for o, copy in enumerate(weight_copies(i)):
            if o == 0:
                copy.wait()
            else:
                copy.wait_recv()

    def pair_copies(kind, s, src, half, dst):
        def cut(owner):
            if half:
                return src.at[..., pl.ds(pl.multiple_of(owner * Dh, 128), Dh)]
            return src

        copies = [pltpu.make_async_copy(cut(dp), dst.at[dp, s], pair_sem.at[0, kind, s])]
        for o, partner in enumerate(partners):
            copies.append(
                pltpu.make_async_remote_copy(
                    cut(partner["dp"]), dst.at[dp, s],
                    pair_sem.at[1 + 2 * o, kind, s], pair_sem.at[2 + 2 * o, kind, s],
                    device_id=partner, device_id_type=MESH,
                )
            )
        return copies

    def pair_of(kind, s):
        return pair_copies(
            kind, s,
            *[
                (X.at[s], True, rows_pair),
                (hid.at[s], False, hid_pair),
                (X.at[s], True, branch_pair),
                (Ab.at[s], False, gate_pair),
                (Bb.at[s], False, up_pair),
                (X.at[s], True, attn_pair),
                (heads_ref.at[:, s], False, head_pair),
            ][kind],
        )

    def pair_start(kind, s):
        for copy in pair_of(kind, s):
            copy.start()

    def pair_sent(kind, s):
        for o, copy in enumerate(pair_of(kind, s)):
            if o == 0:
                copy.wait()
            else:
                copy.wait_send()

    def pair_received(kind, s):
        for copy in pair_of(kind, s)[1:]:
            copy.wait_recv()

    def rs_copy(s, side, k, j):
        if side == 0:
            slot, peer = j, right
        else:
            slot, peer = jnp.where(j == t - 1, T, j), left
        return pltpu.make_async_remote_copy(
            Pb.at[s, j], Rb.at[s, slot], rs_send.at[s, side, k], rs_recv.at[s, side, k],
            device_id=peer, device_id_type=MESH,
        )

    def rs_block(side, k):
        return (T - 1 - k + t) if side == 0 else (k - (T - 1 - t))

    def rs_sends(side, k):
        return (t <= k) if side == 0 else (T - 1 - t <= k)

    def ag_copy(s, side, k, j):
        return pltpu.make_async_remote_copy(
            X.at[s, j], X.at[s, j], ag_send.at[s, side, k], ag_recv.at[s, side, k],
            device_id=right if side == 0 else left, device_id_type=MESH,
        )

    def ag_block(side, k):
        return (t - k) if side == 0 else (t + k)

    def ag_sends(side, k):
        return (t >= k) & has_right if side == 0 else (t + k <= T - 1) & has_left

    def rs_start(s):
        for side in (0, 1):

            @pl.when(rs_sends(side, 0))
            def _():
                rs_copy(s, side, 0, rs_block(side, 0)).start()

    def rs_step(s, k):
        for side in (0, 1):
            j = rs_block(side, k)
            came = has_left if side == 0 else has_right

            @pl.when(rs_sends(side, k))
            def _():
                @pl.when(came)
                def _():
                    rs_copy(s, side, k - 1, j).wait_recv()
                    Pb[s, j] = (Pb[s, j].astype(F32) + Rb[s, j].astype(F32)).astype(BF)

                rs_copy(s, side, k, j).start()

    def rs_sent(s):
        for side in (0, 1):
            for k in range(T - 1):

                @pl.when(rs_sends(side, k))
                def _():
                    rs_copy(s, side, k, rs_block(side, k)).wait_send()

    def rs_finish(s):
        acc[...] = Pb[s, t].astype(F32)

        @pl.when(has_left)
        def _():
            rs_copy(s, 0, T - 2, t).wait_recv()
            acc[...] += Rb[s, t].astype(F32)

        @pl.when(has_right)
        def _():
            rs_copy(s, 1, T - 2, t).wait_recv()
            acc[...] += Rb[s, T].astype(F32)

    def ag_start(s):
        for side in (0, 1):

            @pl.when(ag_sends(side, 0))
            def _():
                ag_copy(s, side, 0, t).start()

    def ag_step(s, k):
        for side in (0, 1):
            j = ag_block(side, k)
            there = (j >= 0) if side == 0 else (j <= T - 1)

            @pl.when(there)
            def _():
                ag_copy(s, side, k - 1, j).wait_recv()
                if k <= T - 2:

                    @pl.when(has_right if side == 0 else has_left)
                    def _():
                        ag_copy(s, side, k, j).start()

    def ag_sent(s):
        for side in (0, 1):
            for k in range(T - 1):

                @pl.when(ag_sends(side, k))
                def _():
                    ag_copy(s, side, k, ag_block(side, k)).wait_send()

    def local_rows(n, s):
        own = pl.ds(pl.multiple_of(s * rc, rc), rc)
        total = acc[...]

        @pl.when(n == 0)
        def _():
            att[s] = total
            middle = x_ref[own].astype(F32) + total * inverse_rms(total) * gain_ref[1:2]
            mid[s] = middle
            X[s, t] = (middle * inverse_rms(middle) * gain_ref[2:3]).astype(BF)

        @pl.when(n == 1)
        def _():
            scale = inverse_rms(total)
            out_ref[own] = (mid[s] + total * scale * gain_ref[3:4]).astype(BF)
            grad, terms = rms_back(total, scale, gain_ref[3:4], ct_ref[own].astype(F32))
            gsum_ref[2:3] += terms
            X[s, t] = grad.astype(BF)

        @pl.when(n == 2)
        def _():
            middle, attention = mid[s], att[s]
            grad, terms = rms_back(middle, inverse_rms(middle), gain_ref[2:3], total)
            gsum_ref[1:2] += terms
            middle_delta = ct_ref[own].astype(F32) + grad
            mdelta_ref[own] = middle_delta
            grad, terms = rms_back(attention, inverse_rms(attention), gain_ref[1:2], middle_delta)
            gsum_ref[0:1] += terms
            X[s, t] = grad.astype(BF)

    def comm(tau, w, a):
        back = tau - a

        @pl.when((back >= 0) & (back < 3 * C))
        def _():
            n, s = back // C, lax.rem(back, C)
            if w <= T - 2:
                rs_step(s, w)
            elif w == T - 1:
                rs_finish(s)
                local_rows(n, s)
                ag_start(s)
            else:
                ag_step(s, w - (T - 1))

    def tiles(width, body):
        tile = tile_of(width)

        def step(i, carry):
            body(pl.ds(pl.multiple_of(i * tile, tile), tile), tile)
            return carry

        lax.fori_loop(0, width // tile, step, 0)

    def rows_of(s):
        return X[s].reshape(M, D)

    def store_part(s, at, tile, value):
        Pb[s, :, :, at] = value.astype(BF).reshape(T, rc, tile)

    def tick(tau, carry):
        n, s = tau // C, lax.rem(tau, C)

        @pl.when((n >= 1) & (n <= 2))
        def _():
            rs_sent(s)

        @pl.when(n == 1)
        def _():
            @pl.when(s == 0)
            def _():
                weight_wait(1)
                weight_wait(2)

            pair_start(0, s)

            def gate_up(at, tile):
                gate = dot_nn(rows_of(s), wg_v[:, at])
                up = dot_nn(rows_of(s), wu_v[:, at])
                inner = jnp.tanh(0.7978845608028654 * (gate + 0.044715 * gate * gate * gate))
                half = 0.5 * (1.0 + inner)
                gelu = gate * half
                slope = half + 0.5 * gate * (1.0 - inner * inner) * (
                    0.7978845608028654 * (1.0 + 0.134145 * gate * gate)
                )
                hid[s, :, at] = (gelu * up).astype(BF)
                Ab[s, :, at] = (up * slope).astype(BF)
                Bb[s, :, at] = gelu.astype(BF)

            tiles(F, gate_up)
            pair_start(1, s)

        @pl.when(n == 2)
        def _():
            pair_start(2, s)

            def gate_up_delta(at, tile):
                delta = dot_nt(rows_of(s), wd_v[at, :])
                Ab[s, :, at] = (delta * Ab[s, :, at].astype(F32)).astype(BF)
                Bb[s, :, at] = (delta * Bb[s, :, at].astype(F32)).astype(BF)

            tiles(F, gate_up_delta)
            pair_start(3, s)
            pair_start(4, s)

        for a in range(1, T):
            comm(tau, 2 * a - 1, a)

        @pl.when(n == 0)
        def _():
            pair_start(6, s)
            heads = heads_ref[:, s].reshape(M, heads_ref.shape[3])
            tiles(D, lambda at, tile: store_part(s, at, tile, dot_nn(heads, wo_v[:, at])))

        @pl.when(n == 1)
        def _():
            @pl.when(s == 0)
            def _():
                weight_wait(3)

            tiles(D, lambda at, tile: store_part(s, at, tile, dot_nn(hid[s], wd_v[:, at])))
            pair_sent(0, s)
            ag_sent(s)

        @pl.when(n == 2)
        def _():
            tiles(
                D,
                lambda at, tile: store_part(
                    s, at, tile, dot_nt(Ab[s], wg_v[at, :]) + dot_nt(Bb[s], wu_v[at, :])
                ),
            )
            pair_sent(2, s)
            ag_sent(s)

        @pl.when(n <= 2)
        def _():
            rs_start(s)

        @pl.when(n == 3)
        def _():
            pair_start(5, s)
            hdelta_ref[:, s] = (
                dot_nt(rows_of(s), wo_v[...]).astype(BF).reshape(T, rc, heads_ref.shape[3])
            )

        for a in range(1, T):
            comm(tau, 2 * a, a)
        return carry

    gsum_ref[...] = jnp.zeros_like(gsum_ref)
    weight_wait(0)
    lax.fori_loop(0, 4 * C, tick, 0)

    for i in range(4):
        for copy in weight_copies(i)[1:]:
            copy.wait_send()

    def close(s, carry):
        for kind in (1, 3, 4, 5, 6):
            pair_sent(kind, s)
        for kind in range(7):
            pair_received(kind, s)
        rs_sent(s)
        ag_sent(s)
        return carry

    lax.fori_loop(0, C, close, 0)


def core_call(layer_in, cotangent, norm_gains, head_flat, w_out, w_gate, w_up, w_down):
    T, NDP = lax.axis_size("tp"), lax.axis_size("dp")
    C = T
    Lr, D = layer_in.shape
    rc = Lr // C
    Hq = w_out.shape[0]
    Dh = D // NDP
    F = w_gate.shape[1]
    M = T * rc
    any_spec = pl.BlockSpec(memory_space=pl.ANY)
    vm = pl.BlockSpec(memory_space=pltpu.VMEM)
    sds = jax.ShapeDtypeStruct
    outs = pl.pallas_call(
        functools.partial(core_kernel, T, C, NDP),
        out_shape=(
            sds((Lr, D), BF), sds((Lr, D), F32), sds((3, D), F32), sds((T, C, rc, Hq), BF),
            sds((NDP, C, T, rc, Dh), BF), sds((NDP, C, M, F), BF), sds((NDP, C, T, rc, Dh), BF),
            sds((NDP, C, M, F), BF), sds((NDP, C, M, F), BF), sds((NDP, C, T, rc, Dh), BF),
            sds((NDP, C, T, rc, Hq), BF),
        ),
        in_specs=[vm, vm, vm, vm] + [any_spec] * 4,
        out_specs=[vm, vm, vm, vm] + [any_spec] * 7,
        scratch_shapes=[
            pltpu.VMEM((Hq, D), BF), pltpu.VMEM((D, F), BF), pltpu.VMEM((D, F), BF), pltpu.VMEM((F, D), BF),
            pltpu.VMEM((C, T, rc, D), BF), pltpu.VMEM((C, T, rc, D), BF), pltpu.VMEM((C, T + 1, rc, D), BF),
            pltpu.VMEM((C, M, F), BF), pltpu.VMEM((C, M, F), BF), pltpu.VMEM((C, M, F), BF),
            pltpu.VMEM((C, rc, D), F32), pltpu.VMEM((C, rc, D), F32), pltpu.VMEM((rc, D), F32),
            pltpu.SemaphoreType.DMA((2 * NDP - 1, 4)),
            pltpu.SemaphoreType.DMA((C, 2, T - 1)), pltpu.SemaphoreType.DMA((C, 2, T - 1)),
            pltpu.SemaphoreType.DMA((C, 2, T - 1)), pltpu.SemaphoreType.DMA((C, 2, T - 1)),
            pltpu.SemaphoreType.DMA((2 * NDP - 1, 7, C)),
        ],
        compiler_params=pltpu.CompilerParams(
            collective_id=0, has_side_effects=True, vmem_limit_bytes=66_000_000
        ),
        name="core",
    )(layer_in, cotangent, norm_gains, head_flat.reshape(T, C, rc, Hq), w_out, w_gate, w_up, w_down)
    out, mdelta, gsum, hdelta, rows, hidden, branch, gate, up, attn, heads = outs
    flat = lambda a: a.reshape(NDP * T * Lr, a.shape[-1])
    return (
        out, mdelta, gsum, hdelta.reshape(T * Lr, Hq),
        flat(rows), flat(hidden), flat(branch), flat(gate), flat(up), flat(attn), flat(heads),
    )


def flip(index, bit):
    return index + bit * (1 - 2 * lax.rem(index // bit, 2))


def flips(index, mask):
    bit = 1
    while bit <= mask:
        if mask & bit:
            index = flip(index, bit)
        bit *= 2
    return index


def dot_tn(former, latter):
    return lax.dot_general(former, latter, (((0,), (0,)), ((), ())), preferred_element_type=F32)


def sub_sums(bits):
    sums = [0]
    for bit in bits:
        sums = sums + [s + bit for s in sums]
    return sums


def bits_below(count):
    return [1 << i for i in range(count.bit_length() - 1)]


def tail_kernel(
    T, NC, NDP, KH, NS,
    x_ref, mdelta_ref, gain_ref, gsum_ref, q_ref, hd_ref, logt_ref, rdelta_ref, cos_ref, sin_ref,
    k_ref, v_ref, rows1_ref, wq_ref, wk_ref, wv_ref,
    rows_ref, branch_ref, attn_ref, head_ref, gate_ref, up_ref, hid_ref,
    igrad_ref, gains_ref, gate_o, up_o, down_o, out_o, q_o, k_o, v_o,
    L, Rc, Hd, RQ, RKV, WQ, WK, WV, Pe, *rest,
):
    m = NC.bit_length() - 1
    Rv, rest = rest[:m], rest[m:]
    (
        st, dq, kvb, kvs, kvr, Pb, Rb, acc, G, GR,
        l_sem, r_sem, w_sem, pair_sem, e_send, e_recv, st_sem, kv_send, kv_recv,
        rs_send, rs_recv, g_send, g_recv, kvb_sem,
    ) = rest
    t, c, dp = lax.axis_index("tp"), lax.axis_index("ctx"), lax.axis_index("dp")
    Lr, D = x_ref.shape
    R, Hq = q_ref.shape
    KVd = KH * HEAD
    GS = Hq // KVd
    Dh, RB = D // NDP, D // NDP // NC
    F = gate_ref.shape[1]
    W = Rc.shape[2] // 2
    NF = F // (2 * W)
    wide_units, units = 3 * NF, 3 * NF + 3
    narrow = Hq // 2
    scale = HEAD**-0.5

    def along(axis, index):
        return {axis: index}

    others = [along("tp", lax.rem(t + o, T)) for o in range(1, T)]
    others += [along("ctx", lax.rem(c + o, NC)) for o in range(1, NC)]
    partners = [along("dp", lax.rem(dp + o, NDP)) for o in range(1, NDP)]
    sem = pltpu.get_barrier_semaphore()
    for peer in others + partners:
        pl.semaphore_signal(sem, inc=1, device_id=peer, device_id_type=MESH)
    pl.semaphore_wait(sem, len(others + partners))

    def remote(src, dst, send, recv, peer):
        return pltpu.make_async_remote_copy(src, dst, send, recv, device_id=peer, device_id_type=MESH)

    firsts = [rows_ref, branch_ref, attn_ref]

    def first_copy(i):
        return pltpu.make_async_copy(firsts[i], L.at[i % 2], l_sem.at[i])

    def half_of(ref, owner):
        return ref.at[:, pl.ds(pl.multiple_of(owner * Dh, 128), Dh)]

    rows_at = pl.ds(pl.multiple_of(dp * Dh, 128), Dh)
    token_at = pl.ds(pl.multiple_of(dp * R, 128), R)
    spread = [
        (lambda owner: half_of(rows1_ref, owner), L.at[2, token_at]),
        (lambda owner: wq_ref, WQ.at[rows_at]),
        (lambda owner: wk_ref, WK.at[rows_at]),
        (lambda owner: wv_ref, WV.at[rows_at]),
    ]

    def spread_local(i):
        return pltpu.make_async_copy(spread[i][0](dp), spread[i][1], w_sem.at[0, i])

    def spread_remote(i, o):
        return remote(
            spread[i][0](partners[o]["dp"]), spread[i][1],
            w_sem.at[1 + 2 * o, i], w_sem.at[2 + 2 * o, i], partners[o],
        )

    kinds = [gate_ref, up_ref, hid_ref]

    def chunk_copy(u, kind):
        at = pl.ds(pl.multiple_of((u - kind * NF) * 2 * W, 128), 2 * W)
        return pltpu.make_async_copy(kinds[kind].at[:, at], Rc.at[lax.rem(u, 2)], r_sem.at[lax.rem(u, 2)])

    def chunk_start(u):
        for kind in range(3):

            @pl.when((u >= kind * NF) & (u < (kind + 1) * NF))
            def _():
                chunk_copy(u, kind).start()

    first_copy(0).start()
    chunk_start(0)
    first_copy(1).start()
    for i in range(4):
        spread_local(i).start()
        for o in range(NDP - 1):
            spread_remote(i, o).start()
    head_copy = pltpu.make_async_copy(head_ref, Hd, l_sem.at[3])
    head_copy.start()

    orders = [bits_below(NC), bits_below(NC)[::-1]]
    first_of = [sum(NC >> (i + 1) for i in range(k)) for k in range(m)]

    def e_copy(u, par, k, n, w):
        order = orders[par]
        kept = sub_sums(order[k + 1:])[n]
        slot = lax.rem(u, NS)
        at = first_of[k] + n
        return remote(
            Pe.at[slot, par, flips(c, kept + order[k]), :, pl.ds(0, w)],
            Rv[k].at[slot, par, n, :, pl.ds(0, w)],
            e_send.at[slot, par, at], e_recv.at[slot, par, at],
            along("ctx", flip(c, order[k])),
        )

    def e_sent(u, w):
        for par in (0, 1):
            for k in range(m):
                for n in range(NC >> (k + 1)):
                    e_copy(u, par, k, n, w).wait_send()

    def e_product(u, w):
        slot = lax.rem(u, NS)

        def store(par, first, second):
            Pe[slot, par, :, :, :w] = dot_tn(first, second).reshape(NC, RB, w).astype(BF)

        if w == W:
            for kind in range(3):

                @pl.when((u >= kind * NF) & (u < (kind + 1) * NF))
                def _():
                    chunk_copy(u, kind).wait()

            @pl.when(u == 0)
            def _():
                first_copy(0).wait()

            @pl.when(u == 2 * NF)
            def _():
                first_copy(1).wait()
                first_copy(2).start()

            chunk_start(u + 1)
            at = jnp.where(u >= 2 * NF, 1, 0)
            for par in (0, 1):
                store(par, L[at], Rc[lax.rem(u, 2), :, par * W:(par + 1) * W])
        else:

            @pl.when(u == wide_units)
            def _():
                first_copy(2).wait()
                head_copy.wait()
                for par in (0, 1):
                    store(par, L[0], Hd[:, par * w:(par + 1) * w])

            @pl.when(u == wide_units + 1)
            def _():
                for par in (0, 1):
                    store(par, L[2], RQ[:, :, par * w:(par + 1) * w].reshape(NDP * R, w))

            @pl.when(u == wide_units + 2)
            def _():
                for par in (0, 1):
                    store(par, L[2], RKV[:, par].reshape(NDP * R, w))

    def e_send_step(u, k, w):
        for par in (0, 1):
            for n in range(NC >> (k + 1)):
                e_copy(u, par, k, n, w).start()

    def e_add(u, k, w):
        slot = lax.rem(u, NS)
        for par in (0, 1):
            for n in range(NC >> (k + 1)):
                e_copy(u, par, k, n, w).wait_recv()
                if k < m - 1:
                    kept = flips(c, sub_sums(orders[par][k + 1:])[n])
                    Pe[slot, par, kept, :, :w] = (
                        Pe[slot, par, kept, :, :w].astype(F32) + Rv[k][slot, par, n, :, :w].astype(F32)
                    ).astype(BF)

    def out_copies(u, w):
        two = lax.rem(u, 2)

        def copy(par, dst):
            return pltpu.make_async_copy(st.at[two, par, :, pl.ds(0, w)], dst, st_sem.at[two, par])

        if w == W:
            pairs = []
            for kind, dst in enumerate([gate_o, up_o, down_o]):
                base = (u - kind * NF) * 2 * W
                pairs.append((
                    (u >= kind * NF) & (u < (kind + 1) * NF),
                    [copy(p, dst.at[:, pl.ds(pl.multiple_of(base + p * W, 128), W)]) for p in (0, 1)],
                ))
            return pairs
        return [
            (u == wide_units, [copy(p, out_o.at[:, pl.ds(p * w, w)]) for p in (0, 1)]),
            (u == wide_units + 1, [copy(p, q_o.at[:, pl.ds(p * w, w)]) for p in (0, 1)]),
            (u == wide_units + 2, [copy(0, k_o), copy(1, v_o)]),
        ]

    def out_wait(u):
        for w in (W, narrow):
            for here, copies in out_copies(u, w):

                @pl.when(here)
                def _():
                    for copy in copies:
                        copy.wait()

    def e_finish(u, w):
        slot, two = lax.rem(u, NS), lax.rem(u, 2)
        e_add(u, m - 1, w)
        out_wait(u - 2)
        for par in (0, 1):
            st[two, par, :, :w] = Pe[slot, par, c, :, :w].astype(F32) + Rv[m - 1][slot, par, 0, :, :w].astype(F32)
        for here, copies in out_copies(u, w):

            @pl.when(here)
            def _():
                for copy in copies:
                    copy.start()

    def by_width(u, body):
        @pl.when((u >= 0) & (u < wide_units))
        def _():
            body(W)

        @pl.when((u >= wide_units) & (u < units))
        def _():
            body(narrow)

    key_tile = min(256, R)

    def kv_copy(d):
        return remote(
            kvs.at[lax.rem(d, kvs.shape[0])], kvr.at[d - 1], kv_send.at[d - 1], kv_recv.at[d - 1],
            along("ctx", jnp.maximum(c - d, 0)),
        )

    def block_copies(block):
        at = pl.ds(pl.multiple_of(block * R, 128), R)
        two = lax.rem(block, 2)
        return [
            pltpu.make_async_copy(ref.at[at], kvb.at[two, i], kvb_sem.at[two, i])
            for i, ref in enumerate((k_ref, v_ref))
        ]

    def block_start(block):
        for copy in block_copies(block):
            copy.start()

    def block_wait(block):
        for copy in block_copies(block):
            copy.wait()

    def attend(two, masked, dst):
        for kh in range(KH):
            cols = slice(kh * HEAD, (kh + 1) * HEAD)

            def key_step(i, carry):
                start = pl.multiple_of(i * key_tile, key_tile)
                at = pl.ds(start, key_tile)
                keys, values = kvb[two, 0, at, cols], kvb[two, 1, at, cols]
                key_sum = jnp.zeros((key_tile, HEAD), F32)
                value_sum = jnp.zeros((key_tile, HEAD), F32)
                for g in range(GS):
                    h = kh * GS + g
                    head = slice(h * HEAD, (h + 1) * HEAD)
                    query, delta = q_ref[:, head], hd_ref[:, head]
                    bent = jnp.tanh(dot_nt(keys, query) * (scale / CAP))
                    prob = jnp.exp(CAP * bent - logt_ref[h:h + 1, :])
                    if masked:
                        key_pos = start + lax.broadcasted_iota(jnp.int32, prob.shape, 0)
                        prob = jnp.where(key_pos <= lax.broadcasted_iota(jnp.int32, prob.shape, 1), prob, 0.0)
                    grad = prob * (dot_nt(values, delta) - rdelta_ref[h:h + 1, :]) * (1.0 - bent * bent)
                    grad = grad.astype(BF)
                    value_sum += dot_nn(prob.astype(BF), delta)
                    key_sum += dot_nn(grad, query)
                    dq[:, head] += dot_tn(grad, keys)
                rows = pl.ds(start, key_tile)
                kvs[dst, 0, rows, cols] = (key_sum * scale).astype(BF)
                kvs[dst, 1, rows, cols] = value_sum.astype(BF)
                return carry

            lax.fori_loop(0, R // key_tile, key_step, 0)

    def attention():
        dq[...] = jnp.zeros_like(dq)
        block_start(0)

        def far(block, carry):
            d = c - block

            @pl.when(block < c)
            def _():
                slot = lax.rem(d, kvs.shape[0])
                block_wait(block)
                block_start(block + 1)

                @pl.when(d + kvs.shape[0] <= c)
                def _():
                    kv_copy(d + kvs.shape[0]).wait_send()

                attend(lax.rem(block, 2), False, slot)
                kv_copy(d).start()

            return carry

        lax.fori_loop(0, NC - 1, far, 0)

        @pl.when(c >= kvs.shape[0])
        def _():
            kv_copy(kvs.shape[0]).wait_send()

        block_wait(c)
        attend(lax.rem(c, 2), True, 0)

    def turned(values, h):
        a, b = values[:, h * HEAD:h * HEAD + HEAD // 2], values[:, h * HEAD + HEAD // 2:(h + 1) * HEAD]
        cosine, sine = cos_ref[...], sin_ref[...]
        return jnp.concatenate([a * cosine + b * sine, b * cosine - a * sine], axis=1).astype(BF)

    def pair_remote(i, o):
        ref = [RQ, RKV][i]
        return remote(ref.at[dp], ref.at[dp], pair_sem.at[2 * o, i], pair_sem.at[2 * o + 1, i], partners[o])

    has_left, has_right = t > 0, t < T - 1

    def rs_copy(side, k, j):
        if side == 0:
            slot, peer = j, jnp.minimum(t + 1, T - 1)
        else:
            slot, peer = jnp.where(j == t - 1, T, j), jnp.maximum(t - 1, 0)
        return remote(Pb.at[j], Rb.at[slot], rs_send.at[side, k], rs_recv.at[side, k], along("tp", peer))

    def rs_block(side, k):
        return (T - 1 - k + t) if side == 0 else (k - (T - 1 - t))

    def rs_sends(side, k):
        return (t <= k) & has_right if side == 0 else (T - 1 - t <= k) & has_left

    def rs_step(k):
        for side in (0, 1):
            j = rs_block(side, k)

            @pl.when(rs_sends(side, k))
            def _():
                if k:

                    @pl.when(has_left if side == 0 else has_right)
                    def _():
                        rs_copy(side, k - 1, j).wait_recv()
                        Pb[j] = (Pb[j].astype(F32) + Rb[j].astype(F32)).astype(BF)

                rs_copy(side, k, j).start()

    def own_keys():
        for which in range(2):
            dst = []
            for kh in range(KH):
                dst.append(kvs[0, which, :, kh * HEAD:(kh + 1) * HEAD].astype(F32))
            acc[which] = jnp.concatenate(dst, axis=1) if KH > 1 else dst[0]

        def come(i, carry):
            d = i + 1

            @pl.when(c + d <= NC - 1)
            def _():
                kv_copy(d).wait_recv()
                for which in range(2):
                    acc[which] += kvr[d - 1, which].astype(F32)

            return carry

        lax.fori_loop(0, NC - 1, come, 0)
        for kh in range(KH):
            cols = slice(kh * HEAD, (kh + 1) * HEAD)
            RKV[dp, 0, :, cols] = turned(acc[0], kh)
        RKV[dp, 1] = acc[1].astype(BF)
        for h in range(Hq // HEAD):
            RQ[dp, :, h * HEAD:(h + 1) * HEAD] = turned(dq[...] * scale, h)
        for i in range(2):
            for o in range(NDP - 1):
                pair_remote(i, o).start()
        for i in range(4):
            spread_local(i).wait()
            for o in range(NDP - 1):
                spread_remote(i, o).wait_recv()
        tile = tile_of(D)

        def part(i, carry):
            at = pl.ds(pl.multiple_of(i * tile, tile), tile)
            terms = dot_nt(RQ[dp], WQ[at, :]) + dot_nt(RKV[dp, 0], WK[at, :]) + dot_nt(RKV[dp, 1], WV[at, :])
            Pb[:, :, at] = terms.astype(BF).reshape(T, Lr, tile)
            return carry

        lax.fori_loop(0, D // tile, part, 0)
        rs_step(0)

    def rs_finish():
        igrad_ref[...] = Pb[t].astype(F32)

        @pl.when(has_left)
        def _():
            rs_copy(0, T - 2, t).wait_recv()
            igrad_ref[...] += Rb[t].astype(F32)

        @pl.when(has_right)
        def _():
            rs_copy(1, T - 2, t).wait_recv()
            igrad_ref[...] += Rb[T].astype(F32)

        rows = x_ref[...].astype(F32)
        grad, terms = rms_back(rows, inverse_rms(rows), gain_ref[0:1], igrad_ref[...])
        igrad_ref[...] = mdelta_ref[...] + grad
        G[0, 0:1] = terms
        G[0, 1:4] = gsum_ref[...]

    meets = [("tp", t, b) for b in bits_below(T)] + [("ctx", c, b) for b in bits_below(NC)]
    meets += [("dp", dp, b) for b in bits_below(NDP)]

    def g_copy(k):
        axis, index, bit = meets[k]
        return remote(G.at[k], GR.at[k], g_send.at[k], g_recv.at[k], along(axis, flip(index, bit)))

    def tick(i, carry):
        def start(w):
            @pl.when(i >= NS)
            def _():
                by_width(i - NS, lambda before: e_sent(i - NS, before))

            e_product(i, w)
            e_send_step(i, 0, w)

        by_width(i, start)

        @pl.when(i == 1)
        def _():
            attention()

        @pl.when(i == 2)
        def _():
            own_keys()

        for k in range(1, T - 1):

            @pl.when(i == 2 + k)
            def _():
                rs_step(k)

        @pl.when(i == 1 + T)
        def _():
            rs_finish()
            g_copy(0).start()

        for k in range(len(meets)):

            @pl.when(i == 2 + T + k)
            def _():
                g_copy(k).wait_recv()
                G[k + 1] = G[k] + GR[k]
                if k + 1 < len(meets):
                    g_copy(k + 1).start()

        @pl.when(i == wide_units)
        def _():
            for p in range(2):
                for o in range(NDP - 1):
                    pair_remote(p, o).wait_recv()

        for k in range(1, m):

            def middle(w):
                e_add(i - k, k - 1, w)
                e_send_step(i - k, k, w)

            by_width(i - k, middle)
        by_width(i - m, lambda w: e_finish(i - m, w))
        return carry

    lax.fori_loop(0, units + m, tick, 0)
    gains_ref[...] = G[len(meets)]

    for u in (units - 2, units - 1):
        out_wait(jnp.int32(u))
    for u in range(units - NS, units):
        by_width(jnp.int32(u), lambda w: e_sent(jnp.int32(u), w))
    for side in (0, 1):
        for k in range(T - 1):

            @pl.when(rs_sends(side, k))
            def _():
                rs_copy(side, k, rs_block(side, k)).wait_send()

    for k in range(len(meets)):
        g_copy(k).wait_send()
    for o in range(NDP - 1):
        for i in range(4):
            spread_remote(i, o).wait_send()
        for i in range(2):
            pair_remote(i, o).wait_send()

    def kv_close(i, carry):
        d = i + 1

        @pl.when((d <= c) & (d < kvs.shape[0]))
        def _():
            kv_copy(d).wait_send()

        return carry

    lax.fori_loop(0, min(NC - 1, kvs.shape[0] - 1), kv_close, 0)


def tail_call(
    layer_in, middle_delta, norm_gains, gain_sums, query, heads_delta, log_totals, row_delta, cosine, sine,
    keys, values, rows_one, w_query, w_key, w_value, rows, branch, attn, heads, gate, up, hidden,
):
    T, NC, NDP = lax.axis_size("tp"), lax.axis_size("ctx"), lax.axis_size("dp")
    Lr, D = layer_in.shape
    R, Hq = query.shape
    KVd = w_key.shape[1]
    KH = KVd // HEAD
    Dh = D // NDP
    RB = Dh // NC
    F = gate.shape[1]
    W = tile_of(F) // 2
    m = NC.bit_length() - 1
    NS = max(4, m + 1)
    tokens = NDP * R
    kv_slots = min(NC, 4)
    meets = sum(n.bit_length() - 1 for n in (T, NC, NDP))
    any_spec = pl.BlockSpec(memory_space=pl.ANY)
    vm = pl.BlockSpec(memory_space=pltpu.VMEM)
    sds = jax.ShapeDtypeStruct
    dma = pltpu.SemaphoreType.DMA
    return pl.pallas_call(
        functools.partial(tail_kernel, T, NC, NDP, KH, NS),
        out_shape=(
            sds((Lr, D), F32), sds((4, D), F32),
            sds((RB, F), F32), sds((RB, F), F32), sds((RB, F), F32), sds((RB, Hq), F32),
            sds((RB, Hq), F32), sds((RB, KVd), F32), sds((RB, KVd), F32),
        ),
        in_specs=[vm] * 10 + [any_spec] * 13,
        out_specs=[vm] * 2 + [any_spec] * 7,
        scratch_shapes=[
            pltpu.VMEM((3, tokens, Dh), BF), pltpu.VMEM((2, tokens, 2 * W), BF), pltpu.VMEM((tokens, Hq), BF),
            pltpu.VMEM((NDP, R, Hq), BF), pltpu.VMEM((NDP, 2, R, KVd), BF),
            pltpu.VMEM((D, Hq), BF), pltpu.VMEM((D, KVd), BF), pltpu.VMEM((D, KVd), BF),
            pltpu.VMEM((NS, 2, NC, RB, W), BF),
            *[pltpu.VMEM((NS, 2, NC >> (k + 1), RB, W), BF) for k in range(m)],
            pltpu.VMEM((2, 2, RB, W), F32), pltpu.VMEM((R, Hq), F32), pltpu.VMEM((2, 2, R, KVd), BF),
            pltpu.VMEM((kv_slots, 2, R, KVd), BF), pltpu.VMEM((NC - 1, 2, R, KVd), BF),
            pltpu.VMEM((T, Lr, D), BF), pltpu.VMEM((T + 1, Lr, D), BF), pltpu.VMEM((2, R, KVd), F32),
            pltpu.VMEM((meets + 1, 4, D), F32), pltpu.VMEM((meets, 4, D), F32),
            dma((4,)), dma((2,)), dma((2 * NDP - 1, 4)), dma((2 * (NDP - 1), 2)),
            dma((NS, 2, NC - 1)), dma((NS, 2, NC - 1)), dma((2, 2)), dma((NC - 1,)), dma((NC - 1,)),
            dma((2, T - 1)), dma((2, T - 1)), dma((meets,)), dma((meets,)), dma((2, 2)),
        ],
        compiler_params=pltpu.CompilerParams(
            collective_id=1, has_side_effects=True, vmem_limit_bytes=66_000_000
        ),
        name="tail",
    )(
        layer_in, middle_delta, norm_gains, gain_sums, query, heads_delta, log_totals, row_delta, cosine, sine,
        keys, values, rows_one, w_query, w_key, w_value, rows, branch, attn, heads, gate, up, hidden,
    )


def rms_scale(values, gain_row):
    return values * lax.rsqrt(jnp.mean(values * values, axis=-1, keepdims=True) + EPS) * gain_row


def rope_tables(positions, head_width):
    half_width = head_width // 2
    frequency = THETA ** (-(jnp.arange(half_width, dtype=jnp.float32) * 2.0) / head_width)
    angles = positions.astype(jnp.float32)[:, None] * frequency[None, :]
    cosine = jnp.concatenate([jnp.cos(angles), jnp.cos(angles)], axis=1)
    sine_table = jnp.concatenate([jnp.sin(angles), jnp.sin(angles)], axis=1)
    return (cosine, sine_table)


def rotate(values, cosine, sine_table, sine_sign):
    half_width = values.shape[-1] // 2
    turned = jnp.concatenate([-values[..., half_width:], values[..., :half_width]], axis=-1)
    return values * cosine[:, None, :] + turned * (sine_sign * sine_table)[:, None, :]


def fetch_weights(query_part, key_part, value_part):
    return (
        lax.all_gather(query_part, "dp", axis=0, tiled=True),
        lax.all_gather(key_part, "dp", axis=0, tiled=True),
        lax.all_gather(value_part, "dp", axis=0, tiled=True),
    )


def spread_rows(rows_part):
    return lax.all_gather(rows_part, "tp", axis=0, tiled=True)


def shards(layer_in, cotangent, norm_gains, w_query, w_key, w_value, w_out, w_gate, w_up, w_down):
    tp_count = lax.axis_size("tp")
    ctx_count = lax.axis_size("ctx")
    local_rows = layer_in.shape[0]
    block_rows = local_rows * tp_count
    seq_rows = block_rows * ctx_count
    positions = lax.axis_index("ctx") * block_rows + jnp.arange(block_rows, dtype=jnp.int32)
    last_pos = positions[block_rows - 1]
    cosine, sine_table = rope_tables(positions, HEAD)
    score_scale = HEAD ** (-0.5)
    query_full, key_full, value_full = fetch_weights(w_query, w_key, w_value)
    query_heads = query_full.shape[1] // HEAD
    key_heads = key_full.shape[1] // HEAD
    group_size = query_heads // key_heads
    input_float = layer_in.astype(jnp.float32)
    normed_one = rms_scale(input_float, norm_gains[0]).astype(jnp.bfloat16)
    rows_one = spread_rows(normed_one)
    query_proj = jnp.dot(rows_one, query_full, preferred_element_type=jnp.float32).reshape(
        block_rows, query_heads, HEAD
    )
    query_rot = (
        rotate(query_proj, cosine, sine_table, 1.0)
        .astype(jnp.bfloat16)
        .reshape(block_rows, key_heads, group_size, HEAD)
    )
    key_proj = jnp.dot(rows_one, key_full, preferred_element_type=jnp.float32).reshape(
        block_rows, key_heads, HEAD
    )
    key_rot = rotate(key_proj, cosine, sine_table, 1.0).astype(jnp.bfloat16)
    value_rows = (
        jnp.dot(rows_one, value_full, preferred_element_type=jnp.float32)
        .astype(jnp.bfloat16)
        .reshape(block_rows, key_heads, HEAD)
    )

    def scores_for(key_block):
        piece_len = key_block.shape[0]
        raw_scores = (
            jnp.einsum("bkgh,lkh->kgbl", query_rot, key_block, preferred_element_type=jnp.float32)
            * score_scale
        )
        capped = CAP * jnp.tanh(raw_scores / CAP)
        key_pos = jnp.arange(piece_len, dtype=jnp.int32)
        allowed = key_pos[None, :] <= positions[:, None]
        return (capped, allowed)

    accum_zero = jnp.zeros((block_rows, key_heads, group_size, HEAD), jnp.float32)
    totals_zero = jnp.zeros((key_heads, group_size, block_rows), jnp.float32)
    accumulated = accum_zero
    totals = totals_zero
    key_block = lax.all_gather(key_rot, "ctx", axis=0, tiled=True)
    value_block = lax.all_gather(value_rows, "ctx", axis=0, tiled=True)

    def attend_compute_piece():
        capped, allowed = scores_for(key_block)
        exp_scores = jnp.where(allowed, jnp.exp(capped), 0.0)
        weights = exp_scores.astype(jnp.bfloat16)
        summed = jnp.einsum(
            "kgbl,lkh->bkgh", weights, value_block, preferred_element_type=jnp.float32
        )
        return (summed, jnp.sum(exp_scores, axis=-1))

    def attend_keep_piece():
        return (accumulated, totals)

    accumulated, totals = lax.cond(
        jnp.int32(0) <= last_pos, attend_compute_piece, attend_keep_piece
    )
    head_rows = (accumulated / jnp.transpose(totals, (2, 0, 1))[..., None]).astype(jnp.bfloat16)
    log_totals = jnp.log(totals)
    head_flat = head_rows.reshape(block_rows, query_heads * HEAD)

    core = core_call(layer_in, cotangent, norm_gains, head_flat, w_out, w_gate, w_up, w_down)
    layer_out, middle_delta, gain_sums, heads_delta, *pairs = core
    rows_pair, hid_pair, branch_pair, gate_pair, up_pair, attn_pair, head_pair = pairs
    heads_delta = heads_delta.reshape(block_rows, key_heads, group_size, HEAD)
    row_delta = jnp.einsum(
        "bkgh,bkgh->kgb", heads_delta, head_rows, preferred_element_type=jnp.float32
    )
    heads_here = query_heads
    input_grad, gain_total, grad_gate, grad_up, down_turned, out_turned, grad_query, grad_key, grad_value = tail_call(
        layer_in,
        middle_delta,
        norm_gains,
        gain_sums,
        query_rot.reshape(block_rows, query_heads * HEAD),
        heads_delta.reshape(block_rows, query_heads * HEAD),
        log_totals.reshape(heads_here, block_rows),
        row_delta.reshape(heads_here, block_rows),
        cosine[:, : HEAD // 2],
        sine_table[:, : HEAD // 2],
        key_block.reshape(seq_rows, key_heads * HEAD),
        value_block.reshape(seq_rows, key_heads * HEAD),
        rows_one,
        w_query,
        w_key,
        w_value,
        rows_pair,
        branch_pair,
        attn_pair,
        head_pair,
        gate_pair,
        up_pair,
        hid_pair,
    )
    grad_down, grad_out = down_turned.T, out_turned.T
    ranks = (lax.axis_index("dp") * ctx_count + lax.axis_index("ctx")) * tp_count + lax.axis_index("tp")
    gain_width = gain_total.shape[1] // (lax.axis_size("dp") * ctx_count * tp_count)
    gain_grads = lax.dynamic_slice_in_dim(gain_total, ranks * gain_width, gain_width, 1)
    return (
        layer_out,
        input_grad,
        gain_grads,
        grad_query,
        grad_key,
        grad_value,
        grad_out,
        grad_gate,
        grad_up,
        grad_down,
    )


def solution(mesh):
    return jax.shard_map(
        shards,
        mesh=mesh,
        in_specs=(
            P(("dp", "ctx", "tp"), None),
            P(("dp", "ctx", "tp"), None),
            P(),
            P("dp", "tp"),
            P("dp", "tp"),
            P("dp", "tp"),
            P("tp", "dp"),
            P("dp", "tp"),
            P("dp", "tp"),
            P("tp", "dp"),
        ),
        out_specs=(
            P(("dp", "ctx", "tp"), None),
            P(("dp", "ctx", "tp"), None),
            P(None, ("dp", "ctx", "tp")),
            P(("dp", "ctx"), "tp"),
            P(("dp", "ctx"), "tp"),
            P(("dp", "ctx"), "tp"),
            P("tp", ("dp", "ctx")),
            P(("dp", "ctx"), "tp"),
            P(("dp", "ctx"), "tp"),
            P("tp", ("dp", "ctx")),
        ),
        check_vma=False,
    )
```

```python
import functools

import jax
import jax.numpy as jnp
from jax import lax
from jax.experimental import pallas as pl
from jax.experimental.pallas import tpu as pltpu
from jax.sharding import PartitionSpec as P

HEAD = 256
EPS = 1e-06
CAP = 50.0
THETA = 10000.0
MESH = pl.DeviceIdType.MESH
BF = jnp.bfloat16
F32 = jnp.float32


def tile_of(width):
    for tile in (768, 512, 256, 128):
        if width % tile == 0:
            return tile
    return width


def inverse_rms(values):
    return lax.rsqrt(jnp.mean(values * values, axis=-1, keepdims=True) + EPS)


def rms_back(values, scale, gain, delta):
    weighted = delta * gain
    inner = jnp.mean(weighted * values, axis=-1, keepdims=True)
    grad = scale * weighted - values * (scale * scale * scale * inner)
    return grad, jnp.sum(delta * values * scale, axis=0, keepdims=True)


def dot_nt(former, latter):
    return lax.dot_general(former, latter, (((1,), (1,)), ((), ())), preferred_element_type=F32)


def dot_nn(former, latter):
    return jnp.dot(former, latter, preferred_element_type=F32)


def barrier(count_of, peers):
    sem = pltpu.get_barrier_semaphore()
    for present, device_id in peers:

        @pl.when(present)
        def _():
            pl.semaphore_signal(sem, inc=1, device_id=device_id, device_id_type=MESH)

    pl.semaphore_wait(sem, count_of)


def core_kernel(
    T, C, NDP,
    x_ref, ct_ref, gain_ref, heads_ref, wo_ref, wg_ref, wu_ref, wd_ref,
    out_ref, mdelta_ref, gsum_ref, hdelta_ref,
    rows_pair, hid_pair, branch_pair, gate_pair, up_pair, attn_pair, head_pair,
    wo_v, wg_v, wu_v, wd_v, X, Pb, Rb, hid, Ab, Bb, att, mid, acc,
    w_sem, rs_send, rs_recv, ag_send, ag_recv, pair_sem,
):
    t = lax.axis_index("tp")
    dp = lax.axis_index("dp")
    D = x_ref.shape[1]
    rc = x_ref.shape[0] // C
    Dh = D // NDP
    F = wg_v.shape[1]
    M = T * rc
    has_left, has_right = t > 0, t < T - 1
    left, right = {"tp": jnp.maximum(t - 1, 0)}, {"tp": jnp.minimum(t + 1, T - 1)}
    partners = [{"dp": lax.rem(dp + o, NDP)} for o in range(1, NDP)]

    barrier(
        has_left.astype(jnp.int32) + has_right.astype(jnp.int32) + (NDP - 1),
        [(has_left, left), (has_right, right)] + [(t >= 0, p) for p in partners],
    )

    rows_at = pl.ds(pl.multiple_of(dp * Dh, 128), Dh)
    weights = [
        (wo_ref, lambda: wo_v.at[:, rows_at]),
        (wg_ref, lambda: wg_v.at[rows_at]),
        (wu_ref, lambda: wu_v.at[rows_at]),
        (wd_ref, lambda: wd_v.at[:, rows_at]),
    ]

    def weight_copies(i):
        src, dst = weights[i]
        copies = [pltpu.make_async_copy(src, dst(), w_sem.at[0, i])]
        for o, partner in enumerate(partners):
            copies.append(
                pltpu.make_async_remote_copy(
                    src, dst(), w_sem.at[1 + 2 * o, i], w_sem.at[2 + 2 * o, i],
                    device_id=partner, device_id_type=MESH,
                )
            )
        return copies

    for i in range(4):
        for copy in weight_copies(i):
            copy.start()

    def weight_wait(i):
        src, dst = weights[i]
        for o, copy in enumerate(weight_copies(i)):
            if o == 0:
                copy.wait()
            else:
                copy.wait_recv()

    def pair_copies(kind, s, src, half, dst):
        def cut(owner):
            if half:
                return src.at[..., pl.ds(pl.multiple_of(owner * Dh, 128), Dh)]
            return src

        copies = [pltpu.make_async_copy(cut(dp), dst.at[dp, s], pair_sem.at[0, kind, s])]
        for o, partner in enumerate(partners):
            copies.append(
                pltpu.make_async_remote_copy(
                    cut(partner["dp"]), dst.at[dp, s],
                    pair_sem.at[1 + 2 * o, kind, s], pair_sem.at[2 + 2 * o, kind, s],
                    device_id=partner, device_id_type=MESH,
                )
            )
        return copies

    def pair_of(kind, s):
        return pair_copies(
            kind, s,
            *[
                (X.at[s], True, rows_pair),
                (hid.at[s], False, hid_pair),
                (X.at[s], True, branch_pair),
                (Ab.at[s], False, gate_pair),
                (Bb.at[s], False, up_pair),
                (X.at[s], True, attn_pair),
                (heads_ref.at[:, s], False, head_pair),
            ][kind],
        )

    def pair_start(kind, s):
        for copy in pair_of(kind, s):
            copy.start()

    def pair_sent(kind, s):
        for o, copy in enumerate(pair_of(kind, s)):
            if o == 0:
                copy.wait()
            else:
                copy.wait_send()

    def pair_received(kind, s):
        for copy in pair_of(kind, s)[1:]:
            copy.wait_recv()

    def rs_copy(s, side, k, j):
        if side == 0:
            slot, peer = j, right
        else:
            slot, peer = jnp.where(j == t - 1, T, j), left
        return pltpu.make_async_remote_copy(
            Pb.at[s, j], Rb.at[s, slot], rs_send.at[s, side, k], rs_recv.at[s, side, k],
            device_id=peer, device_id_type=MESH,
        )

    def rs_block(side, k):
        return (T - 1 - k + t) if side == 0 else (k - (T - 1 - t))

    def rs_sends(side, k):
        return (t <= k) if side == 0 else (T - 1 - t <= k)

    def ag_copy(s, side, k, j):
        return pltpu.make_async_remote_copy(
            X.at[s, j], X.at[s, j], ag_send.at[s, side, k], ag_recv.at[s, side, k],
            device_id=right if side == 0 else left, device_id_type=MESH,
        )

    def ag_block(side, k):
        return (t - k) if side == 0 else (t + k)

    def ag_sends(side, k):
        return (t >= k) & has_right if side == 0 else (t + k <= T - 1) & has_left

    def rs_start(s):
        for side in (0, 1):

            @pl.when(rs_sends(side, 0))
            def _():
                rs_copy(s, side, 0, rs_block(side, 0)).start()

    def rs_step(s, k):
        for side in (0, 1):
            j = rs_block(side, k)
            came = has_left if side == 0 else has_right

            @pl.when(rs_sends(side, k))
            def _():
                @pl.when(came)
                def _():
                    rs_copy(s, side, k - 1, j).wait_recv()
                    Pb[s, j] = (Pb[s, j].astype(F32) + Rb[s, j].astype(F32)).astype(BF)

                rs_copy(s, side, k, j).start()

    def rs_sent(s):
        for side in (0, 1):
            for k in range(T - 1):

                @pl.when(rs_sends(side, k))
                def _():
                    rs_copy(s, side, k, rs_block(side, k)).wait_send()

    def rs_finish(s):
        acc[...] = Pb[s, t].astype(F32)

        @pl.when(has_left)
        def _():
            rs_copy(s, 0, T - 2, t).wait_recv()
            acc[...] += Rb[s, t].astype(F32)

        @pl.when(has_right)
        def _():
            rs_copy(s, 1, T - 2, t).wait_recv()
            acc[...] += Rb[s, T].astype(F32)

    def ag_start(s):
        for side in (0, 1):

            @pl.when(ag_sends(side, 0))
            def _():
                ag_copy(s, side, 0, t).start()

    def ag_step(s, k):
        for side in (0, 1):
            j = ag_block(side, k)
            there = (j >= 0) if side == 0 else (j <= T - 1)

            @pl.when(there)
            def _():
                ag_copy(s, side, k - 1, j).wait_recv()
                if k <= T - 2:

                    @pl.when(has_right if side == 0 else has_left)
                    def _():
                        ag_copy(s, side, k, j).start()

    def ag_sent(s):
        for side in (0, 1):
            for k in range(T - 1):

                @pl.when(ag_sends(side, k))
                def _():
                    ag_copy(s, side, k, ag_block(side, k)).wait_send()

    def local_rows(n, s):
        own = pl.ds(pl.multiple_of(s * rc, rc), rc)
        total = acc[...]

        @pl.when(n == 0)
        def _():
            att[s] = total
            middle = x_ref[own].astype(F32) + total * inverse_rms(total) * gain_ref[1:2]
            mid[s] = middle
            X[s, t] = (middle * inverse_rms(middle) * gain_ref[2:3]).astype(BF)

        @pl.when(n == 1)
        def _():
            scale = inverse_rms(total)
            out_ref[own] = (mid[s] + total * scale * gain_ref[3:4]).astype(BF)
            grad, terms = rms_back(total, scale, gain_ref[3:4], ct_ref[own].astype(F32))
            gsum_ref[2:3] += terms
            X[s, t] = grad.astype(BF)

        @pl.when(n == 2)
        def _():
            middle, attention = mid[s], att[s]
            grad, terms = rms_back(middle, inverse_rms(middle), gain_ref[2:3], total)
            gsum_ref[1:2] += terms
            middle_delta = ct_ref[own].astype(F32) + grad
            mdelta_ref[own] = middle_delta
            grad, terms = rms_back(attention, inverse_rms(attention), gain_ref[1:2], middle_delta)
            gsum_ref[0:1] += terms
            X[s, t] = grad.astype(BF)

    def comm(tau, w, a):
        back = tau - a

        @pl.when((back >= 0) & (back < 3 * C))
        def _():
            n, s = back // C, lax.rem(back, C)
            if w <= T - 2:
                rs_step(s, w)
            elif w == T - 1:
                rs_finish(s)
                local_rows(n, s)
                ag_start(s)
            else:
                ag_step(s, w - (T - 1))

    def tiles(width, body):
        tile = tile_of(width)

        def step(i, carry):
            body(pl.ds(pl.multiple_of(i * tile, tile), tile), tile)
            return carry

        lax.fori_loop(0, width // tile, step, 0)

    def rows_of(s):
        return X[s].reshape(M, D)

    def store_part(s, at, tile, value):
        Pb[s, :, :, at] = value.astype(BF).reshape(T, rc, tile)

    def tick(tau, carry):
        n, s = tau // C, lax.rem(tau, C)

        @pl.when((n >= 1) & (n <= 2))
        def _():
            rs_sent(s)

        @pl.when(n == 1)
        def _():
            @pl.when(s == 0)
            def _():
                weight_wait(1)
                weight_wait(2)

            pair_start(0, s)

            def gate_up(at, tile):
                gate = dot_nn(rows_of(s), wg_v[:, at])
                up = dot_nn(rows_of(s), wu_v[:, at])
                inner = jnp.tanh(0.7978845608028654 * (gate + 0.044715 * gate * gate * gate))
                half = 0.5 * (1.0 + inner)
                gelu = gate * half
                slope = half + 0.5 * gate * (1.0 - inner * inner) * (
                    0.7978845608028654 * (1.0 + 0.134145 * gate * gate)
                )
                hid[s, :, at] = (gelu * up).astype(BF)
                Ab[s, :, at] = (up * slope).astype(BF)
                Bb[s, :, at] = gelu.astype(BF)

            tiles(F, gate_up)
            pair_start(1, s)

        @pl.when(n == 2)
        def _():
            pair_start(2, s)

            def gate_up_delta(at, tile):
                delta = dot_nt(rows_of(s), wd_v[at, :])
                Ab[s, :, at] = (delta * Ab[s, :, at].astype(F32)).astype(BF)
                Bb[s, :, at] = (delta * Bb[s, :, at].astype(F32)).astype(BF)

            tiles(F, gate_up_delta)
            pair_start(3, s)
            pair_start(4, s)

        for a in range(1, T):
            comm(tau, 2 * a - 1, a)

        @pl.when(n == 0)
        def _():
            pair_start(6, s)
            heads = heads_ref[:, s].reshape(M, heads_ref.shape[3])
            tiles(D, lambda at, tile: store_part(s, at, tile, dot_nn(heads, wo_v[:, at])))

        @pl.when(n == 1)
        def _():
            @pl.when(s == 0)
            def _():
                weight_wait(3)

            tiles(D, lambda at, tile: store_part(s, at, tile, dot_nn(hid[s], wd_v[:, at])))
            pair_sent(0, s)
            ag_sent(s)

        @pl.when(n == 2)
        def _():
            tiles(
                D,
                lambda at, tile: store_part(
                    s, at, tile, dot_nt(Ab[s], wg_v[at, :]) + dot_nt(Bb[s], wu_v[at, :])
                ),
            )
            pair_sent(2, s)
            ag_sent(s)

        @pl.when(n <= 2)
        def _():
            rs_start(s)

        @pl.when(n == 3)
        def _():
            pair_start(5, s)
            hdelta_ref[:, s] = (
                dot_nt(rows_of(s), wo_v[...]).astype(BF).reshape(T, rc, heads_ref.shape[3])
            )

        for a in range(1, T):
            comm(tau, 2 * a, a)
        return carry

    gsum_ref[...] = jnp.zeros_like(gsum_ref)
    weight_wait(0)
    lax.fori_loop(0, 4 * C, tick, 0)

    for i in range(4):
        for copy in weight_copies(i)[1:]:
            copy.wait_send()

    def close(s, carry):
        for kind in (1, 3, 4, 5, 6):
            pair_sent(kind, s)
        for kind in range(7):
            pair_received(kind, s)
        rs_sent(s)
        ag_sent(s)
        return carry

    lax.fori_loop(0, C, close, 0)


def core_call(layer_in, cotangent, norm_gains, head_flat, w_out, w_gate, w_up, w_down):
    T, NDP = lax.axis_size("tp"), lax.axis_size("dp")
    C = T
    Lr, D = layer_in.shape
    rc = Lr // C
    Hq = w_out.shape[0]
    Dh = D // NDP
    F = w_gate.shape[1]
    M = T * rc
    any_spec = pl.BlockSpec(memory_space=pl.ANY)
    vm = pl.BlockSpec(memory_space=pltpu.VMEM)
    sds = jax.ShapeDtypeStruct
    outs = pl.pallas_call(
        functools.partial(core_kernel, T, C, NDP),
        out_shape=(
            sds((Lr, D), BF), sds((Lr, D), F32), sds((3, D), F32), sds((T, C, rc, Hq), BF),
            sds((NDP, C, T, rc, Dh), BF), sds((NDP, C, M, F), BF), sds((NDP, C, T, rc, Dh), BF),
            sds((NDP, C, M, F), BF), sds((NDP, C, M, F), BF), sds((NDP, C, T, rc, Dh), BF),
            sds((NDP, C, T, rc, Hq), BF),
        ),
        in_specs=[vm, vm, vm, vm] + [any_spec] * 4,
        out_specs=[vm, vm, vm, vm] + [any_spec] * 7,
        scratch_shapes=[
            pltpu.VMEM((Hq, D), BF), pltpu.VMEM((D, F), BF), pltpu.VMEM((D, F), BF), pltpu.VMEM((F, D), BF),
            pltpu.VMEM((C, T, rc, D), BF), pltpu.VMEM((C, T, rc, D), BF), pltpu.VMEM((C, T + 1, rc, D), BF),
            pltpu.VMEM((C, M, F), BF), pltpu.VMEM((C, M, F), BF), pltpu.VMEM((C, M, F), BF),
            pltpu.VMEM((C, rc, D), F32), pltpu.VMEM((C, rc, D), F32), pltpu.VMEM((rc, D), F32),
            pltpu.SemaphoreType.DMA((2 * NDP - 1, 4)),
            pltpu.SemaphoreType.DMA((C, 2, T - 1)), pltpu.SemaphoreType.DMA((C, 2, T - 1)),
            pltpu.SemaphoreType.DMA((C, 2, T - 1)), pltpu.SemaphoreType.DMA((C, 2, T - 1)),
            pltpu.SemaphoreType.DMA((2 * NDP - 1, 7, C)),
        ],
        compiler_params=pltpu.CompilerParams(
            collective_id=0, has_side_effects=True, vmem_limit_bytes=66_000_000
        ),
        name="core",
    )(layer_in, cotangent, norm_gains, head_flat.reshape(T, C, rc, Hq), w_out, w_gate, w_up, w_down)
    out, mdelta, gsum, hdelta, rows, hidden, branch, gate, up, attn, heads = outs
    flat = lambda a: a.reshape(NDP * T * Lr, a.shape[-1])
    return (
        out, mdelta, gsum, hdelta.reshape(T * Lr, Hq),
        flat(rows), flat(hidden), flat(branch), flat(gate), flat(up), flat(attn), flat(heads),
    )


def front_kernel(
    T, NC, NDP, KH, C,
    x_ref, gain_ref, freq_ref, wq_ref, wk_ref, wv_ref,
    q_o, heads_o, logt_o, cos_o, sin_o, kv_o, rows1_o,
    X, WQ, WK, WV, KV, turned_sum, totals,
    w_sem, ag_send, ag_recv, pair_sem, kv_send, kv_recv, out_sem,
):
    t, c, dp = lax.axis_index("tp"), lax.axis_index("ctx"), lax.axis_index("dp")
    Lr, D = x_ref.shape
    R, Hq = q_o.shape
    rc = Lr // C
    KVd = KH * HEAD
    GS = Hq // KVd
    Dh = D // NDP
    scale = HEAD**-0.5
    has_left, has_right = t > 0, t < T - 1

    def remote(src, dst, send, recv, axis, index):
        return pltpu.make_async_remote_copy(
            src, dst, send, recv, device_id={axis: index}, device_id_type=MESH
        )

    partners = [lax.rem(dp + o, NDP) for o in range(1, NDP)]
    peers = [("tp", lax.rem(t + o, T)) for o in range(1, T)]
    peers += [("ctx", lax.rem(c + o, NC)) for o in range(1, NC)]
    peers += [("dp", p) for p in partners]
    sem = pltpu.get_barrier_semaphore()
    for axis, index in peers:
        pl.semaphore_signal(sem, inc=1, device_id={axis: index}, device_id_type=MESH)
    pl.semaphore_wait(sem, len(peers))

    rows_at = pl.ds(pl.multiple_of(dp * Dh, 128), Dh)
    weights = [(wq_ref, WQ), (wk_ref, WK), (wv_ref, WV)]

    def weight_local(i):
        return pltpu.make_async_copy(weights[i][0], weights[i][1].at[rows_at], w_sem.at[0, i])

    def weight_remote(i, o):
        return remote(
            weights[i][0], weights[i][1].at[rows_at], w_sem.at[1 + 2 * o, i], w_sem.at[2 + 2 * o, i],
            "dp", partners[o],
        )

    for i in range(3):
        weight_local(i).start()
        for o in range(NDP - 1):
            weight_remote(i, o).start()

    def ag_copy(s, side, k, j):
        at = pl.ds(s * rc, rc)
        peer = jnp.minimum(t + 1, T - 1) if side == 0 else jnp.maximum(t - 1, 0)
        return remote(X.at[j, at], X.at[j, at], ag_send.at[s, side, k], ag_recv.at[s, side, k], "tp", peer)

    def ag_block(side, k):
        return (t - k) if side == 0 else (t + k)

    def ag_there(side, k):
        return (t >= k) if side == 0 else (t + k <= T - 1)

    def onward(side):
        return has_right if side == 0 else has_left

    rows = x_ref[...].astype(F32)
    X[t] = (rows * inverse_rms(rows) * gain_ref[0:1]).astype(BF)
    for s in range(C):
        for side in (0, 1):

            @pl.when(onward(side))
            def _():
                ag_copy(s, side, 0, t).start()

    position = (c * R + lax.broadcasted_iota(jnp.int32, (R, HEAD // 2), 0)).astype(F32)
    angles = position * freq_ref[...]
    cos_o[...] = jnp.cos(angles)
    sin_o[...] = jnp.sin(angles)
    for i in range(3):
        weight_local(i).wait()
        for o in range(NDP - 1):
            weight_remote(i, o).wait_recv()

    def kv_copy(d, j):
        return remote(
            KV.at[c, j], KV.at[c, j], kv_send.at[d - 1, j], kv_recv.at[d - 1, j],
            "ctx", jnp.minimum(c + d, NC - 1),
        )

    def kv_from(b, j):
        d = c - b
        return remote(KV.at[b, j], KV.at[b, j], kv_send.at[d - 1, j], kv_recv.at[d - 1, j], "ctx", c)

    def pair_copies(j):
        def half(owner):
            return X.at[j, :, pl.ds(pl.multiple_of(owner * Dh, 128), Dh)]

        copies = [pltpu.make_async_copy(half(dp), rows1_o.at[dp, j], pair_sem.at[0, j])]
        for o, partner in enumerate(partners):
            copies.append(
                remote(
                    half(partner), rows1_o.at[dp, j], pair_sem.at[1 + 2 * o, j], pair_sem.at[2 + 2 * o, j],
                    "dp", partner,
                )
            )
        return copies

    def turned(values, h, at):
        a, b = values[:, h * HEAD:h * HEAD + HEAD // 2], values[:, h * HEAD + HEAD // 2:(h + 1) * HEAD]
        cosine, sine = cos_o[at], sin_o[at]
        return jnp.concatenate([a * cosine - b * sine, b * cosine + a * sine], axis=1).astype(BF)

    def project(j):
        for copy in pair_copies(j):
            copy.start()
        at = pl.ds(pl.multiple_of(j * Lr, Lr), Lr)
        values = dot_nn(X[j], WK[...])
        for kh in range(KH):
            KV[c, j, 0, :, kh * HEAD:(kh + 1) * HEAD] = turned(values, kh, at)
        KV[c, j, 1] = dot_nn(X[j], WV[...]).astype(BF)

        def push(i, carry):
            @pl.when(c + 1 + i <= NC - 1)
            def _():
                kv_copy(i + 1, j).start()

            return carry

        lax.fori_loop(0, NC - 1, push, 0)
        values = dot_nn(X[j], WQ[...])
        for h in range(Hq // HEAD):
            q_o[at, h * HEAD:(h + 1) * HEAD] = turned(values, h, at)

    def gather(k, carry):
        for side in (0, 1):

            @pl.when(ag_there(side, k) & (k > 0))
            def _():
                for s in range(C):
                    ag_copy(s, side, k - 1, ag_block(side, k)).wait_recv()

                    @pl.when(onward(side) & (k <= T - 2))
                    def _():
                        ag_copy(s, side, k, ag_block(side, k)).start()

        for side in (0, 1):

            @pl.when(ag_there(side, k) & ((k > 0) | (side == 0)))
            def _():
                project(ag_block(side, k))

        return carry

    lax.fori_loop(0, T, gather, 0)

    per = max(1, 256 // Lr)
    tile = per * Lr
    turned_sum[...] = jnp.zeros_like(turned_sum)
    totals[...] = jnp.zeros_like(totals)

    def out_copy(b):
        return pltpu.make_async_copy(KV.at[b], kv_o.at[b], out_sem.at[b])

    def key_step(b, p, masked):
        for kh in range(KH):
            cols = slice(kh * HEAD, (kh + 1) * HEAD)
            keys = KV[b, pl.ds(p * per, per), 0, :, cols].reshape(tile, HEAD)
            values = KV[b, pl.ds(p * per, per), 1, :, cols].reshape(tile, HEAD)
            for g in range(GS):
                h = kh * GS + g
                scores = dot_nt(keys, q_o[:, h * HEAD:(h + 1) * HEAD])
                weights = jnp.exp(CAP * jnp.tanh(scores * (scale / CAP)))
                if masked:
                    key_pos = p * tile + lax.broadcasted_iota(jnp.int32, weights.shape, 0)
                    allowed = key_pos <= lax.broadcasted_iota(jnp.int32, weights.shape, 1)
                    weights = jnp.where(allowed, weights, 0.0)
                totals[h:h + 1] += jnp.sum(weights, axis=0, keepdims=True)
                turned_sum[h] += dot_tn(values, weights.astype(BF))

    def own_step(p, carry):
        key_step(c, p, True)
        return carry

    out_copy(c).start()
    lax.fori_loop(0, T // per, own_step, 0)

    def far_block(i, carry):
        @pl.when(i < c)
        def _():
            b = c - 1 - i
            for j in range(T):
                kv_from(b, j).wait_recv()
            out_copy(b).start()

            def far_step(p, carry):
                key_step(b, p, False)
                return carry

            lax.fori_loop(0, T // per, far_step, 0)

        return carry

    lax.fori_loop(0, NC - 1, far_block, 0)
    for h in range(Hq // HEAD):
        heads_o[:, h * HEAD:(h + 1) * HEAD] = (turned_sum[h] / totals[h:h + 1]).T.astype(BF)
    logt_o[...] = jnp.log(totals[...])

    for i in range(3):
        for o in range(NDP - 1):
            weight_remote(i, o).wait_send()
    for s in range(C):
        for side in (0, 1):
            for k in range(T - 1):

                @pl.when(ag_there(side, k) & onward(side))
                def _():
                    ag_copy(s, side, k, ag_block(side, k)).wait_send()

    for j in range(T):
        copies = pair_copies(j)
        copies[0].wait()
        for copy in copies[1:]:
            copy.wait()

    def close(i, carry):
        @pl.when(c + 1 + i <= NC - 1)
        def _():
            for j in range(T):
                kv_copy(i + 1, j).wait_send()

        return carry

    lax.fori_loop(0, NC - 1, close, 0)

    def close_out(b, carry):
        @pl.when(b <= c)
        def _():
            out_copy(b).wait()

        return carry

    lax.fori_loop(0, NC, close_out, 0)


def front_call(layer_in, norm_gains, frequency, w_query, w_key, w_value):
    T, NC, NDP = lax.axis_size("tp"), lax.axis_size("ctx"), lax.axis_size("dp")
    C = T
    Lr, D = layer_in.shape
    R = T * Lr
    Hq, KVd = w_query.shape[1], w_key.shape[1]
    Dh = D // NDP
    H = Hq // HEAD
    any_spec = pl.BlockSpec(memory_space=pl.ANY)
    vm = pl.BlockSpec(memory_space=pltpu.VMEM)
    sds = jax.ShapeDtypeStruct
    dma = pltpu.SemaphoreType.DMA
    return pl.pallas_call(
        functools.partial(front_kernel, T, NC, NDP, KVd // HEAD, C),
        out_shape=(
            sds((R, Hq), BF), sds((R, Hq), BF), sds((H, R), F32),
            sds((R, HEAD // 2), F32), sds((R, HEAD // 2), F32),
            sds((NC, T, 2, Lr, KVd), BF), sds((NDP, T, Lr, Dh), BF),
        ),
        in_specs=[vm] * 3 + [any_spec] * 3,
        out_specs=[vm] * 5 + [any_spec] * 2,
        scratch_shapes=[
            pltpu.VMEM((T, Lr, D), BF), pltpu.VMEM((D, Hq), BF), pltpu.VMEM((D, KVd), BF), pltpu.VMEM((D, KVd), BF),
            pltpu.VMEM((NC, T, 2, Lr, KVd), BF), pltpu.VMEM((H, HEAD, R), F32), pltpu.VMEM((H, R), F32),
            dma((2 * NDP - 1, 3)), dma((C, 2, T - 1)), dma((C, 2, T - 1)), dma((2 * NDP - 1, T)),
            dma((NC - 1, T)), dma((NC - 1, T)), dma((NC,)),
        ],
        compiler_params=pltpu.CompilerParams(
            collective_id=2, has_side_effects=True, vmem_limit_bytes=66_000_000
        ),
        name="front",
    )(layer_in, norm_gains, frequency, w_query, w_key, w_value)


def flip(index, bit):
    return index + bit * (1 - 2 * lax.rem(index // bit, 2))


def flips(index, mask):
    bit = 1
    while bit <= mask:
        if mask & bit:
            index = flip(index, bit)
        bit *= 2
    return index


def dot_tn(former, latter):
    return lax.dot_general(former, latter, (((0,), (0,)), ((), ())), preferred_element_type=F32)


def sub_sums(bits):
    sums = [0]
    for bit in bits:
        sums = sums + [s + bit for s in sums]
    return sums


def bits_below(count):
    return [1 << i for i in range(count.bit_length() - 1)]


def tail_kernel(
    T, NC, NDP, KH, NS,
    x_ref, mdelta_ref, gain_ref, gsum_ref, q_ref, hd_ref, heads_ref, logt_ref, cos_ref, sin_ref,
    kv_ref, rows1_ref, wq_ref, wk_ref, wv_ref,
    rows_ref, branch_ref, attn_ref, head_ref, gate_ref, up_ref, hid_ref,
    igrad_ref, gains_ref, gate_o, up_o, down_o, out_o, q_o, k_o, v_o,
    L, Rc, Hd, RQ, RKV, WQ, WK, WV, Pe, *rest,
):
    m = NC.bit_length() - 1
    Rv, rest = rest[:m], rest[m:]
    (
        st, dq, rdelta, kvb, kvs, kvr, Pb, Rb, acc, G, GR,
        l_sem, r_sem, w_sem, pair_sem, e_send, e_recv, st_sem, kv_send, kv_recv,
        rs_send, rs_recv, g_send, g_recv, kvb_sem,
    ) = rest
    t, c, dp = lax.axis_index("tp"), lax.axis_index("ctx"), lax.axis_index("dp")
    Lr, D = x_ref.shape
    R, Hq = q_ref.shape
    KVd = KH * HEAD
    GS = Hq // KVd
    Dh, RB = D // NDP, D // NDP // NC
    F = gate_ref.shape[1]
    W = Rc.shape[2] // 2
    NF = F // (2 * W)
    wide_units, units = 3 * NF, 3 * NF + 3
    narrow = Hq // 2
    scale = HEAD**-0.5

    def along(axis, index):
        return {axis: index}

    others = [along("tp", lax.rem(t + o, T)) for o in range(1, T)]
    others += [along("ctx", lax.rem(c + o, NC)) for o in range(1, NC)]
    partners = [along("dp", lax.rem(dp + o, NDP)) for o in range(1, NDP)]
    sem = pltpu.get_barrier_semaphore()
    for peer in others + partners:
        pl.semaphore_signal(sem, inc=1, device_id=peer, device_id_type=MESH)
    pl.semaphore_wait(sem, len(others + partners))

    def remote(src, dst, send, recv, peer):
        return pltpu.make_async_remote_copy(src, dst, send, recv, device_id=peer, device_id_type=MESH)

    firsts = [rows_ref, branch_ref, attn_ref]

    def first_copy(i):
        return pltpu.make_async_copy(firsts[i], L.at[i % 2], l_sem.at[i % 2])

    rows_at = pl.ds(pl.multiple_of(dp * Dh, 128), Dh)
    spread = [
        (lambda owner: wq_ref, WQ.at[rows_at]),
        (lambda owner: wk_ref, WK.at[rows_at]),
        (lambda owner: wv_ref, WV.at[rows_at]),
    ]

    def spread_local(i):
        return pltpu.make_async_copy(spread[i][0](dp), spread[i][1], w_sem.at[0, i])

    def spread_remote(i, o):
        return remote(
            spread[i][0](partners[o]["dp"]), spread[i][1],
            w_sem.at[1 + 2 * o, i], w_sem.at[2 + 2 * o, i], partners[o],
        )

    kinds = [gate_ref, up_ref, hid_ref]

    def chunk_copy(u, kind):
        at = pl.ds(pl.multiple_of((u - kind * NF) * 2 * W, 128), 2 * W)
        return pltpu.make_async_copy(kinds[kind].at[:, at], Rc.at[lax.rem(u, 2)], r_sem.at[lax.rem(u, 2)])

    def chunk_start(u):
        for kind in range(3):

            @pl.when((u >= kind * NF) & (u < (kind + 1) * NF))
            def _():
                chunk_copy(u, kind).start()

    first_copy(0).start()
    chunk_start(0)
    first_copy(1).start()
    for i in range(3):
        spread_local(i).start()
        for o in range(NDP - 1):
            spread_remote(i, o).start()
    head_copy = pltpu.make_async_copy(head_ref, Hd, l_sem.at[3])
    head_copy.start()
    rows1_copy = pltpu.make_async_copy(rows1_ref, L.at[2], l_sem.at[2])
    rows1_copy.start()

    orders = [bits_below(NC), bits_below(NC)[::-1]]
    first_of = [sum(NC >> (i + 1) for i in range(k)) for k in range(m)]

    def e_copy(u, par, k, n, w):
        order = orders[par]
        kept = sub_sums(order[k + 1:])[n]
        slot = lax.rem(u, NS)
        at = first_of[k] + n
        return remote(
            Pe.at[slot, par, flips(c, kept + order[k]), :, pl.ds(0, w)],
            Rv[k].at[slot, par, n, :, pl.ds(0, w)],
            e_send.at[slot, par, at], e_recv.at[slot, par, at],
            along("ctx", flip(c, order[k])),
        )

    def e_sent(u, w):
        for par in (0, 1):
            for k in range(m):
                for n in range(NC >> (k + 1)):
                    e_copy(u, par, k, n, w).wait_send()

    def e_product(u, w):
        slot = lax.rem(u, NS)

        def store(par, first, second):
            Pe[slot, par, :, :, :w] = dot_tn(first, second).reshape(NC, RB, w).astype(BF)

        if w == W:
            for kind in range(3):

                @pl.when((u >= kind * NF) & (u < (kind + 1) * NF))
                def _():
                    chunk_copy(u, kind).wait()

            @pl.when(u == 0)
            def _():
                first_copy(0).wait()

            @pl.when(u == 2 * NF)
            def _():
                first_copy(1).wait()
                first_copy(2).start()

            chunk_start(u + 1)
            at = jnp.where(u >= 2 * NF, 1, 0)
            for par in (0, 1):
                store(par, L[at], Rc[lax.rem(u, 2), :, par * W:(par + 1) * W])
        else:

            @pl.when(u == wide_units)
            def _():
                first_copy(2).wait()
                head_copy.wait()
                for par in (0, 1):
                    store(par, L[0], Hd[:, par * w:(par + 1) * w])

            @pl.when(u == wide_units + 1)
            def _():
                rows1_copy.wait()
                for par in (0, 1):
                    store(par, L[2], RQ[:, :, par * w:(par + 1) * w].reshape(NDP * R, w))

            @pl.when(u == wide_units + 2)
            def _():
                for par in (0, 1):
                    store(par, L[2], RKV[:, par].reshape(NDP * R, w))

    def e_send_step(u, k, w):
        for par in (0, 1):
            for n in range(NC >> (k + 1)):
                e_copy(u, par, k, n, w).start()

    def e_add(u, k, w):
        slot = lax.rem(u, NS)
        for par in (0, 1):
            for n in range(NC >> (k + 1)):
                e_copy(u, par, k, n, w).wait_recv()
                if k < m - 1:
                    kept = flips(c, sub_sums(orders[par][k + 1:])[n])
                    Pe[slot, par, kept, :, :w] = (
                        Pe[slot, par, kept, :, :w].astype(F32) + Rv[k][slot, par, n, :, :w].astype(F32)
                    ).astype(BF)

    def out_copies(u, w):
        two = lax.rem(u, 2)

        def copy(par, dst):
            return pltpu.make_async_copy(st.at[two, par, :, pl.ds(0, w)], dst, st_sem.at[two, par])

        if w == W:
            pairs = []
            for kind, dst in enumerate([gate_o, up_o, down_o]):
                base = (u - kind * NF) * 2 * W
                pairs.append((
                    (u >= kind * NF) & (u < (kind + 1) * NF),
                    [copy(p, dst.at[:, pl.ds(pl.multiple_of(base + p * W, 128), W)]) for p in (0, 1)],
                ))
            return pairs
        return [
            (u == wide_units, [copy(p, out_o.at[:, pl.ds(p * w, w)]) for p in (0, 1)]),
            (u == wide_units + 1, [copy(p, q_o.at[:, pl.ds(p * w, w)]) for p in (0, 1)]),
            (u == wide_units + 2, [copy(0, k_o), copy(1, v_o)]),
        ]

    def out_wait(u):
        for w in (W, narrow):
            for here, copies in out_copies(u, w):

                @pl.when(here)
                def _():
                    for copy in copies:
                        copy.wait()

    def e_finish(u, w):
        slot, two = lax.rem(u, NS), lax.rem(u, 2)
        e_add(u, m - 1, w)
        out_wait(u - 2)
        for par in (0, 1):
            st[two, par, :, :w] = Pe[slot, par, c, :, :w].astype(F32) + Rv[m - 1][slot, par, 0, :, :w].astype(F32)
        for here, copies in out_copies(u, w):

            @pl.when(here)
            def _():
                for copy in copies:
                    copy.start()

    def by_width(u, body):
        @pl.when((u >= 0) & (u < wide_units))
        def _():
            body(W)

        @pl.when((u >= wide_units) & (u < units))
        def _():
            body(narrow)

    per = max(1, 256 // Lr)
    key_tile = per * Lr

    def kv_copy(d):
        return remote(
            kvs.at[lax.rem(d, kvs.shape[0])], kvr.at[d - 1], kv_send.at[d - 1], kv_recv.at[d - 1],
            along("ctx", jnp.maximum(c - d, 0)),
        )

    def block_copy(block):
        two = lax.rem(block, 2)
        return pltpu.make_async_copy(kv_ref.at[block], kvb.at[two], kvb_sem.at[two])

    def attend(two, masked, dst):
        for kh in range(KH):
            cols = slice(kh * HEAD, (kh + 1) * HEAD)

            def key_step(i, carry):
                start = pl.multiple_of(i * key_tile, key_tile)
                at = pl.ds(i * per, per)
                keys = kvb[two, at, 0, :, cols].reshape(key_tile, HEAD)
                values = kvb[two, at, 1, :, cols].reshape(key_tile, HEAD)
                key_sum = jnp.zeros((key_tile, HEAD), F32)
                value_sum = jnp.zeros((key_tile, HEAD), F32)
                for g in range(GS):
                    h = kh * GS + g
                    head = slice(h * HEAD, (h + 1) * HEAD)
                    query, delta = q_ref[:, head], hd_ref[:, head]
                    bent = jnp.tanh(dot_nt(keys, query) * (scale / CAP))
                    prob = jnp.exp(CAP * bent - logt_ref[h:h + 1, :])
                    if masked:
                        key_pos = start + lax.broadcasted_iota(jnp.int32, prob.shape, 0)
                        prob = jnp.where(key_pos <= lax.broadcasted_iota(jnp.int32, prob.shape, 1), prob, 0.0)
                    grad = prob * (dot_nt(values, delta) - rdelta[h:h + 1, :]) * (1.0 - bent * bent)
                    grad = grad.astype(BF)
                    value_sum += dot_nn(prob.astype(BF), delta)
                    key_sum += dot_nn(grad, query)
                    dq[:, head] += dot_tn(grad, keys)
                rows = pl.ds(start, key_tile)
                kvs[dst, 0, rows, cols] = (key_sum * scale).astype(BF)
                kvs[dst, 1, rows, cols] = value_sum.astype(BF)
                return carry

            lax.fori_loop(0, R // key_tile, key_step, 0)

    def attention():
        dq[...] = jnp.zeros_like(dq)
        for h in range(Hq // HEAD):
            head = slice(h * HEAD, (h + 1) * HEAD)
            product = hd_ref[:, head].astype(F32) * heads_ref[:, head].astype(F32)
            rdelta[h:h + 1] = jnp.sum(product.T, axis=0, keepdims=True)
        block_copy(0).start()

        def far(block, carry):
            d = c - block

            @pl.when(block < c)
            def _():
                slot = lax.rem(d, kvs.shape[0])
                block_copy(block).wait()
                block_copy(block + 1).start()

                @pl.when(d + kvs.shape[0] <= c)
                def _():
                    kv_copy(d + kvs.shape[0]).wait_send()

                attend(lax.rem(block, 2), False, slot)
                kv_copy(d).start()

            return carry

        lax.fori_loop(0, NC - 1, far, 0)

        @pl.when(c >= kvs.shape[0])
        def _():
            kv_copy(kvs.shape[0]).wait_send()

        block_copy(c).wait()
        attend(lax.rem(c, 2), True, 0)

    def turned(values, h):
        a, b = values[:, h * HEAD:h * HEAD + HEAD // 2], values[:, h * HEAD + HEAD // 2:(h + 1) * HEAD]
        cosine, sine = cos_ref[...], sin_ref[...]
        return jnp.concatenate([a * cosine + b * sine, b * cosine - a * sine], axis=1).astype(BF)

    def pair_remote(i, o):
        ref = [RQ, RKV][i]
        return remote(ref.at[dp], ref.at[dp], pair_sem.at[2 * o, i], pair_sem.at[2 * o + 1, i], partners[o])

    has_left, has_right = t > 0, t < T - 1

    def rs_copy(side, k, j):
        if side == 0:
            slot, peer = j, jnp.minimum(t + 1, T - 1)
        else:
            slot, peer = jnp.where(j == t - 1, T, j), jnp.maximum(t - 1, 0)
        return remote(Pb.at[j], Rb.at[slot], rs_send.at[side, k], rs_recv.at[side, k], along("tp", peer))

    def rs_block(side, k):
        return (T - 1 - k + t) if side == 0 else (k - (T - 1 - t))

    def rs_sends(side, k):
        return (t <= k) & has_right if side == 0 else (T - 1 - t <= k) & has_left

    def rs_step(k):
        for side in (0, 1):
            j = rs_block(side, k)

            @pl.when(rs_sends(side, k))
            def _():
                if k:

                    @pl.when(has_left if side == 0 else has_right)
                    def _():
                        rs_copy(side, k - 1, j).wait_recv()
                        Pb[j] = (Pb[j].astype(F32) + Rb[j].astype(F32)).astype(BF)

                rs_copy(side, k, j).start()

    def own_keys():
        for which in range(2):
            dst = []
            for kh in range(KH):
                dst.append(kvs[0, which, :, kh * HEAD:(kh + 1) * HEAD].astype(F32))
            acc[which] = jnp.concatenate(dst, axis=1) if KH > 1 else dst[0]

        def come(i, carry):
            d = i + 1

            @pl.when(c + d <= NC - 1)
            def _():
                kv_copy(d).wait_recv()
                for which in range(2):
                    acc[which] += kvr[d - 1, which].astype(F32)

            return carry

        lax.fori_loop(0, NC - 1, come, 0)
        for kh in range(KH):
            cols = slice(kh * HEAD, (kh + 1) * HEAD)
            RKV[dp, 0, :, cols] = turned(acc[0], kh)
        RKV[dp, 1] = acc[1].astype(BF)
        for h in range(Hq // HEAD):
            RQ[dp, :, h * HEAD:(h + 1) * HEAD] = turned(dq[...] * scale, h)
        for i in range(2):
            for o in range(NDP - 1):
                pair_remote(i, o).start()
        for i in range(3):
            spread_local(i).wait()
            for o in range(NDP - 1):
                spread_remote(i, o).wait_recv()
        tile = tile_of(D)

        def part(i, carry):
            at = pl.ds(pl.multiple_of(i * tile, tile), tile)
            terms = dot_nt(RQ[dp], WQ[at, :]) + dot_nt(RKV[dp, 0], WK[at, :]) + dot_nt(RKV[dp, 1], WV[at, :])
            Pb[:, :, at] = terms.astype(BF).reshape(T, Lr, tile)
            return carry

        lax.fori_loop(0, D // tile, part, 0)
        rs_step(0)

    def rs_finish():
        igrad_ref[...] = Pb[t].astype(F32)

        @pl.when(has_left)
        def _():
            rs_copy(0, T - 2, t).wait_recv()
            igrad_ref[...] += Rb[t].astype(F32)

        @pl.when(has_right)
        def _():
            rs_copy(1, T - 2, t).wait_recv()
            igrad_ref[...] += Rb[T].astype(F32)

        rows = x_ref[...].astype(F32)
        grad, terms = rms_back(rows, inverse_rms(rows), gain_ref[0:1], igrad_ref[...])
        igrad_ref[...] = mdelta_ref[...] + grad
        G[0, 0:1] = terms
        G[0, 1:4] = gsum_ref[...]

    meets = [("tp", t, b) for b in bits_below(T)] + [("ctx", c, b) for b in bits_below(NC)]
    meets += [("dp", dp, b) for b in bits_below(NDP)]

    def g_copy(k):
        axis, index, bit = meets[k]
        return remote(G.at[k], GR.at[k], g_send.at[k], g_recv.at[k], along(axis, flip(index, bit)))

    def tick(i, carry):
        def start(w):
            @pl.when(i >= NS)
            def _():
                by_width(i - NS, lambda before: e_sent(i - NS, before))

            e_product(i, w)
            e_send_step(i, 0, w)

        by_width(i, start)

        @pl.when(i == 1)
        def _():
            attention()

        @pl.when(i == 2)
        def _():
            own_keys()

        for k in range(1, T - 1):

            @pl.when(i == 2 + k)
            def _():
                rs_step(k)

        @pl.when(i == 1 + T)
        def _():
            rs_finish()
            g_copy(0).start()

        for k in range(len(meets)):

            @pl.when(i == 2 + T + k)
            def _():
                g_copy(k).wait_recv()
                G[k + 1] = G[k] + GR[k]
                if k + 1 < len(meets):
                    g_copy(k + 1).start()

        @pl.when(i == wide_units)
        def _():
            for p in range(2):
                for o in range(NDP - 1):
                    pair_remote(p, o).wait_recv()

        for k in range(1, m):

            def middle(w):
                e_add(i - k, k - 1, w)
                e_send_step(i - k, k, w)

            by_width(i - k, middle)
        by_width(i - m, lambda w: e_finish(i - m, w))
        return carry

    lax.fori_loop(0, units + m, tick, 0)
    gains_ref[...] = G[len(meets)]

    for u in (units - 2, units - 1):
        out_wait(jnp.int32(u))
    for u in range(units - NS, units):
        by_width(jnp.int32(u), lambda w: e_sent(jnp.int32(u), w))
    for side in (0, 1):
        for k in range(T - 1):

            @pl.when(rs_sends(side, k))
            def _():
                rs_copy(side, k, rs_block(side, k)).wait_send()

    for k in range(len(meets)):
        g_copy(k).wait_send()
    for o in range(NDP - 1):
        for i in range(3):
            spread_remote(i, o).wait_send()
        for i in range(2):
            pair_remote(i, o).wait_send()

    def kv_close(i, carry):
        d = i + 1

        @pl.when((d <= c) & (d < kvs.shape[0]))
        def _():
            kv_copy(d).wait_send()

        return carry

    lax.fori_loop(0, min(NC - 1, kvs.shape[0] - 1), kv_close, 0)


def tail_call(
    layer_in, middle_delta, norm_gains, gain_sums, query, heads_delta, head_rows, log_totals, cosine, sine,
    keys_values, rows_one, w_query, w_key, w_value, rows, branch, attn, heads, gate, up, hidden,
):
    T, NC, NDP = lax.axis_size("tp"), lax.axis_size("ctx"), lax.axis_size("dp")
    Lr, D = layer_in.shape
    R, Hq = query.shape
    KVd = w_key.shape[1]
    KH = KVd // HEAD
    Dh = D // NDP
    RB = Dh // NC
    F = gate.shape[1]
    W = tile_of(F) // 2
    m = NC.bit_length() - 1
    NS = max(4, m + 1)
    tokens = NDP * R
    kv_slots = min(NC, 4)
    meets = sum(n.bit_length() - 1 for n in (T, NC, NDP))
    any_spec = pl.BlockSpec(memory_space=pl.ANY)
    vm = pl.BlockSpec(memory_space=pltpu.VMEM)
    sds = jax.ShapeDtypeStruct
    dma = pltpu.SemaphoreType.DMA
    return pl.pallas_call(
        functools.partial(tail_kernel, T, NC, NDP, KH, NS),
        out_shape=(
            sds((Lr, D), F32), sds((4, D), F32),
            sds((RB, F), F32), sds((RB, F), F32), sds((RB, F), F32), sds((RB, Hq), F32),
            sds((RB, Hq), F32), sds((RB, KVd), F32), sds((RB, KVd), F32),
        ),
        in_specs=[vm] * 10 + [any_spec] * 12,
        out_specs=[vm] * 2 + [any_spec] * 7,
        scratch_shapes=[
            pltpu.VMEM((3, tokens, Dh), BF), pltpu.VMEM((2, tokens, 2 * W), BF), pltpu.VMEM((tokens, Hq), BF),
            pltpu.VMEM((NDP, R, Hq), BF), pltpu.VMEM((NDP, 2, R, KVd), BF),
            pltpu.VMEM((D, Hq), BF), pltpu.VMEM((D, KVd), BF), pltpu.VMEM((D, KVd), BF),
            pltpu.VMEM((NS, 2, NC, RB, W), BF),
            *[pltpu.VMEM((NS, 2, NC >> (k + 1), RB, W), BF) for k in range(m)],
            pltpu.VMEM((2, 2, RB, W), F32), pltpu.VMEM((R, Hq), F32), pltpu.VMEM((Hq // HEAD, R), F32), pltpu.VMEM((2, T, 2, Lr, KVd), BF),
            pltpu.VMEM((kv_slots, 2, R, KVd), BF), pltpu.VMEM((NC - 1, 2, R, KVd), BF),
            pltpu.VMEM((T, Lr, D), BF), pltpu.VMEM((T + 1, Lr, D), BF), pltpu.VMEM((2, R, KVd), F32),
            pltpu.VMEM((meets + 1, 4, D), F32), pltpu.VMEM((meets, 4, D), F32),
            dma((4,)), dma((2,)), dma((2 * NDP - 1, 3)), dma((2 * (NDP - 1), 2)),
            dma((NS, 2, NC - 1)), dma((NS, 2, NC - 1)), dma((2, 2)), dma((NC - 1,)), dma((NC - 1,)),
            dma((2, T - 1)), dma((2, T - 1)), dma((meets,)), dma((meets,)), dma((2,)),
        ],
        compiler_params=pltpu.CompilerParams(
            collective_id=1, has_side_effects=True, vmem_limit_bytes=66_000_000
        ),
        name="tail",
    )(
        layer_in, middle_delta, norm_gains, gain_sums, query, heads_delta, head_rows, log_totals, cosine, sine,
        keys_values, rows_one, w_query, w_key, w_value, rows, branch, attn, heads, gate, up, hidden,
    )


def shards(layer_in, cotangent, norm_gains, w_query, w_key, w_value, w_out, w_gate, w_up, w_down):
    tp_count, ctx_count, dp_count = lax.axis_size("tp"), lax.axis_size("ctx"), lax.axis_size("dp")
    half_width = HEAD // 2
    frequency = THETA ** (-(jnp.arange(half_width, dtype=F32) * 2.0) / HEAD)
    query, head_rows, log_totals, cosine, sine, keys_values, rows_one = front_call(
        layer_in, norm_gains, frequency[None, :], w_query, w_key, w_value
    )
    core = core_call(layer_in, cotangent, norm_gains, head_rows, w_out, w_gate, w_up, w_down)
    layer_out, middle_delta, gain_sums, heads_delta, rows, hidden, branch, gate, up, attn, heads = core
    input_grad, gains, grad_gate, grad_up, down_turned, out_turned, grad_query, grad_key, grad_value = tail_call(
        layer_in, middle_delta, norm_gains, gain_sums, query, heads_delta, head_rows, log_totals, cosine, sine,
        keys_values, rows_one.reshape(-1, rows_one.shape[-1]), w_query, w_key, w_value,
        rows, branch, attn, heads, gate, up, hidden,
    )
    rank = (lax.axis_index("dp") * ctx_count + lax.axis_index("ctx")) * tp_count + lax.axis_index("tp")
    width = gains.shape[1] // (dp_count * ctx_count * tp_count)
    gain_grads = lax.dynamic_slice_in_dim(gains, rank * width, width, 1)
    return (
        layer_out, input_grad, gain_grads, grad_query, grad_key, grad_value,
        out_turned.T, grad_gate, grad_up, down_turned.T,
    )


def solution(mesh):
    return jax.shard_map(
        shards,
        mesh=mesh,
        in_specs=(
            P(("dp", "ctx", "tp"), None),
            P(("dp", "ctx", "tp"), None),
            P(),
            P("dp", "tp"),
            P("dp", "tp"),
            P("dp", "tp"),
            P("tp", "dp"),
            P("dp", "tp"),
            P("dp", "tp"),
            P("tp", "dp"),
        ),
        out_specs=(
            P(("dp", "ctx", "tp"), None),
            P(("dp", "ctx", "tp"), None),
            P(None, ("dp", "ctx", "tp")),
            P(("dp", "ctx"), "tp"),
            P(("dp", "ctx"), "tp"),
            P(("dp", "ctx"), "tp"),
            P("tp", ("dp", "ctx")),
            P(("dp", "ctx"), "tp"),
            P(("dp", "ctx"), "tp"),
            P("tp", ("dp", "ctx")),
        ),
        check_vma=False,
    )
```

```python
import functools

import jax
import jax.numpy as jnp
from jax import lax
from jax.experimental import pallas as pl
from jax.experimental.pallas import tpu as pltpu
from jax.sharding import PartitionSpec as P

HEAD = 256
EPS = 1e-06
CAP = 50.0
THETA = 10000.0
MESH = pl.DeviceIdType.MESH
BF = jnp.bfloat16
F32 = jnp.float32


def tile_of(width):
    for tile in (768, 512, 256, 128):
        if width % tile == 0:
            return tile
    return width


def inverse_rms(values):
    return lax.rsqrt(jnp.mean(values * values, axis=-1, keepdims=True) + EPS)


def rms_back(values, scale, gain, delta):
    weighted = delta * gain
    inner = jnp.mean(weighted * values, axis=-1, keepdims=True)
    grad = scale * weighted - values * (scale * scale * scale * inner)
    return grad, jnp.sum(delta * values * scale, axis=0, keepdims=True)


def dot_nt(former, latter):
    return lax.dot_general(former, latter, (((1,), (1,)), ((), ())), preferred_element_type=F32)


def dot_nn(former, latter):
    return jnp.dot(former, latter, preferred_element_type=F32)


def barrier(count_of, peers):
    sem = pltpu.get_barrier_semaphore()
    for present, device_id in peers:

        @pl.when(present)
        def _():
            pl.semaphore_signal(sem, inc=1, device_id=device_id, device_id_type=MESH)

    pl.semaphore_wait(sem, count_of)


def flip(index, bit):
    return index + bit * (1 - 2 * lax.rem(index // bit, 2))


def flips(index, mask):
    bit = 1
    while bit <= mask:
        if mask & bit:
            index = flip(index, bit)
        bit *= 2
    return index


def dot_tn(former, latter):
    return lax.dot_general(former, latter, (((0,), (0,)), ((), ())), preferred_element_type=F32)


def sub_sums(bits):
    sums = [0]
    for bit in bits:
        sums = sums + [s + bit for s in sums]
    return sums


def bits_below(count):
    return [1 << i for i in range(count.bit_length() - 1)]


def core_kernel(
    T, C, NC, NDP,
    x_ref, ct_ref, gain_ref, heads_ref, wo_ref, wg_ref, wu_ref, wd_ref,
    out_ref, mdelta_ref, gsum_ref, hdelta_ref,
    rows_pair, hid_pair, branch_pair, gate_pair, up_pair, attn_pair, head_pair, down_o,
    wo_v, wg_v, wu_v, wd_v, X, Pb, Rb, hid, Ab, Bb, att, mid, acc,
    L, Rc, st, w_sem, rs_send, rs_recv, ag_send, ag_recv, pair_sem, l_sem, e_send, e_recv, st_sem, free_sem,
):
    t = lax.axis_index("tp")
    dp = lax.axis_index("dp")
    c = lax.axis_index("ctx")
    D = x_ref.shape[1]
    rc = x_ref.shape[0] // C
    Dh = D // NDP
    F = wg_v.shape[1]
    M = T * rc
    has_left, has_right = t > 0, t < T - 1
    left, right = {"tp": jnp.maximum(t - 1, 0)}, {"tp": jnp.minimum(t + 1, T - 1)}
    partners = [{"dp": lax.rem(dp + o, NDP)} for o in range(1, NDP)]
    meets = [{"ctx": flip(c, bit)} for bit in bits_below(NC)]

    barrier(
        has_left.astype(jnp.int32) + has_right.astype(jnp.int32) + len(partners + meets),
        [(has_left, left), (has_right, right)] + [(t >= 0, p) for p in partners + meets],
    )

    rows_at = pl.ds(pl.multiple_of(dp * Dh, 128), Dh)
    weights = [
        (wo_ref, lambda: wo_v.at[:, rows_at]),
        (wg_ref, lambda: wg_v.at[rows_at]),
        (wu_ref, lambda: wu_v.at[rows_at]),
        (wd_ref, lambda: wd_v.at[:, rows_at]),
    ]

    def weight_copies(i):
        src, dst = weights[i]
        copies = [pltpu.make_async_copy(src, dst(), w_sem.at[0, i])]
        for o, partner in enumerate(partners):
            copies.append(
                pltpu.make_async_remote_copy(
                    src, dst(), w_sem.at[1 + 2 * o, i], w_sem.at[2 + 2 * o, i],
                    device_id=partner, device_id_type=MESH,
                )
            )
        return copies

    for i in range(4):
        for copy in weight_copies(i):
            copy.start()

    def weight_wait(i):
        src, dst = weights[i]
        for o, copy in enumerate(weight_copies(i)):
            if o == 0:
                copy.wait()
            else:
                copy.wait_recv()

    def pair_copies(kind, s, src, half, dst):
        def cut(owner):
            if half:
                return src.at[..., pl.ds(pl.multiple_of(owner * Dh, 128), Dh)]
            return src

        copies = [pltpu.make_async_copy(cut(dp), dst.at[dp, s], pair_sem.at[0, kind, s])]
        for o, partner in enumerate(partners):
            copies.append(
                pltpu.make_async_remote_copy(
                    cut(partner["dp"]), dst.at[dp, s],
                    pair_sem.at[1 + 2 * o, kind, s], pair_sem.at[2 + 2 * o, kind, s],
                    device_id=partner, device_id_type=MESH,
                )
            )
        return copies

    def pair_of(kind, s):
        return pair_copies(
            kind, s,
            *[
                (X.at[s], True, rows_pair),
                (hid.at[s], False, hid_pair),
                (X.at[s], True, branch_pair),
                (Ab.at[s], False, gate_pair),
                (Bb.at[s], False, up_pair),
                (X.at[s], True, attn_pair),
                (heads_ref.at[:, s], False, head_pair),
            ][kind],
        )

    def pair_start(kind, s):
        for copy in pair_of(kind, s):
            copy.start()

    def pair_kept(kind, s):
        pair_of(kind, s)[0].wait()

    def pair_away(kind, s):
        for copy in pair_of(kind, s)[1:]:
            copy.wait_send()

    def pair_received(kind, s):
        for copy in pair_of(kind, s)[1:]:
            copy.wait_recv()

    def rs_copy(s, side, k, j):
        if side == 0:
            slot, peer = j, right
        else:
            slot, peer = jnp.where(j == t - 1, T, j), left
        return pltpu.make_async_remote_copy(
            Pb.at[s, j], Rb.at[s, slot], rs_send.at[s, side, k], rs_recv.at[s, side, k],
            device_id=peer, device_id_type=MESH,
        )

    def rs_block(side, k):
        return (T - 1 - k + t) if side == 0 else (k - (T - 1 - t))

    def rs_sends(side, k):
        return (t <= k) if side == 0 else (T - 1 - t <= k)

    def ag_copy(s, side, k, j):
        return pltpu.make_async_remote_copy(
            X.at[s, j], X.at[s, j], ag_send.at[s, side, k], ag_recv.at[s, side, k],
            device_id=right if side == 0 else left, device_id_type=MESH,
        )

    def ag_block(side, k):
        return (t - k) if side == 0 else (t + k)

    def ag_sends(side, k):
        return (t >= k) & has_right if side == 0 else (t + k <= T - 1) & has_left

    def rs_start(s):
        for side in (0, 1):

            @pl.when(rs_sends(side, 0))
            def _():
                rs_copy(s, side, 0, rs_block(side, 0)).start()

    def rs_step(s, k):
        for side in (0, 1):
            j = rs_block(side, k)
            came = has_left if side == 0 else has_right

            @pl.when(rs_sends(side, k))
            def _():
                @pl.when(came)
                def _():
                    rs_copy(s, side, k - 1, j).wait_recv()
                    Pb[s, j] = (Pb[s, j].astype(F32) + Rb[s, j].astype(F32)).astype(BF)

                rs_copy(s, side, k, j).start()

    def rs_sent(s):
        for side in (0, 1):
            for k in range(T - 1):

                @pl.when(rs_sends(side, k))
                def _():
                    rs_copy(s, side, k, rs_block(side, k)).wait_send()

    def rs_finish(s):
        acc[...] = Pb[s, t].astype(F32)

        @pl.when(has_left)
        def _():
            rs_copy(s, 0, T - 2, t).wait_recv()
            acc[...] += Rb[s, t].astype(F32)

        @pl.when(has_right)
        def _():
            rs_copy(s, 1, T - 2, t).wait_recv()
            acc[...] += Rb[s, T].astype(F32)

    def ag_start(s):
        for side in (0, 1):

            @pl.when(ag_sends(side, 0))
            def _():
                ag_copy(s, side, 0, t).start()

    def ag_step(s, k):
        for side in (0, 1):
            j = ag_block(side, k)
            there = (j >= 0) if side == 0 else (j <= T - 1)

            @pl.when(there)
            def _():
                ag_copy(s, side, k - 1, j).wait_recv()
                if k <= T - 2:

                    @pl.when(has_right if side == 0 else has_left)
                    def _():
                        ag_copy(s, side, k, j).start()

    def ag_sent(s):
        for side in (0, 1):
            for k in range(T - 1):

                @pl.when(ag_sends(side, k))
                def _():
                    ag_copy(s, side, k, ag_block(side, k)).wait_send()

    def local_rows(n, s):
        own = pl.ds(pl.multiple_of(s * rc, rc), rc)
        total = acc[...]

        @pl.when(n == 0)
        def _():
            att[s] = total
            middle = x_ref[own].astype(F32) + total * inverse_rms(total) * gain_ref[1:2]
            mid[s] = middle
            X[s, t] = (middle * inverse_rms(middle) * gain_ref[2:3]).astype(BF)

        @pl.when(n == 1)
        def _():
            scale = inverse_rms(total)
            out_ref[own] = (mid[s] + total * scale * gain_ref[3:4]).astype(BF)
            grad, terms = rms_back(total, scale, gain_ref[3:4], ct_ref[own].astype(F32))
            gsum_ref[2:3] += terms
            X[s, t] = grad.astype(BF)

        @pl.when(n == 2)
        def _():
            middle, attention = mid[s], att[s]
            grad, terms = rms_back(middle, inverse_rms(middle), gain_ref[2:3], total)
            gsum_ref[1:2] += terms
            middle_delta = ct_ref[own].astype(F32) + grad
            mdelta_ref[own] = middle_delta
            grad, terms = rms_back(attention, inverse_rms(attention), gain_ref[1:2], middle_delta)
            gsum_ref[0:1] += terms
            X[s, t] = grad.astype(BF)

    def comm(tau, w, a):
        back = tau - a

        @pl.when((back >= 0) & (back < 3 * C))
        def _():
            n, s = back // C, lax.rem(back, C)
            if w <= T - 2:
                rs_step(s, w)
            elif w == T - 1:
                rs_finish(s)
                local_rows(n, s)
                ag_start(s)
            else:
                ag_step(s, w - (T - 1))

    def tiles(width, body):
        tile = tile_of(width)

        def step(i, carry):
            body(pl.ds(pl.multiple_of(i * tile, tile), tile), tile)
            return carry

        lax.fori_loop(0, width // tile, step, 0)

    def rows_of(s):
        return X[s].reshape(M, D)

    def store_part(s, at, tile, value):
        Pb[s, :, :, at] = value.astype(BF).reshape(T, rc, tile)

    m = NC.bit_length() - 1
    RB = Dh // NC
    W = Rc.shape[-1] // 2
    units = F // (2 * W)
    begin = 3 * C - 1
    pitch = -(-RB // 16) * 16
    orders = [bits_below(NC), bits_below(NC)[::-1]]
    first_of = [sum(NC >> (i + 1) for i in range(k)) for k in range(m)]

    def block_of(ref, i):
        down = ref.shape[0] // pitch
        row = pl.multiple_of(lax.rem(i, down) * pitch, 16)
        return ref.at[pl.ds(row, RB), pl.ds(pl.multiple_of((i // down) * W, 128), W)]

    def part_of(u, par, owner):
        return block_of(wd_v, (u * 2 + par) * NC + owner)

    def came_of(u, par, at):
        return block_of(wu_v, (u * 2 + par) * (NC - 1) + at)

    def e_copy(u, par, k, n):
        order = orders[par]
        at = first_of[k] + n
        return pltpu.make_async_remote_copy(
            part_of(u, par, flips(c, sub_sums(order[k + 1:])[n] + order[k])), came_of(u, par, at),
            e_send.at[u, par, at], e_recv.at[u, par, at],
            device_id={"ctx": flip(c, order[k])}, device_id_type=MESH,
        )

    def e_each(u, k, act):
        for par in (0, 1):
            for n in range(NC >> (k + 1)):
                act(par, n)

    def e_add(u, k):
        def one(par, n):
            e_copy(u, par, k, n).wait_recv()
            if k < m - 1:
                ref = part_of(u, par, flips(c, sub_sums(orders[par][k + 1:])[n]))
                ref[...] = (ref[...].astype(F32) + came_of(u, par, first_of[k] + n)[...].astype(F32)).astype(BF)

        e_each(u, k, one)

    def chunk_load(u):
        at = pl.ds(pl.multiple_of(u * 2 * W, 128), 2 * W)
        return pltpu.make_async_copy(hid_pair.at[:, :, :, at], Rc, l_sem.at[1])

    def first_all():
        return pltpu.make_async_copy(branch_pair, L, l_sem.at[0])

    def out_copy(u, par):
        at = pl.ds(pl.multiple_of((2 * u + par) * W, 128), W)
        return pltpu.make_async_copy(st.at[par], down_o.at[:, at], st_sem.at[par])

    def engine(tau):
        u = tau - begin

        @pl.when((u >= 0) & (u < units))
        def _():
            @pl.when(u == 0)
            def _():
                first_all().wait()
                pl.semaphore_wait(free_sem, len(meets))

            chunk_load(u).wait()
            rows = NDP * C * M
            for par in (0, 1):
                product = dot_tn(L[...].reshape(rows, Dh), Rc[:, :, :, par * W:(par + 1) * W].reshape(rows, W))
                for owner in range(NC):
                    part_of(u, par, owner)[...] = product[owner * RB:(owner + 1) * RB].astype(BF)

            @pl.when(u + 1 < units)
            def _():
                chunk_load(u + 1).start()

            e_each(u, 0, lambda par, n: e_copy(u, par, 0, n).start())

        for k in range(1, m):

            @pl.when((u - k >= 0) & (u - k < units))
            def _():
                e_add(u - k, k - 1)
                e_each(u - k, k, lambda par, n: e_copy(u - k, par, k, n).start())

        @pl.when((u - m >= 0) & (u - m < units))
        def _():
            e_add(u - m, m - 1)
            for par in (0, 1):

                @pl.when(u - m > 0)
                def _():
                    out_copy(u - m - 1, par).wait()

                st[par] = (
                    part_of(u - m, par, c)[...].astype(F32) + came_of(u - m, par, first_of[m - 1])[...].astype(F32)
                )
                out_copy(u - m, par).start()

    def engine_open():
        pair_kept(2, C - 1)

        def each(s, carry):
            pair_kept(1, s)
            pair_received(1, s)
            pair_received(2, s)
            return carry

        lax.fori_loop(0, C, each, 0)
        first_all().start()
        chunk_load(0).start()

    def tick(tau, carry):
        n, s = tau // C, lax.rem(tau, C)

        @pl.when((n >= 1) & (n <= 2))
        def _():
            rs_sent(s)

        @pl.when(n == 1)
        def _():
            @pl.when(s == 0)
            def _():
                weight_wait(1)
                weight_wait(2)

            pair_start(0, s)

            def gate_up(at, tile):
                gate = dot_nn(rows_of(s), wg_v[:, at])
                up = dot_nn(rows_of(s), wu_v[:, at])
                inner = jnp.tanh(0.7978845608028654 * (gate + 0.044715 * gate * gate * gate))
                half = 0.5 * (1.0 + inner)
                gelu = gate * half
                slope = half + 0.5 * gate * (1.0 - inner * inner) * (
                    0.7978845608028654 * (1.0 + 0.134145 * gate * gate)
                )
                hid[s, :, at] = (gelu * up).astype(BF)
                Ab[s, :, at] = (up * slope).astype(BF)
                Bb[s, :, at] = gelu.astype(BF)

            tiles(F, gate_up)
            pair_start(1, s)

        @pl.when(n == 2)
        def _():
            pair_start(2, s)

            def gate_up_delta(at, tile):
                delta = dot_nt(rows_of(s), wd_v[at, :])
                Ab[s, :, at] = (delta * Ab[s, :, at].astype(F32)).astype(BF)
                Bb[s, :, at] = (delta * Bb[s, :, at].astype(F32)).astype(BF)

            tiles(F, gate_up_delta)
            pair_start(3, s)
            pair_start(4, s)

            @pl.when(s == C - 1)
            def _():
                engine_open()

        for a in range(1, T):
            comm(tau, 2 * a - 1, a)

        @pl.when(n == 0)
        def _():
            pair_start(6, s)
            heads = heads_ref[:, s].reshape(M, heads_ref.shape[3])
            tiles(D, lambda at, tile: store_part(s, at, tile, dot_nn(heads, wo_v[:, at])))

        @pl.when(n == 1)
        def _():
            @pl.when(s == 0)
            def _():
                weight_wait(3)

            tiles(D, lambda at, tile: store_part(s, at, tile, dot_nn(hid[s], wd_v[:, at])))
            pair_kept(0, s)
            pair_away(0, s)
            ag_sent(s)

        @pl.when(n == 2)
        def _():
            tiles(
                D,
                lambda at, tile: store_part(
                    s, at, tile, dot_nt(Ab[s], wg_v[at, :]) + dot_nt(Bb[s], wu_v[at, :])
                ),
            )
            pair_away(2, s)

            @pl.when(s < C - 1)
            def _():
                pair_kept(2, s)

            ag_sent(s)

            @pl.when(s == C - 1)
            def _():
                for meet in meets:
                    pl.semaphore_signal(free_sem, inc=1, device_id=meet, device_id_type=MESH)

        @pl.when(n <= 2)
        def _():
            rs_start(s)

        engine(tau)

        @pl.when(n == 3)
        def _():
            pair_start(5, s)
            hdelta_ref[:, s] = (
                dot_nt(rows_of(s), wo_v[...]).astype(BF).reshape(T, rc, heads_ref.shape[3])
            )

        for a in range(1, T):
            comm(tau, 2 * a, a)
        return carry

    gsum_ref[...] = jnp.zeros_like(gsum_ref)
    weight_wait(0)
    lax.fori_loop(0, max(4 * C, begin + units + m), tick, 0)

    for i in range(4):
        for copy in weight_copies(i)[1:]:
            copy.wait_send()

    def close(s, carry):
        for kind in (3, 4, 5, 6):
            pair_kept(kind, s)
            pair_received(kind, s)
            pair_away(kind, s)
        pair_received(0, s)
        pair_away(1, s)
        rs_sent(s)
        ag_sent(s)
        return carry

    lax.fori_loop(0, C, close, 0)

    def close_engine(u, carry):
        for k in range(m):
            e_each(u, k, lambda par, n: e_copy(u, par, k, n).wait_send())
        return carry

    lax.fori_loop(0, units, close_engine, 0)
    for par in (0, 1):
        out_copy(units - 1, par).wait()


def core_call(layer_in, cotangent, norm_gains, head_flat, w_out, w_gate, w_up, w_down):
    T, NC, NDP = lax.axis_size("tp"), lax.axis_size("ctx"), lax.axis_size("dp")
    C = T
    Lr, D = layer_in.shape
    rc = Lr // C
    Hq = w_out.shape[0]
    RB = D // NDP // NC
    Dh = D // NDP
    F = w_gate.shape[1]
    M = T * rc
    W = tile_of(F) // 2
    any_spec = pl.BlockSpec(memory_space=pl.ANY)
    vm = pl.BlockSpec(memory_space=pltpu.VMEM)
    sds = jax.ShapeDtypeStruct
    outs = pl.pallas_call(
        functools.partial(core_kernel, T, C, NC, NDP),
        out_shape=(
            sds((Lr, D), BF), sds((Lr, D), F32), sds((3, D), F32), sds((T, C, rc, Hq), BF),
            sds((NDP, C, T, rc, Dh), BF), sds((NDP, C, M, F), BF), sds((NDP, C, T, rc, Dh), BF),
            sds((NDP, C, M, F), BF), sds((NDP, C, M, F), BF), sds((NDP, C, T, rc, Dh), BF),
            sds((NDP, C, T, rc, Hq), BF), sds((RB, F), F32),
        ),
        in_specs=[vm, vm, vm, vm] + [any_spec] * 4,
        out_specs=[vm, vm, vm, vm] + [any_spec] * 8,
        scratch_shapes=[
            pltpu.VMEM((Hq, D), BF), pltpu.VMEM((D, F), BF), pltpu.VMEM((D, F), BF), pltpu.VMEM((F, D), BF),
            pltpu.VMEM((C, T, rc, D), BF), pltpu.VMEM((C, T, rc, D), BF), pltpu.VMEM((C, T + 1, rc, D), BF),
            pltpu.VMEM((C, M, F), BF), pltpu.VMEM((C, M, F), BF), pltpu.VMEM((C, M, F), BF),
            pltpu.VMEM((C, rc, D), F32), pltpu.VMEM((C, rc, D), F32), pltpu.VMEM((rc, D), F32),
            pltpu.VMEM((NDP, C, T, rc, Dh), BF), pltpu.VMEM((NDP, C, M, 2 * W), BF), pltpu.VMEM((2, RB, W), F32),
            pltpu.SemaphoreType.DMA((2 * NDP - 1, 4)),
            pltpu.SemaphoreType.DMA((C, 2, T - 1)), pltpu.SemaphoreType.DMA((C, 2, T - 1)),
            pltpu.SemaphoreType.DMA((C, 2, T - 1)), pltpu.SemaphoreType.DMA((C, 2, T - 1)),
            pltpu.SemaphoreType.DMA((2 * NDP - 1, 7, C)),
            pltpu.SemaphoreType.DMA((2,)), pltpu.SemaphoreType.DMA((F // (2 * W), 2, NC - 1)),
            pltpu.SemaphoreType.DMA((F // (2 * W), 2, NC - 1)), pltpu.SemaphoreType.DMA((2,)),
            pltpu.SemaphoreType.REGULAR,
        ],
        compiler_params=pltpu.CompilerParams(
            collective_id=0, has_side_effects=True, vmem_limit_bytes=67_043_328
        ),
        name="core",
    )(layer_in, cotangent, norm_gains, head_flat.reshape(T, C, rc, Hq), w_out, w_gate, w_up, w_down)
    out, mdelta, gsum, hdelta, rows, hidden, branch, gate, up, attn, heads, down = outs
    flat = lambda a: a.reshape(NDP * T * Lr, a.shape[-1])
    return (
        out, mdelta, gsum, hdelta.reshape(T * Lr, Hq),
        flat(rows), flat(gate), flat(up), flat(attn), flat(heads), down,
    )


def front_kernel(
    T, NC, NDP, KH, C,
    x_ref, gain_ref, freq_ref, wq_ref, wk_ref, wv_ref,
    q_o, heads_o, logt_o, cos_o, sin_o, kv_o, rows1_o,
    X, WQ, WK, WV, KV, turned_sum, totals,
    w_sem, ag_send, ag_recv, pair_sem, kv_send, kv_recv, out_sem,
):
    t, c, dp = lax.axis_index("tp"), lax.axis_index("ctx"), lax.axis_index("dp")
    Lr, D = x_ref.shape
    R, Hq = q_o.shape
    rc = Lr // C
    KVd = KH * HEAD
    GS = Hq // KVd
    Dh = D // NDP
    scale = HEAD**-0.5
    has_left, has_right = t > 0, t < T - 1

    def remote(src, dst, send, recv, axis, index):
        return pltpu.make_async_remote_copy(
            src, dst, send, recv, device_id={axis: index}, device_id_type=MESH
        )

    partners = [lax.rem(dp + o, NDP) for o in range(1, NDP)]
    peers = [("tp", lax.rem(t + o, T)) for o in range(1, T)]
    peers += [("ctx", lax.rem(c + o, NC)) for o in range(1, NC)]
    peers += [("dp", p) for p in partners]
    sem = pltpu.get_barrier_semaphore()
    for axis, index in peers:
        pl.semaphore_signal(sem, inc=1, device_id={axis: index}, device_id_type=MESH)
    pl.semaphore_wait(sem, len(peers))

    rows_at = pl.ds(pl.multiple_of(dp * Dh, 128), Dh)
    weights = [(wq_ref, WQ), (wk_ref, WK), (wv_ref, WV)]

    def weight_local(i):
        return pltpu.make_async_copy(weights[i][0], weights[i][1].at[rows_at], w_sem.at[0, i])

    def weight_remote(i, o):
        return remote(
            weights[i][0], weights[i][1].at[rows_at], w_sem.at[1 + 2 * o, i], w_sem.at[2 + 2 * o, i],
            "dp", partners[o],
        )

    for i in range(3):
        weight_local(i).start()
        for o in range(NDP - 1):
            weight_remote(i, o).start()

    def ag_copy(s, side, k, j):
        at = pl.ds(s * rc, rc)
        peer = jnp.minimum(t + 1, T - 1) if side == 0 else jnp.maximum(t - 1, 0)
        return remote(X.at[j, at], X.at[j, at], ag_send.at[s, side, k], ag_recv.at[s, side, k], "tp", peer)

    def ag_block(side, k):
        return (t - k) if side == 0 else (t + k)

    def ag_there(side, k):
        return (t >= k) if side == 0 else (t + k <= T - 1)

    def onward(side):
        return has_right if side == 0 else has_left

    rows = x_ref[...].astype(F32)
    X[t] = (rows * inverse_rms(rows) * gain_ref[0:1]).astype(BF)
    for s in range(C):
        for side in (0, 1):

            @pl.when(onward(side))
            def _():
                ag_copy(s, side, 0, t).start()

    position = (c * R + lax.broadcasted_iota(jnp.int32, (R, HEAD // 2), 0)).astype(F32)
    angles = position * freq_ref[...]
    cos_o[...] = jnp.cos(angles)
    sin_o[...] = jnp.sin(angles)
    for i in range(3):
        weight_local(i).wait()
        for o in range(NDP - 1):
            weight_remote(i, o).wait_recv()

    def kv_copy(d, j):
        return remote(
            KV.at[c, j], KV.at[c, j], kv_send.at[d - 1, j], kv_recv.at[d - 1, j],
            "ctx", jnp.minimum(c + d, NC - 1),
        )

    def kv_from(b, j):
        d = c - b
        return remote(KV.at[b, j], KV.at[b, j], kv_send.at[d - 1, j], kv_recv.at[d - 1, j], "ctx", c)

    def pair_copies(j):
        def half(owner):
            return X.at[j, :, pl.ds(pl.multiple_of(owner * Dh, 128), Dh)]

        copies = [pltpu.make_async_copy(half(dp), rows1_o.at[dp, j], pair_sem.at[0, j])]
        for o, partner in enumerate(partners):
            copies.append(
                remote(
                    half(partner), rows1_o.at[dp, j], pair_sem.at[1 + 2 * o, j], pair_sem.at[2 + 2 * o, j],
                    "dp", partner,
                )
            )
        return copies

    def turned(values, h, at):
        a, b = values[:, h * HEAD:h * HEAD + HEAD // 2], values[:, h * HEAD + HEAD // 2:(h + 1) * HEAD]
        cosine, sine = cos_o[at], sin_o[at]
        return jnp.concatenate([a * cosine - b * sine, b * cosine + a * sine], axis=1).astype(BF)

    def project(j):
        for copy in pair_copies(j):
            copy.start()
        at = pl.ds(pl.multiple_of(j * Lr, Lr), Lr)
        values = dot_nn(X[j], WK[...])
        for kh in range(KH):
            KV[c, j, 0, :, kh * HEAD:(kh + 1) * HEAD] = turned(values, kh, at)
        KV[c, j, 1] = dot_nn(X[j], WV[...]).astype(BF)

        def push(i, carry):
            @pl.when(c + 1 + i <= NC - 1)
            def _():
                kv_copy(i + 1, j).start()

            return carry

        lax.fori_loop(0, NC - 1, push, 0)
        values = dot_nn(X[j], WQ[...])
        for h in range(Hq // HEAD):
            q_o[at, h * HEAD:(h + 1) * HEAD] = turned(values, h, at)

    def gather(k, carry):
        for side in (0, 1):

            @pl.when(ag_there(side, k) & (k > 0))
            def _():
                for s in range(C):
                    ag_copy(s, side, k - 1, ag_block(side, k)).wait_recv()

                    @pl.when(onward(side) & (k <= T - 2))
                    def _():
                        ag_copy(s, side, k, ag_block(side, k)).start()

        for side in (0, 1):

            @pl.when(ag_there(side, k) & ((k > 0) | (side == 0)))
            def _():
                project(ag_block(side, k))

        return carry

    lax.fori_loop(0, T, gather, 0)

    per = max(1, 256 // Lr)
    tile = per * Lr
    turned_sum[...] = jnp.zeros_like(turned_sum)
    totals[...] = jnp.zeros_like(totals)

    def out_copy(b):
        return pltpu.make_async_copy(KV.at[b], kv_o.at[b], out_sem.at[b])

    def key_step(b, p, masked):
        for kh in range(KH):
            cols = slice(kh * HEAD, (kh + 1) * HEAD)
            keys = KV[b, pl.ds(p * per, per), 0, :, cols].reshape(tile, HEAD)
            values = KV[b, pl.ds(p * per, per), 1, :, cols].reshape(tile, HEAD)
            for g in range(GS):
                h = kh * GS + g
                scores = dot_nt(keys, q_o[:, h * HEAD:(h + 1) * HEAD])
                weights = jnp.exp(CAP * jnp.tanh(scores * (scale / CAP)))
                if masked:
                    key_pos = p * tile + lax.broadcasted_iota(jnp.int32, weights.shape, 0)
                    allowed = key_pos <= lax.broadcasted_iota(jnp.int32, weights.shape, 1)
                    weights = jnp.where(allowed, weights, 0.0)
                totals[h:h + 1] += jnp.sum(weights, axis=0, keepdims=True)
                turned_sum[h] += dot_tn(values, weights.astype(BF))

    def own_step(p, carry):
        key_step(c, p, True)
        return carry

    out_copy(c).start()
    lax.fori_loop(0, T // per, own_step, 0)

    def far_block(i, carry):
        @pl.when(i < c)
        def _():
            b = c - 1 - i
            for j in range(T):
                kv_from(b, j).wait_recv()
            out_copy(b).start()

            def far_step(p, carry):
                key_step(b, p, False)
                return carry

            lax.fori_loop(0, T // per, far_step, 0)

        return carry

    lax.fori_loop(0, NC - 1, far_block, 0)
    for h in range(Hq // HEAD):
        heads_o[:, h * HEAD:(h + 1) * HEAD] = (turned_sum[h] / totals[h:h + 1]).T.astype(BF)
    logt_o[...] = jnp.log(totals[...])

    for i in range(3):
        for o in range(NDP - 1):
            weight_remote(i, o).wait_send()
    for s in range(C):
        for side in (0, 1):
            for k in range(T - 1):

                @pl.when(ag_there(side, k) & onward(side))
                def _():
                    ag_copy(s, side, k, ag_block(side, k)).wait_send()

    for j in range(T):
        copies = pair_copies(j)
        copies[0].wait()
        for copy in copies[1:]:
            copy.wait()

    def close(i, carry):
        @pl.when(c + 1 + i <= NC - 1)
        def _():
            for j in range(T):
                kv_copy(i + 1, j).wait_send()

        return carry

    lax.fori_loop(0, NC - 1, close, 0)

    def close_out(b, carry):
        @pl.when(b <= c)
        def _():
            out_copy(b).wait()

        return carry

    lax.fori_loop(0, NC, close_out, 0)


def front_call(layer_in, norm_gains, frequency, w_query, w_key, w_value):
    T, NC, NDP = lax.axis_size("tp"), lax.axis_size("ctx"), lax.axis_size("dp")
    C = T
    Lr, D = layer_in.shape
    R = T * Lr
    Hq, KVd = w_query.shape[1], w_key.shape[1]
    Dh = D // NDP
    H = Hq // HEAD
    any_spec = pl.BlockSpec(memory_space=pl.ANY)
    vm = pl.BlockSpec(memory_space=pltpu.VMEM)
    sds = jax.ShapeDtypeStruct
    dma = pltpu.SemaphoreType.DMA
    return pl.pallas_call(
        functools.partial(front_kernel, T, NC, NDP, KVd // HEAD, C),
        out_shape=(
            sds((R, Hq), BF), sds((R, Hq), BF), sds((H, R), F32),
            sds((R, HEAD // 2), F32), sds((R, HEAD // 2), F32),
            sds((NC, T, 2, Lr, KVd), BF), sds((NDP, T, Lr, Dh), BF),
        ),
        in_specs=[vm] * 3 + [any_spec] * 3,
        out_specs=[vm] * 5 + [any_spec] * 2,
        scratch_shapes=[
            pltpu.VMEM((T, Lr, D), BF), pltpu.VMEM((D, Hq), BF), pltpu.VMEM((D, KVd), BF), pltpu.VMEM((D, KVd), BF),
            pltpu.VMEM((NC, T, 2, Lr, KVd), BF), pltpu.VMEM((H, HEAD, R), F32), pltpu.VMEM((H, R), F32),
            dma((2 * NDP - 1, 3)), dma((C, 2, T - 1)), dma((C, 2, T - 1)), dma((2 * NDP - 1, T)),
            dma((NC - 1, T)), dma((NC - 1, T)), dma((NC,)),
        ],
        compiler_params=pltpu.CompilerParams(
            collective_id=2, has_side_effects=True, vmem_limit_bytes=66_000_000
        ),
        name="front",
    )(layer_in, norm_gains, frequency, w_query, w_key, w_value)


def tail_kernel(
    T, NC, NDP, KH, NS,
    x_ref, mdelta_ref, gain_ref, gsum_ref, q_ref, hd_ref, heads_ref, logt_ref, cos_ref, sin_ref,
    kv_ref, rows1_ref, wq_ref, wk_ref, wv_ref,
    rows_ref, attn_ref, head_ref, gate_ref, up_ref,
    igrad_ref, gains_ref, gate_o, up_o, out_o, q_o, k_o, v_o,
    L, Rc, Hd, RQ, RKV, WQ, WK, WV, Pe, *rest,
):
    m = NC.bit_length() - 1
    Rv, rest = rest[:m], rest[m:]
    (
        st, dq, rdelta, kvb, kvs, kvr, Pb, Rb, acc, G, GR,
        l_sem, r_sem, w_sem, pair_sem, e_send, e_recv, st_sem, kv_send, kv_recv,
        rs_send, rs_recv, g_send, g_recv, kvb_sem,
    ) = rest
    t, c, dp = lax.axis_index("tp"), lax.axis_index("ctx"), lax.axis_index("dp")
    Lr, D = x_ref.shape
    R, Hq = q_ref.shape
    KVd = KH * HEAD
    GS = Hq // KVd
    Dh, RB = D // NDP, D // NDP // NC
    F = gate_ref.shape[1]
    W = Rc.shape[-1] // 2
    NF = F // (2 * W)
    wide_units, units = 2 * NF, 2 * NF + 3
    narrow = Hq // 2
    scale = HEAD**-0.5

    def along(axis, index):
        return {axis: index}

    others = [along("tp", lax.rem(t + o, T)) for o in range(1, T)]
    others += [along("ctx", lax.rem(c + o, NC)) for o in range(1, NC)]
    partners = [along("dp", lax.rem(dp + o, NDP)) for o in range(1, NDP)]
    sem = pltpu.get_barrier_semaphore()
    for peer in others + partners:
        pl.semaphore_signal(sem, inc=1, device_id=peer, device_id_type=MESH)
    pl.semaphore_wait(sem, len(others + partners))

    def remote(src, dst, send, recv, peer):
        return pltpu.make_async_remote_copy(src, dst, send, recv, device_id=peer, device_id_type=MESH)

    firsts = [rows_ref, attn_ref, rows1_ref]

    def first_copy(i):
        return pltpu.make_async_copy(firsts[i], L.at[i], l_sem.at[i])

    rows_at = pl.ds(pl.multiple_of(dp * Dh, 128), Dh)
    spread = [
        (lambda owner: wq_ref, WQ.at[rows_at]),
        (lambda owner: wk_ref, WK.at[rows_at]),
        (lambda owner: wv_ref, WV.at[rows_at]),
    ]

    def spread_local(i):
        return pltpu.make_async_copy(spread[i][0](dp), spread[i][1], w_sem.at[0, i])

    def spread_remote(i, o):
        return remote(
            spread[i][0](partners[o]["dp"]), spread[i][1],
            w_sem.at[1 + 2 * o, i], w_sem.at[2 + 2 * o, i], partners[o],
        )

    kinds = [gate_ref, up_ref]

    def chunk_copy(u, kind):
        at = pl.ds(pl.multiple_of((u - kind * NF) * 2 * W, 128), 2 * W)
        return pltpu.make_async_copy(kinds[kind].at[:, at], Rc.at[lax.rem(u, 2)], r_sem.at[lax.rem(u, 2)])

    def chunk_start(u):
        for kind in range(2):

            @pl.when((u >= kind * NF) & (u < (kind + 1) * NF))
            def _():
                chunk_copy(u, kind).start()

    first_copy(0).start()
    chunk_start(0)
    first_copy(1).start()
    for i in range(3):
        spread_local(i).start()
        for o in range(NDP - 1):
            spread_remote(i, o).start()
    head_copy = pltpu.make_async_copy(head_ref, Hd, l_sem.at[3])
    head_copy.start()
    first_copy(2).start()

    orders = [bits_below(NC), bits_below(NC)[::-1]]
    first_of = [sum(NC >> (i + 1) for i in range(k)) for k in range(m)]

    def e_copy(u, par, k, n, w):
        order = orders[par]
        kept = sub_sums(order[k + 1:])[n]
        slot = lax.rem(u, NS)
        at = first_of[k] + n
        return remote(
            Pe.at[slot, par, flips(c, kept + order[k]), :, pl.ds(0, w)],
            Rv[k].at[slot, par, n, :, pl.ds(0, w)],
            e_send.at[slot, par, at], e_recv.at[slot, par, at],
            along("ctx", flip(c, order[k])),
        )

    def e_sent(u, w):
        for par in (0, 1):
            for k in range(m):
                for n in range(NC >> (k + 1)):
                    e_copy(u, par, k, n, w).wait_send()

    def e_product(u, w):
        slot = lax.rem(u, NS)

        def store(par, first, second):
            Pe[slot, par, :, :, :w] = dot_tn(first, second).reshape(NC, RB, w).astype(BF)

        if w == W:
            for kind in range(2):

                @pl.when((u >= kind * NF) & (u < (kind + 1) * NF))
                def _():
                    chunk_copy(u, kind).wait()

            @pl.when(u == 0)
            def _():
                first_copy(0).wait()

            chunk_start(u + 1)
            for par in (0, 1):
                store(par, L[0], Rc[lax.rem(u, 2), :, par * W:(par + 1) * W])
        else:

            @pl.when(u == wide_units)
            def _():
                first_copy(1).wait()
                head_copy.wait()
                for par in (0, 1):
                    store(par, L[1], Hd[:, par * w:(par + 1) * w])

            @pl.when(u == wide_units + 1)
            def _():
                first_copy(2).wait()
                for par in (0, 1):
                    store(par, L[2], RQ[:, :, par * w:(par + 1) * w].reshape(NDP * R, w))

            @pl.when(u == wide_units + 2)
            def _():
                for par in (0, 1):
                    store(par, L[2], RKV[:, par].reshape(NDP * R, w))

    def e_send_step(u, k, w):
        for par in (0, 1):
            for n in range(NC >> (k + 1)):
                e_copy(u, par, k, n, w).start()

    def e_add(u, k, w):
        slot = lax.rem(u, NS)
        for par in (0, 1):
            for n in range(NC >> (k + 1)):
                e_copy(u, par, k, n, w).wait_recv()
                if k < m - 1:
                    kept = flips(c, sub_sums(orders[par][k + 1:])[n])
                    Pe[slot, par, kept, :, :w] = (
                        Pe[slot, par, kept, :, :w].astype(F32) + Rv[k][slot, par, n, :, :w].astype(F32)
                    ).astype(BF)

    def out_copies(u, w):
        two = lax.rem(u, 2)

        def copy(par, dst):
            return pltpu.make_async_copy(st.at[two, par, :, pl.ds(0, w)], dst, st_sem.at[two, par])

        if w == W:
            pairs = []
            for kind, dst in enumerate([gate_o, up_o]):
                base = (u - kind * NF) * 2 * W
                pairs.append((
                    (u >= kind * NF) & (u < (kind + 1) * NF),
                    [copy(p, dst.at[:, pl.ds(pl.multiple_of(base + p * W, 128), W)]) for p in (0, 1)],
                ))
            return pairs
        return [
            (u == wide_units, [copy(p, out_o.at[:, pl.ds(p * w, w)]) for p in (0, 1)]),
            (u == wide_units + 1, [copy(p, q_o.at[:, pl.ds(p * w, w)]) for p in (0, 1)]),
            (u == wide_units + 2, [copy(0, k_o), copy(1, v_o)]),
        ]

    def out_wait(u):
        for w in (W, narrow):
            for here, copies in out_copies(u, w):

                @pl.when(here)
                def _():
                    for copy in copies:
                        copy.wait()

    def e_finish(u, w):
        slot, two = lax.rem(u, NS), lax.rem(u, 2)
        e_add(u, m - 1, w)
        out_wait(u - 2)
        for par in (0, 1):
            st[two, par, :, :w] = Pe[slot, par, c, :, :w].astype(F32) + Rv[m - 1][slot, par, 0, :, :w].astype(F32)
        for here, copies in out_copies(u, w):

            @pl.when(here)
            def _():
                for copy in copies:
                    copy.start()

    def by_width(u, body):
        @pl.when((u >= 0) & (u < wide_units))
        def _():
            body(W)

        @pl.when((u >= wide_units) & (u < units))
        def _():
            body(narrow)

    per = max(1, 256 // Lr)
    key_tile = per * Lr

    def kv_copy(d):
        return remote(
            kvs.at[lax.rem(d, kvs.shape[0])], kvr.at[d - 1], kv_send.at[d - 1], kv_recv.at[d - 1],
            along("ctx", jnp.maximum(c - d, 0)),
        )

    def block_copy(block):
        two = lax.rem(block, 2)
        return pltpu.make_async_copy(kv_ref.at[block], kvb.at[two], kvb_sem.at[two])

    def attend(two, masked, dst):
        for kh in range(KH):
            cols = slice(kh * HEAD, (kh + 1) * HEAD)

            def key_step(i, carry):
                start = pl.multiple_of(i * key_tile, key_tile)
                at = pl.ds(i * per, per)
                keys = kvb[two, at, 0, :, cols].reshape(key_tile, HEAD)
                values = kvb[two, at, 1, :, cols].reshape(key_tile, HEAD)
                key_sum = jnp.zeros((key_tile, HEAD), F32)
                value_sum = jnp.zeros((key_tile, HEAD), F32)
                for g in range(GS):
                    h = kh * GS + g
                    head = slice(h * HEAD, (h + 1) * HEAD)
                    query, delta = q_ref[:, head], hd_ref[:, head]
                    bent = jnp.tanh(dot_nt(keys, query) * (scale / CAP))
                    prob = jnp.exp(CAP * bent - logt_ref[h:h + 1, :])
                    if masked:
                        key_pos = start + lax.broadcasted_iota(jnp.int32, prob.shape, 0)
                        prob = jnp.where(key_pos <= lax.broadcasted_iota(jnp.int32, prob.shape, 1), prob, 0.0)
                    grad = prob * (dot_nt(values, delta) - rdelta[h:h + 1, :]) * (1.0 - bent * bent)
                    grad = grad.astype(BF)
                    value_sum += dot_nn(prob.astype(BF), delta)
                    key_sum += dot_nn(grad, query)
                    dq[:, head] += dot_tn(grad, keys)
                rows = pl.ds(start, key_tile)
                kvs[dst, 0, rows, cols] = (key_sum * scale).astype(BF)
                kvs[dst, 1, rows, cols] = value_sum.astype(BF)
                return carry

            lax.fori_loop(0, R // key_tile, key_step, 0)

    def attention():
        dq[...] = jnp.zeros_like(dq)
        for h in range(Hq // HEAD):
            head = slice(h * HEAD, (h + 1) * HEAD)
            product = hd_ref[:, head].astype(F32) * heads_ref[:, head].astype(F32)
            rdelta[h:h + 1] = jnp.sum(product.T, axis=0, keepdims=True)
        block_copy(0).start()

        def far(block, carry):
            d = c - block

            @pl.when(block < c)
            def _():
                slot = lax.rem(d, kvs.shape[0])
                block_copy(block).wait()
                block_copy(block + 1).start()

                @pl.when(d + kvs.shape[0] <= c)
                def _():
                    kv_copy(d + kvs.shape[0]).wait_send()

                attend(lax.rem(block, 2), False, slot)
                kv_copy(d).start()

            return carry

        lax.fori_loop(0, NC - 1, far, 0)

        @pl.when(c >= kvs.shape[0])
        def _():
            kv_copy(kvs.shape[0]).wait_send()

        block_copy(c).wait()
        attend(lax.rem(c, 2), True, 0)

    def turned(values, h):
        a, b = values[:, h * HEAD:h * HEAD + HEAD // 2], values[:, h * HEAD + HEAD // 2:(h + 1) * HEAD]
        cosine, sine = cos_ref[...], sin_ref[...]
        return jnp.concatenate([a * cosine + b * sine, b * cosine - a * sine], axis=1).astype(BF)

    def pair_remote(i, o):
        ref = [RQ, RKV][i]
        return remote(ref.at[dp], ref.at[dp], pair_sem.at[2 * o, i], pair_sem.at[2 * o + 1, i], partners[o])

    has_left, has_right = t > 0, t < T - 1

    def rs_copy(side, k, j):
        if side == 0:
            slot, peer = j, jnp.minimum(t + 1, T - 1)
        else:
            slot, peer = jnp.where(j == t - 1, T, j), jnp.maximum(t - 1, 0)
        return remote(Pb.at[j], Rb.at[slot], rs_send.at[side, k], rs_recv.at[side, k], along("tp", peer))

    def rs_block(side, k):
        return (T - 1 - k + t) if side == 0 else (k - (T - 1 - t))

    def rs_sends(side, k):
        return (t <= k) & has_right if side == 0 else (T - 1 - t <= k) & has_left

    def rs_step(k):
        for side in (0, 1):
            j = rs_block(side, k)

            @pl.when(rs_sends(side, k))
            def _():
                if k:

                    @pl.when(has_left if side == 0 else has_right)
                    def _():
                        rs_copy(side, k - 1, j).wait_recv()
                        Pb[j] = (Pb[j].astype(F32) + Rb[j].astype(F32)).astype(BF)

                rs_copy(side, k, j).start()

    def own_keys():
        for which in range(2):
            dst = []
            for kh in range(KH):
                dst.append(kvs[0, which, :, kh * HEAD:(kh + 1) * HEAD].astype(F32))
            acc[which] = jnp.concatenate(dst, axis=1) if KH > 1 else dst[0]

        def come(i, carry):
            d = i + 1

            @pl.when(c + d <= NC - 1)
            def _():
                kv_copy(d).wait_recv()
                for which in range(2):
                    acc[which] += kvr[d - 1, which].astype(F32)

            return carry

        lax.fori_loop(0, NC - 1, come, 0)
        for kh in range(KH):
            cols = slice(kh * HEAD, (kh + 1) * HEAD)
            RKV[dp, 0, :, cols] = turned(acc[0], kh)
        RKV[dp, 1] = acc[1].astype(BF)
        for h in range(Hq // HEAD):
            RQ[dp, :, h * HEAD:(h + 1) * HEAD] = turned(dq[...] * scale, h)
        for i in range(2):
            for o in range(NDP - 1):
                pair_remote(i, o).start()
        for i in range(3):
            spread_local(i).wait()
            for o in range(NDP - 1):
                spread_remote(i, o).wait_recv()
        tile = tile_of(D)

        def part(i, carry):
            at = pl.ds(pl.multiple_of(i * tile, tile), tile)
            terms = dot_nt(RQ[dp], WQ[at, :]) + dot_nt(RKV[dp, 0], WK[at, :]) + dot_nt(RKV[dp, 1], WV[at, :])
            Pb[:, :, at] = terms.astype(BF).reshape(T, Lr, tile)
            return carry

        lax.fori_loop(0, D // tile, part, 0)
        rs_step(0)

    def rs_finish():
        igrad_ref[...] = Pb[t].astype(F32)

        @pl.when(has_left)
        def _():
            rs_copy(0, T - 2, t).wait_recv()
            igrad_ref[...] += Rb[t].astype(F32)

        @pl.when(has_right)
        def _():
            rs_copy(1, T - 2, t).wait_recv()
            igrad_ref[...] += Rb[T].astype(F32)

        rows = x_ref[...].astype(F32)
        grad, terms = rms_back(rows, inverse_rms(rows), gain_ref[0:1], igrad_ref[...])
        igrad_ref[...] = mdelta_ref[...] + grad
        G[0, 0:1] = terms
        G[0, 1:4] = gsum_ref[...]

    meets = [("tp", t, b) for b in bits_below(T)] + [("ctx", c, b) for b in bits_below(NC)]
    meets += [("dp", dp, b) for b in bits_below(NDP)]

    def g_copy(k):
        axis, index, bit = meets[k]
        return remote(G.at[k], GR.at[k], g_send.at[k], g_recv.at[k], along(axis, flip(index, bit)))

    def tick(i, carry):
        def start(w):
            @pl.when(i >= NS)
            def _():
                by_width(i - NS, lambda before: e_sent(i - NS, before))

            e_product(i, w)
            e_send_step(i, 0, w)

        by_width(i, start)

        @pl.when(i == 1)
        def _():
            attention()

        @pl.when(i == 2)
        def _():
            own_keys()

        for k in range(1, T - 1):

            @pl.when(i == 2 + k)
            def _():
                rs_step(k)

        @pl.when(i == 1 + T)
        def _():
            rs_finish()
            g_copy(0).start()

        for k in range(len(meets)):

            @pl.when(i == 2 + T + k)
            def _():
                g_copy(k).wait_recv()
                G[k + 1] = G[k] + GR[k]
                if k + 1 < len(meets):
                    g_copy(k + 1).start()

        @pl.when(i == wide_units)
        def _():
            for p in range(2):
                for o in range(NDP - 1):
                    pair_remote(p, o).wait_recv()

        for k in range(1, m):

            def middle(w):
                e_add(i - k, k - 1, w)
                e_send_step(i - k, k, w)

            by_width(i - k, middle)
        by_width(i - m, lambda w: e_finish(i - m, w))
        return carry

    lax.fori_loop(0, units + m, tick, 0)
    gains_ref[...] = G[len(meets)]

    for u in (units - 2, units - 1):
        out_wait(jnp.int32(u))
    for u in range(units - NS, units):
        by_width(jnp.int32(u), lambda w: e_sent(jnp.int32(u), w))
    for side in (0, 1):
        for k in range(T - 1):

            @pl.when(rs_sends(side, k))
            def _():
                rs_copy(side, k, rs_block(side, k)).wait_send()

    for k in range(len(meets)):
        g_copy(k).wait_send()
    for o in range(NDP - 1):
        for i in range(3):
            spread_remote(i, o).wait_send()
        for i in range(2):
            pair_remote(i, o).wait_send()

    def kv_close(i, carry):
        d = i + 1

        @pl.when((d <= c) & (d < kvs.shape[0]))
        def _():
            kv_copy(d).wait_send()

        return carry

    lax.fori_loop(0, min(NC - 1, kvs.shape[0] - 1), kv_close, 0)


def tail_call(
    layer_in, middle_delta, norm_gains, gain_sums, query, heads_delta, head_rows, log_totals, cosine, sine,
    keys_values, rows_one, w_query, w_key, w_value, rows, attn, heads, gate, up,
):
    T, NC, NDP = lax.axis_size("tp"), lax.axis_size("ctx"), lax.axis_size("dp")
    Lr, D = layer_in.shape
    R, Hq = query.shape
    KVd = w_key.shape[1]
    KH = KVd // HEAD
    Dh = D // NDP
    RB = Dh // NC
    F = gate.shape[1]
    W = tile_of(F) // 2
    m = NC.bit_length() - 1
    NS = max(4, m + 1)
    tokens = NDP * R
    kv_slots = min(NC, 4)
    meets = sum(n.bit_length() - 1 for n in (T, NC, NDP))
    any_spec = pl.BlockSpec(memory_space=pl.ANY)
    vm = pl.BlockSpec(memory_space=pltpu.VMEM)
    sds = jax.ShapeDtypeStruct
    dma = pltpu.SemaphoreType.DMA
    return pl.pallas_call(
        functools.partial(tail_kernel, T, NC, NDP, KH, NS),
        out_shape=(
            sds((Lr, D), F32), sds((4, D), F32),
            sds((RB, F), F32), sds((RB, F), F32), sds((RB, Hq), F32),
            sds((RB, Hq), F32), sds((RB, KVd), F32), sds((RB, KVd), F32),
        ),
        in_specs=[vm] * 10 + [any_spec] * 10,
        out_specs=[vm] * 2 + [any_spec] * 6,
        scratch_shapes=[
            pltpu.VMEM((3, tokens, Dh), BF), pltpu.VMEM((2, tokens, 2 * W), BF), pltpu.VMEM((tokens, Hq), BF),
            pltpu.VMEM((NDP, R, Hq), BF), pltpu.VMEM((NDP, 2, R, KVd), BF),
            pltpu.VMEM((D, Hq), BF), pltpu.VMEM((D, KVd), BF), pltpu.VMEM((D, KVd), BF),
            pltpu.VMEM((NS, 2, NC, RB, W), BF),
            *[pltpu.VMEM((NS, 2, NC >> (k + 1), RB, W), BF) for k in range(m)],
            pltpu.VMEM((2, 2, RB, W), F32), pltpu.VMEM((R, Hq), F32), pltpu.VMEM((Hq // HEAD, R), F32), pltpu.VMEM((2, T, 2, Lr, KVd), BF),
            pltpu.VMEM((kv_slots, 2, R, KVd), BF), pltpu.VMEM((NC - 1, 2, R, KVd), BF),
            pltpu.VMEM((T, Lr, D), BF), pltpu.VMEM((T + 1, Lr, D), BF), pltpu.VMEM((2, R, KVd), F32),
            pltpu.VMEM((meets + 1, 4, D), F32), pltpu.VMEM((meets, 4, D), F32),
            dma((4,)), dma((2,)), dma((2 * NDP - 1, 3)), dma((2 * (NDP - 1), 2)),
            dma((NS, 2, NC - 1)), dma((NS, 2, NC - 1)), dma((2, 2)), dma((NC - 1,)), dma((NC - 1,)),
            dma((2, T - 1)), dma((2, T - 1)), dma((meets,)), dma((meets,)), dma((2,)),
        ],
        compiler_params=pltpu.CompilerParams(
            collective_id=1, has_side_effects=True, vmem_limit_bytes=66_000_000
        ),
        name="tail",
    )(
        layer_in, middle_delta, norm_gains, gain_sums, query, heads_delta, head_rows, log_totals, cosine, sine,
        keys_values, rows_one, w_query, w_key, w_value, rows, attn, heads, gate, up,
    )


def shards(layer_in, cotangent, norm_gains, w_query, w_key, w_value, w_out, w_gate, w_up, w_down):
    tp_count, ctx_count, dp_count = lax.axis_size("tp"), lax.axis_size("ctx"), lax.axis_size("dp")
    half_width = HEAD // 2
    frequency = THETA ** (-(jnp.arange(half_width, dtype=F32) * 2.0) / HEAD)
    query, head_rows, log_totals, cosine, sine, keys_values, rows_one = front_call(
        layer_in, norm_gains, frequency[None, :], w_query, w_key, w_value
    )
    core = core_call(layer_in, cotangent, norm_gains, head_rows, w_out, w_gate, w_up, w_down)
    layer_out, middle_delta, gain_sums, heads_delta, rows, gate, up, attn, heads, down_turned = core
    input_grad, gains, grad_gate, grad_up, out_turned, grad_query, grad_key, grad_value = tail_call(
        layer_in, middle_delta, norm_gains, gain_sums, query, heads_delta, head_rows, log_totals, cosine, sine,
        keys_values, rows_one.reshape(-1, rows_one.shape[-1]), w_query, w_key, w_value,
        rows, attn, heads, gate, up,
    )
    rank = (lax.axis_index("dp") * ctx_count + lax.axis_index("ctx")) * tp_count + lax.axis_index("tp")
    width = gains.shape[1] // (dp_count * ctx_count * tp_count)
    gain_grads = lax.dynamic_slice_in_dim(gains, rank * width, width, 1)
    return (
        layer_out, input_grad, gain_grads, grad_query, grad_key, grad_value,
        out_turned.T, grad_gate, grad_up, down_turned.T,
    )


def solution(mesh):
    return jax.shard_map(
        shards,
        mesh=mesh,
        in_specs=(
            P(("dp", "ctx", "tp"), None),
            P(("dp", "ctx", "tp"), None),
            P(),
            P("dp", "tp"),
            P("dp", "tp"),
            P("dp", "tp"),
            P("tp", "dp"),
            P("dp", "tp"),
            P("dp", "tp"),
            P("tp", "dp"),
        ),
        out_specs=(
            P(("dp", "ctx", "tp"), None),
            P(("dp", "ctx", "tp"), None),
            P(None, ("dp", "ctx", "tp")),
            P(("dp", "ctx"), "tp"),
            P(("dp", "ctx"), "tp"),
            P(("dp", "ctx"), "tp"),
            P("tp", ("dp", "ctx")),
            P(("dp", "ctx"), "tp"),
            P(("dp", "ctx"), "tp"),
            P("tp", ("dp", "ctx")),
        ),
        check_vma=False,
    )
```

```python
import functools

import jax
import jax.numpy as jnp
from jax import lax
from jax.experimental import pallas as pl
from jax.experimental.pallas import tpu as pltpu
from jax.sharding import PartitionSpec as P

HEAD = 256
EPS = 1e-06
CAP = 50.0
THETA = 10000.0
MESH = pl.DeviceIdType.MESH
BF = jnp.bfloat16
F32 = jnp.float32


def tile_of(width):
    for tile in (768, 512, 256, 128):
        if width % tile == 0:
            return tile
    return width


def inverse_rms(values):
    return lax.rsqrt(jnp.mean(values * values, axis=-1, keepdims=True) + EPS)


def rms_back(values, scale, gain, delta):
    weighted = delta * gain
    inner = jnp.mean(weighted * values, axis=-1, keepdims=True)
    grad = scale * weighted - values * (scale * scale * scale * inner)
    return grad, jnp.sum(delta * values * scale, axis=0, keepdims=True)


def dot_nt(former, latter):
    return lax.dot_general(former, latter, (((1,), (1,)), ((), ())), preferred_element_type=F32)


def dot_nn(former, latter):
    return jnp.dot(former, latter, preferred_element_type=F32)


def barrier(count_of, peers):
    sem = pltpu.get_barrier_semaphore()
    for present, device_id in peers:

        @pl.when(present)
        def _():
            pl.semaphore_signal(sem, inc=1, device_id=device_id, device_id_type=MESH)

    pl.semaphore_wait(sem, count_of)


def flip(index, bit):
    return index + bit * (1 - 2 * lax.rem(index // bit, 2))


def flips(index, mask):
    bit = 1
    while bit <= mask:
        if mask & bit:
            index = flip(index, bit)
        bit *= 2
    return index


def dot_tn(former, latter):
    return lax.dot_general(former, latter, (((0,), (0,)), ((), ())), preferred_element_type=F32)


def sub_sums(bits):
    sums = [0]
    for bit in bits:
        sums = sums + [s + bit for s in sums]
    return sums


def bits_below(count):
    return [1 << i for i in range(count.bit_length() - 1)]


def core_kernel(
    T, C, NC, NDP,
    x_ref, ct_ref, gain_ref, heads_ref, wo_ref, wg_ref, wo_other, wg_other, wut_ref, wdt_ref,
    out_ref, mdelta_ref, gsum_ref, hdelta_ref,
    rows_pair, hid_pair, branch_pair, gate_pair, up_pair, attn_pair, head_pair, down_o,
    wo_v, wg_v, wu_v, wd_v, X, Pb, Rb, hid, Ab, Bb, att, mid, acc,
    L, Rc, st, w_sem, rs_send, rs_recv, ag_send, ag_recv, pair_sem, l_sem, e_send, e_recv, st_sem, free_sem,
):
    t = lax.axis_index("tp")
    dp = lax.axis_index("dp")
    c = lax.axis_index("ctx")
    D = x_ref.shape[1]
    rc = x_ref.shape[0] // C
    Dh = D // NDP
    F = wg_v.shape[1]
    M = T * rc
    has_left, has_right = t > 0, t < T - 1
    left, right = {"tp": jnp.maximum(t - 1, 0)}, {"tp": jnp.minimum(t + 1, T - 1)}
    partners = [{"dp": lax.rem(dp + o, NDP)} for o in range(1, NDP)]
    meets = [{"ctx": flip(c, bit)} for bit in bits_below(NC)]

    def columns_of(ref, owner):
        return ref.at[:, pl.ds(pl.multiple_of(owner * Dh, 128), Dh)]

    def rows_part(ref, owner):
        return ref.at[pl.ds(pl.multiple_of(owner * Dh, 128), Dh)]

    owners = [p["dp"] for p in partners]
    loads = [
        [pltpu.make_async_copy(wo_ref, columns_of(wo_v, dp), w_sem.at[0, 0])]
        + [
            pltpu.make_async_copy(columns_of(wo_other, p), columns_of(wo_v, p), w_sem.at[1 + o, 0])
            for o, p in enumerate(owners)
        ],
        [pltpu.make_async_copy(wg_ref, rows_part(wg_v, dp), w_sem.at[0, 1])]
        + [
            pltpu.make_async_copy(rows_part(wg_other, p), rows_part(wg_v, p), w_sem.at[1 + o, 1])
            for o, p in enumerate(owners)
        ],
        [pltpu.make_async_copy(wut_ref, wu_v, w_sem.at[0, 2])],
        [pltpu.make_async_copy(wdt_ref, wd_v, w_sem.at[0, 3])],
    ]
    for load in loads:
        for copy in load:
            copy.start()

    barrier(
        has_left.astype(jnp.int32) + has_right.astype(jnp.int32) + len(partners + meets),
        [(has_left, left), (has_right, right)] + [(t >= 0, p) for p in partners + meets],
    )

    def weight_wait(i):
        for copy in loads[i]:
            copy.wait()

    def pair_copies(kind, s, src, half, dst):
        def cut(owner):
            if half:
                return src.at[..., pl.ds(pl.multiple_of(owner * Dh, 128), Dh)]
            return src

        copies = [pltpu.make_async_copy(cut(dp), dst.at[dp, s], pair_sem.at[0, kind, s])]
        for o, partner in enumerate(partners):
            copies.append(
                pltpu.make_async_remote_copy(
                    cut(partner["dp"]), dst.at[dp, s],
                    pair_sem.at[1 + 2 * o, kind, s], pair_sem.at[2 + 2 * o, kind, s],
                    device_id=partner, device_id_type=MESH,
                )
            )
        return copies

    def pair_of(kind, s):
        return pair_copies(
            kind, s,
            *[
                (X.at[s], True, rows_pair),
                (hid.at[s], False, hid_pair),
                (X.at[s], True, branch_pair),
                (Ab.at[s], False, gate_pair),
                (Bb.at[s], False, up_pair),
                (X.at[s], True, attn_pair),
                (heads_ref.at[:, s], False, head_pair),
            ][kind],
        )

    def pair_start(kind, s):
        for copy in pair_of(kind, s):
            copy.start()

    def pair_kept(kind, s):
        pair_of(kind, s)[0].wait()

    def pair_away(kind, s):
        for copy in pair_of(kind, s)[1:]:
            copy.wait_send()

    def pair_received(kind, s):
        for copy in pair_of(kind, s)[1:]:
            copy.wait_recv()

    def rs_copy(s, side, k, j):
        if side == 0:
            slot, peer = j, right
        else:
            slot, peer = jnp.where(j == t - 1, T, j), left
        return pltpu.make_async_remote_copy(
            Pb.at[s, j], Rb.at[s, slot], rs_send.at[s, side, k], rs_recv.at[s, side, k],
            device_id=peer, device_id_type=MESH,
        )

    def rs_block(side, k):
        return (T - 1 - k + t) if side == 0 else (k - (T - 1 - t))

    def rs_sends(side, k):
        return (t <= k) if side == 0 else (T - 1 - t <= k)

    def ag_copy(s, side, k, j):
        return pltpu.make_async_remote_copy(
            X.at[s, j], X.at[s, j], ag_send.at[s, side, k], ag_recv.at[s, side, k],
            device_id=right if side == 0 else left, device_id_type=MESH,
        )

    def ag_block(side, k):
        return (t - k) if side == 0 else (t + k)

    def ag_sends(side, k):
        return (t >= k) & has_right if side == 0 else (t + k <= T - 1) & has_left

    def rs_start(s):
        for side in (0, 1):

            @pl.when(rs_sends(side, 0))
            def _():
                rs_copy(s, side, 0, rs_block(side, 0)).start()

    def rs_step(s, k):
        for side in (0, 1):
            j = rs_block(side, k)
            came = has_left if side == 0 else has_right

            @pl.when(rs_sends(side, k))
            def _():
                @pl.when(came)
                def _():
                    rs_copy(s, side, k - 1, j).wait_recv()
                    Pb[s, j] = (Pb[s, j].astype(F32) + Rb[s, j].astype(F32)).astype(BF)

                rs_copy(s, side, k, j).start()

    def rs_sent(s):
        for side in (0, 1):
            for k in range(T - 1):

                @pl.when(rs_sends(side, k))
                def _():
                    rs_copy(s, side, k, rs_block(side, k)).wait_send()

    def rs_finish(s):
        acc[...] = Pb[s, t].astype(F32)

        @pl.when(has_left)
        def _():
            rs_copy(s, 0, T - 2, t).wait_recv()
            acc[...] += Rb[s, t].astype(F32)

        @pl.when(has_right)
        def _():
            rs_copy(s, 1, T - 2, t).wait_recv()
            acc[...] += Rb[s, T].astype(F32)

    def ag_start(s):
        for side in (0, 1):

            @pl.when(ag_sends(side, 0))
            def _():
                ag_copy(s, side, 0, t).start()

    def ag_step(s, k):
        for side in (0, 1):
            j = ag_block(side, k)
            there = (j >= 0) if side == 0 else (j <= T - 1)

            @pl.when(there)
            def _():
                ag_copy(s, side, k - 1, j).wait_recv()
                if k <= T - 2:

                    @pl.when(has_right if side == 0 else has_left)
                    def _():
                        ag_copy(s, side, k, j).start()

    def ag_sent(s):
        for side in (0, 1):
            for k in range(T - 1):

                @pl.when(ag_sends(side, k))
                def _():
                    ag_copy(s, side, k, ag_block(side, k)).wait_send()

    def local_rows(n, s):
        own = pl.ds(pl.multiple_of(s * rc, rc), rc)
        total = acc[...]

        @pl.when(n == 0)
        def _():
            att[s] = total
            middle = x_ref[own].astype(F32) + total * inverse_rms(total) * gain_ref[1:2]
            mid[s] = middle
            X[s, t] = (middle * inverse_rms(middle) * gain_ref[2:3]).astype(BF)

        @pl.when(n == 1)
        def _():
            scale = inverse_rms(total)
            out_ref[own] = (mid[s] + total * scale * gain_ref[3:4]).astype(BF)
            grad, terms = rms_back(total, scale, gain_ref[3:4], ct_ref[own].astype(F32))
            gsum_ref[2:3] += terms
            X[s, t] = grad.astype(BF)

        @pl.when(n == 2)
        def _():
            middle, attention = mid[s], att[s]
            grad, terms = rms_back(middle, inverse_rms(middle), gain_ref[2:3], total)
            gsum_ref[1:2] += terms
            middle_delta = ct_ref[own].astype(F32) + grad
            mdelta_ref[own] = middle_delta
            grad, terms = rms_back(attention, inverse_rms(attention), gain_ref[1:2], middle_delta)
            gsum_ref[0:1] += terms
            X[s, t] = grad.astype(BF)

    def comm(tau, w, a):
        back = tau - a

        @pl.when((back >= 0) & (back < 3 * C))
        def _():
            n, s = back // C, lax.rem(back, C)
            if w <= T - 2:
                rs_step(s, w)
            elif w == T - 1:
                rs_finish(s)
                local_rows(n, s)
                ag_start(s)
            else:
                ag_step(s, w - (T - 1))

    def tiles(width, body):
        tile = tile_of(width)

        def step(i, carry):
            body(pl.ds(pl.multiple_of(i * tile, tile), tile), tile)
            return carry

        lax.fori_loop(0, width // tile, step, 0)

    def rows_of(s):
        return X[s].reshape(M, D)

    def store_part(s, at, tile, value):
        Pb[s, :, :, at] = value.astype(BF).reshape(T, rc, tile)

    m = NC.bit_length() - 1
    RB = Dh // NC
    W = Rc.shape[-1] // 2
    units = F // (2 * W)
    begin = 3 * C - 1
    pitch = -(-RB // 16) * 16
    orders = [bits_below(NC), bits_below(NC)[::-1]]
    first_of = [sum(NC >> (i + 1) for i in range(k)) for k in range(m)]

    def block_of(ref, i):
        down = ref.shape[0] // pitch
        row = pl.multiple_of(lax.rem(i, down) * pitch, 16)
        return ref.at[pl.ds(row, RB), pl.ds(pl.multiple_of((i // down) * W, 128), W)]

    def part_of(u, par, owner):
        return block_of(wd_v, (u * 2 + par) * NC + owner)

    early = units * 2 * (2 * NC - 1) <= (D // pitch) * (F // W)

    def came_of(u, par, at):
        i = (u * 2 + par) * (NC - 1) + at
        return block_of(wd_v, units * 2 * NC + i) if early else block_of(wu_v, i)

    def free():
        for meet in meets:
            pl.semaphore_signal(free_sem, inc=1, device_id=meet, device_id_type=MESH)

    def e_copy(u, par, k, n):
        order = orders[par]
        at = first_of[k] + n
        return pltpu.make_async_remote_copy(
            part_of(u, par, flips(c, sub_sums(order[k + 1:])[n] + order[k])), came_of(u, par, at),
            e_send.at[u, par, at], e_recv.at[u, par, at],
            device_id={"ctx": flip(c, order[k])}, device_id_type=MESH,
        )

    def e_each(u, k, act):
        for par in (0, 1):
            for n in range(NC >> (k + 1)):
                act(par, n)

    def e_add(u, k):
        def one(par, n):
            e_copy(u, par, k, n).wait_recv()
            if k < m - 1:
                ref = part_of(u, par, flips(c, sub_sums(orders[par][k + 1:])[n]))
                ref[...] = (ref[...].astype(F32) + came_of(u, par, first_of[k] + n)[...].astype(F32)).astype(BF)

        e_each(u, k, one)

    def chunk_load(u):
        at = pl.ds(pl.multiple_of(u * 2 * W, 128), 2 * W)
        return pltpu.make_async_copy(hid_pair.at[:, :, :, at], Rc, l_sem.at[1])

    def first_all():
        return pltpu.make_async_copy(branch_pair, L, l_sem.at[0])

    def out_copy(u, par):
        at = pl.ds(pl.multiple_of((2 * u + par) * W, 128), W)
        return pltpu.make_async_copy(st.at[par], down_o.at[:, at], st_sem.at[par])

    def engine(tau):
        u = tau - begin

        @pl.when((u >= 0) & (u < units))
        def _():
            @pl.when(u == 0)
            def _():
                first_all().wait()
                pl.semaphore_wait(free_sem, len(meets))

            chunk_load(u).wait()
            rows = NDP * C * M
            for par in (0, 1):
                product = dot_tn(L[...].reshape(rows, Dh), Rc[:, :, :, par * W:(par + 1) * W].reshape(rows, W))
                for owner in range(NC):
                    part_of(u, par, owner)[...] = product[owner * RB:(owner + 1) * RB].astype(BF)

            @pl.when(u + 1 < units)
            def _():
                chunk_load(u + 1).start()

            e_each(u, 0, lambda par, n: e_copy(u, par, 0, n).start())

        for k in range(1, m):

            @pl.when((u - k >= 0) & (u - k < units))
            def _():
                e_add(u - k, k - 1)
                e_each(u - k, k, lambda par, n: e_copy(u - k, par, k, n).start())

        @pl.when((u - m >= 0) & (u - m < units))
        def _():
            e_add(u - m, m - 1)
            for par in (0, 1):

                @pl.when(u - m > 0)
                def _():
                    out_copy(u - m - 1, par).wait()

                st[par] = (
                    part_of(u - m, par, c)[...].astype(F32) + came_of(u - m, par, first_of[m - 1])[...].astype(F32)
                ).astype(BF)
                out_copy(u - m, par).start()

    def engine_open():
        pair_kept(2, C - 1)

        def each(s, carry):
            pair_kept(1, s)
            pair_received(1, s)
            pair_received(2, s)
            return carry

        lax.fori_loop(0, C, each, 0)
        first_all().start()
        chunk_load(0).start()

    def tick(tau, carry):
        n, s = tau // C, lax.rem(tau, C)

        @pl.when((n >= 1) & (n <= 2))
        def _():
            rs_sent(s)

        @pl.when(n == 1)
        def _():
            @pl.when(s == 0)
            def _():
                weight_wait(1)
                weight_wait(2)

            pair_start(0, s)

            def gate_up(at, tile):
                gate = dot_nn(rows_of(s), wg_v[:, at])
                up = dot_nt(rows_of(s), wu_v[at, :])
                inner = jnp.tanh(0.7978845608028654 * (gate + 0.044715 * gate * gate * gate))
                half = 0.5 * (1.0 + inner)
                gelu = gate * half
                slope = half + 0.5 * gate * (1.0 - inner * inner) * (
                    0.7978845608028654 * (1.0 + 0.134145 * gate * gate)
                )
                hid[s, :, at] = (gelu * up).astype(BF)
                Ab[s, :, at] = (up * slope).astype(BF)
                Bb[s, :, at] = gelu.astype(BF)

            tiles(F, gate_up)
            pair_start(1, s)

        @pl.when(n == 2)
        def _():
            pair_start(2, s)

            def gate_up_delta(at, tile):
                delta = dot_nn(rows_of(s), wd_v[:, at])
                Ab[s, :, at] = (delta * Ab[s, :, at].astype(F32)).astype(BF)
                Bb[s, :, at] = (delta * Bb[s, :, at].astype(F32)).astype(BF)

            tiles(F, gate_up_delta)
            pair_start(3, s)
            pair_start(4, s)

            @pl.when(s == C - 1)
            def _():
                if early:
                    free()
                engine_open()

        if early:
            engine(tau)

        for a in range(1, T):
            comm(tau, 2 * a - 1, a)

        @pl.when(n == 0)
        def _():
            pair_start(6, s)
            heads = heads_ref[:, s].reshape(M, heads_ref.shape[3])
            tiles(D, lambda at, tile: store_part(s, at, tile, dot_nn(heads, wo_v[:, at])))

        @pl.when(n == 1)
        def _():
            @pl.when(s == 0)
            def _():
                weight_wait(3)

            tiles(D, lambda at, tile: store_part(s, at, tile, dot_nt(hid[s], wd_v[at, :])))
            pair_kept(0, s)
            pair_away(0, s)
            ag_sent(s)

        @pl.when(n == 2)
        def _():
            tiles(
                D,
                lambda at, tile: store_part(
                    s, at, tile, dot_nt(Ab[s], wg_v[at, :]) + dot_nn(Bb[s], wu_v[:, at])
                ),
            )
            pair_away(2, s)

            @pl.when(s < C - 1)
            def _():
                pair_kept(2, s)

            ag_sent(s)

            if not early:
                pl.when(s == C - 1)(free)

        @pl.when(n <= 2)
        def _():
            rs_start(s)

        if not early:
            engine(tau)

        @pl.when(n == 3)
        def _():
            pair_start(5, s)
            hdelta_ref[:, s] = (
                dot_nt(rows_of(s), wo_v[...]).astype(BF).reshape(T, rc, heads_ref.shape[3])
            )

        for a in range(1, T):
            comm(tau, 2 * a, a)
        return carry

    gsum_ref[...] = jnp.zeros_like(gsum_ref)
    weight_wait(0)
    lax.fori_loop(0, max(4 * C, begin + units + m), tick, 0)

    def close(s, carry):
        for kind in (3, 4, 5, 6):
            pair_kept(kind, s)
            pair_received(kind, s)
            pair_away(kind, s)
        pair_received(0, s)
        pair_away(1, s)
        rs_sent(s)
        ag_sent(s)
        return carry

    lax.fori_loop(0, C, close, 0)

    def close_engine(u, carry):
        for k in range(m):
            e_each(u, k, lambda par, n: e_copy(u, par, k, n).wait_send())
        return carry

    lax.fori_loop(0, units, close_engine, 0)
    for par in (0, 1):
        out_copy(units - 1, par).wait()


def core_call(layer_in, cotangent, norm_gains, head_flat, w_out, w_gate, *weights):
    T, NC, NDP = lax.axis_size("tp"), lax.axis_size("ctx"), lax.axis_size("dp")
    C = T
    Lr, D = layer_in.shape
    rc = Lr // C
    Hq = w_out.shape[0]
    RB = D // NDP // NC
    Dh = D // NDP
    F = w_gate.shape[1]
    M = T * rc
    W = tile_of(F) // 2
    any_spec = pl.BlockSpec(memory_space=pl.ANY)
    vm = pl.BlockSpec(memory_space=pltpu.VMEM)
    sds = jax.ShapeDtypeStruct
    outs = pl.pallas_call(
        functools.partial(core_kernel, T, C, NC, NDP),
        out_shape=(
            sds((Lr, D), BF), sds((Lr, D), F32), sds((3, D), F32), sds((T, C, rc, Hq), BF),
            sds((NDP, C, T, rc, Dh), BF), sds((NDP, C, M, F), BF), sds((NDP, C, T, rc, Dh), BF),
            sds((NDP, C, M, F), BF), sds((NDP, C, M, F), BF), sds((NDP, C, T, rc, Dh), BF),
            sds((NDP, C, T, rc, Hq), BF), sds((RB, F), BF),
        ),
        in_specs=[vm, vm, vm, vm] + [any_spec] * 6,
        out_specs=[vm, vm, vm, vm] + [any_spec] * 8,
        scratch_shapes=[
            pltpu.VMEM((Hq, D), BF), pltpu.VMEM((D, F), BF), pltpu.VMEM((D, F), BF), pltpu.VMEM((F, D), BF),
            pltpu.VMEM((C, T, rc, D), BF), pltpu.VMEM((C, T, rc, D), BF), pltpu.VMEM((C, T + 1, rc, D), BF),
            pltpu.VMEM((C, M, F), BF), pltpu.VMEM((C, M, F), BF), pltpu.VMEM((C, M, F), BF),
            pltpu.VMEM((C, rc, D), F32), pltpu.VMEM((C, rc, D), F32), pltpu.VMEM((rc, D), F32),
            pltpu.VMEM((NDP, C, T, rc, Dh), BF), pltpu.VMEM((NDP, C, M, 2 * W), BF), pltpu.VMEM((2, RB, W), BF),
            pltpu.SemaphoreType.DMA((NDP, 4)),
            pltpu.SemaphoreType.DMA((C, 2, T - 1)), pltpu.SemaphoreType.DMA((C, 2, T - 1)),
            pltpu.SemaphoreType.DMA((C, 2, T - 1)), pltpu.SemaphoreType.DMA((C, 2, T - 1)),
            pltpu.SemaphoreType.DMA((2 * NDP - 1, 7, C)),
            pltpu.SemaphoreType.DMA((2,)), pltpu.SemaphoreType.DMA((F // (2 * W), 2, NC - 1)),
            pltpu.SemaphoreType.DMA((F // (2 * W), 2, NC - 1)), pltpu.SemaphoreType.DMA((2,)),
            pltpu.SemaphoreType.REGULAR,
        ],
        compiler_params=pltpu.CompilerParams(
            collective_id=0, has_side_effects=True, vmem_limit_bytes=67_043_328
        ),
        name="core",
    )(layer_in, cotangent, norm_gains, head_flat.reshape(T, C, rc, Hq), w_out, w_gate, *weights)
    out, mdelta, gsum, hdelta, rows, hidden, branch, gate, up, attn, heads, down = outs
    flat = lambda a: a.reshape(NDP * T * Lr, a.shape[-1])
    return (
        out, mdelta, gsum, hdelta.reshape(T * Lr, Hq),
        flat(rows), flat(gate), flat(up), flat(attn), flat(heads), down,
    )


def front_kernel(
    T, NC, NDP, KH, C,
    x_ref, gain_ref, freq_ref, wq_ref, wk_ref, wv_ref, wo_ref, wg_ref, wu_ref, wd_ref,
    q_o, heads_o, logt_o, cos_o, sin_o, kv_o, rows1_o, wo_o, wg_o, wut_o, wdt_o,
    X, WQ, WK, WV, KV, turned_sum, totals, up_v, upt_v, down_v, downt_v,
    w_sem, ag_send, ag_recv, pair_sem, kv_send, kv_recv, out_sem, t_sem, p_sem,
):
    t, c, dp = lax.axis_index("tp"), lax.axis_index("ctx"), lax.axis_index("dp")
    Lr, D = x_ref.shape
    R, Hq = q_o.shape
    rc = Lr // C
    KVd = KH * HEAD
    GS = Hq // KVd
    Dh = D // NDP
    scale = HEAD**-0.5
    has_left, has_right = t > 0, t < T - 1

    def remote(src, dst, send, recv, axis, index):
        return pltpu.make_async_remote_copy(
            src, dst, send, recv, device_id={axis: index}, device_id_type=MESH
        )

    partners = [lax.rem(dp + o, NDP) for o in range(1, NDP)]
    peers = [("tp", lax.rem(t + o, T)) for o in range(1, T)]
    peers += [("ctx", lax.rem(c + o, NC)) for o in range(1, NC)]
    peers += [("dp", p) for p in partners]
    sem = pltpu.get_barrier_semaphore()
    for axis, index in peers:
        pl.semaphore_signal(sem, inc=1, device_id={axis: index}, device_id_type=MESH)

    rows_at = pl.ds(pl.multiple_of(dp * Dh, 128), Dh)
    weights = [(wq_ref, WQ), (wk_ref, WK), (wv_ref, WV)]

    def weight_local(i):
        return pltpu.make_async_copy(weights[i][0], weights[i][1].at[rows_at], w_sem.at[0, i])

    def weight_remote(i, o):
        return remote(
            weights[i][0], weights[i][1].at[rows_at], w_sem.at[1 + 2 * o, i], w_sem.at[2 + 2 * o, i],
            "dp", partners[o],
        )

    turns = [
        pltpu.make_async_copy(wu_ref, up_v, t_sem.at[0]),
        pltpu.make_async_copy(wd_ref, down_v, t_sem.at[1]),
    ]
    for i in range(3):
        weight_local(i).start()
    for copy in turns:
        copy.start()
    rows = x_ref[...].astype(F32)
    X[t] = (rows * inverse_rms(rows) * gain_ref[0:1]).astype(BF)
    pl.semaphore_wait(sem, len(peers))

    def ag_copy(s, side, k, j):
        at = pl.ds(s * rc, rc)
        peer = jnp.minimum(t + 1, T - 1) if side == 0 else jnp.maximum(t - 1, 0)
        return remote(X.at[j, at], X.at[j, at], ag_send.at[s, side, k], ag_recv.at[s, side, k], "tp", peer)

    def ag_block(side, k):
        return (t - k) if side == 0 else (t + k)

    def ag_there(side, k):
        return (t >= k) if side == 0 else (t + k <= T - 1)

    def onward(side):
        return has_right if side == 0 else has_left

    for s in range(C):
        for side in (0, 1):

            @pl.when(onward(side))
            def _():
                ag_copy(s, side, 0, t).start()

    for i in range(3):
        for o in range(NDP - 1):
            weight_remote(i, o).start()

    def parts(ref, i):
        height = ref.shape[0] // T
        return pl.ds(pl.multiple_of(i * height, 16), height), height

    def part_dst(dst, ref, i, columns):
        at, height = parts(ref, i)
        if columns:
            return dst.at[at, rows_at]
        return dst.at[pl.ds(pl.multiple_of(dp * Dh + i * height, 16), height)]

    moved = [(wo_ref, wo_o, True, False), (wg_ref, wg_o, False, False)]
    moved += [(upt_v, wut_o, True, True), (downt_v, wdt_o, False, True)]

    def part_remote(w, i, o):
        src, dst, columns, _ = moved[w]
        return remote(
            src.at[parts(src, i)[0]], part_dst(dst, src, i, columns),
            p_sem.at[1 + 2 * o, w, i], p_sem.at[2 + 2 * o, w, i], "dp", partners[o],
        )

    def part_local(w, i):
        src, dst, columns, _ = moved[w]
        return pltpu.make_async_copy(src.at[parts(src, i)[0]], part_dst(dst, src, i, columns), p_sem.at[0, w, i])

    def part_start(w, i):
        for o in range(NDP - 1):
            part_remote(w, i, o).start()
        if moved[w][3]:
            part_local(w, i).start()

    def turn():
        for copy, src, dst in zip(turns, (up_v, down_v), (upt_v, downt_v), strict=True):
            copy.wait()
            height = src.shape[0] // T

            def some(i, carry):
                at = pl.ds(pl.multiple_of(i * height, 128), height)
                dst[:, at] = src[at, :].T
                return carry

            if height % 128 == 0:
                lax.fori_loop(0, T, some, 0)
            else:
                dst[...] = src[...].T

    position = (c * R + lax.broadcasted_iota(jnp.int32, (R, HEAD // 2), 0)).astype(F32)
    angles = position * freq_ref[...]
    cos_o[...] = jnp.cos(angles)
    sin_o[...] = jnp.sin(angles)
    for i in range(3):
        weight_local(i).wait()
        for o in range(NDP - 1):
            weight_remote(i, o).wait_recv()

    def kv_copy(d, j):
        return remote(
            KV.at[c, j], KV.at[c, j], kv_send.at[d - 1, j], kv_recv.at[d - 1, j],
            "ctx", jnp.minimum(c + d, NC - 1),
        )

    def kv_from(b, j):
        d = c - b
        return remote(KV.at[b, j], KV.at[b, j], kv_send.at[d - 1, j], kv_recv.at[d - 1, j], "ctx", c)

    def pair_copies(j):
        def half(owner):
            return X.at[j, :, pl.ds(pl.multiple_of(owner * Dh, 128), Dh)]

        copies = [pltpu.make_async_copy(half(dp), rows1_o.at[dp, j], pair_sem.at[0, j])]
        for o, partner in enumerate(partners):
            copies.append(
                remote(
                    half(partner), rows1_o.at[dp, j], pair_sem.at[1 + 2 * o, j], pair_sem.at[2 + 2 * o, j],
                    "dp", partner,
                )
            )
        return copies

    def turned(values, h, at):
        a, b = values[:, h * HEAD:h * HEAD + HEAD // 2], values[:, h * HEAD + HEAD // 2:(h + 1) * HEAD]
        cosine, sine = cos_o[at], sin_o[at]
        return jnp.concatenate([a * cosine - b * sine, b * cosine + a * sine], axis=1).astype(BF)

    def project(j):
        for copy in pair_copies(j):
            copy.start()
        at = pl.ds(pl.multiple_of(j * Lr, Lr), Lr)
        values = dot_nn(X[j], WK[...])
        for kh in range(KH):
            KV[c, j, 0, :, kh * HEAD:(kh + 1) * HEAD] = turned(values, kh, at)
        KV[c, j, 1] = dot_nn(X[j], WV[...]).astype(BF)

        def push(i, carry):
            @pl.when(c + 1 + i <= NC - 1)
            def _():
                kv_copy(i + 1, j).start()

            return carry

        lax.fori_loop(0, NC - 1, push, 0)
        values = dot_nn(X[j], WQ[...])
        for h in range(Hq // HEAD):
            q_o[at, h * HEAD:(h + 1) * HEAD] = turned(values, h, at)

    def gather(k, carry):
        for side in (0, 1):

            @pl.when(ag_there(side, k) & (k > 0))
            def _():
                for s in range(C):
                    ag_copy(s, side, k - 1, ag_block(side, k)).wait_recv()

                    @pl.when(onward(side) & (k <= T - 2))
                    def _():
                        ag_copy(s, side, k, ag_block(side, k)).start()

        for side in (0, 1):

            @pl.when(ag_there(side, k) & ((k > 0) | (side == 0)))
            def _():
                project(ag_block(side, k))

        part_start(0, k)
        part_start(1, k)

        @pl.when(k == 0)
        def _():
            turn()

        part_start(2, k)
        part_start(3, k)
        return carry

    lax.fori_loop(0, T, gather, 0)

    per = max(1, 256 // Lr)
    tile = per * Lr
    turned_sum[...] = jnp.zeros_like(turned_sum)
    totals[...] = jnp.zeros_like(totals)

    def out_copy(b):
        return pltpu.make_async_copy(KV.at[b], kv_o.at[b], out_sem.at[b])

    def key_step(b, p, masked):
        for kh in range(KH):
            cols = slice(kh * HEAD, (kh + 1) * HEAD)
            keys = KV[b, pl.ds(p * per, per), 0, :, cols].reshape(tile, HEAD)
            values = KV[b, pl.ds(p * per, per), 1, :, cols].reshape(tile, HEAD)
            for g in range(GS):
                h = kh * GS + g
                scores = dot_nt(keys, q_o[:, h * HEAD:(h + 1) * HEAD])
                weights = jnp.exp(CAP * jnp.tanh(scores * (scale / CAP)))
                if masked:
                    key_pos = p * tile + lax.broadcasted_iota(jnp.int32, weights.shape, 0)
                    allowed = key_pos <= lax.broadcasted_iota(jnp.int32, weights.shape, 1)
                    weights = jnp.where(allowed, weights, 0.0)
                totals[h:h + 1] += jnp.sum(weights, axis=0, keepdims=True)
                turned_sum[h] += dot_tn(values, weights.astype(BF))

    def own_step(p, carry):
        key_step(c, p, True)
        return carry

    out_copy(c).start()
    lax.fori_loop(0, T // per, own_step, 0)

    def far_block(i, carry):
        @pl.when(i < c)
        def _():
            b = c - 1 - i
            for j in range(T):
                kv_from(b, j).wait_recv()
            out_copy(b).start()

            def far_step(p, carry):
                key_step(b, p, False)
                return carry

            lax.fori_loop(0, T // per, far_step, 0)

        return carry

    lax.fori_loop(0, NC - 1, far_block, 0)
    for h in range(Hq // HEAD):
        heads_o[:, h * HEAD:(h + 1) * HEAD] = (turned_sum[h] / totals[h:h + 1]).T.astype(BF)
    logt_o[...] = jnp.log(totals[...])

    for i in range(3):
        for o in range(NDP - 1):
            weight_remote(i, o).wait_send()

    def close_parts(i, carry):
        for w in range(4):
            for o in range(NDP - 1):
                part_remote(w, i, o).wait()
            if moved[w][3]:
                part_local(w, i).wait()
        return carry

    lax.fori_loop(0, T, close_parts, 0)
    for s in range(C):
        for side in (0, 1):
            for k in range(T - 1):

                @pl.when(ag_there(side, k) & onward(side))
                def _():
                    ag_copy(s, side, k, ag_block(side, k)).wait_send()

    for j in range(T):
        copies = pair_copies(j)
        copies[0].wait()
        for copy in copies[1:]:
            copy.wait()

    def close(i, carry):
        @pl.when(c + 1 + i <= NC - 1)
        def _():
            for j in range(T):
                kv_copy(i + 1, j).wait_send()

        return carry

    lax.fori_loop(0, NC - 1, close, 0)

    def close_out(b, carry):
        @pl.when(b <= c)
        def _():
            out_copy(b).wait()

        return carry

    lax.fori_loop(0, NC, close_out, 0)


def front_call(layer_in, norm_gains, frequency, w_query, w_key, w_value, w_out, w_gate, w_up, w_down):
    T, NC, NDP = lax.axis_size("tp"), lax.axis_size("ctx"), lax.axis_size("dp")
    C = T
    Lr, D = layer_in.shape
    R = T * Lr
    Hq, KVd = w_query.shape[1], w_key.shape[1]
    Dh = D // NDP
    F = w_gate.shape[1]
    H = Hq // HEAD
    any_spec = pl.BlockSpec(memory_space=pl.ANY)
    vm = pl.BlockSpec(memory_space=pltpu.VMEM)
    sds = jax.ShapeDtypeStruct
    dma = pltpu.SemaphoreType.DMA
    return pl.pallas_call(
        functools.partial(front_kernel, T, NC, NDP, KVd // HEAD, C),
        out_shape=(
            sds((R, Hq), BF), sds((R, Hq), BF), sds((H, R), F32),
            sds((R, HEAD // 2), F32), sds((R, HEAD // 2), F32),
            sds((NC, T, 2, Lr, KVd), BF), sds((NDP, T, Lr, Dh), BF),
            sds((Hq, D), BF), sds((D, F), BF), sds((F, D), BF), sds((D, F), BF),
        ),
        in_specs=[vm] * 3 + [any_spec] * 7,
        out_specs=[vm] * 5 + [any_spec] * 6,
        scratch_shapes=[
            pltpu.VMEM((T, Lr, D), BF), pltpu.VMEM((D, Hq), BF), pltpu.VMEM((D, KVd), BF), pltpu.VMEM((D, KVd), BF),
            pltpu.VMEM((NC, T, 2, Lr, KVd), BF), pltpu.VMEM((H, HEAD, R), F32), pltpu.VMEM((H, R), F32),
            pltpu.VMEM((Dh, F), BF), pltpu.VMEM((F, Dh), BF), pltpu.VMEM((F, Dh), BF), pltpu.VMEM((Dh, F), BF),
            dma((2 * NDP - 1, 3)), dma((C, 2, T - 1)), dma((C, 2, T - 1)), dma((2 * NDP - 1, T)),
            dma((NC - 1, T)), dma((NC - 1, T)), dma((NC,)), dma((2,)), dma((2 * NDP - 1, 4, T)),
        ],
        compiler_params=pltpu.CompilerParams(
            collective_id=2, has_side_effects=True, vmem_limit_bytes=66_000_000
        ),
        name="front",
    )(layer_in, norm_gains, frequency, w_query, w_key, w_value, w_out, w_gate, w_up, w_down)


def tail_kernel(
    T, NC, NDP, KH, NS,
    x_ref, mdelta_ref, gain_ref, gsum_ref, q_ref, hd_ref, heads_ref, logt_ref, cos_ref, sin_ref,
    kv_ref, rows1_ref, wq_ref, wk_ref, wv_ref,
    rows_ref, attn_ref, head_ref, gate_ref, up_ref,
    igrad_ref, gains_ref, gate_o, up_o, out_o, q_o, k_o, v_o,
    L, Rc, Hd, RQ, RKV, WQ, WK, WV, Pe, *rest,
):
    m = NC.bit_length() - 1
    Rv, rest = rest[:m], rest[m:]
    (
        st, dq, rdelta, kvb, kvs, kvr, Pb, Rb, acc, G, GR,
        l_sem, r_sem, w_sem, pair_sem, e_send, e_recv, st_sem, kv_send, kv_recv,
        rs_send, rs_recv, g_send, g_recv, kvb_sem,
    ) = rest
    t, c, dp = lax.axis_index("tp"), lax.axis_index("ctx"), lax.axis_index("dp")
    Lr, D = x_ref.shape
    R, Hq = q_ref.shape
    KVd = KH * HEAD
    GS = Hq // KVd
    Dh, RB = D // NDP, D // NDP // NC
    F = gate_ref.shape[1]
    W = Rc.shape[-1] // 2
    NF = F // (2 * W)
    wide_units, units = 2 * NF, 2 * NF + 3
    narrow = Hq // 2
    scale = HEAD**-0.5

    def along(axis, index):
        return {axis: index}

    others = [along("tp", lax.rem(t + o, T)) for o in range(1, T)]
    others += [along("ctx", lax.rem(c + o, NC)) for o in range(1, NC)]
    partners = [along("dp", lax.rem(dp + o, NDP)) for o in range(1, NDP)]
    def remote(src, dst, send, recv, peer):
        return pltpu.make_async_remote_copy(src, dst, send, recv, device_id=peer, device_id_type=MESH)

    firsts = [rows_ref, attn_ref, rows1_ref]

    def first_copy(i):
        return pltpu.make_async_copy(firsts[i], L.at[i], l_sem.at[i])

    rows_at = pl.ds(pl.multiple_of(dp * Dh, 128), Dh)
    spread = [
        (lambda owner: wq_ref, WQ.at[rows_at]),
        (lambda owner: wk_ref, WK.at[rows_at]),
        (lambda owner: wv_ref, WV.at[rows_at]),
    ]

    def spread_local(i):
        return pltpu.make_async_copy(spread[i][0](dp), spread[i][1], w_sem.at[0, i])

    def spread_remote(i, o):
        return remote(
            spread[i][0](partners[o]["dp"]), spread[i][1],
            w_sem.at[1 + 2 * o, i], w_sem.at[2 + 2 * o, i], partners[o],
        )

    kinds = [gate_ref, up_ref]

    def chunk_copy(u, kind):
        at = pl.ds(pl.multiple_of((u - kind * NF) * 2 * W, 128), 2 * W)
        return pltpu.make_async_copy(kinds[kind].at[:, at], Rc.at[lax.rem(u, 2)], r_sem.at[lax.rem(u, 2)])

    def chunk_start(u):
        for kind in range(2):

            @pl.when((u >= kind * NF) & (u < (kind + 1) * NF))
            def _():
                chunk_copy(u, kind).start()

    first_copy(0).start()
    chunk_start(0)
    sem = pltpu.get_barrier_semaphore()
    for peer in others + partners:
        pl.semaphore_signal(sem, inc=1, device_id=peer, device_id_type=MESH)
    pl.semaphore_wait(sem, len(others + partners))
    first_copy(1).start()
    head_copy = pltpu.make_async_copy(head_ref, Hd, l_sem.at[3])
    head_copy.start()
    first_copy(2).start()

    orders = [bits_below(NC), bits_below(NC)[::-1]]
    first_of = [sum(NC >> (i + 1) for i in range(k)) for k in range(m)]

    def e_copy(u, par, k, n, w):
        order = orders[par]
        kept = sub_sums(order[k + 1:])[n]
        slot = lax.rem(u, NS)
        at = first_of[k] + n
        return remote(
            Pe.at[slot, par, flips(c, kept + order[k]), :, pl.ds(0, w)],
            Rv[k].at[slot, par, n, :, pl.ds(0, w)],
            e_send.at[slot, par, at], e_recv.at[slot, par, at],
            along("ctx", flip(c, order[k])),
        )

    def e_sent(u, w):
        for par in (0, 1):
            for k in range(m):
                for n in range(NC >> (k + 1)):
                    e_copy(u, par, k, n, w).wait_send()

    def e_product(u, w):
        slot = lax.rem(u, NS)

        def store(par, first, second):
            Pe[slot, par, :, :, :w] = dot_tn(first, second).reshape(NC, RB, w).astype(BF)

        if w == W:
            for kind in range(2):

                @pl.when((u >= kind * NF) & (u < (kind + 1) * NF))
                def _():
                    chunk_copy(u, kind).wait()

            @pl.when(u == 0)
            def _():
                first_copy(0).wait()

            chunk_start(u + 1)
            for par in (0, 1):
                store(par, L[0], Rc[lax.rem(u, 2), :, par * W:(par + 1) * W])
        else:

            @pl.when(u == wide_units)
            def _():
                first_copy(1).wait()
                head_copy.wait()
                for par in (0, 1):
                    store(par, L[1], Hd[:, par * w:(par + 1) * w])

            @pl.when(u == wide_units + 1)
            def _():
                first_copy(2).wait()
                for par in (0, 1):
                    store(par, L[2], RQ[:, :, par * w:(par + 1) * w].reshape(NDP * R, w))

            @pl.when(u == wide_units + 2)
            def _():
                for par in (0, 1):
                    store(par, L[2], RKV[:, par].reshape(NDP * R, w))

    def e_send_step(u, k, w):
        for par in (0, 1):
            for n in range(NC >> (k + 1)):
                e_copy(u, par, k, n, w).start()

    def e_add(u, k, w):
        slot = lax.rem(u, NS)
        for par in (0, 1):
            for n in range(NC >> (k + 1)):
                e_copy(u, par, k, n, w).wait_recv()
                if k < m - 1:
                    kept = flips(c, sub_sums(orders[par][k + 1:])[n])
                    Pe[slot, par, kept, :, :w] = (
                        Pe[slot, par, kept, :, :w].astype(F32) + Rv[k][slot, par, n, :, :w].astype(F32)
                    ).astype(BF)

    def out_copies(u, w):
        two = lax.rem(u, 2)

        def copy(par, dst):
            return pltpu.make_async_copy(st.at[two, par, :, pl.ds(0, w)], dst, st_sem.at[two, par])

        if w == W:
            pairs = []
            for kind, dst in enumerate([gate_o, up_o]):
                base = (u - kind * NF) * 2 * W
                pairs.append((
                    (u >= kind * NF) & (u < (kind + 1) * NF),
                    [copy(p, dst.at[:, pl.ds(pl.multiple_of(base + p * W, 128), W)]) for p in (0, 1)],
                ))
            return pairs
        return [
            (u == wide_units, [copy(p, out_o.at[:, pl.ds(p * w, w)]) for p in (0, 1)]),
            (u == wide_units + 1, [copy(p, q_o.at[:, pl.ds(p * w, w)]) for p in (0, 1)]),
            (u == wide_units + 2, [copy(0, k_o), copy(1, v_o)]),
        ]

    def out_wait(u):
        for w in (W, narrow):
            for here, copies in out_copies(u, w):

                @pl.when(here)
                def _():
                    for copy in copies:
                        copy.wait()

    def e_finish(u, w):
        slot, two = lax.rem(u, NS), lax.rem(u, 2)
        e_add(u, m - 1, w)
        out_wait(u - 2)
        for par in (0, 1):
            total = Pe[slot, par, c, :, :w].astype(F32) + Rv[m - 1][slot, par, 0, :, :w].astype(F32)
            st[two, par, :, :w] = total.astype(BF)
        for here, copies in out_copies(u, w):

            @pl.when(here)
            def _():
                for copy in copies:
                    copy.start()

    def by_width(u, body):
        @pl.when((u >= 0) & (u < wide_units))
        def _():
            body(W)

        @pl.when((u >= wide_units) & (u < units))
        def _():
            body(narrow)

    per = max(1, 256 // Lr)
    key_tile = per * Lr

    def kv_copy(d):
        return remote(
            kvs.at[lax.rem(d, kvs.shape[0])], kvr.at[d - 1], kv_send.at[d - 1], kv_recv.at[d - 1],
            along("ctx", jnp.maximum(c - d, 0)),
        )

    def block_copy(block):
        two = lax.rem(block, 2)
        return pltpu.make_async_copy(kv_ref.at[block], kvb.at[two], kvb_sem.at[two])

    def attend(two, masked, dst):
        for kh in range(KH):
            cols = slice(kh * HEAD, (kh + 1) * HEAD)

            def key_step(i, carry):
                start = pl.multiple_of(i * key_tile, key_tile)
                at = pl.ds(i * per, per)
                keys = kvb[two, at, 0, :, cols].reshape(key_tile, HEAD)
                values = kvb[two, at, 1, :, cols].reshape(key_tile, HEAD)
                key_sum = jnp.zeros((key_tile, HEAD), F32)
                value_sum = jnp.zeros((key_tile, HEAD), F32)
                for g in range(GS):
                    h = kh * GS + g
                    head = slice(h * HEAD, (h + 1) * HEAD)
                    query, delta = q_ref[:, head], hd_ref[:, head]
                    bent = jnp.tanh(dot_nt(keys, query) * (scale / CAP))
                    prob = jnp.exp(CAP * bent - logt_ref[h:h + 1, :])
                    if masked:
                        key_pos = start + lax.broadcasted_iota(jnp.int32, prob.shape, 0)
                        prob = jnp.where(key_pos <= lax.broadcasted_iota(jnp.int32, prob.shape, 1), prob, 0.0)
                    grad = prob * (dot_nt(values, delta) - rdelta[h:h + 1, :]) * (1.0 - bent * bent)
                    grad = grad.astype(BF)
                    value_sum += dot_nn(prob.astype(BF), delta)
                    key_sum += dot_nn(grad, query)
                    dq[:, head] += dot_tn(grad, keys)
                rows = pl.ds(start, key_tile)
                kvs[dst, 0, rows, cols] = (key_sum * scale).astype(BF)
                kvs[dst, 1, rows, cols] = value_sum.astype(BF)
                return carry

            lax.fori_loop(0, R // key_tile, key_step, 0)

    def attention():
        dq[...] = jnp.zeros_like(dq)
        for h in range(Hq // HEAD):
            head = slice(h * HEAD, (h + 1) * HEAD)
            product = hd_ref[:, head].astype(F32) * heads_ref[:, head].astype(F32)
            rdelta[h:h + 1] = jnp.sum(product.T, axis=0, keepdims=True)
        block_copy(0).start()

        def far(block, carry):
            d = c - block

            @pl.when(block < c)
            def _():
                slot = lax.rem(d, kvs.shape[0])
                block_copy(block).wait()
                block_copy(block + 1).start()

                @pl.when(d + kvs.shape[0] <= c)
                def _():
                    kv_copy(d + kvs.shape[0]).wait_send()

                attend(lax.rem(block, 2), False, slot)
                kv_copy(d).start()

            return carry

        lax.fori_loop(0, NC - 1, far, 0)

        @pl.when(c >= kvs.shape[0])
        def _():
            kv_copy(kvs.shape[0]).wait_send()

        block_copy(c).wait()
        attend(lax.rem(c, 2), True, 0)

    def turned(values, h):
        a, b = values[:, h * HEAD:h * HEAD + HEAD // 2], values[:, h * HEAD + HEAD // 2:(h + 1) * HEAD]
        cosine, sine = cos_ref[...], sin_ref[...]
        return jnp.concatenate([a * cosine + b * sine, b * cosine - a * sine], axis=1).astype(BF)

    def pair_remote(i, o):
        ref = [RQ, RKV][i]
        return remote(ref.at[dp], ref.at[dp], pair_sem.at[2 * o, i], pair_sem.at[2 * o + 1, i], partners[o])

    has_left, has_right = t > 0, t < T - 1

    def rs_copy(side, k, j):
        if side == 0:
            slot, peer = j, jnp.minimum(t + 1, T - 1)
        else:
            slot, peer = jnp.where(j == t - 1, T, j), jnp.maximum(t - 1, 0)
        return remote(Pb.at[j], Rb.at[slot], rs_send.at[side, k], rs_recv.at[side, k], along("tp", peer))

    def rs_block(side, k):
        return (T - 1 - k + t) if side == 0 else (k - (T - 1 - t))

    def rs_sends(side, k):
        return (t <= k) & has_right if side == 0 else (T - 1 - t <= k) & has_left

    def rs_step(k):
        for side in (0, 1):
            j = rs_block(side, k)

            @pl.when(rs_sends(side, k))
            def _():
                if k:

                    @pl.when(has_left if side == 0 else has_right)
                    def _():
                        rs_copy(side, k - 1, j).wait_recv()
                        Pb[j] = (Pb[j].astype(F32) + Rb[j].astype(F32)).astype(BF)

                rs_copy(side, k, j).start()

    def own_keys():
        for which in range(2):
            dst = []
            for kh in range(KH):
                dst.append(kvs[0, which, :, kh * HEAD:(kh + 1) * HEAD].astype(F32))
            acc[which] = jnp.concatenate(dst, axis=1) if KH > 1 else dst[0]

        def come(i, carry):
            d = i + 1

            @pl.when(c + d <= NC - 1)
            def _():
                kv_copy(d).wait_recv()
                for which in range(2):
                    acc[which] += kvr[d - 1, which].astype(F32)

            return carry

        lax.fori_loop(0, NC - 1, come, 0)
        for kh in range(KH):
            cols = slice(kh * HEAD, (kh + 1) * HEAD)
            RKV[dp, 0, :, cols] = turned(acc[0], kh)
        RKV[dp, 1] = acc[1].astype(BF)
        for h in range(Hq // HEAD):
            RQ[dp, :, h * HEAD:(h + 1) * HEAD] = turned(dq[...] * scale, h)
        for i in range(2):
            for o in range(NDP - 1):
                pair_remote(i, o).start()
        for i in range(3):
            spread_local(i).wait()
            for o in range(NDP - 1):
                spread_remote(i, o).wait_recv()
        tile = tile_of(D)

        def part(i, carry):
            at = pl.ds(pl.multiple_of(i * tile, tile), tile)
            terms = dot_nt(RQ[dp], WQ[at, :]) + dot_nt(RKV[dp, 0], WK[at, :]) + dot_nt(RKV[dp, 1], WV[at, :])
            Pb[:, :, at] = terms.astype(BF).reshape(T, Lr, tile)
            return carry

        lax.fori_loop(0, D // tile, part, 0)
        rs_step(0)

    def rs_finish():
        igrad_ref[...] = Pb[t].astype(F32)

        @pl.when(has_left)
        def _():
            rs_copy(0, T - 2, t).wait_recv()
            igrad_ref[...] += Rb[t].astype(F32)

        @pl.when(has_right)
        def _():
            rs_copy(1, T - 2, t).wait_recv()
            igrad_ref[...] += Rb[T].astype(F32)

        rows = x_ref[...].astype(F32)
        grad, terms = rms_back(rows, inverse_rms(rows), gain_ref[0:1], igrad_ref[...])
        igrad_ref[...] = mdelta_ref[...] + grad
        G[0, 0:1] = terms
        G[0, 1:4] = gsum_ref[...]

    meets = [("tp", t, b) for b in bits_below(T)] + [("ctx", c, b) for b in bits_below(NC)]
    meets += [("dp", dp, b) for b in bits_below(NDP)]

    def g_copy(k):
        axis, index, bit = meets[k]
        return remote(G.at[k], GR.at[k], g_send.at[k], g_recv.at[k], along(axis, flip(index, bit)))

    def tick(i, carry):
        def start(w):
            @pl.when(i >= NS)
            def _():
                by_width(i - NS, lambda before: e_sent(i - NS, before))

            e_product(i, w)
            e_send_step(i, 0, w)

        by_width(i, start)

        @pl.when(i == 1)
        def _():
            for w in range(3):
                spread_local(w).start()
                for o in range(NDP - 1):
                    spread_remote(w, o).start()
            attention()

        @pl.when(i == 2)
        def _():
            own_keys()

        for k in range(1, T - 1):

            @pl.when(i == 2 + k)
            def _():
                rs_step(k)

        @pl.when(i == 1 + T)
        def _():
            rs_finish()
            g_copy(0).start()

        for k in range(len(meets)):

            @pl.when(i == 2 + T + k)
            def _():
                g_copy(k).wait_recv()
                G[k + 1] = G[k] + GR[k]
                if k + 1 < len(meets):
                    g_copy(k + 1).start()

        @pl.when(i == wide_units)
        def _():
            for p in range(2):
                for o in range(NDP - 1):
                    pair_remote(p, o).wait_recv()

        for k in range(1, m):

            def middle(w):
                e_add(i - k, k - 1, w)
                e_send_step(i - k, k, w)

            by_width(i - k, middle)
        by_width(i - m, lambda w: e_finish(i - m, w))
        return carry

    lax.fori_loop(0, units + m, tick, 0)
    gains_ref[...] = G[len(meets)]

    for u in (units - 2, units - 1):
        out_wait(jnp.int32(u))
    for u in range(units - NS, units):
        by_width(jnp.int32(u), lambda w: e_sent(jnp.int32(u), w))
    for side in (0, 1):
        for k in range(T - 1):

            @pl.when(rs_sends(side, k))
            def _():
                rs_copy(side, k, rs_block(side, k)).wait_send()

    for k in range(len(meets)):
        g_copy(k).wait_send()
    for o in range(NDP - 1):
        for i in range(3):
            spread_remote(i, o).wait_send()
        for i in range(2):
            pair_remote(i, o).wait_send()

    def kv_close(i, carry):
        d = i + 1

        @pl.when((d <= c) & (d < kvs.shape[0]))
        def _():
            kv_copy(d).wait_send()

        return carry

    lax.fori_loop(0, min(NC - 1, kvs.shape[0] - 1), kv_close, 0)


def tail_call(
    layer_in, middle_delta, norm_gains, gain_sums, query, heads_delta, head_rows, log_totals, cosine, sine,
    keys_values, rows_one, w_query, w_key, w_value, rows, attn, heads, gate, up,
):
    T, NC, NDP = lax.axis_size("tp"), lax.axis_size("ctx"), lax.axis_size("dp")
    Lr, D = layer_in.shape
    R, Hq = query.shape
    KVd = w_key.shape[1]
    KH = KVd // HEAD
    Dh = D // NDP
    RB = Dh // NC
    F = gate.shape[1]
    W = tile_of(F) // 2
    m = NC.bit_length() - 1
    NS = max(4, m + 1)
    tokens = NDP * R
    kv_slots = min(NC, 4)
    meets = sum(n.bit_length() - 1 for n in (T, NC, NDP))
    any_spec = pl.BlockSpec(memory_space=pl.ANY)
    vm = pl.BlockSpec(memory_space=pltpu.VMEM)
    sds = jax.ShapeDtypeStruct
    dma = pltpu.SemaphoreType.DMA
    return pl.pallas_call(
        functools.partial(tail_kernel, T, NC, NDP, KH, NS),
        out_shape=(
            sds((Lr, D), F32), sds((4, D), F32),
            sds((RB, F), BF), sds((RB, F), BF), sds((RB, Hq), BF),
            sds((RB, Hq), BF), sds((RB, KVd), BF), sds((RB, KVd), BF),
        ),
        in_specs=[vm] * 10 + [any_spec] * 10,
        out_specs=[vm] * 2 + [any_spec] * 6,
        scratch_shapes=[
            pltpu.VMEM((3, tokens, Dh), BF), pltpu.VMEM((2, tokens, 2 * W), BF), pltpu.VMEM((tokens, Hq), BF),
            pltpu.VMEM((NDP, R, Hq), BF), pltpu.VMEM((NDP, 2, R, KVd), BF),
            pltpu.VMEM((D, Hq), BF), pltpu.VMEM((D, KVd), BF), pltpu.VMEM((D, KVd), BF),
            pltpu.VMEM((NS, 2, NC, RB, W), BF),
            *[pltpu.VMEM((NS, 2, NC >> (k + 1), RB, W), BF) for k in range(m)],
            pltpu.VMEM((2, 2, RB, W), BF), pltpu.VMEM((R, Hq), F32), pltpu.VMEM((Hq // HEAD, R), F32), pltpu.VMEM((2, T, 2, Lr, KVd), BF),
            pltpu.VMEM((kv_slots, 2, R, KVd), BF), pltpu.VMEM((NC - 1, 2, R, KVd), BF),
            pltpu.VMEM((T, Lr, D), BF), pltpu.VMEM((T + 1, Lr, D), BF), pltpu.VMEM((2, R, KVd), F32),
            pltpu.VMEM((meets + 1, 4, D), F32), pltpu.VMEM((meets, 4, D), F32),
            dma((4,)), dma((2,)), dma((2 * NDP - 1, 3)), dma((2 * (NDP - 1), 2)),
            dma((NS, 2, NC - 1)), dma((NS, 2, NC - 1)), dma((2, 2)), dma((NC - 1,)), dma((NC - 1,)),
            dma((2, T - 1)), dma((2, T - 1)), dma((meets,)), dma((meets,)), dma((2,)),
        ],
        compiler_params=pltpu.CompilerParams(
            collective_id=1, has_side_effects=True, vmem_limit_bytes=66_000_000
        ),
        name="tail",
    )(
        layer_in, middle_delta, norm_gains, gain_sums, query, heads_delta, head_rows, log_totals, cosine, sine,
        keys_values, rows_one, w_query, w_key, w_value, rows, attn, heads, gate, up,
    )


def finish_kernel(width, count, gains_ref, *refs):
    n = count
    srcs, gain_o, dsts = refs[:n], refs[n], refs[n + 1:2 * n + 1]
    held, wide, sems = refs[2 * n + 1:3 * n + 1], refs[3 * n + 1:-1], refs[-1]
    for i in range(n):
        pltpu.make_async_copy(srcs[i], held[i], sems.at[0, i]).start()
    rank = lax.axis_index("dp")
    for axis in ("ctx", "tp"):
        rank = rank * lax.axis_size(axis) + lax.axis_index(axis)
    gains = gains_ref[...]
    total = gains.shape[1]
    gain_o[...] = pltpu.roll(gains, lax.rem(total - rank * width, total), axis=1)[:4, :width]
    buffers = []
    for i in range(n):
        pltpu.make_async_copy(srcs[i], held[i], sems.at[0, i]).wait()
        buffer = held[i]
        if held[i].dtype != dsts[i].dtype:
            buffer = wide[len([b for b in buffers if b])]
            buffer[...] = held[i][...].astype(buffer.dtype)
        buffers.append(buffer is not held[i])
        pltpu.make_async_copy(buffer, dsts[i], sems.at[1, i]).start()
    used = 0
    for i in range(n):
        buffer = wide[used] if buffers[i] else held[i]
        used += buffers[i]
        pltpu.make_async_copy(buffer, dsts[i], sems.at[1, i]).wait()


def finish_call(gains, arrays, dtypes):
    width = gains.shape[1] // (lax.axis_size("tp") * lax.axis_size("ctx") * lax.axis_size("dp"))
    any_spec = pl.BlockSpec(memory_space=pl.ANY)
    vm = pl.BlockSpec(memory_space=pltpu.VMEM)
    sds = jax.ShapeDtypeStruct
    n = len(arrays)
    return pl.pallas_call(
        functools.partial(finish_kernel, width, n),
        out_shape=[sds((4, width), F32)] + [sds(a.shape, d) for a, d in zip(arrays, dtypes, strict=True)],
        in_specs=[vm] + [any_spec] * n,
        out_specs=[vm] + [any_spec] * n,
        scratch_shapes=[pltpu.VMEM(a.shape, a.dtype) for a in arrays]
        + [pltpu.VMEM(a.shape, d) for a, d in zip(arrays, dtypes, strict=True) if a.dtype != d]
        + [pltpu.SemaphoreType.DMA((2, n))],
        compiler_params=pltpu.CompilerParams(vmem_limit_bytes=66_000_000),
        name="finish",
    )(gains, *arrays)


def shards(layer_in, cotangent, norm_gains, w_query, w_key, w_value, w_out, w_gate, w_up, w_down):
    half_width = HEAD // 2
    frequency = THETA ** (-(jnp.arange(half_width, dtype=F32) * 2.0) / HEAD)
    query, head_rows, log_totals, cosine, sine, keys_values, rows_one, *weights = front_call(
        layer_in, norm_gains, frequency[None, :], w_query, w_key, w_value, w_out, w_gate, w_up, w_down
    )
    core = core_call(layer_in, cotangent, norm_gains, head_rows, w_out, w_gate, *weights)
    layer_out, middle_delta, gain_sums, heads_delta, rows, gate, up, attn, heads, down_sum = core
    input_grad, gains, *sums = tail_call(
        layer_in, middle_delta, norm_gains, gain_sums, query, heads_delta, head_rows, log_totals, cosine, sine,
        keys_values, rows_one.reshape(-1, rows_one.shape[-1]), w_query, w_key, w_value,
        rows, attn, heads, gate, up,
    )
    arrays = [layer_out, input_grad, down_sum, *sums]
    gain_grads, layer_out, input_grad, down_turned, grad_gate, grad_up, out_turned, *rest = finish_call(
        gains, arrays, [BF] + [F32] * (len(arrays) - 1)
    )
    return (layer_out, input_grad, gain_grads, *rest, out_turned.T, grad_gate, grad_up, down_turned.T)


def solution(mesh):
    return jax.shard_map(
        shards,
        mesh=mesh,
        in_specs=(
            P(("dp", "ctx", "tp"), None),
            P(("dp", "ctx", "tp"), None),
            P(),
            P("dp", "tp"),
            P("dp", "tp"),
            P("dp", "tp"),
            P("tp", "dp"),
            P("dp", "tp"),
            P("dp", "tp"),
            P("tp", "dp"),
        ),
        out_specs=(
            P(("dp", "ctx", "tp"), None),
            P(("dp", "ctx", "tp"), None),
            P(None, ("dp", "ctx", "tp")),
            P(("dp", "ctx"), "tp"),
            P(("dp", "ctx"), "tp"),
            P(("dp", "ctx"), "tp"),
            P("tp", ("dp", "ctx")),
            P(("dp", "ctx"), "tp"),
            P(("dp", "ctx"), "tp"),
            P("tp", ("dp", "ctx")),
        ),
        check_vma=False,
    )
```

```python
import functools

import jax
import jax.numpy as jnp
from jax import lax
from jax.experimental import pallas as pl
from jax.experimental.pallas import tpu as pltpu
from jax.sharding import PartitionSpec as P

HEAD = 256
EPS = 1e-06
CAP = 50.0
THETA = 10000.0
MESH = pl.DeviceIdType.MESH
BF = jnp.bfloat16
F32 = jnp.float32


def tile_of(width):
    for tile in (768, 512, 256, 128):
        if width % tile == 0:
            return tile
    return width


def inverse_rms(values):
    return lax.rsqrt(jnp.mean(values * values, axis=-1, keepdims=True) + EPS)


def rms_back(values, scale, gain, delta):
    weighted = delta * gain
    inner = jnp.mean(weighted * values, axis=-1, keepdims=True)
    grad = scale * weighted - values * (scale * scale * scale * inner)
    return grad, jnp.sum(delta * values * scale, axis=0, keepdims=True)


def dot_nt(former, latter):
    return lax.dot_general(former, latter, (((1,), (1,)), ((), ())), preferred_element_type=F32)


def dot_nn(former, latter):
    return jnp.dot(former, latter, preferred_element_type=F32)


def flip(index, bit):
    return index + bit * (1 - 2 * lax.rem(index // bit, 2))


def flips(index, mask):
    bit = 1
    while bit <= mask:
        if mask & bit:
            index = flip(index, bit)
        bit *= 2
    return index


def dot_tn(former, latter):
    return lax.dot_general(former, latter, (((0,), (0,)), ((), ())), preferred_element_type=F32)


def sub_sums(bits):
    sums = [0]
    for bit in bits:
        sums = sums + [s + bit for s in sums]
    return sums


def bits_below(count):
    return [1 << i for i in range(count.bit_length() - 1)]


def main_kernel(
    T, C, NC, NDP, KH, NP, NR,
    x_ref, ct_ref, gain_ref, heads_ref,
    wo_ref, wg_ref, wo_other, wg_other, wut_ref, wdt_ref, q_ref, logt_ref, cos_ref, sin_ref, kv_ref, rows1_ref,
    wq_ref, wk_ref, wv_ref,
    out_ref, igrad_ref, gains_ref,
    down_o, gate_o, up_o, out_o, q_o, k_o, v_o,
    rows_pair, hid_pair, branch_pair, gate_pair, up_pair, attn_pair, head_pair,
    wo_v, wd_v, X, Pb, Rb, att, mid, acc, mdelta, gsum, hdelta, Ab, Bb, L0, Rc, st, G, GR,
    w_sem, f_sem, rs_send, rs_recv, ag_send, ag_recv, pair_sem, l_sem, r_sem, e_send, e_recv, st_sem,
    s_sem, q_sem, kv_send, kv_recv, last_send, last_recv, g_send, g_recv, kvb_sem, free_sem, enter_sem,
):
    t, c, dp = lax.axis_index("tp"), lax.axis_index("ctx"), lax.axis_index("dp")
    Lr, D = x_ref.shape
    rc = Lr // C
    R, Hq = q_ref.shape
    KVd = KH * HEAD
    GS = Hq // KVd
    Dh, RB = D // NDP, D // NDP // NC
    F = wg_ref.shape[1]
    M = T * rc
    tokens = NDP * R
    W = Rc.shape[-1] // 2
    m = NC.bit_length() - 1
    NF = F // (2 * W)
    narrow = min(W, Hq // 2)
    wide_units = 3 * NF
    n_out, n_kv = Hq // (2 * narrow), KVd // narrow
    q_first, kv_first = wide_units + n_out, wide_units + 2 * n_out
    units = kv_first + n_kv
    begin = 3 * C - 1
    scale = HEAD**-0.5
    has_left, has_right = t > 0, t < T - 1
    left, right = {"tp": jnp.maximum(t - 1, 0)}, {"tp": jnp.minimum(t + 1, T - 1)}
    partners = [{"dp": lax.rem(dp + o, NDP)} for o in range(1, NDP)]
    later = [{"ctx": lax.rem(c + o, NC)} for o in range(1, NC)]
    others = [{"tp": lax.rem(t + o, T)} for o in range(1, T)] + later + partners
    ctx_meets = [{"ctx": flip(c, bit)} for bit in bits_below(NC)]

    def along(axis, index):
        return {axis: index}

    def remote(src, dst, send, recv, peer):
        return pltpu.make_async_remote_copy(src, dst, send, recv, device_id=peer, device_id_type=MESH)

    def signal_all(sem, peers):
        for peer in peers:
            pl.semaphore_signal(sem, inc=1, device_id=peer, device_id_type=MESH)

    def columns_of(ref, owner):
        return ref.at[:, pl.ds(pl.multiple_of(owner * Dh, 128), Dh)]

    owners = [p["dp"] for p in partners]
    out_loads = [pltpu.make_async_copy(wo_ref, columns_of(wo_v, dp), w_sem.at[0])] + [
        pltpu.make_async_copy(columns_of(wo_other, p), columns_of(wo_v, p), w_sem.at[1 + o])
        for o, p in enumerate(owners)
    ]
    for copy in out_loads:
        copy.start()
    entry = pltpu.get_barrier_semaphore()
    signal_all(entry, others)
    gsum[...] = jnp.zeros_like(gsum)
    pl.semaphore_wait(entry, len(others))

    def pair_copies(kind, s, src, half, dst):
        def cut(owner):
            if half:
                return src.at[..., pl.ds(pl.multiple_of(owner * Dh, 128), Dh)]
            return src

        copies = [pltpu.make_async_copy(cut(dp), dst.at[dp, s], pair_sem.at[0, kind, s])]
        for o, partner in enumerate(partners):
            copies.append(
                pltpu.make_async_remote_copy(
                    cut(partner["dp"]), dst.at[dp, s],
                    pair_sem.at[1 + 2 * o, kind, s], pair_sem.at[2 + 2 * o, kind, s],
                    device_id=partner, device_id_type=MESH,
                )
            )
        return copies

    env = {}

    def pair_of(kind, s):
        src = [
            lambda: X.at[s], lambda: env["hid"].at[s], lambda: X.at[s], lambda: Ab.at[s],
            lambda: Bb.at[s], lambda: X.at[s], lambda: heads_ref.at[:, s],
        ][kind]()
        return pair_copies(kind, s, src, kind in (0, 2, 5), pairs[kind])

    pairs = [rows_pair, hid_pair, branch_pair, gate_pair, up_pair, attn_pair, head_pair]

    def pair_start(kind, s):
        for copy in pair_of(kind, s):
            copy.start()

    def pair_kept(kind, s):
        pair_of(kind, s)[0].wait()

    def pair_away(kind, s):
        for copy in pair_of(kind, s)[1:]:
            copy.wait_send()

    def pair_received(kind, s):
        for o, partner in enumerate(partners):
            place = pairs[kind].at[dp, s]
            remote(
                place, place, pair_sem.at[1 + 2 * o, kind, s], pair_sem.at[2 + 2 * o, kind, s], partner
            ).wait_recv()

    def rs_copy(s, side, k, j):
        if side == 0:
            slot, peer = j, right
        else:
            slot, peer = jnp.where(j == t - 1, T, j), left
        return pltpu.make_async_remote_copy(
            Pb.at[s, j], Rb.at[s, slot], rs_send.at[s, side, k], rs_recv.at[s, side, k],
            device_id=peer, device_id_type=MESH,
        )

    def rs_block(side, k):
        return (T - 1 - k + t) if side == 0 else (k - (T - 1 - t))

    def rs_sends(side, k):
        return (t <= k) if side == 0 else (T - 1 - t <= k)

    def ag_copy(s, side, k, j):
        return pltpu.make_async_remote_copy(
            X.at[s, j], X.at[s, j], ag_send.at[s, side, k], ag_recv.at[s, side, k],
            device_id=right if side == 0 else left, device_id_type=MESH,
        )

    def ag_block(side, k):
        return (t - k) if side == 0 else (t + k)

    def ag_sends(side, k):
        return (t >= k) & has_right if side == 0 else (t + k <= T - 1) & has_left

    def rs_start(s):
        for side in (0, 1):

            @pl.when(rs_sends(side, 0))
            def _():
                rs_copy(s, side, 0, rs_block(side, 0)).start()

    def rs_step(s, k):
        for side in (0, 1):
            j = rs_block(side, k)
            came = has_left if side == 0 else has_right

            @pl.when(rs_sends(side, k))
            def _():
                @pl.when(came)
                def _():
                    rs_copy(s, side, k - 1, j).wait_recv()
                    Pb[s, j] = (Pb[s, j].astype(F32) + Rb[s, j].astype(F32)).astype(BF)

                rs_copy(s, side, k, j).start()

    def rs_sent(s):
        for side in (0, 1):
            for k in range(T - 1):

                @pl.when(rs_sends(side, k))
                def _():
                    rs_copy(s, side, k, rs_block(side, k)).wait_send()

    def rs_finish(s):
        acc[...] = Pb[s, t].astype(F32)

        @pl.when(has_left)
        def _():
            rs_copy(s, 0, T - 2, t).wait_recv()
            acc[...] += Rb[s, t].astype(F32)

        @pl.when(has_right)
        def _():
            rs_copy(s, 1, T - 2, t).wait_recv()
            acc[...] += Rb[s, T].astype(F32)

    def ag_start(s):
        for side in (0, 1):

            @pl.when(ag_sends(side, 0))
            def _():
                ag_copy(s, side, 0, t).start()

    def ag_step(s, k):
        for side in (0, 1):
            j = ag_block(side, k)
            there = (j >= 0) if side == 0 else (j <= T - 1)

            @pl.when(there)
            def _():
                ag_copy(s, side, k - 1, j).wait_recv()
                if k <= T - 2:

                    @pl.when(has_right if side == 0 else has_left)
                    def _():
                        ag_copy(s, side, k, j).start()

    def ag_sent(s):
        for side in (0, 1):
            for k in range(T - 1):

                @pl.when(ag_sends(side, k))
                def _():
                    ag_copy(s, side, k, ag_block(side, k)).wait_send()

    def local_rows(n, s):
        own = pl.ds(pl.multiple_of(s * rc, rc), rc)
        total = acc[...]

        @pl.when(n == 0)
        def _():
            att[s] = total
            middle = x_ref[own].astype(F32) + total * inverse_rms(total) * gain_ref[1:2]
            mid[s] = middle
            X[s, t] = (middle * inverse_rms(middle) * gain_ref[2:3]).astype(BF)

        @pl.when(n == 1)
        def _():
            scale = inverse_rms(total)
            out_ref[own] = (mid[s] + total * scale * gain_ref[3:4]).astype(BF)
            grad, terms = rms_back(total, scale, gain_ref[3:4], ct_ref[own].astype(F32))
            gsum[2:3] += terms
            X[s, t] = grad.astype(BF)

        @pl.when(n == 2)
        def _():
            middle, attention = mid[s], att[s]
            grad, terms = rms_back(middle, inverse_rms(middle), gain_ref[2:3], total)
            gsum[1:2] += terms
            middle_delta = ct_ref[own].astype(F32) + grad
            mdelta[own] = middle_delta
            grad, terms = rms_back(attention, inverse_rms(attention), gain_ref[1:2], middle_delta)
            gsum[0:1] += terms
            X[s, t] = grad.astype(BF)

    def comm(tau, w, a):
        back = tau - a

        @pl.when((back >= 0) & (back < 3 * C))
        def _():
            n, s = back // C, lax.rem(back, C)
            if w <= T - 2:
                rs_step(s, w)
            elif w == T - 1:
                rs_finish(s)
                local_rows(n, s)
                ag_start(s)
            else:
                ag_step(s, w - (T - 1))

    def tiles(width, body):
        tile = tile_of(width)

        def step(i, carry):
            body(pl.ds(pl.multiple_of(i * tile, tile), tile), tile)
            return carry

        lax.fori_loop(0, width // tile, step, 0)

    def rows_of(s):
        return X[s].reshape(M, D)

    def store_part(s, at, tile, value):
        Pb[s, :, :, at] = value.astype(BF).reshape(T, rc, tile)

    pitch = -(-RB // 16) * 16
    orders = [bits_below(NC), bits_below(NC)[::-1]]
    first_of = [sum(NC >> (i + 1) for i in range(k)) for k in range(m)]

    def block_of(i, w):
        down = D // pitch
        row = pl.multiple_of(lax.rem(i, down) * pitch, 16)
        return wd_v.at[pl.ds(row, RB), pl.ds(pl.multiple_of((i // down) * W, 128), w)]

    def part_of(u, par, owner, w):
        return block_of((lax.rem(u, NP) * 2 + par) * NC + owner, w)

    def came_of(u, par, at, w):
        return block_of(NP * 2 * NC + (lax.rem(u, NR) * 2 + par) * (NC - 1) + at, w)

    def e_copy(u, par, k, n, w):
        order = orders[par]
        at = first_of[k] + n
        return remote(
            part_of(u, par, flips(c, sub_sums(order[k + 1:])[n] + order[k]), w), came_of(u, par, at, w),
            e_send.at[lax.rem(u, NP), par, at], e_recv.at[lax.rem(u, NR), par, at],
            along("ctx", flip(c, order[k])),
        )

    def e_each(k, act):
        for par in (0, 1):
            for n in range(NC >> (k + 1)):
                act(par, n)

    def e_sent(u, w):
        for k in range(m):
            e_each(k, lambda par, n: e_copy(u, par, k, n, w).wait_send())

    def e_send_step(u, k, w):
        e_each(k, lambda par, n: e_copy(u, par, k, n, w).start())

    def e_add(u, k, w):
        def one(par, n):
            e_copy(u, par, k, n, w).wait_recv()
            if k < m - 1:
                ref = part_of(u, par, flips(c, sub_sums(orders[par][k + 1:])[n]), w)
                ref[...] = (ref[...].astype(F32) + came_of(u, par, first_of[k] + n, w)[...].astype(F32)).astype(BF)

        e_each(k, one)

    chunks = [hid_pair, gate_pair, up_pair]

    def chunk_copy(u, kind):
        at = pl.ds(pl.multiple_of((u - kind * NF) * 2 * W, 128), 2 * W)
        return pltpu.make_async_copy(chunks[kind].at[:, :, :, at], Rc, r_sem.at[0])

    def for_kind(u, act):
        for kind in range(3):

            @pl.when((u >= kind * NF) & (u < (kind + 1) * NF))
            def _():
                act(kind)

    branch_load = pltpu.make_async_copy(branch_pair, L0, l_sem.at[0])

    def store(u, par, w, first, second):
        product = dot_tn(first.reshape(tokens, Dh), second)
        for owner in range(NC):
            part_of(u, par, owner, w)[...] = product[owner * RB:(owner + 1) * RB].astype(BF)

    def wide_product(u):
        for_kind(u, lambda kind: chunk_copy(u, kind).wait())
        def each(par, carry):
            second = Rc[:, :, :, pl.ds(pl.multiple_of(par * W, 128), W)].reshape(tokens, W)

            @pl.when(u < NF)
            def _():
                store(u, par, W, L0[...], second)

            if "L" in env:

                @pl.when(u >= NF)
                def _():
                    store(u, par, W, env["L"][0], second)

            return carry

        lax.fori_loop(0, 2, each, 0)
        for_kind(u + 1, lambda kind: chunk_copy(u + 1, kind).start())

    def out_copies(u, w):
        two = lax.rem(u, 2)

        def copy(par, dst):
            return pltpu.make_async_copy(st.at[two, par, :, pl.ds(0, w)], dst, st_sem.at[two, par])

        def columns(dst, base):
            return dst.at[:, pl.ds(pl.multiple_of(base, 128), w)]

        if w == W and w != narrow:
            spans = [(0, NF, down_o), (NF, 2 * NF, gate_o), (2 * NF, 3 * NF, up_o)]
        elif w == W:
            spans = [(0, NF, down_o), (NF, 2 * NF, gate_o), (2 * NF, 3 * NF, up_o)]
            spans += [(wide_units, q_first, out_o), (q_first, kv_first, q_o)]
        else:
            spans = [(wide_units, q_first, out_o), (q_first, kv_first, q_o)]
        found = [
            (
                (u >= low) & (u < high),
                [copy(p, columns(dst, (u - low) * 2 * w + p * w)) for p in (0, 1)],
            )
            for low, high, dst in spans
        ]
        if w == narrow:
            base = (u - kv_first) * w
            found.append(((u >= kv_first) & (u < units), [copy(0, columns(k_o, base)), copy(1, columns(v_o, base))]))
        return found

    widths = [W] if W == narrow else [W, narrow]

    def out_wait(u):
        for w in widths:
            for here, copies in out_copies(u, w):

                @pl.when(here)
                def _():
                    for copy in copies:
                        copy.wait()

    def e_finish(u, w):
        e_add(u, m - 1, w)
        out_wait(u - 2)
        for par in (0, 1):
            total = part_of(u, par, c, w)[...].astype(F32) + came_of(u, par, first_of[m - 1], w)[...].astype(F32)
            st[lax.rem(u, 2), par, :, :w] = total.astype(BF)
        for here, copies in out_copies(u, w):

            @pl.when(here)
            def _():
                for copy in copies:
                    copy.start()

    def by_width(u, body):
        @pl.when((u >= 0) & (u < wide_units))
        def _():
            body(W)

        @pl.when((u >= wide_units) & (u < units))
        def _():
            body(narrow)

    def compute_open(s):
        signal_all(free_sem, ctx_meets)
        pair_kept(2, s)

        def each(i, carry):
            pair_kept(1, i)
            pair_received(1, i)
            pair_received(2, i)
            return carry

        lax.fori_loop(0, C, each, 0)
        branch_load.start()
        chunk_copy(jnp.int32(0), 0).start()

    def stages(wg_v, wu_v, hid):
        env.update(hid=hid)
        def load_copies(i):
            height, turned_height = D // (2 * T), F // (2 * T)
            part = pl.ds(pl.multiple_of(i * height, 16), height)
            turned_part = pl.ds(pl.multiple_of(i * turned_height, 16), turned_height)
            inner = pl.ds(pl.multiple_of(lax.rem(i * height, Dh), 16), height)
            return (
                pltpu.make_async_copy(wg_ref.at[inner], wg_v.at[part], f_sem.at[0, i]),
                pltpu.make_async_copy(wg_other.at[part], wg_v.at[part], f_sem.at[0, i]),
                pltpu.make_async_copy(wut_ref.at[turned_part], wu_v.at[turned_part], f_sem.at[1, i]),
                pltpu.make_async_copy(wdt_ref.at[part], wd_v.at[part], f_sem.at[2, i]),
            )

        def load_start(i):
            own, other, up_part, down_part = load_copies(i)
            here = (i * (D // (2 * T))) // Dh == dp
            pl.when(here)(own.start)
            pl.when(jnp.logical_not(here))(other.start)
            up_part.start()
            down_part.start()

        def load_wait(which):
            def each(i, carry):
                load_copies(i)[which + 1].wait()
                return carry

            lax.fori_loop(0, 2 * T, each, 0)

        def gate_up(s, at):
            gate = dot_nn(rows_of(s), wg_v[:, at])
            up = dot_nt(rows_of(s), wu_v[at, :])
            inner = jnp.tanh(0.7978845608028654 * (gate + 0.044715 * gate * gate * gate))
            half = 0.5 * (1.0 + inner)
            gelu = gate * half
            slope = half + 0.5 * gate * (1.0 - inner * inner) * (
                0.7978845608028654 * (1.0 + 0.134145 * gate * gate)
            )
            hid[s, :, at] = (gelu * up).astype(BF)
            Ab[s, :, at] = (up * slope).astype(BF)
            Bb[s, :, at] = gelu.astype(BF)

        def gate_up_delta(s, at):
            delta = dot_nn(rows_of(s), wd_v[:, at])
            Ab[s, :, at] = (delta * Ab[s, :, at].astype(F32)).astype(BF)
            Bb[s, :, at] = (delta * Bb[s, :, at].astype(F32)).astype(BF)

        def tick(tau, carry):
            n, s = tau // C, lax.rem(tau, C)

            @pl.when(n >= 1)
            def _():
                rs_sent(s)

            @pl.when(n == 0)
            def _():
                load_start(2 * tau)

            @pl.when(n == 1)
            def _():
                @pl.when(s == 0)
                def _():
                    load_wait(0)
                    load_wait(1)

                pair_start(0, s)
                tiles(F, lambda at, tile: gate_up(s, at))
                pair_start(1, s)

            @pl.when(n == 2)
            def _():
                pair_start(2, s)
                tiles(F, lambda at, tile: gate_up_delta(s, at))
                pair_start(3, s)
                pair_start(4, s)

            @pl.when(tau == begin)
            def _():
                compute_open(s)
                branch_load.wait()
                wide_product(jnp.int32(0))
                pl.semaphore_wait(free_sem, len(ctx_meets))
                e_send_step(jnp.int32(0), 0, W)

            for a in range(1, T):
                comm(tau, 2 * a - 1, a)

            @pl.when(n == 0)
            def _():
                load_start(2 * tau + 1)
                pair_start(6, s)
                heads = heads_ref[:, s].reshape(M, Hq)
                tiles(D, lambda at, tile: store_part(s, at, tile, dot_nn(heads, wo_v[:, at])))

            @pl.when(n == 1)
            def _():
                @pl.when(s == 0)
                def _():
                    load_wait(2)

                tiles(D, lambda at, tile: store_part(s, at, tile, dot_nt(hid[s], wd_v[at, :])))
                pair_kept(0, s)
                pair_away(0, s)
                ag_sent(s)

            @pl.when(n == 2)
            def _():
                tiles(
                    D,
                    lambda at, tile: store_part(
                        s, at, tile, dot_nt(Ab[s], wg_v[at, :]) + dot_nn(Bb[s], wu_v[:, at])
                    ),
                )
                pair_away(2, s)

                @pl.when(s < C - 1)
                def _():
                    pair_kept(2, s)

                ag_sent(s)

            rs_start(s)
            for a in range(1, T):
                comm(tau, 2 * a, a)
            return carry

        lax.fori_loop(0, 3 * C, tick, 0)

        def leave(s, carry):
            pair_away(1, s)
            return carry

        lax.fori_loop(0, C, leave, 0)
        del env["hid"]

    def finishing(L, Hd, RQ, RKV, WQ, WK, WV, dq, rdelta, kvb, kvs, kvr, acc2, qv, cos_v, sin_v):
        env["L"] = L
        signal_all(enter_sem, later + partners)
        rows_load = pltpu.make_async_copy(rows_pair, L.at[0], l_sem.at[1])
        attn_load = pltpu.make_async_copy(attn_pair, L.at[1], l_sem.at[2])
        rows1_load = pltpu.make_async_copy(rows1_ref, L.at[0], l_sem.at[1])
        head_load = pltpu.make_async_copy(head_pair, Hd, l_sem.at[3])
        small_loads = [
            pltpu.make_async_copy(src, dst, q_sem.at[i])
            for i, (src, dst) in enumerate([(q_ref, qv), (cos_ref, cos_v), (sin_ref, sin_v)])
        ]
        for copy in small_loads:
            copy.start()

        rows_at = pl.ds(pl.multiple_of(dp * Dh, 128), Dh)
        spread = [(wq_ref, WQ.at[rows_at]), (wk_ref, WK.at[rows_at]), (wv_ref, WV.at[rows_at])]

        def spread_local(i):
            return pltpu.make_async_copy(*spread[i], s_sem.at[0, i])

        def spread_remote(i, o):
            return remote(*spread[i], s_sem.at[1 + 2 * o, i], s_sem.at[2 + 2 * o, i], partners[o])

        def pair_remote(i, o):
            ref = [RQ, RKV][i]
            return remote(ref.at[dp], ref.at[dp], q_sem.at[3 + 4 * o + 2 * i], q_sem.at[4 + 4 * o + 2 * i], partners[o])

        def deltas_of(head):
            return hdelta[:, :, :, head].reshape(R, HEAD)

        per = max(1, 256 // Lr)
        key_tile = per * Lr

        def kv_copy(d):
            return remote(
                kvs.at[lax.rem(d, kvs.shape[0])], kvr.at[d - 1], kv_send.at[d - 1], kv_recv.at[d - 1],
                along("ctx", jnp.maximum(c - d, 0)),
            )

        def block_copy(block):
            two = lax.rem(block, 2)
            return pltpu.make_async_copy(kv_ref.at[block], kvb.at[two], kvb_sem.at[two])

        def attend(two, masked, dst):
            for kh in range(KH):
                cols = slice(kh * HEAD, (kh + 1) * HEAD)

                def key_step(i, carry):
                    start = pl.multiple_of(i * key_tile, key_tile)
                    at = pl.ds(i * per, per)
                    keys = kvb[two, at, 0, :, cols].reshape(key_tile, HEAD)
                    values = kvb[two, at, 1, :, cols].reshape(key_tile, HEAD)
                    key_sum = jnp.zeros((key_tile, HEAD), F32)
                    value_sum = jnp.zeros((key_tile, HEAD), F32)
                    for g in range(GS):
                        h = kh * GS + g
                        head = slice(h * HEAD, (h + 1) * HEAD)
                        query, delta = qv[:, head], deltas_of(head)
                        bent = jnp.tanh(dot_nt(keys, query) * (scale / CAP))
                        prob = jnp.exp(CAP * bent - logt_ref[h:h + 1, :])
                        if masked:
                            key_pos = start + lax.broadcasted_iota(jnp.int32, prob.shape, 0)
                            prob = jnp.where(key_pos <= lax.broadcasted_iota(jnp.int32, prob.shape, 1), prob, 0.0)
                        grad = prob * (dot_nt(values, delta) - rdelta[h:h + 1, :]) * (1.0 - bent * bent)
                        grad = grad.astype(BF)
                        value_sum += dot_nn(prob.astype(BF), delta)
                        key_sum += dot_nn(grad, query)
                        dq[:, head] += dot_tn(grad, keys)
                    rows = pl.ds(start, key_tile)
                    kvs[dst, 0, rows, cols] = (key_sum * scale).astype(BF)
                    kvs[dst, 1, rows, cols] = value_sum.astype(BF)
                    return carry

                lax.fori_loop(0, R // key_tile, key_step, 0)

        def attention():
            dq[...] = jnp.zeros_like(dq)
            for h in range(Hq // HEAD):
                head = slice(h * HEAD, (h + 1) * HEAD)
                product = deltas_of(head).astype(F32) * heads_ref[:, :, :, head].reshape(R, HEAD).astype(F32)
                rdelta[h:h + 1] = jnp.sum(product.T, axis=0, keepdims=True)
            block_copy(0).start()

            def far(block, carry):
                d = c - block

                @pl.when(block < c)
                def _():
                    slot = lax.rem(d, kvs.shape[0])
                    block_copy(block).wait()
                    block_copy(block + 1).start()

                    @pl.when(d + kvs.shape[0] <= c)
                    def _():
                        kv_copy(d + kvs.shape[0]).wait_send()

                    attend(lax.rem(block, 2), False, slot)
                    kv_copy(d).start()

                return carry

            lax.fori_loop(0, NC - 1, far, 0)

            @pl.when(c >= kvs.shape[0])
            def _():
                kv_copy(kvs.shape[0]).wait_send()

            block_copy(c).wait()
            attend(lax.rem(c, 2), True, 0)

        def turned(values, h):
            a, b = values[:, h * HEAD:h * HEAD + HEAD // 2], values[:, h * HEAD + HEAD // 2:(h + 1) * HEAD]
            cosine, sine = cos_v[...], sin_v[...]
            return jnp.concatenate([a * cosine + b * sine, b * cosine - a * sine], axis=1).astype(BF)

        def last_copy(side, k, j):
            if side == 0:
                slot, peer = j, right
            else:
                slot, peer = jnp.where(j == t - 1, T, j), left
            return remote(Pb.at[:, j], Rb.at[:, slot], last_send.at[side, k], last_recv.at[side, k], peer)

        def last_step(k):
            for side in (0, 1):
                j = rs_block(side, k)

                @pl.when(rs_sends(side, k))
                def _():
                    if k:

                        @pl.when(has_left if side == 0 else has_right)
                        def _():
                            last_copy(side, k - 1, j).wait_recv()
                            Pb[:, j] = (Pb[:, j].astype(F32) + Rb[:, j].astype(F32)).astype(BF)

                    last_copy(side, k, j).start()

        def own_keys():
            for which in range(2):
                dst = []
                for kh in range(KH):
                    dst.append(kvs[0, which, :, kh * HEAD:(kh + 1) * HEAD].astype(F32))
                acc2[which] = jnp.concatenate(dst, axis=1) if KH > 1 else dst[0]

            def come(i, carry):
                d = i + 1

                @pl.when(c + d <= NC - 1)
                def _():
                    kv_copy(d).wait_recv()
                    for which in range(2):
                        acc2[which] += kvr[d - 1, which].astype(F32)

                return carry

            lax.fori_loop(0, NC - 1, come, 0)
            for kh in range(KH):
                cols = slice(kh * HEAD, (kh + 1) * HEAD)
                RKV[dp, 0, :, cols] = turned(acc2[0], kh)
            RKV[dp, 1] = acc2[1].astype(BF)
            for h in range(Hq // HEAD):
                RQ[dp, :, h * HEAD:(h + 1) * HEAD] = turned(dq[...] * scale, h)
            for i in range(2):
                for o in range(NDP - 1):
                    pair_remote(i, o).start()
            for i in range(3):
                spread_local(i).wait()
                for o in range(NDP - 1):
                    spread_remote(i, o).wait_recv()
            tile = tile_of(D)

            def part(i, carry):
                at = pl.ds(pl.multiple_of(i * tile, tile), tile)
                terms = dot_nt(RQ[dp], WQ[at, :]) + dot_nt(RKV[dp, 0], WK[at, :]) + dot_nt(RKV[dp, 1], WV[at, :])
                terms = terms.astype(BF).reshape(T, C, rc, tile)
                for s in range(C):
                    Pb[s, :, :, at] = terms[:, s]
                return carry

            lax.fori_loop(0, D // tile, part, 0)
            last_step(0)

        def last_finish():
            igrad_ref[...] = Pb[:, t].reshape(Lr, D).astype(F32)

            @pl.when(has_left)
            def _():
                last_copy(0, T - 2, t).wait_recv()
                igrad_ref[...] += Rb[:, t].reshape(Lr, D).astype(F32)

            @pl.when(has_right)
            def _():
                last_copy(1, T - 2, t).wait_recv()
                igrad_ref[...] += Rb[:, T].reshape(Lr, D).astype(F32)

            rows = x_ref[...].astype(F32)
            grad, terms = rms_back(rows, inverse_rms(rows), gain_ref[0:1], igrad_ref[...])
            igrad_ref[...] = mdelta[...] + grad
            G[0, 0:1] = terms
            G[0, 1:4] = gsum[...]

        meets = [("tp", t, b) for b in bits_below(T)] + [("ctx", c, b) for b in bits_below(NC)]
        meets += [("dp", dp, b) for b in bits_below(NDP)]

        def g_copy(k):
            axis, index, bit = meets[k]
            return remote(G.at[k], GR.at[k], g_send.at[k], g_recv.at[k], along(axis, flip(index, bit)))

        def g_steps(i, half):
            for k in range(half, len(meets), 2):

                @pl.when(i == C + T + 2 + k // 2)
                def _():
                    g_copy(k).wait_recv()
                    G[k + 1] = G[k] + GR[k]
                    if k + 1 < len(meets):
                        g_copy(k + 1).start()

        def up_open():
            def each(s, carry):
                for kind in (3, 4):
                    pair_kept(kind, s)
                    pair_received(kind, s)
                pair_received(0, s)
                return carry

            lax.fori_loop(0, C, each, 0)
            rows_load.start()

        def attn_open():
            def each(s, carry):
                for kind in (5, 6):
                    pair_kept(kind, s)
                    pair_received(kind, s)
                return carry

            lax.fori_loop(0, C, each, 0)
            attn_load.start()
            head_load.start()

        def product(u, w):
            @pl.when(u < wide_units)
            def _():
                @pl.when(u == NF)
                def _():
                    rows_load.wait()

                @pl.when(u == NF - 1)
                def _():
                    up_open()

                wide_product(u)

                @pl.when(u == wide_units - 1)
                def _():
                    attn_open()

            if w == narrow:

                def columns(first, par):
                    return pl.ds(pl.multiple_of(((u - first) * 2 + par) * narrow, 128), narrow)

                @pl.when((u >= wide_units) & (u < q_first))
                def _():
                    @pl.when(u == wide_units)
                    def _():
                        attn_load.wait()
                        head_load.wait()
                        rows1_load.start()

                    def out_part(par, carry):
                        second = Hd[:, :, :, :, columns(wide_units, par)]
                        store(u, par, narrow, L[1], second.reshape(tokens, narrow))
                        return carry

                    lax.fori_loop(0, 2, out_part, 0)

                @pl.when(u == q_first)
                def _():
                    rows1_load.wait()
                    for p in range(2):
                        for o in range(NDP - 1):
                            pair_remote(p, o).wait_recv()

                @pl.when((u >= q_first) & (u < kv_first))
                def _():
                    def query_part(par, carry):
                        store(u, par, narrow, L[0], RQ[:, :, columns(q_first, par)].reshape(tokens, narrow))
                        return carry

                    lax.fori_loop(0, 2, query_part, 0)

                @pl.when(u >= kv_first)
                def _():
                    at = pl.ds(pl.multiple_of((u - kv_first) * narrow, 128), narrow)
                    def key_part(par, carry):
                        store(u, par, narrow, L[0], RKV[:, par, :, at].reshape(tokens, narrow))
                        return carry

                    lax.fori_loop(0, 2, key_part, 0)

        def tick(i, carry):
            u = i + 1

            def start(w):
                @pl.when(u >= NP)
                def _():
                    by_width(u - NP, lambda before: e_sent(u - NP, before))

                product(u, w)
                e_send_step(u, 0, w)

            by_width(u, start)
            g_steps(i, 0)

            @pl.when(i == 1)
            def _():
                pl.semaphore_wait(enter_sem, len(later + partners))
                for w in range(3):
                    spread_local(w).start()
                    for o in range(NDP - 1):
                        spread_remote(w, o).start()

            @pl.when(i < C)
            def _():
                tau = 3 * C + i
                for a in range(1, T):
                    comm(tau, 2 * a - 1, a)
                pair_start(5, i)
                hdelta[:, i] = dot_nt(rows_of(i), wo_v[...]).astype(BF).reshape(T, rc, Hq)
                rs_sent(i)
                for a in range(1, T):
                    comm(tau, 2 * a, a)

            @pl.when(i == C)
            def _():
                for copy in small_loads:
                    copy.wait()
                attention()

            @pl.when(i == C + 2)
            def _():
                own_keys()

            for k in range(1, T - 1):

                @pl.when(i == C + 2 + k)
                def _():
                    last_step(k)

            @pl.when(i == C + T + 1)
            def _():
                last_finish()
                g_copy(0).start()

            for k in range(1, m):

                def middle(w):
                    e_add(u - k, k - 1, w)
                    e_send_step(u - k, k, w)

                by_width(u - k, middle)
            by_width(u - m, lambda w: e_finish(u - m, w))
            g_steps(i, 1)
            return carry

        lax.fori_loop(0, units + m - 1, tick, 0)
        gains_ref[...] = G[len(meets)]

        for u in (units - 2, units - 1):
            out_wait(jnp.int32(u))
        for u in range(units - NP, units):
            by_width(jnp.int32(u), lambda w: e_sent(jnp.int32(u), w))
        for side in (0, 1):
            for k in range(T - 1):

                @pl.when(rs_sends(side, k))
                def _():
                    last_copy(side, k, rs_block(side, k)).wait_send()

        for k in range(len(meets)):
            g_copy(k).wait_send()
        for o in range(NDP - 1):
            for i in range(3):
                spread_remote(i, o).wait_send()
            for i in range(2):
                pair_remote(i, o).wait_send()

        def kv_close(i, carry):
            d = i + 1

            @pl.when((d <= c) & (d < kvs.shape[0]))
            def _():
                kv_copy(d).wait_send()

            return carry

        lax.fori_loop(0, min(NC - 1, kvs.shape[0] - 1), kv_close, 0)

        def close(s, carry):
            for kind in (3, 4, 5, 6):
                pair_away(kind, s)
            ag_sent(s)
            return carry

        lax.fori_loop(0, C, close, 0)

    for copy in out_loads:
        copy.wait()
    vmem = pltpu.VMEM
    pl.run_scoped(
        stages, vmem((D, F), BF), vmem((F, D), BF), vmem((C, M, F), BF)
    )
    kv_slots = min(NC, 3)
    pl.run_scoped(
        finishing,
        vmem((2, NDP, C, T, rc, Dh), BF), vmem((NDP, C, T, rc, Hq), BF),
        vmem((NDP, R, Hq), BF), vmem((NDP, 2, R, KVd), BF),
        vmem((D, Hq), BF), vmem((D, KVd), BF), vmem((D, KVd), BF),
        vmem((R, Hq), F32), vmem((Hq // HEAD, R), F32), vmem((2, T, 2, Lr, KVd), BF),
        vmem((kv_slots, 2, R, KVd), BF), vmem((NC - 1, 2, R, KVd), BF), vmem((2, R, KVd), F32),
        vmem((R, Hq), BF), vmem((R, HEAD // 2), F32), vmem((R, HEAD // 2), F32),
    )


def main_call(
    layer_in, cotangent, norm_gains, head_rows, w_out, w_gate, out_other, gate_other, up_turned, down_turned,
    query, log_totals, cosine, sine, keys_values, rows_one, w_query, w_key, w_value,
):
    T, NC, NDP = lax.axis_size("tp"), lax.axis_size("ctx"), lax.axis_size("dp")
    C = T
    Lr, D = layer_in.shape
    rc = Lr // C
    R, Hq = query.shape
    KVd = w_key.shape[1]
    Dh, RB = D // NDP, D // NDP // NC
    F = w_gate.shape[1]
    M = T * rc
    m = NC.bit_length() - 1
    NP, NR = m + 1, 4
    pitch = -(-RB // 16) * 16
    blocks = NP * 2 * NC + NR * 2 * (NC - 1)
    W = next(w for w in (tile_of(F) // 2, 256, 128) if F % (2 * w) == 0 and blocks <= (D // pitch) * (F // w))
    meets = sum(n.bit_length() - 1 for n in (T, NC, NDP))
    any_spec = pl.BlockSpec(memory_space=pl.ANY)
    vm = pl.BlockSpec(memory_space=pltpu.VMEM)
    sds = jax.ShapeDtypeStruct
    dma = pltpu.SemaphoreType.DMA
    vmem = pltpu.VMEM
    half_rows = sds((NDP, C, T, rc, Dh), BF)
    hidden_rows = sds((NDP, C, M, F), BF)
    outs = pl.pallas_call(
        functools.partial(main_kernel, T, C, NC, NDP, KVd // HEAD, NP, NR),
        out_shape=(
            sds((Lr, D), BF), sds((Lr, D), F32), sds((4, D), F32),
            sds((RB, F), BF), sds((RB, F), BF), sds((RB, F), BF), sds((RB, Hq), BF),
            sds((RB, Hq), BF), sds((RB, KVd), BF), sds((RB, KVd), BF),
            half_rows, hidden_rows, half_rows, hidden_rows, hidden_rows, half_rows, sds((NDP, C, T, rc, Hq), BF),
        ),
        in_specs=[vm] * 4 + [any_spec] * 7 + [vm] + [any_spec] * 7,
        out_specs=[vm] * 3 + [any_spec] * 14,
        scratch_shapes=[
            vmem((Hq, D), BF), vmem((D, F), BF), vmem((C, T, rc, D), BF), vmem((C, T, rc, D), BF),
            vmem((C, T + 1, rc, D), BF), vmem((C, rc, D), F32), vmem((C, rc, D), F32), vmem((rc, D), F32),
            vmem((Lr, D), F32), vmem((3, D), F32), vmem((T, C, rc, Hq), BF), vmem((C, M, F), BF), vmem((C, M, F), BF),
            vmem((NDP, C, T, rc, Dh), BF), vmem((NDP, C, M, 2 * W), BF), vmem((2, 2, RB, W), BF),
            vmem((meets + 1, 4, D), F32), vmem((meets, 4, D), F32),
            dma((NDP,)), dma((3, 2 * T)), dma((C, 2, T - 1)), dma((C, 2, T - 1)), dma((C, 2, T - 1)), dma((C, 2, T - 1)),
            dma((2 * NDP - 1, 7, C)), dma((4,)), dma((1,)), dma((NP, 2, NC - 1)), dma((NR, 2, NC - 1)), dma((2, 2)),
            dma((2 * NDP - 1, 3)), dma((3 + 4 * (NDP - 1),)), dma((NC - 1,)), dma((NC - 1,)),
            dma((2, T - 1)), dma((2, T - 1)), dma((meets,)), dma((meets,)), dma((2,)),
            pltpu.SemaphoreType.REGULAR, pltpu.SemaphoreType.REGULAR,
        ],
        compiler_params=pltpu.CompilerParams(
            collective_id=0, has_side_effects=True, vmem_limit_bytes=67_043_328
        ),
        name="main",
    )(
        layer_in, cotangent, norm_gains, head_rows.reshape(T, C, rc, Hq), w_out, w_gate, out_other, gate_other,
        up_turned, down_turned, query, log_totals, cosine, sine, keys_values,
        rows_one.reshape(NDP, C, T, rc, Dh), w_query, w_key, w_value,
    )
    return outs[:10]


def front_kernel(
    T, NC, NDP, KH, C,
    x_ref, gain_ref, freq_ref, wq_ref, wk_ref, wv_ref, wo_ref, wg_ref, wu_ref, wd_ref,
    q_o, heads_o, logt_o, cos_o, sin_o, kv_o, rows1_o, wo_o, wg_o, wut_o, wdt_o,
    X, WQ, WK, WV, KV, turned_sum, totals, up_v, upt_v, down_v, downt_v,
    w_sem, ag_send, ag_recv, pair_sem, kv_send, kv_recv, out_sem, t_sem, p_sem,
):
    t, c, dp = lax.axis_index("tp"), lax.axis_index("ctx"), lax.axis_index("dp")
    Lr, D = x_ref.shape
    R, Hq = q_o.shape
    rc = Lr // C
    KVd = KH * HEAD
    GS = Hq // KVd
    Dh = D // NDP
    scale = HEAD**-0.5
    has_left, has_right = t > 0, t < T - 1

    def remote(src, dst, send, recv, axis, index):
        return pltpu.make_async_remote_copy(
            src, dst, send, recv, device_id={axis: index}, device_id_type=MESH
        )

    partners = [lax.rem(dp + o, NDP) for o in range(1, NDP)]
    peers = [("tp", lax.rem(t + o, T)) for o in range(1, T)]
    peers += [("ctx", lax.rem(c + o, NC)) for o in range(1, NC)]
    peers += [("dp", p) for p in partners]
    sem = pltpu.get_barrier_semaphore()
    for axis, index in peers:
        pl.semaphore_signal(sem, inc=1, device_id={axis: index}, device_id_type=MESH)

    rows_at = pl.ds(pl.multiple_of(dp * Dh, 128), Dh)
    weights = [(wq_ref, WQ), (wk_ref, WK), (wv_ref, WV)]

    def weight_local(i):
        return pltpu.make_async_copy(weights[i][0], weights[i][1].at[rows_at], w_sem.at[0, i])

    def weight_remote(i, o):
        return remote(
            weights[i][0], weights[i][1].at[rows_at], w_sem.at[1 + 2 * o, i], w_sem.at[2 + 2 * o, i],
            "dp", partners[o],
        )

    turns = [
        pltpu.make_async_copy(wu_ref, up_v, t_sem.at[0]),
        pltpu.make_async_copy(wd_ref, down_v, t_sem.at[1]),
    ]
    for i in range(3):
        weight_local(i).start()
    for copy in turns:
        copy.start()
    rows = x_ref[...].astype(F32)
    X[t] = (rows * inverse_rms(rows) * gain_ref[0:1]).astype(BF)
    pl.semaphore_wait(sem, len(peers))

    def ag_copy(s, side, k, j):
        at = pl.ds(s * rc, rc)
        peer = jnp.minimum(t + 1, T - 1) if side == 0 else jnp.maximum(t - 1, 0)
        return remote(X.at[j, at], X.at[j, at], ag_send.at[s, side, k], ag_recv.at[s, side, k], "tp", peer)

    def ag_block(side, k):
        return (t - k) if side == 0 else (t + k)

    def ag_there(side, k):
        return (t >= k) if side == 0 else (t + k <= T - 1)

    def onward(side):
        return has_right if side == 0 else has_left

    for s in range(C):
        for side in (0, 1):

            @pl.when(onward(side))
            def _():
                ag_copy(s, side, 0, t).start()

    for i in range(3):
        for o in range(NDP - 1):
            weight_remote(i, o).start()

    def parts(ref, i):
        height = ref.shape[0] // T
        return pl.ds(pl.multiple_of(i * height, 16), height), height

    def part_dst(dst, ref, i, columns):
        at, height = parts(ref, i)
        if columns:
            return dst.at[at, rows_at]
        return dst.at[pl.ds(pl.multiple_of(dp * Dh + i * height, 16), height)]

    moved = [(wo_ref, wo_o, True, False), (wg_ref, wg_o, False, False)]
    moved += [(upt_v, wut_o, True, True), (downt_v, wdt_o, False, True)]

    def part_remote(w, i, o):
        src, dst, columns, _ = moved[w]
        return remote(
            src.at[parts(src, i)[0]], part_dst(dst, src, i, columns),
            p_sem.at[1 + 2 * o, w, i], p_sem.at[2 + 2 * o, w, i], "dp", partners[o],
        )

    def part_local(w, i):
        src, dst, columns, _ = moved[w]
        return pltpu.make_async_copy(src.at[parts(src, i)[0]], part_dst(dst, src, i, columns), p_sem.at[0, w, i])

    def part_start(w, i):
        for o in range(NDP - 1):
            part_remote(w, i, o).start()
        if moved[w][3]:
            part_local(w, i).start()

    def turn():
        for copy, src, dst in zip(turns, (up_v, down_v), (upt_v, downt_v), strict=True):
            copy.wait()
            height = src.shape[0] // T

            def some(i, carry):
                at = pl.ds(pl.multiple_of(i * height, 128), height)
                dst[:, at] = src[at, :].T
                return carry

            if height % 128 == 0:
                lax.fori_loop(0, T, some, 0)
            else:
                dst[...] = src[...].T

    position = (c * R + lax.broadcasted_iota(jnp.int32, (R, HEAD // 2), 0)).astype(F32)
    angles = position * freq_ref[...]
    cos_o[...] = jnp.cos(angles)
    sin_o[...] = jnp.sin(angles)
    for i in range(3):
        weight_local(i).wait()
        for o in range(NDP - 1):
            weight_remote(i, o).wait_recv()

    def kv_copy(d, j):
        return remote(
            KV.at[c, j], KV.at[c, j], kv_send.at[d - 1, j], kv_recv.at[d - 1, j],
            "ctx", jnp.minimum(c + d, NC - 1),
        )

    def kv_from(b, j):
        d = c - b
        return remote(KV.at[b, j], KV.at[b, j], kv_send.at[d - 1, j], kv_recv.at[d - 1, j], "ctx", c)

    def pair_copies(j):
        def half(owner):
            return X.at[j, :, pl.ds(pl.multiple_of(owner * Dh, 128), Dh)]

        copies = [pltpu.make_async_copy(half(dp), rows1_o.at[dp, j], pair_sem.at[0, j])]
        for o, partner in enumerate(partners):
            copies.append(
                remote(
                    half(partner), rows1_o.at[dp, j], pair_sem.at[1 + 2 * o, j], pair_sem.at[2 + 2 * o, j],
                    "dp", partner,
                )
            )
        return copies

    def turned(values, h, at):
        a, b = values[:, h * HEAD:h * HEAD + HEAD // 2], values[:, h * HEAD + HEAD // 2:(h + 1) * HEAD]
        cosine, sine = cos_o[at], sin_o[at]
        return jnp.concatenate([a * cosine - b * sine, b * cosine + a * sine], axis=1).astype(BF)

    def project(j):
        for copy in pair_copies(j):
            copy.start()
        at = pl.ds(pl.multiple_of(j * Lr, Lr), Lr)
        values = dot_nn(X[j], WK[...])
        for kh in range(KH):
            KV[c, j, 0, :, kh * HEAD:(kh + 1) * HEAD] = turned(values, kh, at)
        KV[c, j, 1] = dot_nn(X[j], WV[...]).astype(BF)

        def push(i, carry):
            @pl.when(c + 1 + i <= NC - 1)
            def _():
                kv_copy(i + 1, j).start()

            return carry

        lax.fori_loop(0, NC - 1, push, 0)
        values = dot_nn(X[j], WQ[...])
        for h in range(Hq // HEAD):
            q_o[at, h * HEAD:(h + 1) * HEAD] = turned(values, h, at)

    def gather(k, carry):
        for side in (0, 1):

            @pl.when(ag_there(side, k) & (k > 0))
            def _():
                for s in range(C):
                    ag_copy(s, side, k - 1, ag_block(side, k)).wait_recv()

                    @pl.when(onward(side) & (k <= T - 2))
                    def _():
                        ag_copy(s, side, k, ag_block(side, k)).start()

        for side in (0, 1):

            @pl.when(ag_there(side, k) & ((k > 0) | (side == 0)))
            def _():
                project(ag_block(side, k))

        part_start(0, k)
        part_start(1, k)

        @pl.when(k == 0)
        def _():
            turn()

        part_start(2, k)
        part_start(3, k)
        return carry

    lax.fori_loop(0, T, gather, 0)

    per = max(1, 256 // Lr)
    tile = per * Lr
    turned_sum[...] = jnp.zeros_like(turned_sum)
    totals[...] = jnp.zeros_like(totals)

    def out_copy(b):
        return pltpu.make_async_copy(KV.at[b], kv_o.at[b], out_sem.at[b])

    def key_step(b, p, masked):
        for kh in range(KH):
            cols = slice(kh * HEAD, (kh + 1) * HEAD)
            keys = KV[b, pl.ds(p * per, per), 0, :, cols].reshape(tile, HEAD)
            values = KV[b, pl.ds(p * per, per), 1, :, cols].reshape(tile, HEAD)
            for g in range(GS):
                h = kh * GS + g
                scores = dot_nt(keys, q_o[:, h * HEAD:(h + 1) * HEAD])
                weights = jnp.exp(CAP * jnp.tanh(scores * (scale / CAP)))
                if masked:
                    key_pos = p * tile + lax.broadcasted_iota(jnp.int32, weights.shape, 0)
                    allowed = key_pos <= lax.broadcasted_iota(jnp.int32, weights.shape, 1)
                    weights = jnp.where(allowed, weights, 0.0)
                totals[h:h + 1] += jnp.sum(weights, axis=0, keepdims=True)
                turned_sum[h] += dot_tn(values, weights.astype(BF))

    def own_step(p, carry):
        key_step(c, p, True)
        return carry

    out_copy(c).start()
    lax.fori_loop(0, T // per, own_step, 0)

    def far_block(i, carry):
        @pl.when(i < c)
        def _():
            b = c - 1 - i
            for j in range(T):
                kv_from(b, j).wait_recv()
            out_copy(b).start()

            def far_step(p, carry):
                key_step(b, p, False)
                return carry

            lax.fori_loop(0, T // per, far_step, 0)

        return carry

    lax.fori_loop(0, NC - 1, far_block, 0)
    for h in range(Hq // HEAD):
        heads_o[:, h * HEAD:(h + 1) * HEAD] = (turned_sum[h] / totals[h:h + 1]).T.astype(BF)
    logt_o[...] = jnp.log(totals[...])

    for i in range(3):
        for o in range(NDP - 1):
            weight_remote(i, o).wait_send()

    def close_parts(i, carry):
        for w in range(4):
            for o in range(NDP - 1):
                part_remote(w, i, o).wait()
            if moved[w][3]:
                part_local(w, i).wait()
        return carry

    lax.fori_loop(0, T, close_parts, 0)
    for s in range(C):
        for side in (0, 1):
            for k in range(T - 1):

                @pl.when(ag_there(side, k) & onward(side))
                def _():
                    ag_copy(s, side, k, ag_block(side, k)).wait_send()

    for j in range(T):
        copies = pair_copies(j)
        copies[0].wait()
        for copy in copies[1:]:
            copy.wait()

    def close(i, carry):
        @pl.when(c + 1 + i <= NC - 1)
        def _():
            for j in range(T):
                kv_copy(i + 1, j).wait_send()

        return carry

    lax.fori_loop(0, NC - 1, close, 0)

    def close_out(b, carry):
        @pl.when(b <= c)
        def _():
            out_copy(b).wait()

        return carry

    lax.fori_loop(0, NC, close_out, 0)


def front_call(layer_in, norm_gains, frequency, w_query, w_key, w_value, w_out, w_gate, w_up, w_down):
    T, NC, NDP = lax.axis_size("tp"), lax.axis_size("ctx"), lax.axis_size("dp")
    C = T
    Lr, D = layer_in.shape
    R = T * Lr
    Hq, KVd = w_query.shape[1], w_key.shape[1]
    Dh = D // NDP
    F = w_gate.shape[1]
    H = Hq // HEAD
    any_spec = pl.BlockSpec(memory_space=pl.ANY)
    vm = pl.BlockSpec(memory_space=pltpu.VMEM)
    sds = jax.ShapeDtypeStruct
    dma = pltpu.SemaphoreType.DMA
    return pl.pallas_call(
        functools.partial(front_kernel, T, NC, NDP, KVd // HEAD, C),
        out_shape=(
            sds((R, Hq), BF), sds((R, Hq), BF), sds((H, R), F32),
            sds((R, HEAD // 2), F32), sds((R, HEAD // 2), F32),
            sds((NC, T, 2, Lr, KVd), BF), sds((NDP, T, Lr, Dh), BF),
            sds((Hq, D), BF), sds((D, F), BF), sds((F, D), BF), sds((D, F), BF),
        ),
        in_specs=[vm] * 3 + [any_spec] * 7,
        out_specs=[vm] * 5 + [any_spec] * 6,
        scratch_shapes=[
            pltpu.VMEM((T, Lr, D), BF), pltpu.VMEM((D, Hq), BF), pltpu.VMEM((D, KVd), BF), pltpu.VMEM((D, KVd), BF),
            pltpu.VMEM((NC, T, 2, Lr, KVd), BF), pltpu.VMEM((H, HEAD, R), F32), pltpu.VMEM((H, R), F32),
            pltpu.VMEM((Dh, F), BF), pltpu.VMEM((F, Dh), BF), pltpu.VMEM((F, Dh), BF), pltpu.VMEM((Dh, F), BF),
            dma((2 * NDP - 1, 3)), dma((C, 2, T - 1)), dma((C, 2, T - 1)), dma((2 * NDP - 1, T)),
            dma((NC - 1, T)), dma((NC - 1, T)), dma((NC,)), dma((2,)), dma((2 * NDP - 1, 4, T)),
        ],
        compiler_params=pltpu.CompilerParams(
            collective_id=2, has_side_effects=True, vmem_limit_bytes=66_000_000
        ),
        name="front",
    )(layer_in, norm_gains, frequency, w_query, w_key, w_value, w_out, w_gate, w_up, w_down)


def finish_kernel(width, count, gains_ref, *refs):
    n = count
    srcs, gain_o, dsts = refs[:n], refs[n], refs[n + 1:2 * n + 1]
    held, wide, sems = refs[2 * n + 1:3 * n + 1], refs[3 * n + 1:-1], refs[-1]
    for i in range(n):
        pltpu.make_async_copy(srcs[i], held[i], sems.at[0, i]).start()
    rank = lax.axis_index("dp")
    for axis in ("ctx", "tp"):
        rank = rank * lax.axis_size(axis) + lax.axis_index(axis)
    gains = gains_ref[...]
    total = gains.shape[1]
    gain_o[...] = pltpu.roll(gains, lax.rem(total - rank * width, total), axis=1)[:4, :width]
    buffers = []
    for i in range(n):
        pltpu.make_async_copy(srcs[i], held[i], sems.at[0, i]).wait()
        buffer = held[i]
        if held[i].dtype != dsts[i].dtype:
            buffer = wide[len([b for b in buffers if b])]
            buffer[...] = held[i][...].astype(buffer.dtype)
        buffers.append(buffer is not held[i])
        pltpu.make_async_copy(buffer, dsts[i], sems.at[1, i]).start()
    used = 0
    for i in range(n):
        buffer = wide[used] if buffers[i] else held[i]
        used += buffers[i]
        pltpu.make_async_copy(buffer, dsts[i], sems.at[1, i]).wait()


def finish_call(gains, arrays, dtypes):
    width = gains.shape[1] // (lax.axis_size("tp") * lax.axis_size("ctx") * lax.axis_size("dp"))
    any_spec = pl.BlockSpec(memory_space=pl.ANY)
    vm = pl.BlockSpec(memory_space=pltpu.VMEM)
    sds = jax.ShapeDtypeStruct
    n = len(arrays)
    return pl.pallas_call(
        functools.partial(finish_kernel, width, n),
        out_shape=[sds((4, width), F32)] + [sds(a.shape, d) for a, d in zip(arrays, dtypes, strict=True)],
        in_specs=[vm] + [any_spec] * n,
        out_specs=[vm] + [any_spec] * n,
        scratch_shapes=[pltpu.VMEM(a.shape, a.dtype) for a in arrays]
        + [pltpu.VMEM(a.shape, d) for a, d in zip(arrays, dtypes, strict=True) if a.dtype != d]
        + [pltpu.SemaphoreType.DMA((2, n))],
        compiler_params=pltpu.CompilerParams(vmem_limit_bytes=66_000_000),
        name="finish",
    )(gains, *arrays)


def shards(layer_in, cotangent, norm_gains, w_query, w_key, w_value, w_out, w_gate, w_up, w_down):
    half_width = HEAD // 2
    frequency = THETA ** (-(jnp.arange(half_width, dtype=F32) * 2.0) / HEAD)
    query, head_rows, log_totals, cosine, sine, keys_values, rows_one, *weights = front_call(
        layer_in, norm_gains, frequency[None, :], w_query, w_key, w_value, w_out, w_gate, w_up, w_down
    )
    layer_out, input_grad, gains, down_sum, *sums = main_call(
        layer_in, cotangent, norm_gains, head_rows, w_out, w_gate, *weights,
        query, log_totals, cosine, sine, keys_values, rows_one, w_query, w_key, w_value,
    )
    arrays = [layer_out, input_grad, down_sum, *sums]
    gain_grads, layer_out, input_grad, down_turned, grad_gate, grad_up, out_turned, *rest = finish_call(
        gains, arrays, [BF] + [F32] * (len(arrays) - 1)
    )
    return (layer_out, input_grad, gain_grads, *rest, out_turned.T, grad_gate, grad_up, down_turned.T)


def solution(mesh):
    return jax.shard_map(
        shards,
        mesh=mesh,
        in_specs=(
            P(("dp", "ctx", "tp"), None),
            P(("dp", "ctx", "tp"), None),
            P(),
            P("dp", "tp"),
            P("dp", "tp"),
            P("dp", "tp"),
            P("tp", "dp"),
            P("dp", "tp"),
            P("dp", "tp"),
            P("tp", "dp"),
        ),
        out_specs=(
            P(("dp", "ctx", "tp"), None),
            P(("dp", "ctx", "tp"), None),
            P(None, ("dp", "ctx", "tp")),
            P(("dp", "ctx"), "tp"),
            P(("dp", "ctx"), "tp"),
            P(("dp", "ctx"), "tp"),
            P("tp", ("dp", "ctx")),
            P(("dp", "ctx"), "tp"),
            P(("dp", "ctx"), "tp"),
            P("tp", ("dp", "ctx")),
        ),
        check_vma=False,
    )
```

```python
import functools

import jax
import jax.numpy as jnp
from jax import lax
from jax.experimental import pallas as pl
from jax.experimental.pallas import tpu as pltpu
from jax.sharding import PartitionSpec as P

HEAD = 256
EPS = 1e-06
CAP = 50.0
THETA = 10000.0
MESH = pl.DeviceIdType.MESH
BF = jnp.bfloat16
F32 = jnp.float32


def tile_of(width):
    for tile in (768, 512, 256, 128):
        if width % tile == 0:
            return tile
    return width


def inverse_rms(values):
    return lax.rsqrt(jnp.mean(values * values, axis=-1, keepdims=True) + EPS)


def rms_back(values, scale, gain, delta):
    weighted = delta * gain
    inner = jnp.mean(weighted * values, axis=-1, keepdims=True)
    grad = scale * weighted - values * (scale * scale * scale * inner)
    return grad, jnp.sum(delta * values * scale, axis=0, keepdims=True)


def dot_nt(former, latter):
    return lax.dot_general(former, latter, (((1,), (1,)), ((), ())), preferred_element_type=F32)


def dot_nn(former, latter):
    return jnp.dot(former, latter, preferred_element_type=F32)


def flip(index, bit):
    return index + bit * (1 - 2 * lax.rem(index // bit, 2))


def flips(index, mask):
    bit = 1
    while bit <= mask:
        if mask & bit:
            index = flip(index, bit)
        bit *= 2
    return index


def dot_tn(former, latter):
    return lax.dot_general(former, latter, (((0,), (0,)), ((), ())), preferred_element_type=F32)


def sub_sums(bits):
    sums = [0]
    for bit in bits:
        sums = sums + [s + bit for s in sums]
    return sums


def bits_below(count):
    return [1 << i for i in range(count.bit_length() - 1)]


def main_kernel(
    T, C, NC, NDP, KH, NP, NR,
    x_ref, ct_ref, gain_ref, heads_ref,
    wo_ref, wg_ref, wo_other, wg_other, wut_ref, wdt_ref, q_ref, logt_ref, cos_ref, sin_ref, kv_ref, rows1_ref,
    wq_ref, wk_ref, wv_ref,
    out_o, igrad_o, gains_ref,
    down_o, gate_o, up_o, wout_o, q_o, k_o, v_o,
    rows_pair, hid_pair, branch_pair, gate_pair, up_pair, attn_pair, head_pair,
    out_ref, igrad_ref, wo_v, wd_v, X, Pb, Rb, att, mid, acc, mdelta, gsum, hdelta, Ab, Bb, L0, Rc, st, G, GR,
    w_sem, f_sem, b_sem, rs_send, rs_recv, ag_send, ag_recv, pair_sem, l_sem, r_sem, e_send, e_recv, st_sem,
    s_sem, q_sem, kv_send, kv_recv, last_send, last_recv, g_send, g_recv, kvb_sem, free_sem, enter_sem,
):
    t, c, dp = lax.axis_index("tp"), lax.axis_index("ctx"), lax.axis_index("dp")
    Lr, D = x_ref.shape
    rc = Lr // C
    R, Hq = q_ref.shape
    KVd = KH * HEAD
    GS = Hq // KVd
    Dh, RB = D // NDP, D // NDP // NC
    F = wg_ref.shape[1]
    M = T * rc
    tokens = NDP * R
    W = Rc.shape[-1] // 2
    m = NC.bit_length() - 1
    NF = F // (2 * W)
    narrow = min(W, Hq // 2)
    wide_units = 3 * NF
    n_out, n_kv = Hq // (2 * narrow), KVd // narrow
    q_first, kv_first = wide_units + n_out, wide_units + 2 * n_out
    units = kv_first + n_kv
    begin = 3 * C - 1
    scale = HEAD**-0.5
    has_left, has_right = t > 0, t < T - 1
    left, right = {"tp": jnp.maximum(t - 1, 0)}, {"tp": jnp.minimum(t + 1, T - 1)}
    partners = [{"dp": lax.rem(dp + o, NDP)} for o in range(1, NDP)]
    later = [{"ctx": lax.rem(c + o, NC)} for o in range(1, NC)]
    others = [{"tp": lax.rem(t + o, T)} for o in range(1, T)] + later + partners
    ctx_meets = [{"ctx": flip(c, bit)} for bit in bits_below(NC)]

    def along(axis, index):
        return {axis: index}

    def remote(src, dst, send, recv, peer):
        return pltpu.make_async_remote_copy(src, dst, send, recv, device_id=peer, device_id_type=MESH)

    def signal_all(sem, peers):
        for peer in peers:
            pl.semaphore_signal(sem, inc=1, device_id=peer, device_id_type=MESH)

    def columns_of(ref, owner):
        return ref.at[:, pl.ds(pl.multiple_of(owner * Dh, 128), Dh)]

    owners = [p["dp"] for p in partners]
    out_loads = [pltpu.make_async_copy(wo_ref, columns_of(wo_v, dp), w_sem.at[0])] + [
        pltpu.make_async_copy(columns_of(wo_other, p), columns_of(wo_v, p), w_sem.at[1 + o])
        for o, p in enumerate(owners)
    ]
    for copy in out_loads:
        copy.start()
    entry = pltpu.get_barrier_semaphore()
    signal_all(entry, others)
    gsum[...] = jnp.zeros_like(gsum)
    pl.semaphore_wait(entry, len(others))

    def pair_copies(kind, s, src, half, dst):
        def cut(owner):
            if half:
                return src.at[..., pl.ds(pl.multiple_of(owner * Dh, 128), Dh)]
            return src

        copies = [pltpu.make_async_copy(cut(dp), dst.at[dp, s], pair_sem.at[0, kind, s])]
        for o, partner in enumerate(partners):
            copies.append(
                pltpu.make_async_remote_copy(
                    cut(partner["dp"]), dst.at[dp, s],
                    pair_sem.at[1 + 2 * o, kind, s], pair_sem.at[2 + 2 * o, kind, s],
                    device_id=partner, device_id_type=MESH,
                )
            )
        return copies

    env = {}

    def pair_of(kind, s):
        src = [
            lambda: X.at[s], lambda: env["hid"].at[s], lambda: X.at[s], lambda: Ab.at[s],
            lambda: Bb.at[s], lambda: X.at[s], lambda: heads_ref.at[:, s],
        ][kind]()
        return pair_copies(kind, s, src, kind in (0, 2, 5), pairs[kind])

    pairs = [rows_pair, hid_pair, branch_pair, gate_pair, up_pair, attn_pair, head_pair]

    def pair_start(kind, s):
        for copy in pair_of(kind, s):
            copy.start()

    def pair_kept(kind, s):
        pair_of(kind, s)[0].wait()

    def pair_away(kind, s):
        for copy in pair_of(kind, s)[1:]:
            copy.wait_send()

    def pair_received(kind, s):
        for o, partner in enumerate(partners):
            place = pairs[kind].at[dp, s]
            remote(
                place, place, pair_sem.at[1 + 2 * o, kind, s], pair_sem.at[2 + 2 * o, kind, s], partner
            ).wait_recv()

    def rs_copy(s, side, k, j):
        if side == 0:
            slot, peer = j, right
        else:
            slot, peer = jnp.where(j == t - 1, T, j), left
        return pltpu.make_async_remote_copy(
            Pb.at[s, j], Rb.at[s, slot], rs_send.at[s, side, k], rs_recv.at[s, side, k],
            device_id=peer, device_id_type=MESH,
        )

    def rs_block(side, k):
        return (T - 1 - k + t) if side == 0 else (k - (T - 1 - t))

    def rs_sends(side, k):
        return (t <= k) if side == 0 else (T - 1 - t <= k)

    def ag_copy(s, side, k, j):
        return pltpu.make_async_remote_copy(
            X.at[s, j], X.at[s, j], ag_send.at[s, side, k], ag_recv.at[s, side, k],
            device_id=right if side == 0 else left, device_id_type=MESH,
        )

    def ag_block(side, k):
        return (t - k) if side == 0 else (t + k)

    def ag_sends(side, k):
        return (t >= k) & has_right if side == 0 else (t + k <= T - 1) & has_left

    def rs_start(s):
        for side in (0, 1):

            @pl.when(rs_sends(side, 0))
            def _():
                rs_copy(s, side, 0, rs_block(side, 0)).start()

    def rs_step(s, k):
        for side in (0, 1):
            j = rs_block(side, k)
            came = has_left if side == 0 else has_right

            @pl.when(rs_sends(side, k))
            def _():
                @pl.when(came)
                def _():
                    rs_copy(s, side, k - 1, j).wait_recv()
                    Pb[s, j] = (Pb[s, j].astype(F32) + Rb[s, j].astype(F32)).astype(BF)

                rs_copy(s, side, k, j).start()

    def rs_sent(s):
        for side in (0, 1):
            for k in range(T - 1):

                @pl.when(rs_sends(side, k))
                def _():
                    rs_copy(s, side, k, rs_block(side, k)).wait_send()

    def rs_finish(s):
        acc[...] = Pb[s, t].astype(F32)

        @pl.when(has_left)
        def _():
            rs_copy(s, 0, T - 2, t).wait_recv()
            acc[...] += Rb[s, t].astype(F32)

        @pl.when(has_right)
        def _():
            rs_copy(s, 1, T - 2, t).wait_recv()
            acc[...] += Rb[s, T].astype(F32)

    def ag_start(s):
        for side in (0, 1):

            @pl.when(ag_sends(side, 0))
            def _():
                ag_copy(s, side, 0, t).start()

    def ag_step(s, k):
        for side in (0, 1):
            j = ag_block(side, k)
            there = (j >= 0) if side == 0 else (j <= T - 1)

            @pl.when(there)
            def _():
                ag_copy(s, side, k - 1, j).wait_recv()
                if k <= T - 2:

                    @pl.when(has_right if side == 0 else has_left)
                    def _():
                        ag_copy(s, side, k, j).start()

    def ag_sent(s):
        for side in (0, 1):
            for k in range(T - 1):

                @pl.when(ag_sends(side, k))
                def _():
                    ag_copy(s, side, k, ag_block(side, k)).wait_send()

    def local_rows(n, s):
        own = pl.ds(pl.multiple_of(s * rc, rc), rc)
        total = acc[...]

        @pl.when(n == 0)
        def _():
            att[s] = total
            middle = x_ref[own].astype(F32) + total * inverse_rms(total) * gain_ref[1:2]
            mid[s] = middle
            X[s, t] = (middle * inverse_rms(middle) * gain_ref[2:3]).astype(BF)

        @pl.when(n == 1)
        def _():
            scale = inverse_rms(total)
            out_ref[own] = (mid[s] + total * scale * gain_ref[3:4]).astype(BF)
            grad, terms = rms_back(total, scale, gain_ref[3:4], ct_ref[own].astype(F32))
            gsum[2:3] += terms
            X[s, t] = grad.astype(BF)

        @pl.when(n == 2)
        def _():
            middle, attention = mid[s], att[s]
            grad, terms = rms_back(middle, inverse_rms(middle), gain_ref[2:3], total)
            gsum[1:2] += terms
            middle_delta = ct_ref[own].astype(F32) + grad
            mdelta[own] = middle_delta
            grad, terms = rms_back(attention, inverse_rms(attention), gain_ref[1:2], middle_delta)
            gsum[0:1] += terms
            X[s, t] = grad.astype(BF)

    def comm(tau, w, a):
        back = tau - a

        @pl.when(((back >= 0) & (back < 2 * C)) | ((back >= begin) & (back < begin + C)))
        def _():
            n = jnp.where(back < 2 * C, back // C, 2)
            s = jnp.where(back < 2 * C, lax.rem(back, C), back - begin)
            if w <= T - 2:
                rs_step(s, w)
            elif w == T - 1:
                rs_finish(s)
                local_rows(n, s)
                ag_start(s)
            else:
                ag_step(s, w - (T - 1))

    def tiles(width, body):
        tile = tile_of(width)

        def step(i, carry):
            body(pl.ds(pl.multiple_of(i * tile, tile), tile), tile)
            return carry

        lax.fori_loop(0, width // tile, step, 0)

    def rows_of(s):
        return X[s].reshape(M, D)

    def store_part(s, at, tile, value):
        Pb[s, :, :, at] = value.astype(BF).reshape(T, rc, tile)

    pitch = -(-RB // 16) * 16
    orders = [bits_below(NC), bits_below(NC)[::-1]]
    first_of = [sum(NC >> (i + 1) for i in range(k)) for k in range(m)]

    def block_of(i, w):
        down = D // pitch
        row = pl.multiple_of(lax.rem(i, down) * pitch, 16)
        return wd_v.at[pl.ds(row, RB), pl.ds(pl.multiple_of((i // down) * W, 128), w)]

    def part_of(u, par, owner, w):
        return block_of((lax.rem(u, NP) * 2 + par) * NC + owner, w)

    def came_of(u, par, at, w):
        return block_of(NP * 2 * NC + (lax.rem(u, NR) * 2 + par) * (NC - 1) + at, w)

    def e_copy(u, par, k, n, w):
        order = orders[par]
        at = first_of[k] + n
        return remote(
            part_of(u, par, flips(c, sub_sums(order[k + 1:])[n] + order[k]), w), came_of(u, par, at, w),
            e_send.at[lax.rem(u, NP), par, at], e_recv.at[lax.rem(u, NR), par, at],
            along("ctx", flip(c, order[k])),
        )

    def e_each(k, act):
        for par in (0, 1):
            for n in range(NC >> (k + 1)):
                act(par, n)

    def e_sent(u, w):
        for k in range(m):
            e_each(k, lambda par, n: e_copy(u, par, k, n, w).wait_send())

    def e_send_step(u, k, w):
        e_each(k, lambda par, n: e_copy(u, par, k, n, w).start())

    def e_add(u, k, w):
        def one(par, n):
            e_copy(u, par, k, n, w).wait_recv()
            if k < m - 1:
                ref = part_of(u, par, flips(c, sub_sums(orders[par][k + 1:])[n]), w)
                ref[...] = (ref[...].astype(F32) + came_of(u, par, first_of[k] + n, w)[...].astype(F32)).astype(BF)

        e_each(k, one)

    chunks = [hid_pair, gate_pair, up_pair]

    def chunk_copy(u, kind):
        at = pl.ds(pl.multiple_of((u - kind * NF) * 2 * W, 128), 2 * W)
        return pltpu.make_async_copy(chunks[kind].at[:, :, :, at], Rc, r_sem.at[0])

    def for_kind(u, act):
        for kind in range(3):

            @pl.when((u >= kind * NF) & (u < (kind + 1) * NF))
            def _():
                act(kind)

    def branch_load(s):
        return pltpu.make_async_copy(branch_pair.at[:, s], L0.at[:, s], b_sem.at[s])

    def store(u, par, w, first, second):
        product = dot_tn(first.reshape(tokens, Dh), second)
        for owner in range(NC):
            part_of(u, par, owner, w)[...] = product[owner * RB:(owner + 1) * RB].astype(BF)

    def wide_product(u):
        for_kind(u, lambda kind: chunk_copy(u, kind).wait())
        def each(par, carry):
            second = Rc[:, :, :, pl.ds(pl.multiple_of(par * W, 128), W)].reshape(tokens, W)

            @pl.when(u < NF)
            def _():
                store(u, par, W, L0[...], second)

            if "L" in env:

                @pl.when(u >= NF)
                def _():
                    store(u, par, W, env["L"][0], second)

            return carry

        lax.fori_loop(0, 2, each, 0)
        for_kind(u + 1, lambda kind: chunk_copy(u + 1, kind).start())

    def out_copies(u, w):
        two = lax.rem(u, 2)

        def copy(par, dst):
            return pltpu.make_async_copy(st.at[two, par, :, pl.ds(0, w)], dst, st_sem.at[two, par])

        def columns(dst, base):
            return dst.at[:, pl.ds(pl.multiple_of(base, 128), w)]

        if w == W and w != narrow:
            spans = [(0, NF, down_o), (NF, 2 * NF, gate_o), (2 * NF, 3 * NF, up_o)]
        elif w == W:
            spans = [(0, NF, down_o), (NF, 2 * NF, gate_o), (2 * NF, 3 * NF, up_o)]
            spans += [(wide_units, q_first, wout_o), (q_first, kv_first, q_o)]
        else:
            spans = [(wide_units, q_first, wout_o), (q_first, kv_first, q_o)]
        found = [
            (
                (u >= low) & (u < high),
                [copy(p, columns(dst, (u - low) * 2 * w + p * w)) for p in (0, 1)],
            )
            for low, high, dst in spans
        ]
        if w == narrow:
            base = (u - kv_first) * w
            found.append(((u >= kv_first) & (u < units), [copy(0, columns(k_o, base)), copy(1, columns(v_o, base))]))
        return found

    widths = [W] if W == narrow else [W, narrow]

    def out_wait(u):
        for w in widths:
            for here, copies in out_copies(u, w):

                @pl.when(here)
                def _():
                    for copy in copies:
                        copy.wait()

    def e_finish(u, w):
        e_add(u, m - 1, w)
        out_wait(u - 2)
        for par in (0, 1):
            total = part_of(u, par, c, w)[...].astype(F32) + came_of(u, par, first_of[m - 1], w)[...].astype(F32)
            st[lax.rem(u, 2), par, :, :w] = total.astype(BF)
        for here, copies in out_copies(u, w):

            @pl.when(here)
            def _():
                for copy in copies:
                    copy.start()

    def by_width(u, body):
        @pl.when((u >= 0) & (u < wide_units))
        def _():
            body(W)

        @pl.when((u >= wide_units) & (u < units))
        def _():
            body(narrow)

    def compute_open(s):
        signal_all(free_sem, ctx_meets)

        def each(i, carry):
            branch_load(i).wait()
            return carry

        lax.fori_loop(0, C, each, 0)

    def stages(wg_v, wu_v, hid):
        env.update(hid=hid)
        def load_copies(i):
            height, turned_height = D // (2 * T), F // (2 * T)
            part = pl.ds(pl.multiple_of(i * height, 16), height)
            turned_part = pl.ds(pl.multiple_of(i * turned_height, 16), turned_height)
            inner = pl.ds(pl.multiple_of(lax.rem(i * height, Dh), 16), height)
            return (
                pltpu.make_async_copy(wg_ref.at[inner], wg_v.at[part], f_sem.at[0, i]),
                pltpu.make_async_copy(wg_other.at[part], wg_v.at[part], f_sem.at[0, i]),
                pltpu.make_async_copy(wut_ref.at[turned_part], wu_v.at[turned_part], f_sem.at[1, i]),
                pltpu.make_async_copy(wdt_ref.at[part], wd_v.at[part], f_sem.at[2, i]),
            )

        def load_start(i):
            own, other, up_part, down_part = load_copies(i)
            here = (i * (D // (2 * T))) // Dh == dp
            pl.when(here)(own.start)
            pl.when(jnp.logical_not(here))(other.start)
            up_part.start()
            down_part.start()

        def load_wait(which):
            def each(i, carry):
                load_copies(i)[which + 1].wait()
                return carry

            lax.fori_loop(0, 2 * T, each, 0)

        def gate_up(s, at):
            gate = dot_nn(rows_of(s), wg_v[:, at])
            up = dot_nt(rows_of(s), wu_v[at, :])
            inner = jnp.tanh(0.7978845608028654 * (gate + 0.044715 * gate * gate * gate))
            half = 0.5 * (1.0 + inner)
            gelu = gate * half
            slope = half + 0.5 * gate * (1.0 - inner * inner) * (
                0.7978845608028654 * (1.0 + 0.134145 * gate * gate)
            )
            hid[s, :, at] = (gelu * up).astype(BF)
            Ab[s, :, at] = (up * slope).astype(BF)
            Bb[s, :, at] = gelu.astype(BF)

        def gate_up_delta(s, at):
            delta = dot_nn(rows_of(s), wd_v[:, at])
            Ab[s, :, at] = (delta * Ab[s, :, at].astype(F32)).astype(BF)
            Bb[s, :, at] = (delta * Bb[s, :, at].astype(F32)).astype(BF)

        def tick(tau, carry):
            n, s = tau // C, lax.rem(tau, C)

            @pl.when(n >= 1)
            def _():
                rs_sent(s)

            @pl.when(n == 0)
            def _():
                load_start(2 * tau)

            @pl.when(n == 1)
            def _():
                @pl.when(s == 0)
                def _():
                    load_wait(0)
                    load_wait(1)

                pair_start(0, s)
                tiles(F, lambda at, tile: gate_up(s, at))
                pair_start(1, s)

            @pl.when(n == 2)
            def _():
                pair_start(2, s)
                tiles(F, lambda at, tile: gate_up_delta(s, at))
                pair_start(3, s)
                pair_start(4, s)
                pair_kept(2, s)
                pair_received(2, s)
                branch_load(s).start()

                @pl.when(s == 0)
                def _():
                    def each(i, carry):
                        pair_kept(1, i)
                        pair_received(1, i)
                        return carry

                    lax.fori_loop(0, C, each, 0)
                    chunk_copy(jnp.int32(0), 0).start()

            @pl.when(tau == begin)
            def _():
                compute_open(s)
                wide_product(jnp.int32(0))
                pl.semaphore_wait(free_sem, len(ctx_meets))
                e_send_step(jnp.int32(0), 0, W)

            for a in range(1, T):
                comm(tau, 2 * a - 1, a)

            @pl.when(n == 0)
            def _():
                load_start(2 * tau + 1)
                pair_start(6, s)
                heads = heads_ref[:, s].reshape(M, Hq)
                tiles(D, lambda at, tile: store_part(s, at, tile, dot_nn(heads, wo_v[:, at])))

            @pl.when(n == 1)
            def _():
                @pl.when(s == 0)
                def _():
                    load_wait(2)

                tiles(D, lambda at, tile: store_part(s, at, tile, dot_nt(hid[s], wd_v[at, :])))
                pair_kept(0, s)
                pair_away(0, s)
                ag_sent(s)

            @pl.when(n == 2)
            def _():
                tiles(
                    D,
                    lambda at, tile: store_part(
                        s, at, tile, dot_nt(Ab[s], wg_v[at, :]) + dot_nn(Bb[s], wu_v[:, at])
                    ),
                )
                pair_away(2, s)
                ag_sent(s)

            @pl.when((n < 2) | (tau == begin))
            def _():
                rs_start(jnp.where(n < 2, s, 0))

            for a in range(1, T):
                comm(tau, 2 * a, a)
            return carry

        lax.fori_loop(0, 3 * C, tick, 0)

        def leave(s, carry):
            pair_away(1, s)
            return carry

        lax.fori_loop(0, C, leave, 0)
        del env["hid"]

    def finishing(L, Hd, RQ, RKV, WQ, WK, WV, dq, rdelta, kvb, kvs, kvr, acc2, qv, cos_v, sin_v):
        env["L"] = L
        signal_all(enter_sem, later + partners)
        rows_load = pltpu.make_async_copy(rows_pair, L.at[0], l_sem.at[1])
        attn_load = pltpu.make_async_copy(attn_pair, L.at[1], l_sem.at[2])
        rows1_load = pltpu.make_async_copy(rows1_ref, L.at[0], l_sem.at[1])
        head_load = pltpu.make_async_copy(head_pair, Hd, l_sem.at[3])
        small_loads = [
            pltpu.make_async_copy(src, dst, q_sem.at[i])
            for i, (src, dst) in enumerate([(q_ref, qv), (cos_ref, cos_v), (sin_ref, sin_v)])
        ]
        for copy in small_loads:
            copy.start()
        out_copy = pltpu.make_async_copy(out_ref, out_o, l_sem.at[4])
        igrad_copy = pltpu.make_async_copy(igrad_ref, igrad_o, l_sem.at[5])
        out_copy.start()

        rows_at = pl.ds(pl.multiple_of(dp * Dh, 128), Dh)
        spread = [(wq_ref, WQ.at[rows_at]), (wk_ref, WK.at[rows_at]), (wv_ref, WV.at[rows_at])]

        def spread_local(i):
            return pltpu.make_async_copy(*spread[i], s_sem.at[0, i])

        def spread_remote(i, o):
            return remote(*spread[i], s_sem.at[1 + 2 * o, i], s_sem.at[2 + 2 * o, i], partners[o])

        def pair_remote(i, o):
            ref = [RQ, RKV][i]
            return remote(ref.at[dp], ref.at[dp], q_sem.at[3 + 4 * o + 2 * i], q_sem.at[4 + 4 * o + 2 * i], partners[o])

        def deltas_of(head):
            return hdelta[:, :, :, head].reshape(R, HEAD)

        per = max(1, 256 // Lr)
        key_tile = per * Lr

        def kv_copy(d):
            return remote(
                kvs.at[lax.rem(d, kvs.shape[0])], kvr.at[d - 1], kv_send.at[d - 1], kv_recv.at[d - 1],
                along("ctx", jnp.maximum(c - d, 0)),
            )

        def block_copy(block):
            two = lax.rem(block, 2)
            return pltpu.make_async_copy(kv_ref.at[block], kvb.at[two], kvb_sem.at[two])

        def attend(two, masked, dst):
            for kh in range(KH):
                cols = slice(kh * HEAD, (kh + 1) * HEAD)

                def key_step(i, carry):
                    start = pl.multiple_of(i * key_tile, key_tile)
                    at = pl.ds(i * per, per)
                    keys = kvb[two, at, 0, :, cols].reshape(key_tile, HEAD)
                    values = kvb[two, at, 1, :, cols].reshape(key_tile, HEAD)
                    key_sum = jnp.zeros((key_tile, HEAD), F32)
                    value_sum = jnp.zeros((key_tile, HEAD), F32)
                    for g in range(GS):
                        h = kh * GS + g
                        head = slice(h * HEAD, (h + 1) * HEAD)
                        query, delta = qv[:, head], deltas_of(head)
                        bent = jnp.tanh(dot_nt(keys, query) * (scale / CAP))
                        prob = jnp.exp(CAP * bent - logt_ref[h:h + 1, :])
                        if masked:
                            key_pos = start + lax.broadcasted_iota(jnp.int32, prob.shape, 0)
                            prob = jnp.where(key_pos <= lax.broadcasted_iota(jnp.int32, prob.shape, 1), prob, 0.0)
                        grad = prob * (dot_nt(values, delta) - rdelta[h:h + 1, :]) * (1.0 - bent * bent)
                        grad = grad.astype(BF)
                        value_sum += dot_nn(prob.astype(BF), delta)
                        key_sum += dot_nn(grad, query)
                        dq[:, head] += dot_tn(grad, keys)
                    rows = pl.ds(start, key_tile)
                    kvs[dst, 0, rows, cols] = (key_sum * scale).astype(BF)
                    kvs[dst, 1, rows, cols] = value_sum.astype(BF)
                    return carry

                lax.fori_loop(0, R // key_tile, key_step, 0)

        def attention():
            dq[...] = jnp.zeros_like(dq)
            for h in range(Hq // HEAD):
                head = slice(h * HEAD, (h + 1) * HEAD)
                product = deltas_of(head).astype(F32) * heads_ref[:, :, :, head].reshape(R, HEAD).astype(F32)
                rdelta[h:h + 1] = jnp.sum(product.T, axis=0, keepdims=True)
            block_copy(0).start()

            def far(block, carry):
                d = c - block

                @pl.when(block < c)
                def _():
                    slot = lax.rem(d, kvs.shape[0])
                    block_copy(block).wait()
                    block_copy(block + 1).start()

                    @pl.when(d + kvs.shape[0] <= c)
                    def _():
                        kv_copy(d + kvs.shape[0]).wait_send()

                    attend(lax.rem(block, 2), False, slot)
                    kv_copy(d).start()

                return carry

            lax.fori_loop(0, NC - 1, far, 0)

            @pl.when(c >= kvs.shape[0])
            def _():
                kv_copy(kvs.shape[0]).wait_send()

            block_copy(c).wait()
            attend(lax.rem(c, 2), True, 0)

        def turned(values, h):
            a, b = values[:, h * HEAD:h * HEAD + HEAD // 2], values[:, h * HEAD + HEAD // 2:(h + 1) * HEAD]
            cosine, sine = cos_v[...], sin_v[...]
            return jnp.concatenate([a * cosine + b * sine, b * cosine - a * sine], axis=1).astype(BF)

        def last_copy(side, k, j):
            if side == 0:
                slot, peer = j, right
            else:
                slot, peer = jnp.where(j == t - 1, T, j), left
            return remote(Pb.at[:, j], Rb.at[:, slot], last_send.at[side, k], last_recv.at[side, k], peer)

        def last_step(k):
            for side in (0, 1):
                j = rs_block(side, k)

                @pl.when(rs_sends(side, k))
                def _():
                    if k:

                        @pl.when(has_left if side == 0 else has_right)
                        def _():
                            last_copy(side, k - 1, j).wait_recv()
                            Pb[:, j] = (Pb[:, j].astype(F32) + Rb[:, j].astype(F32)).astype(BF)

                    last_copy(side, k, j).start()

        def own_keys():
            for which in range(2):
                dst = []
                for kh in range(KH):
                    dst.append(kvs[0, which, :, kh * HEAD:(kh + 1) * HEAD].astype(F32))
                acc2[which] = jnp.concatenate(dst, axis=1) if KH > 1 else dst[0]

            def come(i, carry):
                d = i + 1

                @pl.when(c + d <= NC - 1)
                def _():
                    kv_copy(d).wait_recv()
                    for which in range(2):
                        acc2[which] += kvr[d - 1, which].astype(F32)

                return carry

            lax.fori_loop(0, NC - 1, come, 0)
            for kh in range(KH):
                cols = slice(kh * HEAD, (kh + 1) * HEAD)
                RKV[dp, 0, :, cols] = turned(acc2[0], kh)
            RKV[dp, 1] = acc2[1].astype(BF)
            for h in range(Hq // HEAD):
                RQ[dp, :, h * HEAD:(h + 1) * HEAD] = turned(dq[...] * scale, h)
            for i in range(2):
                for o in range(NDP - 1):
                    pair_remote(i, o).start()
            for i in range(3):
                spread_local(i).wait()
                for o in range(NDP - 1):
                    spread_remote(i, o).wait_recv()
            tile = tile_of(D)

            def part(i, carry):
                at = pl.ds(pl.multiple_of(i * tile, tile), tile)
                terms = dot_nt(RQ[dp], WQ[at, :]) + dot_nt(RKV[dp, 0], WK[at, :]) + dot_nt(RKV[dp, 1], WV[at, :])
                terms = terms.astype(BF).reshape(T, C, rc, tile)
                for s in range(C):
                    Pb[s, :, :, at] = terms[:, s]
                return carry

            lax.fori_loop(0, D // tile, part, 0)
            last_step(0)

        def last_finish():
            igrad_ref[...] = Pb[:, t].reshape(Lr, D).astype(F32)

            @pl.when(has_left)
            def _():
                last_copy(0, T - 2, t).wait_recv()
                igrad_ref[...] += Rb[:, t].reshape(Lr, D).astype(F32)

            @pl.when(has_right)
            def _():
                last_copy(1, T - 2, t).wait_recv()
                igrad_ref[...] += Rb[:, T].reshape(Lr, D).astype(F32)

            rows = x_ref[...].astype(F32)
            grad, terms = rms_back(rows, inverse_rms(rows), gain_ref[0:1], igrad_ref[...])
            igrad_ref[...] = mdelta[...] + grad
            G[0, 0:1] = terms
            G[0, 1:4] = gsum[...]

        meets = [("tp", t, T), ("ctx", c, NC), ("dp", dp, NDP)]
        g_base = [0, T - 1, T + NC - 2]

        def g_copies(k):
            axis, index, count = meets[k]
            return [
                remote(
                    G.at[k], GR.at[g_base[k] + o - 1], g_send.at[g_base[k] + o - 1], g_recv.at[g_base[k] + o - 1],
                    along(axis, lax.rem(index + o, count)),
                )
                for o in range(1, count)
            ]

        def g_start(k):
            for copy in g_copies(k):
                copy.start()

        def g_steps(i, place):
            for k in range(len(meets)):
                if k != place:
                    continue

                @pl.when(i == attend_at + T + 2)
                def _():
                    total = G[k]
                    for o, copy in enumerate(g_copies(k)):
                        copy.wait_recv()
                        total += GR[g_base[k] + o]
                    G[k + 1] = total
                    if k + 1 < len(meets):
                        g_start(k + 1)

        def up_open():
            def each(s, carry):
                for kind in (3, 4):
                    pair_kept(kind, s)
                    pair_received(kind, s)
                pair_received(0, s)
                return carry

            lax.fori_loop(0, C, each, 0)
            rows_load.start()

        def attn_open():
            def each(s, carry):
                for kind in (5, 6):
                    pair_kept(kind, s)
                    pair_received(kind, s)
                return carry

            lax.fori_loop(0, C, each, 0)
            attn_load.start()
            head_load.start()

        def product(u, w):
            @pl.when(u < wide_units)
            def _():
                @pl.when(u == NF)
                def _():
                    rows_load.wait()

                @pl.when(u == NF - 1)
                def _():
                    up_open()

                wide_product(u)

                @pl.when(u == wide_units - 1)
                def _():
                    attn_open()

            if w == narrow:

                def columns(first, par):
                    return pl.ds(pl.multiple_of(((u - first) * 2 + par) * narrow, 128), narrow)

                @pl.when((u >= wide_units) & (u < q_first))
                def _():
                    @pl.when(u == wide_units)
                    def _():
                        attn_load.wait()
                        head_load.wait()
                        rows1_load.start()

                    def out_part(par, carry):
                        second = Hd[:, :, :, :, columns(wide_units, par)]
                        store(u, par, narrow, L[1], second.reshape(tokens, narrow))
                        return carry

                    lax.fori_loop(0, 2, out_part, 0)

                @pl.when(u == q_first)
                def _():
                    rows1_load.wait()
                    for p in range(2):
                        for o in range(NDP - 1):
                            pair_remote(p, o).wait_recv()

                @pl.when((u >= q_first) & (u < kv_first))
                def _():
                    def query_part(par, carry):
                        store(u, par, narrow, L[0], RQ[:, :, columns(q_first, par)].reshape(tokens, narrow))
                        return carry

                    lax.fori_loop(0, 2, query_part, 0)

                @pl.when(u >= kv_first)
                def _():
                    at = pl.ds(pl.multiple_of((u - kv_first) * narrow, 128), narrow)
                    def key_part(par, carry):
                        store(u, par, narrow, L[0], RKV[:, par, :, at].reshape(tokens, narrow))
                        return carry

                    lax.fori_loop(0, 2, key_part, 0)

        attend_at = C + 1

        def first_tick(i):
            return begin + 1 + i + jnp.minimum(i // 2, C - 2)

        def line_tick(tau):
            for a in range(1, T):
                comm(tau, 2 * a - 1, a)

            @pl.when(tau < begin + C)
            def _():
                rs_start(tau - begin)

            @pl.when(tau >= begin + C)
            def _():
                s = tau - begin - C
                pair_start(5, s)
                hdelta[:, s] = dot_nt(rows_of(s), wo_v[...]).astype(BF).reshape(T, rc, Hq)
                rs_sent(s)

            for a in range(1, T):
                comm(tau, 2 * a, a)

        def tick(i, carry):
            u = i + 1

            def start(w):
                @pl.when(u >= NP)
                def _():
                    by_width(u - NP, lambda before: e_sent(u - NP, before))

                product(u, w)
                e_send_step(u, 0, w)

            by_width(u, start)
            g_steps(i, 0)

            @pl.when(i == 1)
            def _():
                pl.semaphore_wait(enter_sem, len(later + partners))
                for w in range(3):
                    spread_local(w).start()
                    for o in range(NDP - 1):
                        spread_remote(w, o).start()

            @pl.when(i < attend_at)
            def _():
                line_tick(first_tick(i))

            @pl.when(i == attend_at)
            def _():
                for copy in small_loads:
                    copy.wait()
                attention()

            @pl.when(i == attend_at + 2)
            def _():
                own_keys()

            for k in range(1, T - 1):

                @pl.when(i == attend_at + 2 + k)
                def _():
                    last_step(k)

            @pl.when(i == attend_at + T + 1)
            def _():
                last_finish()
                igrad_copy.start()
                g_start(0)

            for k in range(1, m):

                def middle(w):
                    e_add(u - k, k - 1, w)
                    e_send_step(u - k, k, w)

                by_width(u - k, middle)

            @pl.when((lax.rem(i, 2) == 1) & (i <= 2 * C - 5))
            def _():
                line_tick(first_tick(i) + 1)

            g_steps(i, 1)
            by_width(u - m, lambda w: e_finish(u - m, w))
            g_steps(i, 2)
            return carry

        lax.fori_loop(0, units + m - 1, tick, 0)
        gains_ref[...] = G[len(meets)]
        out_copy.wait()
        igrad_copy.wait()

        for u in (units - 2, units - 1):
            out_wait(jnp.int32(u))
        for u in range(units - NP, units):
            by_width(jnp.int32(u), lambda w: e_sent(jnp.int32(u), w))
        for side in (0, 1):
            for k in range(T - 1):

                @pl.when(rs_sends(side, k))
                def _():
                    last_copy(side, k, rs_block(side, k)).wait_send()

        for k in range(len(meets)):
            for copy in g_copies(k):
                copy.wait_send()
        for o in range(NDP - 1):
            for i in range(3):
                spread_remote(i, o).wait_send()
            for i in range(2):
                pair_remote(i, o).wait_send()

        def kv_close(i, carry):
            d = i + 1

            @pl.when((d <= c) & (d < kvs.shape[0]))
            def _():
                kv_copy(d).wait_send()

            return carry

        lax.fori_loop(0, min(NC - 1, kvs.shape[0] - 1), kv_close, 0)

        def close(s, carry):
            for kind in (3, 4, 5, 6):
                pair_away(kind, s)
            ag_sent(s)
            return carry

        lax.fori_loop(0, C, close, 0)

    for copy in out_loads:
        copy.wait()
    vmem = pltpu.VMEM
    pl.run_scoped(
        stages, vmem((D, F), BF), vmem((F, D), BF), vmem((C, M, F), BF)
    )
    kv_slots = NC if NC <= 4 else 3
    pl.run_scoped(
        finishing,
        vmem((2, NDP, C, T, rc, Dh), BF), vmem((NDP, C, T, rc, Hq), BF),
        vmem((NDP, R, Hq), BF), vmem((NDP, 2, R, KVd), BF),
        vmem((D, Hq), BF), vmem((D, KVd), BF), vmem((D, KVd), BF),
        vmem((R, Hq), F32), vmem((Hq // HEAD, R), F32), vmem((2, T, 2, Lr, KVd), BF),
        vmem((kv_slots, 2, R, KVd), BF), vmem((NC - 1, 2, R, KVd), BF), vmem((2, R, KVd), F32),
        vmem((R, Hq), BF), vmem((R, HEAD // 2), F32), vmem((R, HEAD // 2), F32),
    )


def main_call(
    layer_in, cotangent, norm_gains, head_rows, w_out, w_gate, out_other, gate_other, up_turned, down_turned,
    query, log_totals, cosine, sine, keys_values, rows_one, w_query, w_key, w_value,
):
    T, NC, NDP = lax.axis_size("tp"), lax.axis_size("ctx"), lax.axis_size("dp")
    C = T
    Lr, D = layer_in.shape
    rc = Lr // C
    R, Hq = query.shape
    KVd = w_key.shape[1]
    Dh, RB = D // NDP, D // NDP // NC
    F = w_gate.shape[1]
    M = T * rc
    m = NC.bit_length() - 1
    NP, NR = m + 1, 4
    pitch = -(-RB // 16) * 16
    blocks = NP * 2 * NC + NR * 2 * (NC - 1)
    W = next(w for w in (tile_of(F) // 2, 256, 128) if F % (2 * w) == 0 and blocks <= (D // pitch) * (F // w))
    meets = T + NC + NDP - 3
    any_spec = pl.BlockSpec(memory_space=pl.ANY)
    vm = pl.BlockSpec(memory_space=pltpu.VMEM)
    sds = jax.ShapeDtypeStruct
    dma = pltpu.SemaphoreType.DMA
    vmem = pltpu.VMEM
    half_rows = sds((NDP, C, T, rc, Dh), BF)
    hidden_rows = sds((NDP, C, M, F), BF)
    outs = pl.pallas_call(
        functools.partial(main_kernel, T, C, NC, NDP, KVd // HEAD, NP, NR),
        out_shape=(
            sds((Lr, D), BF), sds((Lr, D), F32), sds((4, D), F32),
            sds((RB, F), BF), sds((RB, F), BF), sds((RB, F), BF), sds((RB, Hq), BF),
            sds((RB, Hq), BF), sds((RB, KVd), BF), sds((RB, KVd), BF),
            half_rows, hidden_rows, half_rows, hidden_rows, hidden_rows, half_rows, sds((NDP, C, T, rc, Hq), BF),
        ),
        in_specs=[vm] * 4 + [any_spec] * 7 + [vm] + [any_spec] * 7,
        out_specs=[any_spec] * 2 + [vm] + [any_spec] * 14,
        scratch_shapes=[
            vmem((Lr, D), BF), vmem((Lr, D), F32),
            vmem((Hq, D), BF), vmem((D, F), BF), vmem((C, T, rc, D), BF), vmem((C, T, rc, D), BF),
            vmem((C, T + 1, rc, D), BF), vmem((C, rc, D), F32), vmem((C, rc, D), F32), vmem((rc, D), F32),
            vmem((Lr, D), F32), vmem((3, D), F32), vmem((T, C, rc, Hq), BF), vmem((C, M, F), BF), vmem((C, M, F), BF),
            vmem((NDP, C, T, rc, Dh), BF), vmem((NDP, C, M, 2 * W), BF), vmem((2, 2, RB, W), BF),
            vmem((4, 4, D), F32), vmem((meets, 4, D), F32),
            dma((NDP,)), dma((3, 2 * T)), dma((C,)), dma((C, 2, T - 1)), dma((C, 2, T - 1)), dma((C, 2, T - 1)), dma((C, 2, T - 1)),
            dma((2 * NDP - 1, 7, C)), dma((6,)), dma((1,)), dma((NP, 2, NC - 1)), dma((NR, 2, NC - 1)), dma((2, 2)),
            dma((2 * NDP - 1, 3)), dma((3 + 4 * (NDP - 1),)), dma((NC - 1,)), dma((NC - 1,)),
            dma((2, T - 1)), dma((2, T - 1)), dma((meets,)), dma((meets,)), dma((2,)),
            pltpu.SemaphoreType.REGULAR, pltpu.SemaphoreType.REGULAR,
        ],
        compiler_params=pltpu.CompilerParams(
            collective_id=0, has_side_effects=True, vmem_limit_bytes=67_043_328
        ),
        name="main",
    )(
        layer_in, cotangent, norm_gains, head_rows.reshape(T, C, rc, Hq), w_out, w_gate, out_other, gate_other,
        up_turned, down_turned, query, log_totals, cosine, sine, keys_values,
        rows_one.reshape(NDP, C, T, rc, Dh), w_query, w_key, w_value,
    )
    return outs[:10]


def front_kernel(
    T, NC, NDP, KH, C,
    x_ref, gain_ref, freq_ref, wq_ref, wk_ref, wv_ref, wo_ref, wg_ref, wu_ref, wd_ref,
    q_o, heads_o, logt_o, cos_o, sin_o, kv_o, rows1_o, wo_o, wg_o, wut_o, wdt_o,
    X, WQ, WK, WV, KV, turned_sum, totals, up_v, upt_v, down_v, downt_v,
    w_sem, ag_send, ag_recv, pair_sem, kv_send, kv_recv, out_sem, t_sem, p_sem,
):
    t, c, dp = lax.axis_index("tp"), lax.axis_index("ctx"), lax.axis_index("dp")
    Lr, D = x_ref.shape
    R, Hq = q_o.shape
    rc = Lr // C
    KVd = KH * HEAD
    GS = Hq // KVd
    Dh = D // NDP
    scale = HEAD**-0.5
    has_left, has_right = t > 0, t < T - 1

    def remote(src, dst, send, recv, axis, index):
        return pltpu.make_async_remote_copy(
            src, dst, send, recv, device_id={axis: index}, device_id_type=MESH
        )

    partners = [lax.rem(dp + o, NDP) for o in range(1, NDP)]
    peers = [("tp", lax.rem(t + o, T)) for o in range(1, T)]
    peers += [("ctx", lax.rem(c + o, NC)) for o in range(1, NC)]
    peers += [("dp", p) for p in partners]
    sem = pltpu.get_barrier_semaphore()
    for axis, index in peers:
        pl.semaphore_signal(sem, inc=1, device_id={axis: index}, device_id_type=MESH)

    rows_at = pl.ds(pl.multiple_of(dp * Dh, 128), Dh)
    weights = [(wq_ref, WQ), (wk_ref, WK), (wv_ref, WV)]

    def weight_local(i):
        return pltpu.make_async_copy(weights[i][0], weights[i][1].at[rows_at], w_sem.at[0, i])

    def weight_remote(i, o):
        return remote(
            weights[i][0], weights[i][1].at[rows_at], w_sem.at[1 + 2 * o, i], w_sem.at[2 + 2 * o, i],
            "dp", partners[o],
        )

    turns = [
        pltpu.make_async_copy(wu_ref, up_v, t_sem.at[0]),
        pltpu.make_async_copy(wd_ref, down_v, t_sem.at[1]),
    ]
    for i in range(3):
        weight_local(i).start()
    for copy in turns:
        copy.start()
    rows = x_ref[...].astype(F32)
    X[t] = (rows * inverse_rms(rows) * gain_ref[0:1]).astype(BF)
    pl.semaphore_wait(sem, len(peers))

    def ag_copy(s, side, k, j):
        at = pl.ds(s * rc, rc)
        peer = jnp.minimum(t + 1, T - 1) if side == 0 else jnp.maximum(t - 1, 0)
        return remote(X.at[j, at], X.at[j, at], ag_send.at[s, side, k], ag_recv.at[s, side, k], "tp", peer)

    def ag_block(side, k):
        return (t - k) if side == 0 else (t + k)

    def ag_there(side, k):
        return (t >= k) if side == 0 else (t + k <= T - 1)

    def onward(side):
        return has_right if side == 0 else has_left

    for s in range(C):
        for side in (0, 1):

            @pl.when(onward(side))
            def _():
                ag_copy(s, side, 0, t).start()

    for i in range(3):
        for o in range(NDP - 1):
            weight_remote(i, o).start()

    def parts(ref, i):
        height = ref.shape[0] // T
        return pl.ds(pl.multiple_of(i * height, 16), height), height

    def part_dst(dst, ref, i, columns):
        at, height = parts(ref, i)
        if columns:
            return dst.at[at, rows_at]
        return dst.at[pl.ds(pl.multiple_of(dp * Dh + i * height, 16), height)]

    moved = [(wo_ref, wo_o, True, False), (wg_ref, wg_o, False, False)]
    moved += [(upt_v, wut_o, True, True), (downt_v, wdt_o, False, True)]

    def part_remote(w, i, o):
        src, dst, columns, _ = moved[w]
        return remote(
            src.at[parts(src, i)[0]], part_dst(dst, src, i, columns),
            p_sem.at[1 + 2 * o, w, i], p_sem.at[2 + 2 * o, w, i], "dp", partners[o],
        )

    def part_local(w, i):
        src, dst, columns, _ = moved[w]
        return pltpu.make_async_copy(src.at[parts(src, i)[0]], part_dst(dst, src, i, columns), p_sem.at[0, w, i])

    def part_start(w, i):
        for o in range(NDP - 1):
            part_remote(w, i, o).start()
        if moved[w][3]:
            part_local(w, i).start()

    def turn():
        for copy, src, dst in zip(turns, (up_v, down_v), (upt_v, downt_v), strict=True):
            copy.wait()
            height = src.shape[0] // T

            def some(i, carry):
                at = pl.ds(pl.multiple_of(i * height, 128), height)
                dst[:, at] = src[at, :].T
                return carry

            if height % 128 == 0:
                lax.fori_loop(0, T, some, 0)
            else:
                dst[...] = src[...].T

    position = (c * R + lax.broadcasted_iota(jnp.int32, (R, HEAD // 2), 0)).astype(F32)
    angles = position * freq_ref[...]
    cos_o[...] = jnp.cos(angles)
    sin_o[...] = jnp.sin(angles)
    for i in range(3):
        weight_local(i).wait()
        for o in range(NDP - 1):
            weight_remote(i, o).wait_recv()

    def kv_copy(d, j):
        return remote(
            KV.at[c, j], KV.at[c, j], kv_send.at[d - 1, j], kv_recv.at[d - 1, j],
            "ctx", jnp.minimum(c + d, NC - 1),
        )

    def kv_from(b, j):
        d = c - b
        return remote(KV.at[b, j], KV.at[b, j], kv_send.at[d - 1, j], kv_recv.at[d - 1, j], "ctx", c)

    def pair_copies(j):
        def half(owner):
            return X.at[j, :, pl.ds(pl.multiple_of(owner * Dh, 128), Dh)]

        copies = [pltpu.make_async_copy(half(dp), rows1_o.at[dp, j], pair_sem.at[0, j])]
        for o, partner in enumerate(partners):
            copies.append(
                remote(
                    half(partner), rows1_o.at[dp, j], pair_sem.at[1 + 2 * o, j], pair_sem.at[2 + 2 * o, j],
                    "dp", partner,
                )
            )
        return copies

    def turned(values, h, at):
        a, b = values[:, h * HEAD:h * HEAD + HEAD // 2], values[:, h * HEAD + HEAD // 2:(h + 1) * HEAD]
        cosine, sine = cos_o[at], sin_o[at]
        return jnp.concatenate([a * cosine - b * sine, b * cosine + a * sine], axis=1).astype(BF)

    def project(j):
        for copy in pair_copies(j):
            copy.start()
        at = pl.ds(pl.multiple_of(j * Lr, Lr), Lr)
        values = dot_nn(X[j], WK[...])
        for kh in range(KH):
            KV[c, j, 0, :, kh * HEAD:(kh + 1) * HEAD] = turned(values, kh, at)
        KV[c, j, 1] = dot_nn(X[j], WV[...]).astype(BF)

        def push(i, carry):
            @pl.when(c + 1 + i <= NC - 1)
            def _():
                kv_copy(i + 1, j).start()

            return carry

        lax.fori_loop(0, NC - 1, push, 0)
        values = dot_nn(X[j], WQ[...])
        for h in range(Hq // HEAD):
            q_o[at, h * HEAD:(h + 1) * HEAD] = turned(values, h, at)

    def gather(k, carry):
        for side in (0, 1):

            @pl.when(ag_there(side, k) & (k > 0))
            def _():
                for s in range(C):
                    ag_copy(s, side, k - 1, ag_block(side, k)).wait_recv()

                    @pl.when(onward(side) & (k <= T - 2))
                    def _():
                        ag_copy(s, side, k, ag_block(side, k)).start()

        for side in (0, 1):

            @pl.when(ag_there(side, k) & ((k > 0) | (side == 0)))
            def _():
                project(ag_block(side, k))

        part_start(0, k)
        part_start(1, k)

        @pl.when(k == 0)
        def _():
            turn()

        part_start(2, k)
        part_start(3, k)
        return carry

    lax.fori_loop(0, T, gather, 0)

    per = max(1, 256 // Lr)
    tile = per * Lr
    turned_sum[...] = jnp.zeros_like(turned_sum)
    totals[...] = jnp.zeros_like(totals)

    def out_copy(b):
        return pltpu.make_async_copy(KV.at[b], kv_o.at[b], out_sem.at[b])

    def key_step(b, p, masked):
        for kh in range(KH):
            cols = slice(kh * HEAD, (kh + 1) * HEAD)
            keys = KV[b, pl.ds(p * per, per), 0, :, cols].reshape(tile, HEAD)
            values = KV[b, pl.ds(p * per, per), 1, :, cols].reshape(tile, HEAD)
            for g in range(GS):
                h = kh * GS + g
                scores = dot_nt(keys, q_o[:, h * HEAD:(h + 1) * HEAD])
                weights = jnp.exp(CAP * jnp.tanh(scores * (scale / CAP)))
                if masked:
                    key_pos = p * tile + lax.broadcasted_iota(jnp.int32, weights.shape, 0)
                    allowed = key_pos <= lax.broadcasted_iota(jnp.int32, weights.shape, 1)
                    weights = jnp.where(allowed, weights, 0.0)
                totals[h:h + 1] += jnp.sum(weights, axis=0, keepdims=True)
                turned_sum[h] += dot_tn(values, weights.astype(BF))

    def own_step(p, carry):
        key_step(c, p, True)
        return carry

    out_copy(c).start()
    lax.fori_loop(0, T // per, own_step, 0)

    def far_block(i, carry):
        @pl.when(i < c)
        def _():
            b = c - 1 - i
            for j in range(T):
                kv_from(b, j).wait_recv()
            out_copy(b).start()

            def far_step(p, carry):
                key_step(b, p, False)
                return carry

            lax.fori_loop(0, T // per, far_step, 0)

        return carry

    lax.fori_loop(0, NC - 1, far_block, 0)
    for h in range(Hq // HEAD):
        heads_o[:, h * HEAD:(h + 1) * HEAD] = (turned_sum[h] / totals[h:h + 1]).T.astype(BF)
    logt_o[...] = jnp.log(totals[...])

    for i in range(3):
        for o in range(NDP - 1):
            weight_remote(i, o).wait_send()

    def close_parts(i, carry):
        for w in range(4):
            for o in range(NDP - 1):
                part_remote(w, i, o).wait()
            if moved[w][3]:
                part_local(w, i).wait()
        return carry

    lax.fori_loop(0, T, close_parts, 0)
    for s in range(C):
        for side in (0, 1):
            for k in range(T - 1):

                @pl.when(ag_there(side, k) & onward(side))
                def _():
                    ag_copy(s, side, k, ag_block(side, k)).wait_send()

    for j in range(T):
        copies = pair_copies(j)
        copies[0].wait()
        for copy in copies[1:]:
            copy.wait()

    def close(i, carry):
        @pl.when(c + 1 + i <= NC - 1)
        def _():
            for j in range(T):
                kv_copy(i + 1, j).wait_send()

        return carry

    lax.fori_loop(0, NC - 1, close, 0)

    def close_out(b, carry):
        @pl.when(b <= c)
        def _():
            out_copy(b).wait()

        return carry

    lax.fori_loop(0, NC, close_out, 0)


def front_call(layer_in, norm_gains, frequency, w_query, w_key, w_value, w_out, w_gate, w_up, w_down):
    T, NC, NDP = lax.axis_size("tp"), lax.axis_size("ctx"), lax.axis_size("dp")
    C = T
    Lr, D = layer_in.shape
    R = T * Lr
    Hq, KVd = w_query.shape[1], w_key.shape[1]
    Dh = D // NDP
    F = w_gate.shape[1]
    H = Hq // HEAD
    any_spec = pl.BlockSpec(memory_space=pl.ANY)
    vm = pl.BlockSpec(memory_space=pltpu.VMEM)
    sds = jax.ShapeDtypeStruct
    dma = pltpu.SemaphoreType.DMA
    return pl.pallas_call(
        functools.partial(front_kernel, T, NC, NDP, KVd // HEAD, C),
        out_shape=(
            sds((R, Hq), BF), sds((R, Hq), BF), sds((H, R), F32),
            sds((R, HEAD // 2), F32), sds((R, HEAD // 2), F32),
            sds((NC, T, 2, Lr, KVd), BF), sds((NDP, T, Lr, Dh), BF),
            sds((Hq, D), BF), sds((D, F), BF), sds((F, D), BF), sds((D, F), BF),
        ),
        in_specs=[vm] * 3 + [any_spec] * 7,
        out_specs=[vm] * 5 + [any_spec] * 6,
        scratch_shapes=[
            pltpu.VMEM((T, Lr, D), BF), pltpu.VMEM((D, Hq), BF), pltpu.VMEM((D, KVd), BF), pltpu.VMEM((D, KVd), BF),
            pltpu.VMEM((NC, T, 2, Lr, KVd), BF), pltpu.VMEM((H, HEAD, R), F32), pltpu.VMEM((H, R), F32),
            pltpu.VMEM((Dh, F), BF), pltpu.VMEM((F, Dh), BF), pltpu.VMEM((F, Dh), BF), pltpu.VMEM((Dh, F), BF),
            dma((2 * NDP - 1, 3)), dma((C, 2, T - 1)), dma((C, 2, T - 1)), dma((2 * NDP - 1, T)),
            dma((NC - 1, T)), dma((NC - 1, T)), dma((NC,)), dma((2,)), dma((2 * NDP - 1, 4, T)),
        ],
        compiler_params=pltpu.CompilerParams(
            collective_id=2, has_side_effects=True, vmem_limit_bytes=66_000_000
        ),
        name="front",
    )(layer_in, norm_gains, frequency, w_query, w_key, w_value, w_out, w_gate, w_up, w_down)


def finish_kernel(width, count, gains_ref, *refs):
    n = count
    srcs, gain_o, dsts = refs[:n], refs[n], refs[n + 1:2 * n + 1]
    held, wide, sems = refs[2 * n + 1:3 * n + 1], refs[3 * n + 1:-1], refs[-1]
    for i in range(n):
        pltpu.make_async_copy(srcs[i], held[i], sems.at[0, i]).start()
    rank = lax.axis_index("dp")
    for axis in ("ctx", "tp"):
        rank = rank * lax.axis_size(axis) + lax.axis_index(axis)
    gains = gains_ref[...]
    total = gains.shape[1]
    gain_o[...] = pltpu.roll(gains, lax.rem(total - rank * width, total), axis=1)[:4, :width]
    buffers = []
    for i in range(n):
        pltpu.make_async_copy(srcs[i], held[i], sems.at[0, i]).wait()
        buffer = held[i]
        if held[i].dtype != dsts[i].dtype:
            buffer = wide[len([b for b in buffers if b])]
            buffer[...] = held[i][...].astype(buffer.dtype)
        buffers.append(buffer is not held[i])
        pltpu.make_async_copy(buffer, dsts[i], sems.at[1, i]).start()
    used = 0
    for i in range(n):
        buffer = wide[used] if buffers[i] else held[i]
        used += buffers[i]
        pltpu.make_async_copy(buffer, dsts[i], sems.at[1, i]).wait()


def finish_call(gains, arrays, dtypes):
    width = gains.shape[1] // (lax.axis_size("tp") * lax.axis_size("ctx") * lax.axis_size("dp"))
    any_spec = pl.BlockSpec(memory_space=pl.ANY)
    vm = pl.BlockSpec(memory_space=pltpu.VMEM)
    sds = jax.ShapeDtypeStruct
    n = len(arrays)
    return pl.pallas_call(
        functools.partial(finish_kernel, width, n),
        out_shape=[sds((4, width), F32)] + [sds(a.shape, d) for a, d in zip(arrays, dtypes, strict=True)],
        in_specs=[vm] + [any_spec] * n,
        out_specs=[vm] + [any_spec] * n,
        scratch_shapes=[pltpu.VMEM(a.shape, a.dtype) for a in arrays]
        + [pltpu.VMEM(a.shape, d) for a, d in zip(arrays, dtypes, strict=True) if a.dtype != d]
        + [pltpu.SemaphoreType.DMA((2, n))],
        compiler_params=pltpu.CompilerParams(vmem_limit_bytes=66_000_000),
        name="finish",
    )(gains, *arrays)


def shards(layer_in, cotangent, norm_gains, w_query, w_key, w_value, w_out, w_gate, w_up, w_down):
    half_width = HEAD // 2
    frequency = THETA ** (-(jnp.arange(half_width, dtype=F32) * 2.0) / HEAD)
    query, head_rows, log_totals, cosine, sine, keys_values, rows_one, *weights = front_call(
        layer_in, norm_gains, frequency[None, :], w_query, w_key, w_value, w_out, w_gate, w_up, w_down
    )
    layer_out, input_grad, gains, down_sum, *sums = main_call(
        layer_in, cotangent, norm_gains, head_rows, w_out, w_gate, *weights,
        query, log_totals, cosine, sine, keys_values, rows_one, w_query, w_key, w_value,
    )
    arrays = [layer_out, input_grad, down_sum, *sums]
    gain_grads, layer_out, input_grad, down_turned, grad_gate, grad_up, out_turned, *rest = finish_call(
        gains, arrays, [BF] + [F32] * (len(arrays) - 1)
    )
    return (layer_out, input_grad, gain_grads, *rest, out_turned.T, grad_gate, grad_up, down_turned.T)


def solution(mesh):
    return jax.shard_map(
        shards,
        mesh=mesh,
        in_specs=(
            P(("dp", "ctx", "tp"), None),
            P(("dp", "ctx", "tp"), None),
            P(),
            P("dp", "tp"),
            P("dp", "tp"),
            P("dp", "tp"),
            P("tp", "dp"),
            P("dp", "tp"),
            P("dp", "tp"),
            P("tp", "dp"),
        ),
        out_specs=(
            P(("dp", "ctx", "tp"), None),
            P(("dp", "ctx", "tp"), None),
            P(None, ("dp", "ctx", "tp")),
            P(("dp", "ctx"), "tp"),
            P(("dp", "ctx"), "tp"),
            P(("dp", "ctx"), "tp"),
            P("tp", ("dp", "ctx")),
            P(("dp", "ctx"), "tp"),
            P(("dp", "ctx"), "tp"),
            P("tp", ("dp", "ctx")),
        ),
        check_vma=False,
    )
```

```python
import functools

import jax
import jax.numpy as jnp
from jax import lax
from jax.experimental import pallas as pl
from jax.experimental.pallas import tpu as pltpu
from jax.sharding import PartitionSpec as P

HEAD = 256
EPS = 1e-06
CAP = 50.0
THETA = 10000.0
MESH = pl.DeviceIdType.MESH
BF = jnp.bfloat16
F32 = jnp.float32


def tile_of(width):
    for tile in (768, 512, 256, 128):
        if width % tile == 0:
            return tile
    return width


def inverse_rms(values):
    return lax.rsqrt(jnp.mean(values * values, axis=-1, keepdims=True) + EPS)


def rms_back(values, scale, gain, delta):
    weighted = delta * gain
    inner = jnp.mean(weighted * values, axis=-1, keepdims=True)
    grad = scale * weighted - values * (scale * scale * scale * inner)
    return grad, jnp.sum(delta * values * scale, axis=0, keepdims=True)


def dot_nt(former, latter):
    return lax.dot_general(former, latter, (((1,), (1,)), ((), ())), preferred_element_type=F32)


def dot_nn(former, latter):
    return jnp.dot(former, latter, preferred_element_type=F32)


def flip(index, bit):
    return index + bit * (1 - 2 * lax.rem(index // bit, 2))


def flips(index, mask):
    bit = 1
    while bit <= mask:
        if mask & bit:
            index = flip(index, bit)
        bit *= 2
    return index


def dot_tn(former, latter):
    return lax.dot_general(former, latter, (((0,), (0,)), ((), ())), preferred_element_type=F32)


def sub_sums(bits):
    sums = [0]
    for bit in bits:
        sums = sums + [s + bit for s in sums]
    return sums


def bits_below(count):
    return [1 << i for i in range(count.bit_length() - 1)]


def main_kernel(
    T, C, NC, NDP, KH, NP, NR,
    x_ref, ct_ref, gain_ref, heads_ref,
    wo_ref, wg_ref, wo_other, wg_other, wut_ref, wdt_ref, q_ref, logt_ref, cos_ref, sin_ref, kv_ref, rows1_ref,
    wq_ref, wk_ref, wv_ref,
    out_o, igrad_o, gains_ref,
    down_o, gate_o, up_o, wout_o, q_o, k_o, v_o,
    rows_pair, hid_pair, branch_pair, gate_pair, up_pair, attn_pair, head_pair,
    out_ref, igrad_ref, wo_v, wd_v, X, Pb, Rb, att, mid, acc, mdelta, gsum, hdelta, Ab, Bb, L0, Rc, st, G, GR,
    w_sem, f_sem, b_sem, rs_send, rs_recv, ag_send, ag_recv, pair_sem, l_sem, r_sem, e_send, e_recv, st_sem,
    s_sem, q_sem, kv_send, kv_recv, last_send, last_recv, g_send, g_recv, kvb_sem, free_sem, enter_sem,
):
    t, c, dp = lax.axis_index("tp"), lax.axis_index("ctx"), lax.axis_index("dp")
    Lr, D = x_ref.shape
    rc = Lr // C
    R, Hq = q_ref.shape
    KVd = KH * HEAD
    GS = Hq // KVd
    Dh, RB = D // NDP, D // NDP // NC
    F = wg_ref.shape[1]
    M = T * rc
    tokens = NDP * R
    W = Rc.shape[-1] // 2
    m = NC.bit_length() - 1
    NF = F // (2 * W)
    narrow = min(W, Hq // 2)
    wide_units = 3 * NF
    n_out, n_kv = Hq // (2 * narrow), KVd // narrow
    q_first, kv_first = wide_units + n_out, wide_units + 2 * n_out
    units = kv_first + n_kv
    begin = 3 * C - 1
    scale = HEAD**-0.5
    has_left, has_right = t > 0, t < T - 1
    left, right = {"tp": jnp.maximum(t - 1, 0)}, {"tp": jnp.minimum(t + 1, T - 1)}
    partners = [{"dp": lax.rem(dp + o, NDP)} for o in range(1, NDP)]
    later = [{"ctx": lax.rem(c + o, NC)} for o in range(1, NC)]
    others = [{"tp": lax.rem(t + o, T)} for o in range(1, T)] + later + partners
    ctx_meets = [{"ctx": flip(c, bit)} for bit in bits_below(NC)]

    def along(axis, index):
        return {axis: index}

    def remote(src, dst, send, recv, peer):
        return pltpu.make_async_remote_copy(src, dst, send, recv, device_id=peer, device_id_type=MESH)

    def signal_all(sem, peers):
        for peer in peers:
            pl.semaphore_signal(sem, inc=1, device_id=peer, device_id_type=MESH)

    def columns_of(ref, owner):
        return ref.at[:, pl.ds(pl.multiple_of(owner * Dh, 128), Dh)]

    owners = [p["dp"] for p in partners]
    out_loads = [pltpu.make_async_copy(wo_ref, columns_of(wo_v, dp), w_sem.at[0])] + [
        pltpu.make_async_copy(columns_of(wo_other, p), columns_of(wo_v, p), w_sem.at[1 + o])
        for o, p in enumerate(owners)
    ]
    for copy in out_loads:
        copy.start()
    entry = pltpu.get_barrier_semaphore()
    signal_all(entry, others)
    gsum[...] = jnp.zeros_like(gsum)
    pl.semaphore_wait(entry, len(others))

    def pair_copies(kind, s, src, half, dst):
        def cut(owner):
            if half:
                return src.at[..., pl.ds(pl.multiple_of(owner * Dh, 128), Dh)]
            return src

        copies = [pltpu.make_async_copy(cut(dp), dst.at[dp, s], pair_sem.at[0, kind, s])]
        for o, partner in enumerate(partners):
            copies.append(
                pltpu.make_async_remote_copy(
                    cut(partner["dp"]), dst.at[dp, s],
                    pair_sem.at[1 + 2 * o, kind, s], pair_sem.at[2 + 2 * o, kind, s],
                    device_id=partner, device_id_type=MESH,
                )
            )
        return copies

    env = {}

    def pair_of(kind, s):
        src = [
            lambda: X.at[s], lambda: env["hid"].at[s], lambda: X.at[s], lambda: Ab.at[s],
            lambda: Bb.at[s], lambda: X.at[s], lambda: heads_ref.at[:, s],
        ][kind]()
        return pair_copies(kind, s, src, kind in (0, 2, 5), pairs[kind])

    pairs = [rows_pair, hid_pair, branch_pair, gate_pair, up_pair, attn_pair, head_pair]

    def pair_start(kind, s):
        for copy in pair_of(kind, s):
            copy.start()

    def pair_kept(kind, s):
        pair_of(kind, s)[0].wait()

    def pair_away(kind, s):
        for copy in pair_of(kind, s)[1:]:
            copy.wait_send()

    def pair_received(kind, s):
        for o, partner in enumerate(partners):
            place = pairs[kind].at[dp, s]
            remote(
                place, place, pair_sem.at[1 + 2 * o, kind, s], pair_sem.at[2 + 2 * o, kind, s], partner
            ).wait_recv()

    def rs_copy(s, side, k, j):
        if side == 0:
            slot, peer = j, right
        else:
            slot, peer = jnp.where(j == t - 1, T, j), left
        return pltpu.make_async_remote_copy(
            Pb.at[s, j], Rb.at[s, slot], rs_send.at[s, side, k], rs_recv.at[s, side, k],
            device_id=peer, device_id_type=MESH,
        )

    def rs_block(side, k):
        return (T - 1 - k + t) if side == 0 else (k - (T - 1 - t))

    def rs_sends(side, k):
        return (t <= k) if side == 0 else (T - 1 - t <= k)

    def ag_copy(s, side, k, j):
        return pltpu.make_async_remote_copy(
            X.at[s, j], X.at[s, j], ag_send.at[s, side, k], ag_recv.at[s, side, k],
            device_id=right if side == 0 else left, device_id_type=MESH,
        )

    def ag_block(side, k):
        return (t - k) if side == 0 else (t + k)

    def ag_sends(side, k):
        return (t >= k) & has_right if side == 0 else (t + k <= T - 1) & has_left

    def rs_start(s):
        for side in (0, 1):

            @pl.when(rs_sends(side, 0))
            def _():
                rs_copy(s, side, 0, rs_block(side, 0)).start()

    def rs_step(s, k):
        for side in (0, 1):
            j = rs_block(side, k)
            came = has_left if side == 0 else has_right

            @pl.when(rs_sends(side, k))
            def _():
                @pl.when(came)
                def _():
                    rs_copy(s, side, k - 1, j).wait_recv()
                    Pb[s, j] = (Pb[s, j].astype(F32) + Rb[s, j].astype(F32)).astype(BF)

                rs_copy(s, side, k, j).start()

    def rs_sent(s):
        for side in (0, 1):
            for k in range(T - 1):

                @pl.when(rs_sends(side, k))
                def _():
                    rs_copy(s, side, k, rs_block(side, k)).wait_send()

    def rs_finish(s):
        acc[...] = Pb[s, t].astype(F32)

        @pl.when(has_left)
        def _():
            rs_copy(s, 0, T - 2, t).wait_recv()
            acc[...] += Rb[s, t].astype(F32)

        @pl.when(has_right)
        def _():
            rs_copy(s, 1, T - 2, t).wait_recv()
            acc[...] += Rb[s, T].astype(F32)

    def ag_start(s):
        for side in (0, 1):

            @pl.when(ag_sends(side, 0))
            def _():
                ag_copy(s, side, 0, t).start()

    def ag_step(s, k):
        for side in (0, 1):
            j = ag_block(side, k)
            there = (j >= 0) if side == 0 else (j <= T - 1)

            @pl.when(there)
            def _():
                ag_copy(s, side, k - 1, j).wait_recv()
                if k <= T - 2:

                    @pl.when(has_right if side == 0 else has_left)
                    def _():
                        ag_copy(s, side, k, j).start()

    def ag_sent(s):
        for side in (0, 1):
            for k in range(T - 1):

                @pl.when(ag_sends(side, k))
                def _():
                    ag_copy(s, side, k, ag_block(side, k)).wait_send()

    def local_rows(n, s):
        own = pl.ds(pl.multiple_of(s * rc, rc), rc)
        total = acc[...]

        @pl.when(n == 0)
        def _():
            att[s] = total
            middle = x_ref[own].astype(F32) + total * inverse_rms(total) * gain_ref[1:2]
            mid[s] = middle
            X[s, t] = (middle * inverse_rms(middle) * gain_ref[2:3]).astype(BF)

        @pl.when(n == 1)
        def _():
            scale = inverse_rms(total)
            out_ref[own] = (mid[s] + total * scale * gain_ref[3:4]).astype(BF)
            grad, terms = rms_back(total, scale, gain_ref[3:4], ct_ref[own].astype(F32))
            gsum[2:3] += terms
            X[s, t] = grad.astype(BF)

        @pl.when(n == 2)
        def _():
            middle, attention = mid[s], att[s]
            grad, terms = rms_back(middle, inverse_rms(middle), gain_ref[2:3], total)
            gsum[1:2] += terms
            middle_delta = ct_ref[own].astype(F32) + grad
            mdelta[own] = middle_delta
            grad, terms = rms_back(attention, inverse_rms(attention), gain_ref[1:2], middle_delta)
            gsum[0:1] += terms
            X[s, t] = grad.astype(BF)

    def comm(tau, w, a):
        back = tau - a

        @pl.when(((back >= 0) & (back < 2 * C)) | ((back >= begin) & (back < begin + C)))
        def _():
            n = jnp.where(back < 2 * C, back // C, 2)
            s = jnp.where(back < 2 * C, lax.rem(back, C), back - begin)
            if w <= T - 2:
                rs_step(s, w)
            elif w == T - 1:
                rs_finish(s)
                local_rows(n, s)
                ag_start(s)
            else:
                ag_step(s, w - (T - 1))

    def tiles(width, body):
        tile = tile_of(width)

        def step(i, carry):
            body(pl.ds(pl.multiple_of(i * tile, tile), tile), tile)
            return carry

        lax.fori_loop(0, width // tile, step, 0)

    def rows_of(s):
        return X[s].reshape(M, D)

    def store_part(s, at, tile, value):
        Pb[s, :, :, at] = value.astype(BF).reshape(T, rc, tile)

    pitch = -(-RB // 16) * 16
    orders = [bits_below(NC), bits_below(NC)[::-1]]
    first_of = [sum(NC >> (i + 1) for i in range(k)) for k in range(m)]

    def block_of(i, w):
        down = D // pitch
        row = pl.multiple_of(lax.rem(i, down) * pitch, 16)
        return wd_v.at[pl.ds(row, RB), pl.ds(pl.multiple_of((i // down) * W, 128), w)]

    def part_of(u, par, owner, w):
        return block_of((lax.rem(u, NP) * 2 + par) * NC + owner, w)

    def came_of(u, par, at, w):
        return block_of(NP * 2 * NC + (lax.rem(u, NR) * 2 + par) * (NC - 1) + at, w)

    def e_copy(u, par, k, n, w):
        order = orders[par]
        at = first_of[k] + n
        return remote(
            part_of(u, par, flips(c, sub_sums(order[k + 1:])[n] + order[k]), w), came_of(u, par, at, w),
            e_send.at[lax.rem(u, NP), par, at], e_recv.at[lax.rem(u, NR), par, at],
            along("ctx", flip(c, order[k])),
        )

    def e_each(k, act):
        for par in (0, 1):
            for n in range(NC >> (k + 1)):
                act(par, n)

    def e_sent(u, w):
        for k in range(m):
            e_each(k, lambda par, n: e_copy(u, par, k, n, w).wait_send())

    def e_send_step(u, k, w):
        e_each(k, lambda par, n: e_copy(u, par, k, n, w).start())

    def e_add(u, k, w):
        def one(par, n):
            e_copy(u, par, k, n, w).wait_recv()
            if k < m - 1:
                ref = part_of(u, par, flips(c, sub_sums(orders[par][k + 1:])[n]), w)
                ref[...] = (ref[...].astype(F32) + came_of(u, par, first_of[k] + n, w)[...].astype(F32)).astype(BF)

        e_each(k, one)

    chunks = [hid_pair, gate_pair, up_pair]

    def chunk_copy(u, kind):
        at = pl.ds(pl.multiple_of((u - kind * NF) * 2 * W, 128), 2 * W)
        return pltpu.make_async_copy(chunks[kind].at[:, :, :, at], Rc, r_sem.at[0])

    def for_kind(u, act):
        for kind in range(3):

            @pl.when((u >= kind * NF) & (u < (kind + 1) * NF))
            def _():
                act(kind)

    def branch_load(s):
        return pltpu.make_async_copy(branch_pair.at[:, s], L0.at[:, s], b_sem.at[s])

    def store(u, par, w, first, second):
        product = dot_tn(first.reshape(tokens, Dh), second)
        for owner in range(NC):
            part_of(u, par, owner, w)[...] = product[owner * RB:(owner + 1) * RB].astype(BF)

    def wide_product(u):
        for_kind(u, lambda kind: chunk_copy(u, kind).wait())
        def each(par, carry):
            second = Rc[:, :, :, pl.ds(pl.multiple_of(par * W, 128), W)].reshape(tokens, W)

            @pl.when(u < NF)
            def _():
                store(u, par, W, L0[...], second)

            if "L" in env:

                @pl.when(u >= NF)
                def _():
                    store(u, par, W, env["L"][0], second)

            return carry

        lax.fori_loop(0, 2, each, 0)
        for_kind(u + 1, lambda kind: chunk_copy(u + 1, kind).start())

    def out_copies(u, w):
        two = lax.rem(u, 2)

        def copy(par, dst):
            return pltpu.make_async_copy(st.at[two, par, :, pl.ds(0, w)], dst, st_sem.at[two, par])

        def columns(dst, base):
            return dst.at[:, pl.ds(pl.multiple_of(base, 128), w)]

        if w == W and w != narrow:
            spans = [(0, NF, down_o), (NF, 2 * NF, gate_o), (2 * NF, 3 * NF, up_o)]
        elif w == W:
            spans = [(0, NF, down_o), (NF, 2 * NF, gate_o), (2 * NF, 3 * NF, up_o)]
            spans += [(wide_units, q_first, wout_o), (q_first, kv_first, q_o)]
        else:
            spans = [(wide_units, q_first, wout_o), (q_first, kv_first, q_o)]
        found = [
            (
                (u >= low) & (u < high),
                [copy(p, columns(dst, (u - low) * 2 * w + p * w)) for p in (0, 1)],
            )
            for low, high, dst in spans
        ]
        if w == narrow:
            base = (u - kv_first) * w
            found.append(((u >= kv_first) & (u < units), [copy(0, columns(k_o, base)), copy(1, columns(v_o, base))]))
        return found

    widths = [W] if W == narrow else [W, narrow]

    def out_wait(u):
        for w in widths:
            for here, copies in out_copies(u, w):

                @pl.when(here)
                def _():
                    for copy in copies:
                        copy.wait()

    def e_finish(u, w):
        e_add(u, m - 1, w)
        out_wait(u - 2)
        for par in (0, 1):
            total = part_of(u, par, c, w)[...].astype(F32) + came_of(u, par, first_of[m - 1], w)[...].astype(F32)
            st[lax.rem(u, 2), par, :, :w] = total.astype(BF)
        for here, copies in out_copies(u, w):

            @pl.when(here)
            def _():
                for copy in copies:
                    copy.start()

    def by_width(u, body):
        @pl.when((u >= 0) & (u < wide_units))
        def _():
            body(W)

        @pl.when((u >= wide_units) & (u < units))
        def _():
            body(narrow)

    def compute_open(s):
        signal_all(free_sem, ctx_meets)

        def each(i, carry):
            branch_load(i).wait()
            return carry

        lax.fori_loop(0, C, each, 0)

    def stages(wg_v, wu_v, hid):
        env.update(hid=hid)
        def load_copies(i):
            height, turned_height = D // (2 * T), F // (2 * T)
            part = pl.ds(pl.multiple_of(i * height, 16), height)
            turned_part = pl.ds(pl.multiple_of(i * turned_height, 16), turned_height)
            inner = pl.ds(pl.multiple_of(lax.rem(i * height, Dh), 16), height)
            return (
                pltpu.make_async_copy(wg_ref.at[inner], wg_v.at[part], f_sem.at[0, i]),
                pltpu.make_async_copy(wg_other.at[part], wg_v.at[part], f_sem.at[0, i]),
                pltpu.make_async_copy(wut_ref.at[turned_part], wu_v.at[turned_part], f_sem.at[1, i]),
                pltpu.make_async_copy(wdt_ref.at[part], wd_v.at[part], f_sem.at[2, i]),
            )

        def load_start(i):
            own, other, up_part, down_part = load_copies(i)
            here = (i * (D // (2 * T))) // Dh == dp
            pl.when(here)(own.start)
            pl.when(jnp.logical_not(here))(other.start)
            up_part.start()
            down_part.start()

        def load_wait(which):
            def each(i, carry):
                load_copies(i)[which + 1].wait()
                return carry

            lax.fori_loop(0, 2 * T, each, 0)

        def gate_up(s, at):
            gate = dot_nn(rows_of(s), wg_v[:, at])
            up = dot_nt(rows_of(s), wu_v[at, :])
            inner = jnp.tanh(0.7978845608028654 * (gate + 0.044715 * gate * gate * gate))
            half = 0.5 * (1.0 + inner)
            gelu = gate * half
            slope = half + 0.5 * gate * (1.0 - inner * inner) * (
                0.7978845608028654 * (1.0 + 0.134145 * gate * gate)
            )
            hid[s, :, at] = (gelu * up).astype(BF)
            Ab[s, :, at] = (up * slope).astype(BF)
            Bb[s, :, at] = gelu.astype(BF)

        def gate_up_delta(s, at):
            delta = dot_nn(rows_of(s), wd_v[:, at])
            Ab[s, :, at] = (delta * Ab[s, :, at].astype(F32)).astype(BF)
            Bb[s, :, at] = (delta * Bb[s, :, at].astype(F32)).astype(BF)

        def tick(tau, carry):
            n, s = tau // C, lax.rem(tau, C)

            @pl.when(n >= 1)
            def _():
                rs_sent(s)

            @pl.when(n == 0)
            def _():
                load_start(2 * tau)

            @pl.when(n == 1)
            def _():
                @pl.when(s == 0)
                def _():
                    load_wait(0)
                    load_wait(1)

                pair_start(0, s)
                tiles(F, lambda at, tile: gate_up(s, at))
                pair_start(1, s)

            @pl.when(n == 2)
            def _():
                pair_start(2, s)
                tiles(F, lambda at, tile: gate_up_delta(s, at))
                pair_start(3, s)
                pair_start(4, s)
                pair_kept(2, s)
                pair_received(2, s)
                branch_load(s).start()

                @pl.when(s == 0)
                def _():
                    def each(i, carry):
                        pair_kept(1, i)
                        pair_received(1, i)
                        return carry

                    lax.fori_loop(0, C, each, 0)
                    chunk_copy(jnp.int32(0), 0).start()

            @pl.when(tau == begin)
            def _():
                compute_open(s)
                wide_product(jnp.int32(0))
                pl.semaphore_wait(free_sem, len(ctx_meets))
                e_send_step(jnp.int32(0), 0, W)

            for a in range(1, T):
                comm(tau, 2 * a - 1, a)

            @pl.when(n == 0)
            def _():
                load_start(2 * tau + 1)
                pair_start(6, s)
                heads = heads_ref[:, s].reshape(M, Hq)
                tiles(D, lambda at, tile: store_part(s, at, tile, dot_nn(heads, wo_v[:, at])))

            @pl.when(n == 1)
            def _():
                @pl.when(s == 0)
                def _():
                    load_wait(2)

                tiles(D, lambda at, tile: store_part(s, at, tile, dot_nt(hid[s], wd_v[at, :])))
                pair_kept(0, s)
                pair_away(0, s)
                ag_sent(s)

            @pl.when(n == 2)
            def _():
                tiles(
                    D,
                    lambda at, tile: store_part(
                        s, at, tile, dot_nt(Ab[s], wg_v[at, :]) + dot_nn(Bb[s], wu_v[:, at])
                    ),
                )
                pair_away(2, s)
                ag_sent(s)

            @pl.when((n < 2) | (tau == begin))
            def _():
                rs_start(jnp.where(n < 2, s, 0))

            for a in range(1, T):
                comm(tau, 2 * a, a)
            return carry

        lax.fori_loop(0, 3 * C, tick, 0)

        def leave(s, carry):
            pair_away(1, s)
            return carry

        lax.fori_loop(0, C, leave, 0)
        del env["hid"]

    def finishing(L, Hd, RQ, RKV, WQ, WK, WV, dq, rdelta, kvb, kvs, kvr, acc2, qv, cos_v, sin_v):
        env["L"] = L
        signal_all(enter_sem, later + partners)
        rows_load = pltpu.make_async_copy(rows_pair, L.at[0], l_sem.at[1])
        attn_load = pltpu.make_async_copy(attn_pair, L.at[1], l_sem.at[2])
        rows1_load = pltpu.make_async_copy(rows1_ref, L.at[0], l_sem.at[1])
        head_load = pltpu.make_async_copy(head_pair, Hd, l_sem.at[3])
        small_loads = [
            pltpu.make_async_copy(src, dst, q_sem.at[i])
            for i, (src, dst) in enumerate([(q_ref, qv), (cos_ref, cos_v), (sin_ref, sin_v)])
        ]
        for copy in small_loads:
            copy.start()
        out_copy = pltpu.make_async_copy(out_ref, out_o, l_sem.at[4])
        igrad_copy = pltpu.make_async_copy(igrad_ref, igrad_o, l_sem.at[5])
        out_copy.start()

        rows_at = pl.ds(pl.multiple_of(dp * Dh, 128), Dh)
        spread = [(wq_ref, WQ.at[rows_at]), (wk_ref, WK.at[rows_at]), (wv_ref, WV.at[rows_at])]

        def spread_local(i):
            return pltpu.make_async_copy(*spread[i], s_sem.at[0, i])

        def spread_remote(i, o):
            return remote(*spread[i], s_sem.at[1 + 2 * o, i], s_sem.at[2 + 2 * o, i], partners[o])

        def pair_remote(i, o):
            ref = [RQ, RKV][i]
            return remote(ref.at[dp], ref.at[dp], q_sem.at[3 + 4 * o + 2 * i], q_sem.at[4 + 4 * o + 2 * i], partners[o])

        def deltas_of(head):
            return hdelta[:, :, :, head].reshape(R, HEAD)

        per = max(1, 256 // Lr)
        key_tile = per * Lr

        def kv_copy(d):
            return remote(
                kvs.at[lax.rem(d, kvs.shape[0])], kvr.at[d - 1], kv_send.at[d - 1], kv_recv.at[d - 1],
                along("ctx", jnp.maximum(c - d, 0)),
            )

        def block_copy(block):
            two = lax.rem(block, 2)
            return pltpu.make_async_copy(kv_ref.at[block], kvb.at[two], kvb_sem.at[two])

        def attend(two, masked, dst):
            for kh in range(KH):
                cols = slice(kh * HEAD, (kh + 1) * HEAD)

                def key_step(i, carry):
                    start = pl.multiple_of(i * key_tile, key_tile)
                    at = pl.ds(i * per, per)
                    keys = kvb[two, at, 0, :, cols].reshape(key_tile, HEAD)
                    values = kvb[two, at, 1, :, cols].reshape(key_tile, HEAD)
                    key_sum = jnp.zeros((key_tile, HEAD), F32)
                    value_sum = jnp.zeros((key_tile, HEAD), F32)
                    for g in range(GS):
                        h = kh * GS + g
                        head = slice(h * HEAD, (h + 1) * HEAD)
                        query, delta = qv[:, head], deltas_of(head)
                        bent = jnp.tanh(dot_nt(keys, query) * (scale / CAP))
                        prob = jnp.exp(CAP * bent - logt_ref[h:h + 1, :])
                        if masked:
                            key_pos = start + lax.broadcasted_iota(jnp.int32, prob.shape, 0)
                            prob = jnp.where(key_pos <= lax.broadcasted_iota(jnp.int32, prob.shape, 1), prob, 0.0)
                        grad = prob * (dot_nt(values, delta) - rdelta[h:h + 1, :]) * (1.0 - bent * bent)
                        grad = grad.astype(BF)
                        value_sum += dot_nn(prob.astype(BF), delta)
                        key_sum += dot_nn(grad, query)
                        dq[:, head] += dot_tn(grad, keys)
                    rows = pl.ds(start, key_tile)
                    kvs[dst, 0, rows, cols] = (key_sum * scale).astype(BF)
                    kvs[dst, 1, rows, cols] = value_sum.astype(BF)
                    return carry

                lax.fori_loop(0, R // key_tile, key_step, 0)

        def attention():
            dq[...] = jnp.zeros_like(dq)
            for h in range(Hq // HEAD):
                head = slice(h * HEAD, (h + 1) * HEAD)
                product = deltas_of(head).astype(F32) * heads_ref[:, :, :, head].reshape(R, HEAD).astype(F32)
                rdelta[h:h + 1] = jnp.sum(product.T, axis=0, keepdims=True)
            block_copy(0).start()

            def far(block, carry):
                d = c - block

                @pl.when(block < c)
                def _():
                    slot = lax.rem(d, kvs.shape[0])
                    block_copy(block).wait()
                    block_copy(block + 1).start()

                    @pl.when(d + kvs.shape[0] <= c)
                    def _():
                        kv_copy(d + kvs.shape[0]).wait_send()

                    attend(lax.rem(block, 2), False, slot)
                    kv_copy(d).start()

                return carry

            lax.fori_loop(0, NC - 1, far, 0)

            @pl.when(c >= kvs.shape[0])
            def _():
                kv_copy(kvs.shape[0]).wait_send()

            block_copy(c).wait()
            attend(lax.rem(c, 2), True, 0)

        def turned(values, h):
            a, b = values[:, h * HEAD:h * HEAD + HEAD // 2], values[:, h * HEAD + HEAD // 2:(h + 1) * HEAD]
            cosine, sine = cos_v[...], sin_v[...]
            return jnp.concatenate([a * cosine + b * sine, b * cosine - a * sine], axis=1).astype(BF)

        def last_copy(side, k, j):
            if side == 0:
                slot, peer = j, right
            else:
                slot, peer = jnp.where(j == t - 1, T, j), left
            return remote(Pb.at[:, j], Rb.at[:, slot], last_send.at[side, k], last_recv.at[side, k], peer)

        def last_step(k):
            for side in (0, 1):
                j = rs_block(side, k)

                @pl.when(rs_sends(side, k))
                def _():
                    if k:

                        @pl.when(has_left if side == 0 else has_right)
                        def _():
                            last_copy(side, k - 1, j).wait_recv()
                            Pb[:, j] = (Pb[:, j].astype(F32) + Rb[:, j].astype(F32)).astype(BF)

                    last_copy(side, k, j).start()

        def own_keys():
            for which in range(2):
                dst = []
                for kh in range(KH):
                    dst.append(kvs[0, which, :, kh * HEAD:(kh + 1) * HEAD].astype(F32))
                acc2[which] = jnp.concatenate(dst, axis=1) if KH > 1 else dst[0]

            def come(i, carry):
                d = i + 1

                @pl.when(c + d <= NC - 1)
                def _():
                    kv_copy(d).wait_recv()
                    for which in range(2):
                        acc2[which] += kvr[d - 1, which].astype(F32)

                return carry

            lax.fori_loop(0, NC - 1, come, 0)
            for kh in range(KH):
                cols = slice(kh * HEAD, (kh + 1) * HEAD)
                RKV[dp, 0, :, cols] = turned(acc2[0], kh)
            RKV[dp, 1] = acc2[1].astype(BF)
            for h in range(Hq // HEAD):
                RQ[dp, :, h * HEAD:(h + 1) * HEAD] = turned(dq[...] * scale, h)
            for i in range(2):
                for o in range(NDP - 1):
                    pair_remote(i, o).start()
            for i in range(3):
                spread_local(i).wait()
                for o in range(NDP - 1):
                    spread_remote(i, o).wait_recv()
            tile = tile_of(D)

            def part(i, carry):
                at = pl.ds(pl.multiple_of(i * tile, tile), tile)
                terms = dot_nt(RQ[dp], WQ[at, :]) + dot_nt(RKV[dp, 0], WK[at, :]) + dot_nt(RKV[dp, 1], WV[at, :])
                terms = terms.astype(BF).reshape(T, C, rc, tile)
                for s in range(C):
                    Pb[s, :, :, at] = terms[:, s]
                return carry

            lax.fori_loop(0, D // tile, part, 0)
            last_step(0)

        def last_finish():
            igrad_ref[...] = Pb[:, t].reshape(Lr, D).astype(F32)

            @pl.when(has_left)
            def _():
                last_copy(0, T - 2, t).wait_recv()
                igrad_ref[...] += Rb[:, t].reshape(Lr, D).astype(F32)

            @pl.when(has_right)
            def _():
                last_copy(1, T - 2, t).wait_recv()
                igrad_ref[...] += Rb[:, T].reshape(Lr, D).astype(F32)

            rows = x_ref[...].astype(F32)
            grad, terms = rms_back(rows, inverse_rms(rows), gain_ref[0:1], igrad_ref[...])
            igrad_ref[...] = mdelta[...] + grad
            G[0, 0:1] = terms
            G[0, 1:4] = gsum[...]

        meets = [("tp", t, T), ("ctx", c, NC), ("dp", dp, NDP)]
        g_base = [0, T - 1, T + NC - 2]

        def g_copies(k):
            axis, index, count = meets[k]
            return [
                remote(
                    G.at[k], GR.at[g_base[k] + o - 1], g_send.at[g_base[k] + o - 1], g_recv.at[g_base[k] + o - 1],
                    along(axis, lax.rem(index + o, count)),
                )
                for o in range(1, count)
            ]

        def g_start(k):
            for copy in g_copies(k):
                copy.start()

        def g_steps(i, place):
            for k in range(len(meets)):
                if k != place:
                    continue

                @pl.when(i == attend_at + T + 2)
                def _():
                    total = G[k]
                    for o, copy in enumerate(g_copies(k)):
                        copy.wait_recv()
                        total += GR[g_base[k] + o]
                    G[k + 1] = total
                    if k + 1 < len(meets):
                        g_start(k + 1)

        def up_open():
            def each(s, carry):
                for kind in (3, 4):
                    pair_kept(kind, s)
                    pair_received(kind, s)
                pair_received(0, s)
                return carry

            lax.fori_loop(0, C, each, 0)
            rows_load.start()

        def attn_open():
            def each(s, carry):
                for kind in (5, 6):
                    pair_kept(kind, s)
                    pair_received(kind, s)
                return carry

            lax.fori_loop(0, C, each, 0)
            attn_load.start()
            head_load.start()

        def product(u, w):
            @pl.when(u < wide_units)
            def _():
                @pl.when(u == NF)
                def _():
                    rows_load.wait()

                @pl.when(u == NF - 1)
                def _():
                    up_open()

                wide_product(u)

                @pl.when(u == wide_units - 1)
                def _():
                    attn_open()

            if w == narrow:

                def columns(first, par):
                    return pl.ds(pl.multiple_of(((u - first) * 2 + par) * narrow, 128), narrow)

                @pl.when((u >= wide_units) & (u < q_first))
                def _():
                    @pl.when(u == wide_units)
                    def _():
                        attn_load.wait()
                        head_load.wait()
                        rows1_load.start()

                    def out_part(par, carry):
                        second = Hd[:, :, :, :, columns(wide_units, par)]
                        store(u, par, narrow, L[1], second.reshape(tokens, narrow))
                        return carry

                    lax.fori_loop(0, 2, out_part, 0)

                @pl.when(u == q_first)
                def _():
                    rows1_load.wait()
                    for p in range(2):
                        for o in range(NDP - 1):
                            pair_remote(p, o).wait_recv()

                @pl.when((u >= q_first) & (u < kv_first))
                def _():
                    def query_part(par, carry):
                        store(u, par, narrow, L[0], RQ[:, :, columns(q_first, par)].reshape(tokens, narrow))
                        return carry

                    lax.fori_loop(0, 2, query_part, 0)

                @pl.when(u >= kv_first)
                def _():
                    at = pl.ds(pl.multiple_of((u - kv_first) * narrow, 128), narrow)
                    def key_part(par, carry):
                        store(u, par, narrow, L[0], RKV[:, par, :, at].reshape(tokens, narrow))
                        return carry

                    lax.fori_loop(0, 2, key_part, 0)

        attend_at = C + 1

        def first_tick(i):
            return begin + 1 + i + jnp.minimum(i // 2, C - 2)

        def line_tick(tau):
            for a in range(1, T):
                comm(tau, 2 * a - 1, a)

            @pl.when(tau < begin + C)
            def _():
                rs_start(tau - begin)

            @pl.when(tau >= begin + C)
            def _():
                s = tau - begin - C
                pair_start(5, s)
                hdelta[:, s] = dot_nt(rows_of(s), wo_v[...]).astype(BF).reshape(T, rc, Hq)
                rs_sent(s)

            for a in range(1, T):
                comm(tau, 2 * a, a)

        def tick(i, carry):
            u = i + 1

            def start(w):
                @pl.when(u >= NP)
                def _():
                    by_width(u - NP, lambda before: e_sent(u - NP, before))

                product(u, w)
                e_send_step(u, 0, w)

            by_width(u, start)
            g_steps(i, 0)

            @pl.when(i == 1)
            def _():
                pl.semaphore_wait(enter_sem, len(later + partners))
                for w in range(3):
                    spread_local(w).start()
                    for o in range(NDP - 1):
                        spread_remote(w, o).start()

            @pl.when(i < attend_at)
            def _():
                line_tick(first_tick(i))

            @pl.when(i == attend_at)
            def _():
                for copy in small_loads:
                    copy.wait()
                attention()

            @pl.when(i == attend_at + 2)
            def _():
                own_keys()

            for k in range(1, T - 1):

                @pl.when(i == attend_at + 2 + k)
                def _():
                    last_step(k)

            @pl.when(i == attend_at + T + 1)
            def _():
                last_finish()
                igrad_copy.start()
                g_start(0)

            for k in range(1, m):

                def middle(w):
                    e_add(u - k, k - 1, w)
                    e_send_step(u - k, k, w)

                by_width(u - k, middle)

            @pl.when((lax.rem(i, 2) == 1) & (i <= 2 * C - 5))
            def _():
                line_tick(first_tick(i) + 1)

            g_steps(i, 1)
            by_width(u - m, lambda w: e_finish(u - m, w))
            g_steps(i, 2)
            return carry

        lax.fori_loop(0, units + m - 1, tick, 0)
        gains_ref[...] = G[len(meets)]
        out_copy.wait()
        igrad_copy.wait()

        for u in (units - 2, units - 1):
            out_wait(jnp.int32(u))
        for u in range(units - NP, units):
            by_width(jnp.int32(u), lambda w: e_sent(jnp.int32(u), w))
        for side in (0, 1):
            for k in range(T - 1):

                @pl.when(rs_sends(side, k))
                def _():
                    last_copy(side, k, rs_block(side, k)).wait_send()

        for k in range(len(meets)):
            for copy in g_copies(k):
                copy.wait_send()
        for o in range(NDP - 1):
            for i in range(3):
                spread_remote(i, o).wait_send()
            for i in range(2):
                pair_remote(i, o).wait_send()

        def kv_close(i, carry):
            d = i + 1

            @pl.when((d <= c) & (d < kvs.shape[0]))
            def _():
                kv_copy(d).wait_send()

            return carry

        lax.fori_loop(0, min(NC - 1, kvs.shape[0] - 1), kv_close, 0)

        def close(s, carry):
            for kind in (3, 4, 5, 6):
                pair_away(kind, s)
            ag_sent(s)
            return carry

        lax.fori_loop(0, C, close, 0)

    for copy in out_loads:
        copy.wait()
    vmem = pltpu.VMEM
    pl.run_scoped(
        stages, vmem((D, F), BF), vmem((F, D), BF), vmem((C, M, F), BF)
    )
    kv_slots = NC if NC <= 4 else 3
    pl.run_scoped(
        finishing,
        vmem((2, NDP, C, T, rc, Dh), BF), vmem((NDP, C, T, rc, Hq), BF),
        vmem((NDP, R, Hq), BF), vmem((NDP, 2, R, KVd), BF),
        vmem((D, Hq), BF), vmem((D, KVd), BF), vmem((D, KVd), BF),
        vmem((R, Hq), F32), vmem((Hq // HEAD, R), F32), vmem((2, T, 2, Lr, KVd), BF),
        vmem((kv_slots, 2, R, KVd), BF), vmem((NC - 1, 2, R, KVd), BF), vmem((2, R, KVd), F32),
        vmem((R, Hq), BF), vmem((R, HEAD // 2), F32), vmem((R, HEAD // 2), F32),
    )


def main_call(
    layer_in, cotangent, norm_gains, head_rows, w_out, w_gate, out_other, gate_other, up_turned, down_turned,
    query, log_totals, cosine, sine, keys_values, rows_one, w_query, w_key, w_value,
):
    T, NC, NDP = lax.axis_size("tp"), lax.axis_size("ctx"), lax.axis_size("dp")
    C = T
    Lr, D = layer_in.shape
    rc = Lr // C
    R, Hq = query.shape
    KVd = w_key.shape[1]
    Dh, RB = D // NDP, D // NDP // NC
    F = w_gate.shape[1]
    M = T * rc
    m = NC.bit_length() - 1
    NP, NR = m + 1, 4
    pitch = -(-RB // 16) * 16
    blocks = NP * 2 * NC + NR * 2 * (NC - 1)
    W = next(w for w in (tile_of(F) // 2, 256, 128) if F % (2 * w) == 0 and blocks <= (D // pitch) * (F // w))
    meets = T + NC + NDP - 3
    any_spec = pl.BlockSpec(memory_space=pl.ANY)
    vm = pl.BlockSpec(memory_space=pltpu.VMEM)
    sds = jax.ShapeDtypeStruct
    dma = pltpu.SemaphoreType.DMA
    vmem = pltpu.VMEM
    half_rows = sds((NDP, C, T, rc, Dh), BF)
    hidden_rows = sds((NDP, C, M, F), BF)
    outs = pl.pallas_call(
        functools.partial(main_kernel, T, C, NC, NDP, KVd // HEAD, NP, NR),
        out_shape=(
            sds((Lr, D), BF), sds((Lr, D), F32), sds((4, D), F32),
            sds((RB, F), BF), sds((RB, F), BF), sds((RB, F), BF), sds((RB, Hq), BF),
            sds((RB, Hq), BF), sds((RB, KVd), BF), sds((RB, KVd), BF),
            half_rows, hidden_rows, half_rows, hidden_rows, hidden_rows, half_rows, sds((NDP, C, T, rc, Hq), BF),
        ),
        in_specs=[vm] * 4 + [any_spec] * 7 + [vm] + [any_spec] * 7,
        out_specs=[any_spec] * 2 + [vm] + [any_spec] * 14,
        scratch_shapes=[
            vmem((Lr, D), BF), vmem((Lr, D), F32),
            vmem((Hq, D), BF), vmem((D, F), BF), vmem((C, T, rc, D), BF), vmem((C, T, rc, D), BF),
            vmem((C, T + 1, rc, D), BF), vmem((C, rc, D), F32), vmem((C, rc, D), F32), vmem((rc, D), F32),
            vmem((Lr, D), F32), vmem((3, D), F32), vmem((T, C, rc, Hq), BF), vmem((C, M, F), BF), vmem((C, M, F), BF),
            vmem((NDP, C, T, rc, Dh), BF), vmem((NDP, C, M, 2 * W), BF), vmem((2, 2, RB, W), BF),
            vmem((4, 4, D), F32), vmem((meets, 4, D), F32),
            dma((NDP,)), dma((3, 2 * T)), dma((C,)), dma((C, 2, T - 1)), dma((C, 2, T - 1)), dma((C, 2, T - 1)), dma((C, 2, T - 1)),
            dma((2 * NDP - 1, 7, C)), dma((6,)), dma((1,)), dma((NP, 2, NC - 1)), dma((NR, 2, NC - 1)), dma((2, 2)),
            dma((2 * NDP - 1, 3)), dma((3 + 4 * (NDP - 1),)), dma((NC - 1,)), dma((NC - 1,)),
            dma((2, T - 1)), dma((2, T - 1)), dma((meets,)), dma((meets,)), dma((2,)),
            pltpu.SemaphoreType.REGULAR, pltpu.SemaphoreType.REGULAR,
        ],
        compiler_params=pltpu.CompilerParams(
            collective_id=0, has_side_effects=True, vmem_limit_bytes=67_043_328
        ),
        name="main",
    )(
        layer_in, cotangent, norm_gains, head_rows.reshape(T, C, rc, Hq), w_out, w_gate, out_other, gate_other,
        up_turned, down_turned, query, log_totals, cosine, sine, keys_values,
        rows_one.reshape(NDP, C, T, rc, Dh), w_query, w_key, w_value,
    )
    return outs[:10]


def front_kernel(
    T, NC, NDP, KH, C,
    x_ref, gain_ref, freq_ref, wq_ref, wk_ref, wv_ref, wo_ref, wg_ref, wu_ref, wd_ref,
    q_o, heads_o, logt_o, cos_o, sin_o, kv_o, rows1_o, wo_o, wg_o, wut_o, wdt_o,
    X, WQ, WK, WV, KV, turned_sum, totals, up_v, upt_v, down_v, downt_v,
    w_sem, ag_send, ag_recv, pair_sem, kv_send, kv_recv, out_sem, t_sem, p_sem,
):
    t, c, dp = lax.axis_index("tp"), lax.axis_index("ctx"), lax.axis_index("dp")
    Lr, D = x_ref.shape
    R, Hq = q_o.shape
    rc = Lr // C
    KVd = KH * HEAD
    GS = Hq // KVd
    Dh = D // NDP
    scale = HEAD**-0.5
    has_left, has_right = t > 0, t < T - 1

    def remote(src, dst, send, recv, axis, index):
        return pltpu.make_async_remote_copy(
            src, dst, send, recv, device_id={axis: index}, device_id_type=MESH
        )

    partners = [lax.rem(dp + o, NDP) for o in range(1, NDP)]
    peers = [("tp", lax.rem(t + o, T)) for o in range(1, T)]
    peers += [("ctx", lax.rem(c + o, NC)) for o in range(1, NC)]
    peers += [("dp", p) for p in partners]
    sem = pltpu.get_barrier_semaphore()
    for axis, index in peers:
        pl.semaphore_signal(sem, inc=1, device_id={axis: index}, device_id_type=MESH)

    rows_at = pl.ds(pl.multiple_of(dp * Dh, 128), Dh)
    weights = [(wq_ref, WQ), (wk_ref, WK), (wv_ref, WV)]

    def weight_local(i):
        return pltpu.make_async_copy(weights[i][0], weights[i][1].at[rows_at], w_sem.at[0, i])

    def weight_remote(i, o):
        return remote(
            weights[i][0], weights[i][1].at[rows_at], w_sem.at[1 + 2 * o, i], w_sem.at[2 + 2 * o, i],
            "dp", partners[o],
        )

    turns = [
        pltpu.make_async_copy(wu_ref, up_v, t_sem.at[0]),
        pltpu.make_async_copy(wd_ref, down_v, t_sem.at[1]),
    ]
    for i in range(3):
        weight_local(i).start()
    for copy in turns:
        copy.start()
    rows = x_ref[...].astype(F32)
    X[t] = (rows * inverse_rms(rows) * gain_ref[0:1]).astype(BF)
    pl.semaphore_wait(sem, len(peers))

    def ag_copy(s, side, k, j):
        at = pl.ds(s * rc, rc)
        peer = jnp.minimum(t + 1, T - 1) if side == 0 else jnp.maximum(t - 1, 0)
        return remote(X.at[j, at], X.at[j, at], ag_send.at[s, side, k], ag_recv.at[s, side, k], "tp", peer)

    def ag_block(side, k):
        return (t - k) if side == 0 else (t + k)

    def ag_there(side, k):
        return (t >= k) if side == 0 else (t + k <= T - 1)

    def onward(side):
        return has_right if side == 0 else has_left

    for s in range(C):
        for side in (0, 1):

            @pl.when(onward(side))
            def _():
                ag_copy(s, side, 0, t).start()

    for i in range(3):
        for o in range(NDP - 1):
            weight_remote(i, o).start()

    def parts(ref, i):
        height = ref.shape[0] // (2 * T)
        return pl.ds(pl.multiple_of(i * height, 16), height), height

    def part_dst(dst, ref, i, columns):
        at, height = parts(ref, i)
        if columns:
            return dst.at[at, rows_at]
        return dst.at[pl.ds(pl.multiple_of(dp * Dh + i * height, 16), height)]

    moved = [(wo_ref, wo_o, True, False), (wg_ref, wg_o, False, False)]
    moved += [(upt_v, wut_o, True, True), (downt_v, wdt_o, False, True)]

    def part_remote(w, i, o):
        src, dst, columns, _ = moved[w]
        return remote(
            src.at[parts(src, i)[0]], part_dst(dst, src, i, columns),
            p_sem.at[1 + 2 * o, w, i], p_sem.at[2 + 2 * o, w, i], "dp", partners[o],
        )

    def part_local(w, i):
        src, dst, columns, _ = moved[w]
        return pltpu.make_async_copy(src.at[parts(src, i)[0]], part_dst(dst, src, i, columns), p_sem.at[0, w, i])

    def part_start(w, i):
        for o in range(NDP - 1):
            part_remote(w, i, o).start()
        if moved[w][3]:
            part_local(w, i).start()

    def turn():
        for copy, src, dst in zip(turns, (up_v, down_v), (upt_v, downt_v), strict=True):
            copy.wait()
            height = src.shape[0] // T

            def some(i, carry):
                at = pl.ds(pl.multiple_of(i * height, 128), height)
                dst[:, at] = src[at, :].T
                return carry

            if height % 128 == 0:
                lax.fori_loop(0, T, some, 0)
            else:
                dst[...] = src[...].T

    position = (c * R + lax.broadcasted_iota(jnp.int32, (R, HEAD // 2), 0)).astype(F32)
    angles = position * freq_ref[...]
    cos_o[...] = jnp.cos(angles)
    sin_o[...] = jnp.sin(angles)
    for i in range(3):
        weight_local(i).wait()
        for o in range(NDP - 1):
            weight_remote(i, o).wait_recv()

    def kv_copy(d, j):
        return remote(
            KV.at[c, j], KV.at[c, j], kv_send.at[d - 1, j], kv_recv.at[d - 1, j],
            "ctx", jnp.minimum(c + d, NC - 1),
        )

    def kv_from(b, j):
        d = c - b
        return remote(KV.at[b, j], KV.at[b, j], kv_send.at[d - 1, j], kv_recv.at[d - 1, j], "ctx", c)

    def pair_copies(j):
        def half(owner):
            return X.at[j, :, pl.ds(pl.multiple_of(owner * Dh, 128), Dh)]

        copies = [pltpu.make_async_copy(half(dp), rows1_o.at[dp, j], pair_sem.at[0, j])]
        for o, partner in enumerate(partners):
            copies.append(
                remote(
                    half(partner), rows1_o.at[dp, j], pair_sem.at[1 + 2 * o, j], pair_sem.at[2 + 2 * o, j],
                    "dp", partner,
                )
            )
        return copies

    def turned(values, h, at):
        a, b = values[:, h * HEAD:h * HEAD + HEAD // 2], values[:, h * HEAD + HEAD // 2:(h + 1) * HEAD]
        cosine, sine = cos_o[at], sin_o[at]
        return jnp.concatenate([a * cosine - b * sine, b * cosine + a * sine], axis=1).astype(BF)

    def project(j):
        for copy in pair_copies(j):
            copy.start()
        at = pl.ds(pl.multiple_of(j * Lr, Lr), Lr)
        values = dot_nn(X[j], WK[...])
        for kh in range(KH):
            KV[c, j, 0, :, kh * HEAD:(kh + 1) * HEAD] = turned(values, kh, at)
        KV[c, j, 1] = dot_nn(X[j], WV[...]).astype(BF)

        def push(i, carry):
            @pl.when(c + 1 + i <= NC - 1)
            def _():
                kv_copy(i + 1, j).start()

            return carry

        lax.fori_loop(0, NC - 1, push, 0)
        values = dot_nn(X[j], WQ[...])
        for h in range(Hq // HEAD):
            q_o[at, h * HEAD:(h + 1) * HEAD] = turned(values, h, at)

    has_late = (t == 0) | (t == T - 1)
    late = jnp.where(t == 0, T - 1, 0)
    late_at = pl.ds(pl.multiple_of(late * Lr, Lr), Lr)

    def out_copy(b):
        return pltpu.make_async_copy(KV.at[b], kv_o.at[b], out_sem.at[b])

    def key_step(b, first, count, masked, queries):
        tile = count * Lr
        for kh in range(KH):
            cols = slice(kh * HEAD, (kh + 1) * HEAD)
            keys = KV[b, pl.ds(first, count), 0, :, cols].reshape(tile, HEAD)
            values = KV[b, pl.ds(first, count), 1, :, cols].reshape(tile, HEAD)
            for g in range(GS):
                h = kh * GS + g
                head = slice(h * HEAD, (h + 1) * HEAD)
                query = q_o[late_at, head] if queries == "late" else q_o[:, head]
                weights = jnp.exp(CAP * jnp.tanh(dot_nt(keys, query) * (scale / CAP)))
                query_pos = lax.broadcasted_iota(jnp.int32, weights.shape, 1)
                if queries == "late":
                    query_pos += late * Lr
                if masked:
                    key_pos = first * Lr + lax.broadcasted_iota(jnp.int32, weights.shape, 0)
                    weights = jnp.where(key_pos <= query_pos, weights, 0.0)
                if queries == "early":
                    weights = jnp.where(query_pos // Lr == late, 0.0, weights)
                at = late_at if queries == "late" else slice(None)
                totals[h:h + 1, at] += jnp.sum(weights, axis=0, keepdims=True)
                turned_sum[h, :, at] += dot_tn(values, weights.astype(BF))

    def by_block(b, body):
        pl.when(b == c)(lambda: body(True))
        pl.when(b < c)(lambda: body(False))

    def early_rows():
        turned_sum[...] = jnp.zeros_like(turned_sum)
        totals[...] = jnp.zeros_like(totals)

        def block(i, carry):
            b = c - i

            @pl.when(b >= 0)
            def _():
                def rows_of(j, inner):
                    @pl.when(jnp.logical_not(has_late) | (j != late))
                    def _():
                        pl.when(b < c)(lambda: kv_from(b, j).wait_recv())
                        by_block(b, lambda masked: key_step(b, j, 1, masked, "all"))

                    return inner

                lax.fori_loop(0, T, rows_of, 0)

            return carry

        lax.fori_loop(0, NC, block, 0)

    def late_rows():
        @pl.when(has_late)
        def _():
            for h in range(Hq // HEAD):
                turned_sum[h, :, late_at] = jnp.zeros((HEAD, Lr), F32)
                totals[h:h + 1, late_at] = jnp.zeros((1, Lr), F32)

        def block(i, carry):
            b = c - i

            @pl.when(b >= 0)
            def _():
                @pl.when(has_late)
                def _():
                    pl.when(b < c)(lambda: kv_from(b, late).wait_recv())

                    def both(masked):
                        key_step(b, 0, T, masked, "late")
                        key_step(b, late, 1, masked, "early")

                    by_block(b, both)

                out_copy(b).start()

            return carry

        lax.fori_loop(0, NC, block, 0)

    def gather(k, carry):
        pl.when(k == T - 1)(early_rows)
        for side in (0, 1):

            @pl.when(ag_there(side, k) & (k > 0))
            def _():
                for s in range(C):
                    ag_copy(s, side, k - 1, ag_block(side, k)).wait_recv()

                    @pl.when(onward(side) & (k <= T - 2))
                    def _():
                        ag_copy(s, side, k, ag_block(side, k)).start()

        for side in (0, 1):

            @pl.when(ag_there(side, k) & ((k > 0) | (side == 0)))
            def _():
                project(ag_block(side, k))

        pl.when(k == 0)(turn)

        def send_parts(i, inner):
            for w in range(4):
                part_start(w, i)
            return inner

        lax.fori_loop((2 * T * k) // (T - 1), jnp.minimum((2 * T * (k + 1)) // (T - 1), 2 * T), send_parts, 0)
        return carry

    lax.fori_loop(0, T, gather, 0)

    late_rows()
    for h in range(Hq // HEAD):
        heads_o[:, h * HEAD:(h + 1) * HEAD] = (turned_sum[h] / totals[h:h + 1]).T.astype(BF)
    logt_o[...] = jnp.log(totals[...])

    for i in range(3):
        for o in range(NDP - 1):
            weight_remote(i, o).wait_send()

    def close_parts(i, carry):
        for w in range(4):
            for o in range(NDP - 1):
                part_remote(w, i, o).wait()
            if moved[w][3]:
                part_local(w, i).wait()
        return carry

    lax.fori_loop(0, 2 * T, close_parts, 0)
    for s in range(C):
        for side in (0, 1):
            for k in range(T - 1):

                @pl.when(ag_there(side, k) & onward(side))
                def _():
                    ag_copy(s, side, k, ag_block(side, k)).wait_send()

    for j in range(T):
        copies = pair_copies(j)
        copies[0].wait()
        for copy in copies[1:]:
            copy.wait()

    def close(i, carry):
        @pl.when(c + 1 + i <= NC - 1)
        def _():
            for j in range(T):
                kv_copy(i + 1, j).wait_send()

        return carry

    lax.fori_loop(0, NC - 1, close, 0)

    def close_out(b, carry):
        @pl.when(b <= c)
        def _():
            out_copy(b).wait()

        return carry

    lax.fori_loop(0, NC, close_out, 0)


def front_call(layer_in, norm_gains, frequency, w_query, w_key, w_value, w_out, w_gate, w_up, w_down):
    T, NC, NDP = lax.axis_size("tp"), lax.axis_size("ctx"), lax.axis_size("dp")
    C = T
    Lr, D = layer_in.shape
    R = T * Lr
    Hq, KVd = w_query.shape[1], w_key.shape[1]
    Dh = D // NDP
    F = w_gate.shape[1]
    H = Hq // HEAD
    any_spec = pl.BlockSpec(memory_space=pl.ANY)
    vm = pl.BlockSpec(memory_space=pltpu.VMEM)
    sds = jax.ShapeDtypeStruct
    dma = pltpu.SemaphoreType.DMA
    return pl.pallas_call(
        functools.partial(front_kernel, T, NC, NDP, KVd // HEAD, C),
        out_shape=(
            sds((R, Hq), BF), sds((R, Hq), BF), sds((H, R), F32),
            sds((R, HEAD // 2), F32), sds((R, HEAD // 2), F32),
            sds((NC, T, 2, Lr, KVd), BF), sds((NDP, T, Lr, Dh), BF),
            sds((Hq, D), BF), sds((D, F), BF), sds((F, D), BF), sds((D, F), BF),
        ),
        in_specs=[vm] * 3 + [any_spec] * 7,
        out_specs=[vm] * 5 + [any_spec] * 6,
        scratch_shapes=[
            pltpu.VMEM((T, Lr, D), BF), pltpu.VMEM((D, Hq), BF), pltpu.VMEM((D, KVd), BF), pltpu.VMEM((D, KVd), BF),
            pltpu.VMEM((NC, T, 2, Lr, KVd), BF), pltpu.VMEM((H, HEAD, R), F32), pltpu.VMEM((H, R), F32),
            pltpu.VMEM((Dh, F), BF), pltpu.VMEM((F, Dh), BF), pltpu.VMEM((F, Dh), BF), pltpu.VMEM((Dh, F), BF),
            dma((2 * NDP - 1, 3)), dma((C, 2, T - 1)), dma((C, 2, T - 1)), dma((2 * NDP - 1, T)),
            dma((NC - 1, T)), dma((NC - 1, T)), dma((NC,)), dma((2,)), dma((2 * NDP - 1, 4, 2 * T)),
        ],
        compiler_params=pltpu.CompilerParams(
            collective_id=2, has_side_effects=True, vmem_limit_bytes=66_000_000
        ),
        name="front",
    )(layer_in, norm_gains, frequency, w_query, w_key, w_value, w_out, w_gate, w_up, w_down)


def finish_kernel(width, count, gains_ref, *refs):
    n = count
    srcs, gain_o, dsts = refs[:n], refs[n], refs[n + 1:2 * n + 1]
    held, wide, sems = refs[2 * n + 1:3 * n + 1], refs[3 * n + 1:-1], refs[-1]
    for i in range(n):
        pltpu.make_async_copy(srcs[i], held[i], sems.at[0, i]).start()
    rank = lax.axis_index("dp")
    for axis in ("ctx", "tp"):
        rank = rank * lax.axis_size(axis) + lax.axis_index(axis)
    gains = gains_ref[...]
    total = gains.shape[1]
    gain_o[...] = pltpu.roll(gains, lax.rem(total - rank * width, total), axis=1)[:4, :width]
    buffers = []
    for i in range(n):
        pltpu.make_async_copy(srcs[i], held[i], sems.at[0, i]).wait()
        buffer = held[i]
        if held[i].dtype != dsts[i].dtype:
            buffer = wide[len([b for b in buffers if b])]
            buffer[...] = held[i][...].astype(buffer.dtype)
        buffers.append(buffer is not held[i])
        pltpu.make_async_copy(buffer, dsts[i], sems.at[1, i]).start()
    used = 0
    for i in range(n):
        buffer = wide[used] if buffers[i] else held[i]
        used += buffers[i]
        pltpu.make_async_copy(buffer, dsts[i], sems.at[1, i]).wait()


def finish_call(gains, arrays, dtypes):
    width = gains.shape[1] // (lax.axis_size("tp") * lax.axis_size("ctx") * lax.axis_size("dp"))
    any_spec = pl.BlockSpec(memory_space=pl.ANY)
    vm = pl.BlockSpec(memory_space=pltpu.VMEM)
    sds = jax.ShapeDtypeStruct
    n = len(arrays)
    return pl.pallas_call(
        functools.partial(finish_kernel, width, n),
        out_shape=[sds((4, width), F32)] + [sds(a.shape, d) for a, d in zip(arrays, dtypes, strict=True)],
        in_specs=[vm] + [any_spec] * n,
        out_specs=[vm] + [any_spec] * n,
        scratch_shapes=[pltpu.VMEM(a.shape, a.dtype) for a in arrays]
        + [pltpu.VMEM(a.shape, d) for a, d in zip(arrays, dtypes, strict=True) if a.dtype != d]
        + [pltpu.SemaphoreType.DMA((2, n))],
        compiler_params=pltpu.CompilerParams(vmem_limit_bytes=66_000_000),
        name="finish",
    )(gains, *arrays)


def shards(layer_in, cotangent, norm_gains, w_query, w_key, w_value, w_out, w_gate, w_up, w_down):
    half_width = HEAD // 2
    frequency = THETA ** (-(jnp.arange(half_width, dtype=F32) * 2.0) / HEAD)
    query, head_rows, log_totals, cosine, sine, keys_values, rows_one, *weights = front_call(
        layer_in, norm_gains, frequency[None, :], w_query, w_key, w_value, w_out, w_gate, w_up, w_down
    )
    layer_out, input_grad, gains, down_sum, *sums = main_call(
        layer_in, cotangent, norm_gains, head_rows, w_out, w_gate, *weights,
        query, log_totals, cosine, sine, keys_values, rows_one, w_query, w_key, w_value,
    )
    arrays = [layer_out, input_grad, down_sum, *sums]
    gain_grads, layer_out, input_grad, down_turned, grad_gate, grad_up, out_turned, *rest = finish_call(
        gains, arrays, [BF] + [F32] * (len(arrays) - 1)
    )
    return (layer_out, input_grad, gain_grads, *rest, out_turned.T, grad_gate, grad_up, down_turned.T)


def solution(mesh):
    return jax.shard_map(
        shards,
        mesh=mesh,
        in_specs=(
            P(("dp", "ctx", "tp"), None),
            P(("dp", "ctx", "tp"), None),
            P(),
            P("dp", "tp"),
            P("dp", "tp"),
            P("dp", "tp"),
            P("tp", "dp"),
            P("dp", "tp"),
            P("dp", "tp"),
            P("tp", "dp"),
        ),
        out_specs=(
            P(("dp", "ctx", "tp"), None),
            P(("dp", "ctx", "tp"), None),
            P(None, ("dp", "ctx", "tp")),
            P(("dp", "ctx"), "tp"),
            P(("dp", "ctx"), "tp"),
            P(("dp", "ctx"), "tp"),
            P("tp", ("dp", "ctx")),
            P(("dp", "ctx"), "tp"),
            P(("dp", "ctx"), "tp"),
            P("tp", ("dp", "ctx")),
        ),
        check_vma=False,
    )
```
